32 devices in a mesh: expert: 8 (over z, x), tensor: 4 (over y, core).
Axes of the slice: x: 2, y: 2, z: 4, core: 2. Of those that a mesh axis runs over, the one named last changes fastest.
Arguments:
- block_in: bfloat16 [2048, 2048], P('expert'), may hold values from -6 to 6
- attention_gain: bfloat16 [2048], P('expert'), may hold values from 0.5 to 1.5
- query_down: bfloat16 [2048, 1536], P('expert'), may hold values from -0.125 to 0.125
- query_gain: bfloat16 [1536], P('expert'), may hold values from 0.5 to 1.5
- query_up: bfloat16 [1536, 3072], P('expert', 'tensor'), may hold values from -0.15625 to 0.15625
- latent_down: bfloat16 [2048, 576], P('expert'), may hold values from -0.125 to 0.125
- latent_gain: bfloat16 [512], P('expert'), may hold values from 0.5 to 1.5
- latent_up: bfloat16 [512, 4096], P('expert', 'tensor'), may hold values from -0.25 to 0.25
- out_proj: bfloat16 [2048, 2048], P('tensor', 'expert'), may hold values from -0.5 to 0.5
- ffn_gain: bfloat16 [2048], P('expert'), may hold values from 0.5 to 1.5
- router: bfloat16 [2048, 64], P('expert'), may hold values from -0.125 to 0.125
- shared_gate: bfloat16 [2048, 2816], P('expert', 'tensor'), may hold values from -0.125 to 0.125
- shared_up: bfloat16 [2048, 2816], P('expert', 'tensor'), may hold values from -0.125 to 0.125
- shared_down: bfloat16 [2816, 2048], P('tensor', 'expert'), may hold values from -0.109375 to 0.109375
- expert_gate: bfloat16 [64, 2048, 1408], P('expert', None, 'tensor'), may hold values from -0.125 to 0.125
- expert_up: bfloat16 [64, 2048, 1408], P('expert', None, 'tensor'), may hold values from -0.125 to 0.125
- expert_down: bfloat16 [64, 1408, 2048], P('expert', 'tensor'), may hold values from -0.15625 to 0.15625
- doc_lengths: int32 [8, 3], P('expert'), may hold values from 1 to 128, 256 in all within a row
- routes: int32 [2048, 6], P('expert'), may hold values from 0 to 63, all different within a row; in each aligned block of 256 rows (0 to 255, 256 to 511, ...) at most 32 rows name the same one
- out_grad: bfloat16 [2048, 2048], P('expert'), may hold values from -6 to 6
Outputs:
- block_out: bfloat16 [2048, 2048], P('expert')
- input_grad: bfloat16 [2048, 2048], P('expert')
- grad_attention_gain: float32 [2048], P('expert')
- grad_query_down: float32 [2048, 1536], P('expert')
- grad_query_gain: float32 [1536], P('expert')
- grad_query_up: float32 [1536, 3072], P('expert', 'tensor')
- grad_latent_down: float32 [2048, 576], P('expert')
- grad_latent_gain: float32 [512], P('expert')
- grad_latent_up: float32 [512, 4096], P('expert', 'tensor')
- grad_out_proj: float32 [2048, 2048], P('tensor', 'expert')
- grad_ffn_gain: float32 [2048], P('expert')
- grad_router: float32 [2048, 64], P('expert')
- grad_shared_gate: float32 [2048, 2816], P('expert', 'tensor')
- grad_shared_up: float32 [2048, 2816], P('expert', 'tensor')
- grad_shared_down: float32 [2816, 2048], P('tensor', 'expert')
- grad_expert_gate: float32 [64, 2048, 1408], P('expert', None, 'tensor')
- grad_expert_up: float32 [64, 2048, 1408], P('expert', None, 'tensor')
- grad_expert_down: float32 [64, 1408, 2048], P('expert', 'tensor')
The draws below stay inside these ranges and needn't reach their ends.
Inputs may be any that keep to these rules, and one draw needn't show every extreme that they name: `doc_lengths`: each block's lengths sum to 256; in every block the longest document has exactly 128 tokens. `routes`: each row names 6 different experts. Among the 256 rows of one block, no expert is named by more than 32 rows, a bound that some block reaches.
All inputs are finite; a program needn't handle non-finite values.
Results may differ from the reference program's by a relative error of at most 0.029.
Values may be sent and summed in bfloat16 or wider, within the bound.
A program may use at most 384 MiB of HBM per device.

```python
import math
import jax
import jax.numpy as jnp
import numpy as np
from jax import lax

D = 2048
HEADS = 16
NOPE = 128
ROPE = 64
VD = 128
QR = 1536
KR = 512
EXPERTS = 64
TOPK = 6
FF = 1408
SFF = 2816
TOK_DEV = 256
SEQS = 3
MAXLEN = 128
CAP = 32
BLOCKS = 8
TOKENS = 2048
FF_PART = 352
N_TENSOR = 4


def shard_levels(own_key, shape, split, smallest, top_value):
    loudness = 1.0
    for axis_at, parts in split:
        draws = jax.random.uniform(jax.random.fold_in(jax.random.fold_in(own_key, 6), axis_at), (parts,), jnp.float32, smallest / len(split), top_value / len(split))
        loudness = loudness * jnp.repeat(jnp.exp(draws), shape[axis_at] // parts).reshape((-1,) + (1,) * (len(shape) - 1 - axis_at))
    return loudness


def profile(number_of, total, limit, slope):
    loads = [(1 << 20) // math.isqrt(rank ** slope) + 1 for rank in range(2, number_of + 1)]
    spare, holding = total - limit - (number_of - 1), [1] * (number_of - 1)
    while spare > 0:
        free = [i for i in range(number_of - 1) if holding[i] < limit]
        pool, remaining = sum([loads[i] for i in free]), spare
        for i in free:
            extra = min(limit - holding[i], max(1, remaining * loads[i] // pool), spare)
            holding[i] = holding[i] + extra
            spare = spare - extra
    return np.array([limit] + holding)


def ragged(own_key, number_of, total, limit, skew):
    if number_of == 2:
        one = jax.random.randint(own_key, (), max(1, total - limit), min(limit, total - 1) + 1)
        return jnp.stack([one, total - one])
    tallies = jnp.asarray(profile(number_of, total, limit, skew), jnp.int32)
    pairs = (number_of - 1) // 2
    donor, sink = tallies[1:1 + 2 * pairs:2], tallies[2:2 + 2 * pairs:2]
    slack = jnp.minimum(donor - 1, limit - sink)
    moved = jax.random.randint(jax.random.fold_in(own_key, 1), (pairs,), 0, 1 << 20) % (slack + 1)
    tallies = tallies.at[1:1 + 2 * pairs:2].set(donor - moved).at[2:2 + 2 * pairs:2].set(sink + moved)
    return tallies[jax.random.permutation(jax.random.fold_in(own_key, 2), number_of)]


def assign_block(key, own, number, rows, count, top, most, slope):
    ranking = jax.random.permutation(key, count)
    crowded, ordinary = portions_of(count, rows * top, most, slope, True), portions_of(count, rows * top, most, slope, False)
    places = jnp.arange(count)

    def named(sizes, offset_by):
        used = int((sizes > 0).sum())
        fixed = max(1, used // 4)
        shifted = fixed + (places - fixed + offset_by * (used - fixed)) % max(1, count - fixed)
        return jnp.zeros((count,), jnp.int32).at[ranking[jnp.where(places < fixed, places, shifted)]].set(jnp.asarray(sizes, jnp.int32))

    sizes = jnp.where(number % 4 == 0, named(crowded, number // 4), named(ordinary, number - number // 4 - 1))
    mixed = jax.random.permutation(jax.random.fold_in(own, 3), count)
    donor, sink = mixed[0:count // 2 * 2:2], mixed[1:count // 2 * 2:2]
    room = jnp.minimum(sizes[donor] - 1, most - sizes[sink]) // 2
    room = jnp.where((donor == ranking[0]) | (sink == ranking[0]) | (sizes[sink] == 0), 0, jnp.maximum(room, 0))
    shifted = jax.random.randint(jax.random.fold_in(own, 4), (count // 2,), 0, 1 << 20) % (room + 1)
    sizes = sizes.at[donor].add(-shifted).at[sink].add(shifted)
    labels = jnp.searchsorted(jnp.cumsum(sizes), jnp.arange(rows * top), side="right").astype(jnp.int32)
    table = labels.reshape(top, rows).T
    table = table[jax.random.permutation(jax.random.fold_in(own, 1), rows)]
    offset_by = jax.random.randint(jax.random.fold_in(own, 2), (rows, 1), 0, top)
    return jnp.take_along_axis(table, (jnp.arange(top)[None, :] + offset_by) % top, axis=1)


def portions_of(number_of, total, reach, skew, full):
    weights = [(1 << 20) // math.isqrt(standing ** skew) + 1 for standing in range(1, number_of + 1)]
    largest = reach if full else min(reach, max(-(-total // number_of), total * weights[0] // sum(weights)))
    least = 1 if total - largest >= number_of - 1 else 0
    holding, surplus = [largest] + [least] * (number_of - 1), total - largest - least * (number_of - 1)
    while surplus > 0:
        movable = [i for i in range(1, number_of) if holding[i] < largest] or [i for i in range(1, number_of) if holding[i] < reach]
        pool, remaining = sum([weights[i] for i in movable]), surplus
        for i in movable:
            addition = min(reach - holding[i], max(1, remaining * weights[i] // pool), surplus)
            holding[i] = holding[i] + addition
            surplus = surplus - addition
    return np.array(holding)


def centred(rng, shape, width, reach, cuts=(), kind=jnp.bfloat16):
    array = width * jax.random.normal(rng, shape, jnp.float32)
    if cuts:
        array = array * shard_levels(rng, shape, cuts, -0.22, 0.18)
    return jnp.clip(array, -reach, reach).astype(kind)


def setup_inputs(seed: int = 0) -> dict:
    streams_of = jax.random.split(jax.random.key(seed), 21)
    block_in = centred(streams_of[0], (TOKENS, D), 1.0, 6.0, ((0, 8),))
    attention_gain = jnp.clip(1.0 + 0.1 * jax.random.normal(streams_of[1], (D,), jnp.float32), 0.5, 1.5).astype(jnp.bfloat16)
    query_down = centred(streams_of[2], (D, QR), D ** -0.5, 0.125, ((0, 8),))
    query_gain = jnp.clip(1.0 + 0.1 * jax.random.normal(streams_of[3], (QR,), jnp.float32), 0.5, 1.5).astype(jnp.bfloat16)
    query_up = centred(streams_of[4], (QR, HEADS * (NOPE + ROPE)), QR ** -0.5, 0.15625, ((0, 8), (1, 4)))
    latent_down = centred(streams_of[5], (D, KR + ROPE), D ** -0.5, 0.125, ((0, 8),))
    latent_gain = jnp.clip(1.0 + 0.1 * jax.random.normal(streams_of[6], (KR,), jnp.float32), 0.5, 1.5).astype(jnp.bfloat16)
    latent_up = centred(streams_of[7], (KR, HEADS * (NOPE + VD)), KR ** -0.5, 0.25, ((0, 8), (1, 4)))
    out_proj = centred(streams_of[8], (HEADS * VD, D), (HEADS * VD // 16) ** -0.5, 0.5, ((0, 4), (1, 8)))
    ffn_gain = jnp.clip(1.0 + 0.1 * jax.random.normal(streams_of[9], (D,), jnp.float32), 0.5, 1.5).astype(jnp.bfloat16)
    router = centred(streams_of[10], (D, EXPERTS), D ** -0.5, 0.125, ((0, 8),))
    shared_gate = centred(streams_of[11], (D, SFF), D ** -0.5, 0.125, ((0, 8), (1, 4)))
    shared_up = centred(streams_of[12], (D, SFF), D ** -0.5, 0.125, ((0, 8), (1, 4)))
    shared_down = centred(streams_of[13], (SFF, D), SFF ** -0.5, 0.109375, ((0, 4), (1, 8)))
    expert_gate = centred(streams_of[14], (EXPERTS, D, FF), D ** -0.5, 0.125, ((0, 8), (2, 4)))
    expert_up = centred(streams_of[15], (EXPERTS, D, FF), D ** -0.5, 0.125, ((0, 8), (2, 4)))
    expert_down = centred(streams_of[16], (EXPERTS, FF, D), FF ** -0.5, 0.15625, ((0, 8), (1, 4)))
    doc_lengths = jax.vmap(lambda own: ragged(own, SEQS, TOK_DEV, MAXLEN, 2))(jax.random.split(streams_of[17], BLOCKS)).reshape((BLOCKS, SEQS)).astype(jnp.int32)
    routes_keys = jax.random.split(jax.random.fold_in(streams_of[18], 1), TOKENS // TOK_DEV)
    routes_turns = jax.random.permutation(jax.random.fold_in(streams_of[18], 3), TOKENS // TOK_DEV)
    routes = jax.vmap(lambda own, number: assign_block(jax.random.fold_in(streams_of[18], 2), own, number, TOK_DEV, EXPERTS, TOPK, CAP, 1))(routes_keys, routes_turns).reshape((TOKENS, TOPK))
    out_grad = centred(streams_of[19], (TOKENS, D), 1.0, 6.0, ((0, 8),))
    return {"block_in": block_in, "attention_gain": attention_gain, "query_down": query_down, "query_gain": query_gain, "query_up": query_up, "latent_down": latent_down, "latent_gain": latent_gain, "latent_up": latent_up, "out_proj": out_proj, "ffn_gain": ffn_gain, "router": router, "shared_gate": shared_gate, "shared_up": shared_up, "shared_down": shared_down, "expert_gate": expert_gate, "expert_up": expert_up, "expert_down": expert_down, "doc_lengths": doc_lengths, "routes": routes, "out_grad": out_grad}


EPSILON = 1e-06
ROPE_BASE = 50000.0
ROUTE_SCALE = 2.446

def matmul(left, right):
    return jnp.dot(left.astype(jnp.float32), right.astype(jnp.float32), preferred_element_type=jnp.float32)

def contract(form, left, right):
    return jnp.einsum(form, left.astype(jnp.float32), right.astype(jnp.float32), preferred_element_type=jnp.float32)

def settle(partial_sum):
    return lax.optimization_barrier(partial_sum.astype(jnp.bfloat16)).astype(jnp.float32)

def rms_forward(values, gain):
    inverse = lax.rsqrt(lax.optimization_barrier(jnp.mean(values * values, axis=-1, keepdims=True)) + EPSILON)
    return (values * inverse * gain.astype(jnp.float32), inverse)

def rms_backward(values, inverse, gain, cotangent):
    scaled = cotangent * gain.astype(jnp.float32)
    normed = values * inverse
    return inverse * (scaled - normed * lax.optimization_barrier(jnp.mean(scaled * normed, axis=-1, keepdims=True)))

def gain_gradient(values, inverse, cotangent):
    return lax.optimization_barrier(jnp.sum(cotangent * (values * inverse), axis=0))

def rotate(values, cosine, sinusoid):
    half_width = values.shape[-1] // 2
    leading = values[..., :half_width]
    trailing = values[..., half_width:]
    return jnp.concatenate([leading * cosine - trailing * sinusoid, trailing * cosine + leading * sinusoid], axis=-1)

def rotate_back(values, cosine, sinusoid):
    half_width = values.shape[-1] // 2
    leading = values[..., :half_width]
    trailing = values[..., half_width:]
    return jnp.concatenate([leading * cosine + trailing * sinusoid, trailing * cosine - leading * sinusoid], axis=-1)

def layout(lengths, row_count):
    doc_count = lengths.shape[0]
    doc_ends = jnp.cumsum(lengths).astype(jnp.int32)
    starts = (doc_ends - lengths).astype(jnp.int32)
    row_index = jnp.arange(row_count, dtype=jnp.int32)
    doc_ids = lax.optimization_barrier(jnp.sum((row_index[:, None] >= doc_ends[None, :]).astype(jnp.int32), axis=1)).astype(jnp.int32)
    owners = doc_ids[:, None] == jnp.arange(doc_count, dtype=jnp.int32)[None, :]
    first_row = lax.optimization_barrier(jnp.sum(jnp.where(owners, starts[None, :], 0), axis=1)).astype(jnp.int32)
    positions = (row_index - first_row).astype(jnp.float32)
    allowed = (doc_ids[:, None] == doc_ids[None, :]) & (row_index[None, :] <= row_index[:, None])
    frequency = jnp.exp(-math.log(ROPE_BASE) * 2.0 * jnp.arange(ROPE // 2, dtype=jnp.float32) / ROPE)
    angles = positions[:, None] * frequency[None, :]
    return (allowed, jnp.cos(angles), jnp.sin(angles))

def latent_stem(residual, stem_weights, cosine, sinusoid):
    attention_gain, query_down, query_gain, latent_down, latent_gain = stem_weights
    normed, inverse_first = rms_forward(residual, attention_gain)
    first_normed = normed.astype(jnp.bfloat16)
    query_lat = matmul(first_normed, query_down)
    query_n, inverse_query = rms_forward(query_lat, query_gain)
    latent_all = matmul(first_normed, latent_down)
    latent = latent_all[:, :KR]
    latent_n, inverse_latent = rms_forward(latent, latent_gain)
    key_rope = rotate(latent_all[:, KR:], cosine, sinusoid)
    return (first_normed, inverse_first, query_lat, inverse_query, query_n.astype(jnp.bfloat16), latent, inverse_latent, latent_n.astype(jnp.bfloat16), key_rope)

def heads_forward(query_n, latent_n, key_rope, query_up, latent_up, allowed, cosine, sinusoid):
    row_count = query_n.shape[0]
    head_width = NOPE + ROPE
    head_count = query_up.shape[1] // head_width
    queries = matmul(query_n, query_up).reshape(row_count, head_count, head_width)
    queries = jnp.concatenate([queries[..., :NOPE], rotate(queries[..., NOPE:], cosine[:, None, :], sinusoid[:, None, :])], axis=-1).astype(jnp.bfloat16)
    keyval = matmul(latent_n, latent_up).reshape(row_count, head_count, NOPE + VD)
    key_rows = jnp.concatenate([keyval[..., :NOPE], jnp.broadcast_to(key_rope[:, None, :], (row_count, head_count, ROPE))], axis=-1).astype(jnp.bfloat16)
    value_rows = keyval[..., NOPE:].astype(jnp.bfloat16)
    scores = contract('qhc,khc->hqk', queries, key_rows) * head_width ** (-0.5)
    scores = jnp.where(allowed[None], scores, -1e+30)
    row_peak = lax.optimization_barrier(jnp.max(scores, axis=-1, keepdims=True))
    powers = jnp.exp(scores - row_peak)
    totals = lax.optimization_barrier(jnp.sum(powers, axis=-1, keepdims=True))
    logsum = row_peak + jnp.log(totals)
    attn_probs = (powers / totals).astype(jnp.bfloat16)
    attended = contract('hqk,khc->qhc', attn_probs, value_rows).reshape(row_count, head_count * VD).astype(jnp.bfloat16)
    return (attended, logsum, queries, key_rows, value_rows)

def heads_backward(attended_grad, logsum, queries, key_rows, value_rows, query_n, latent_n, query_up, latent_up, allowed, cosine, sinusoid):
    row_count = queries.shape[0]
    head_count = queries.shape[1]
    head_width = NOPE + ROPE
    attended_rows = attended_grad.reshape(row_count, head_count, VD)
    scores = contract('qhc,khc->hqk', queries, key_rows) * head_width ** (-0.5)
    attn_probs = jnp.where(allowed[None], jnp.exp(scores - logsum), 0.0)
    dvalues = contract('hqk,qhc->khc', attn_probs.astype(jnp.bfloat16), attended_rows)
    dprobs = contract('qhc,khc->hqk', attended_rows, value_rows)
    row_delta = lax.optimization_barrier(jnp.sum(attn_probs * dprobs, axis=-1, keepdims=True))
    dscores = (attn_probs * (dprobs - row_delta) * head_width ** (-0.5)).astype(jnp.bfloat16)
    dquery = contract('hqk,khc->qhc', dscores, key_rows)
    dkey_rows = contract('hqk,qhc->khc', dscores, queries)
    dquery = jnp.concatenate([dquery[..., :NOPE], rotate_back(dquery[..., NOPE:], cosine[:, None, :], sinusoid[:, None, :])], axis=-1)
    dquery = dquery.reshape(row_count, head_count * head_width).astype(jnp.bfloat16)
    dkey_rope = rotate_back(lax.optimization_barrier(jnp.sum(dkey_rows[..., NOPE:], axis=1)), cosine, sinusoid)
    dkeyval = jnp.concatenate([dkey_rows[..., :NOPE], dvalues], axis=-1).reshape(row_count, head_count * (NOPE + VD)).astype(jnp.bfloat16)
    grad_query_up = matmul(query_n.T, dquery)
    grad_latent_up = matmul(latent_n.T, dkeyval)
    dquery_n = matmul(dquery, query_up.T)
    dlatent_n = matmul(dkeyval, latent_up.T)
    return (dquery_n, dlatent_n, dkey_rope, grad_query_up, grad_latent_up)

def latent_stem_back(residual, stashed, stem_weights, dquery_n, dlatent_n, dkey_rope):
    attention_gain, query_down, query_gain, latent_down, latent_gain = stem_weights
    first_normed = stashed[0]
    dquery_lat = rms_backward(stashed[2], stashed[3], query_gain, dquery_n).astype(jnp.bfloat16)
    grad_query_gain = gain_gradient(stashed[2], stashed[3], dquery_n)
    dlatent_all = jnp.concatenate([rms_backward(stashed[5], stashed[6], latent_gain, dlatent_n), dkey_rope], axis=-1).astype(jnp.bfloat16)
    grad_latent_gain = gain_gradient(stashed[5], stashed[6], dlatent_n)
    grad_query_down = matmul(first_normed.T, dquery_lat)
    grad_latent_down = matmul(first_normed.T, dlatent_all)
    dfirst = matmul(dquery_lat, query_down.T) + matmul(dlatent_all, latent_down.T)
    dresidual = rms_backward(residual, stashed[1], attention_gain, dfirst)
    grad_attention_gain = gain_gradient(residual, stashed[1], dfirst)
    return (dresidual, (grad_attention_gain, grad_query_down, grad_query_gain, grad_latent_down, grad_latent_gain))

def swiglu_forward(row_inputs, gate_weight, up_weight):
    gate_pre = matmul(row_inputs, gate_weight)
    up_pre = matmul(row_inputs, up_weight)
    hidden = (gate_pre * jax.nn.sigmoid(gate_pre) * up_pre).astype(jnp.bfloat16)
    return (gate_pre, up_pre, hidden)

def swiglu_backward(row_inputs, cotangent, gate_pre, up_pre, hidden, down_weight):
    sigmoid_gate = jax.nn.sigmoid(gate_pre)
    dhidden = matmul(cotangent, down_weight.T)
    gate_grad = (dhidden * up_pre * sigmoid_gate * (1.0 + gate_pre * (1.0 - sigmoid_gate))).astype(jnp.bfloat16)
    up_grad = (dhidden * gate_pre * sigmoid_gate).astype(jnp.bfloat16)
    return (gate_grad, up_grad, matmul(row_inputs.T, gate_grad), matmul(row_inputs.T, up_grad), matmul(hidden.T, cotangent))

def router_forward(second_normed, router_weight, route_rows):
    sigmoid_all = jax.nn.sigmoid(matmul(second_normed, router_weight))
    route_hot = route_rows[:, :, None] == jnp.arange(EXPERTS, dtype=jnp.int32)[None, None, :]
    chosen = lax.optimization_barrier(jnp.sum(jnp.where(route_hot, sigmoid_all[:, None, :], 0.0), axis=-1))
    totals = lax.optimization_barrier(jnp.sum(chosen, axis=-1, keepdims=True))
    return (route_hot, chosen, totals, ROUTE_SCALE * chosen / totals)

def router_backward(route_hot, chosen, totals, dweights):
    dchosen = ROUTE_SCALE / totals * (dweights - lax.optimization_barrier(jnp.sum(dweights * chosen, axis=-1, keepdims=True)) / totals)
    dpicked = dchosen * chosen * (1.0 - chosen)
    return lax.optimization_barrier(jnp.sum(jnp.where(route_hot, dpicked[:, :, None], 0.0), axis=1)).astype(jnp.bfloat16)

def slot_positions(route_rows, capacity):
    flat_routes = route_rows.reshape(-1).astype(jnp.int32)
    route_hot = (flat_routes[:, None] == jnp.arange(EXPERTS, dtype=jnp.int32)[None, :]).astype(jnp.int32)
    earlier = (jnp.cumsum(route_hot, axis=0) - route_hot).astype(jnp.int32)
    slot_rank = lax.optimization_barrier(jnp.sum(earlier * route_hot, axis=1)).astype(jnp.int32)
    return (flat_routes * capacity + slot_rank).astype(jnp.int32)

def expert_pass(packed):
    row_inputs, cotangent, gate_weight, up_weight, down_weight = packed
    row_count = row_inputs.shape[0]
    gate_pre, up_pre, hidden = swiglu_forward(row_inputs, gate_weight, up_weight)
    partials = contract('rqf,qfd->qrd', hidden.reshape(row_count, N_TENSOR, FF_PART), down_weight.reshape(N_TENSOR, FF_PART, D))
    routed = lax.optimization_barrier(jnp.sum(settle(partials), axis=0))
    gate_grad, up_grad, grad_gate, grad_up, grad_down = swiglu_backward(row_inputs, cotangent, gate_pre, up_pre, hidden, down_weight)
    dpartials = contract('rqf,dqf->qrd', gate_grad.reshape(row_count, N_TENSOR, FF_PART), gate_weight.reshape(D, N_TENSOR, FF_PART))
    dpartials = dpartials + contract('rqf,dqf->qrd', up_grad.reshape(row_count, N_TENSOR, FF_PART), up_weight.reshape(D, N_TENSOR, FF_PART))
    drows = lax.optimization_barrier(jnp.sum(settle(dpartials), axis=0))
    return (routed, drows, grad_gate, grad_up, grad_down)

def reference(block_in, attention_gain, query_down, query_gain, query_up, latent_down, latent_gain, latent_up, out_proj, ffn_gain, router, shared_gate, shared_up, shared_down, expert_gate, expert_up, expert_down, doc_lengths, routes, out_grad):
    groups = BLOCKS
    head_group = HEADS // N_TENSOR
    query_cols = head_group * (NOPE + ROPE)
    latent_cols = head_group * (NOPE + VD)
    output_rows = head_group * VD
    stem_weights = (attention_gain, query_down, query_gain, latent_down, latent_gain)
    blocks_in = block_in.reshape(groups, TOK_DEV, D)

    def attention_block(residual, lengths):
        allowed, cosine, sinusoid = layout(lengths, TOK_DEV)
        stashed = latent_stem(residual, stem_weights, cosine, sinusoid)
        pieces = []
        for section in range(N_TENSOR):
            pieces.append(heads_forward(stashed[4], stashed[7], stashed[8], query_up[:, section * query_cols:(section + 1) * query_cols], latent_up[:, section * latent_cols:(section + 1) * latent_cols], allowed, cosine, sinusoid))
        return (allowed, cosine, sinusoid, stashed, pieces)

    def forward_block(packed):
        residual = packed[0].astype(jnp.float32)
        allowed, cosine, sinusoid, stashed, pieces = attention_block(residual, packed[1])
        attention_sum = jnp.zeros_like(residual)
        for section in range(N_TENSOR):
            attention_sum = attention_sum + matmul(pieces[section][0], out_proj[section * output_rows:(section + 1) * output_rows])
        return residual + attention_sum
    middle = lax.map(forward_block, (blocks_in, doc_lengths)).reshape(TOKENS, D)
    second_f, inverse_ffn = rms_forward(middle, ffn_gain)
    second_normed = second_f.astype(jnp.bfloat16)
    route_hot, chosen, totals, route_weights = router_forward(second_normed, router, routes)
    shared_gate_pre, shared_up_pre, shared_hidden = swiglu_forward(second_normed, shared_gate, shared_up)
    shared_out = matmul(shared_hidden, shared_down)
    gradient = out_grad.astype(jnp.float32)
    scaled = (route_weights[:, :, None] * gradient[:, None, :]).astype(jnp.bfloat16)
    slot_index = jax.vmap(lambda block_routes: slot_positions(block_routes, CAP))(routes.reshape(groups, TOK_DEV, TOPK))

    def place_rows(block_rows, block_slots):
        return jnp.zeros((EXPERTS * CAP, D), jnp.bfloat16).at[block_slots].set(block_rows)
    copies = jnp.broadcast_to(second_normed[:, None, :], (TOKENS, TOPK, D)).reshape(groups, TOK_DEV * TOPK, D)
    outgoing = jax.vmap(place_rows)(copies, slot_index)
    outgoing_grad = jax.vmap(place_rows)(scaled.reshape(groups, TOK_DEV * TOPK, D), slot_index)

    def per_expert(buffer):
        return buffer.reshape(groups, EXPERTS, CAP, D).transpose(1, 0, 2, 3).reshape(EXPERTS, groups * CAP, D)
    routed_slots, drows_slots, grad_expert_gate, grad_expert_up, grad_expert_down = lax.map(expert_pass, (per_expert(outgoing), per_expert(outgoing_grad), expert_gate, expert_up, expert_down))

    def take_rows(buffer):
        by_source = buffer.reshape(EXPERTS, groups, CAP, D).transpose(1, 0, 2, 3).reshape(groups, EXPERTS * CAP, D)
        return jax.vmap(lambda block_buffer, block_slots: block_buffer[block_slots])(by_source, slot_index).reshape(TOKENS, TOPK, D)
    routed = take_rows(routed_slots)
    drouted = take_rows(drows_slots)
    mixed = shared_out + lax.optimization_barrier(jnp.sum(route_weights[:, :, None] * routed, axis=1))
    block_out = (middle + mixed).astype(jnp.bfloat16)
    dweights = lax.optimization_barrier(jnp.sum(gradient[:, None, :] * routed, axis=-1))
    dlogits = router_backward(route_hot, chosen, totals, dweights)
    shared_gate_grad, shared_up_grad, grad_shared_gate, grad_shared_up, grad_shared_down = swiglu_backward(second_normed, out_grad, shared_gate_pre, shared_up_pre, shared_hidden, shared_down)
    dsecond = matmul(shared_gate_grad, shared_gate.T) + matmul(shared_up_grad, shared_up.T) + lax.optimization_barrier(jnp.sum(drouted, axis=1)) + matmul(dlogits, router.T)
    grad_router = matmul(second_normed.T, dlogits)
    grad_ffn_gain = gain_gradient(middle, inverse_ffn, dsecond)
    middle_grad = gradient + rms_backward(middle, inverse_ffn, ffn_gain, dsecond)

    def backward_block(running, packed):
        block_input, lengths, block_grad = packed
        residual = block_input.astype(jnp.float32)
        allowed, cosine, sinusoid, stashed, pieces = attention_block(residual, lengths)
        attention_grad = block_grad.astype(jnp.bfloat16)
        dresidual = block_grad
        grad_attention_gain, grad_query_down, grad_query_gain, grad_latent_down, grad_latent_gain, grad_query_up, grad_latent_up, grad_out_proj = running
        for section in range(N_TENSOR):
            attended, logsum, queries, key_rows, value_rows = pieces[section]
            query_slice = slice(section * query_cols, (section + 1) * query_cols)
            latent_slice = slice(section * latent_cols, (section + 1) * latent_cols)
            output_slice = slice(section * output_rows, (section + 1) * output_rows)
            grad_out_proj = grad_out_proj.at[output_slice].add(matmul(attended.T, attention_grad))
            attended_grad = matmul(attention_grad, out_proj[output_slice].T).astype(jnp.bfloat16)
            dquery_n, dlatent_n, dkey_rope, section_query_up, section_latent_up = heads_backward(attended_grad, logsum, queries, key_rows, value_rows, stashed[4], stashed[7], query_up[:, query_slice], latent_up[:, latent_slice], allowed, cosine, sinusoid)
            grad_query_up = grad_query_up.at[:, query_slice].add(section_query_up)
            grad_latent_up = grad_latent_up.at[:, latent_slice].add(section_latent_up)
            dpart, stem_grads = latent_stem_back(residual, stashed, stem_weights, dquery_n, dlatent_n, dkey_rope)
            dresidual = dresidual + dpart
            grad_attention_gain = grad_attention_gain + stem_grads[0]
            grad_query_down = grad_query_down + stem_grads[1]
            grad_query_gain = grad_query_gain + stem_grads[2]
            grad_latent_down = grad_latent_down + stem_grads[3]
            grad_latent_gain = grad_latent_gain + stem_grads[4]
        updated = (grad_attention_gain, grad_query_down, grad_query_gain, grad_latent_down, grad_latent_gain, grad_query_up, grad_latent_up, grad_out_proj)
        return (updated, dresidual.astype(jnp.bfloat16))
    start_sums = (jnp.zeros((D,), jnp.float32), jnp.zeros((D, QR), jnp.float32), jnp.zeros((QR,), jnp.float32), jnp.zeros((D, KR + ROPE), jnp.float32), jnp.zeros((KR,), jnp.float32), jnp.zeros((QR, HEADS * (NOPE + ROPE)), jnp.float32), jnp.zeros((KR, HEADS * (NOPE + VD)), jnp.float32), jnp.zeros((HEADS * VD, D), jnp.float32))
    sums, input_blocks = lax.scan(backward_block, start_sums, (blocks_in, doc_lengths, middle_grad.reshape(groups, TOK_DEV, D)))
    input_grad = input_blocks.reshape(TOKENS, D)
    return (block_out, input_grad, sums[0], sums[1], sums[2], sums[5], sums[3], sums[4], sums[6], sums[7], grad_ffn_gain, grad_router, grad_shared_gate, grad_shared_up, grad_shared_down, grad_expert_gate, grad_expert_up, grad_expert_down)
```

```python
import functools
import math

import jax
import jax.numpy as jnp
from jax import lax
from jax.experimental import pallas as pl
from jax.experimental.pallas import tpu as pltpu
from jax.sharding import PartitionSpec as P

NOPE = 128
ROPE = 64
VD = 128
CAP = 32
LANES = 128
VMEM_BYTES = 60 * 2**20

EPSILON = 1e-06
ROPE_BASE = 50000.0
ROUTE_SCALE = 2.446


def matmul(left, right):
    return jnp.dot(left, right, preferred_element_type=jnp.float32)


def contract(form, left, right):
    return jnp.einsum(form, left, right, preferred_element_type=jnp.float32)


def matmul_nt(left, right):
    return lax.dot_general(left, right, (((1,), (1,)), ((), ())), preferred_element_type=jnp.float32)


def matmul_tn(left, right):
    return lax.dot_general(left, right, (((0,), (0,)), ((), ())), preferred_element_type=jnp.float32)


def rms_forward(values, gain):
    inverse = lax.rsqrt(jnp.mean(values * values, axis=-1, keepdims=True) + EPSILON)
    return (values * inverse * gain, inverse)


def rms_backward(values, inverse, gain, cotangent):
    scaled = cotangent * gain
    normed = values * inverse
    return inverse * (scaled - normed * jnp.mean(scaled * normed, axis=-1, keepdims=True))


def gain_gradient(values, inverse, cotangent):
    return jnp.sum(cotangent * (values * inverse), axis=0)


def rotate(values, cosine, sinusoid):
    half_width = values.shape[-1] // 2
    leading = values[..., :half_width]
    trailing = values[..., half_width:]
    return jnp.concatenate(
        [leading * cosine - trailing * sinusoid, trailing * cosine + leading * sinusoid], axis=-1
    )


def rotate_back(values, cosine, sinusoid):
    return rotate(values, cosine, -sinusoid)


def layout(lengths, row_count):
    doc_count = lengths.shape[0]
    doc_ends = jnp.cumsum(lengths)
    starts = doc_ends - lengths
    row_index = jnp.arange(row_count, dtype=jnp.int32)
    doc_ids = jnp.sum((row_index[:, None] >= doc_ends[None, :]).astype(jnp.int32), axis=1)
    owners = doc_ids[:, None] == jnp.arange(doc_count, dtype=jnp.int32)[None, :]
    first_row = jnp.sum(jnp.where(owners, starts[None, :], 0), axis=1)
    positions = (row_index - first_row).astype(jnp.float32)
    allowed = (doc_ids[:, None] == doc_ids[None, :]) & (row_index[None, :] <= row_index[:, None])
    frequency = jnp.exp(
        -math.log(ROPE_BASE) * 2.0 * jnp.arange(ROPE // 2, dtype=jnp.float32) / ROPE
    )
    angles = positions[:, None] * frequency[None, :]
    return (allowed, jnp.cos(angles), jnp.sin(angles))


def heads_forward(query_n, latent_n, key_rope, query_up, latent_up, allowed, cosine, sinusoid):
    row_count = query_n.shape[0]
    head_width = NOPE + ROPE
    head_count = query_up.shape[1] // head_width
    queries = matmul(query_n, query_up).reshape(row_count, head_count, head_width)
    queries = jnp.concatenate(
        [
            queries[..., :NOPE],
            rotate(queries[..., NOPE:], cosine[:, None, :], sinusoid[:, None, :]),
        ],
        axis=-1,
    ).astype(jnp.bfloat16)
    keyval = matmul(latent_n, latent_up).reshape(row_count, head_count, NOPE + VD)
    key_rows = jnp.concatenate(
        [keyval[..., :NOPE], jnp.broadcast_to(key_rope[:, None, :], (row_count, head_count, ROPE))],
        axis=-1,
    ).astype(jnp.bfloat16)
    value_rows = keyval[..., NOPE:].astype(jnp.bfloat16)
    scores = contract("qhc,khc->hqk", queries, key_rows) * head_width ** (-0.5)
    scores = jnp.where(allowed[None], scores, -1e30)
    row_peak = jnp.max(scores, axis=-1, keepdims=True)
    powers = jnp.exp(scores - row_peak)
    totals = jnp.sum(powers, axis=-1, keepdims=True)
    logsum = row_peak + jnp.log(totals)
    attn_probs = (powers / totals).astype(jnp.bfloat16)
    attended = (
        contract("hqk,khc->qhc", attn_probs, value_rows)
        .reshape(row_count, head_count * VD)
        .astype(jnp.bfloat16)
    )
    return (attended, logsum, queries, key_rows, value_rows)


def heads_backward(
    attended_grad,
    logsum,
    queries,
    key_rows,
    value_rows,
    query_n,
    latent_n,
    query_up,
    latent_up,
    allowed,
    cosine,
    sinusoid,
):
    row_count = queries.shape[0]
    head_count = queries.shape[1]
    head_width = NOPE + ROPE
    attended_rows = attended_grad.reshape(row_count, head_count, VD)
    scores = contract("qhc,khc->hqk", queries, key_rows) * head_width ** (-0.5)
    attn_probs = jnp.where(allowed[None], jnp.exp(scores - logsum), 0.0)
    dvalues = contract("hqk,qhc->khc", attn_probs.astype(jnp.bfloat16), attended_rows)
    dprobs = contract("qhc,khc->hqk", attended_rows, value_rows)
    row_delta = jnp.sum(attn_probs * dprobs, axis=-1, keepdims=True)
    dscores = (attn_probs * (dprobs - row_delta) * head_width ** (-0.5)).astype(jnp.bfloat16)
    dquery = contract("hqk,khc->qhc", dscores, key_rows)
    dkey_rows = contract("hqk,qhc->khc", dscores, queries)
    dquery = jnp.concatenate(
        [
            dquery[..., :NOPE],
            rotate_back(dquery[..., NOPE:], cosine[:, None, :], sinusoid[:, None, :]),
        ],
        axis=-1,
    )
    dquery = dquery.reshape(row_count, head_count * head_width).astype(jnp.bfloat16)
    dkey_rope = rotate_back(jnp.sum(dkey_rows[..., NOPE:], axis=1), cosine, sinusoid)
    dkeyval = (
        jnp.concatenate([dkey_rows[..., :NOPE], dvalues], axis=-1)
        .reshape(row_count, head_count * (NOPE + VD))
        .astype(jnp.bfloat16)
    )
    grad_query_up = matmul(query_n.T, dquery)
    grad_latent_up = matmul(latent_n.T, dkeyval)
    dquery_n = matmul(dquery, query_up.T)
    dlatent_n = matmul(dkeyval, latent_up.T)
    return (dquery_n, dlatent_n, dkey_rope, grad_query_up, grad_latent_up)


def swiglu(gate_pre, up_pre):
    sigmoid_gate = jax.nn.sigmoid(gate_pre)
    return (sigmoid_gate, (gate_pre * sigmoid_gate * up_pre).astype(jnp.bfloat16))


def swiglu_back(dhidden, gate_pre, up_pre, sigmoid_gate):
    gate_grad = dhidden * up_pre * sigmoid_gate * (1.0 + gate_pre * (1.0 - sigmoid_gate))
    up_grad = dhidden * gate_pre * sigmoid_gate
    return (gate_grad.astype(jnp.bfloat16), up_grad.astype(jnp.bfloat16))


def expert_kernel(
    x_ref, g_ref, w_ref, gate_ref, up_ref, down_ref, y_ref, dr_ref, dw_ref, gg_ref, gu_ref, gd_ref
):
    blocks, _, cap, width = x_ref.shape
    rows = blocks * cap
    row_inputs = x_ref[...].reshape(rows, width)
    gradient = g_ref[...].reshape(rows, width).astype(jnp.float32)
    weight = w_ref[...].reshape(rows, 1)
    gate, up, down = gate_ref[0], up_ref[0], down_ref[0]
    gate_pre = matmul_nt(row_inputs, gate)
    up_pre = matmul_nt(row_inputs, up)
    sigmoid_gate, hidden = swiglu(gate_pre, up_pre)
    produced = matmul(hidden, down)
    dw_ref[...] = jnp.sum(gradient * produced, axis=1, keepdims=True).reshape(dw_ref.shape)
    y_ref[...] = (weight * produced).astype(jnp.bfloat16).reshape(y_ref.shape)
    cotangent = (weight * gradient).astype(jnp.bfloat16)
    dhidden = matmul_nt(cotangent, down)
    gate_grad, up_grad = swiglu_back(dhidden, gate_pre, up_pre, sigmoid_gate)
    back = matmul(gate_grad, gate) + matmul(up_grad, up)
    dr_ref[...] = back.astype(jnp.bfloat16).reshape(dr_ref.shape)
    first = pl.program_id(1) == 0

    def accumulate(ref, left, right):
        part = matmul_tn(left, right)

        @pl.when(first)
        def _():
            ref[0] = part

        @pl.when(jnp.logical_not(first))
        def _():
            ref[0] += part

    accumulate(gg_ref, gate_grad, row_inputs)
    accumulate(gu_ref, up_grad, row_inputs)
    accumulate(gd_ref, hidden, cotangent)


def expert_stage(row_inputs, gradients, weights, gate_t, up_t, down):
    blocks, local, cap, width = row_inputs.shape
    units = gate_t.shape[1]
    step = min(blocks, 256 // cap)
    rows_spec = pl.BlockSpec((step, 1, cap, width), lambda j, r: (r, j, 0, 0))
    slot_spec = pl.BlockSpec((step, 1, cap, 1), lambda j, r: (r, j, 0, 0))
    unit_spec = pl.BlockSpec((1, units, width), lambda j, r: (j, 0, 0))
    rows_shape = jax.ShapeDtypeStruct(row_inputs.shape, jnp.bfloat16)
    unit_shape = jax.ShapeDtypeStruct((local, units, width), jnp.float32)
    flops = 18 * blocks * local * cap * width * units
    moved = 8 * blocks * local * cap * width + 18 * local * units * width
    return pl.pallas_call(
        expert_kernel,
        grid=(local, blocks // step),
        in_specs=[rows_spec, rows_spec, slot_spec, unit_spec, unit_spec, unit_spec],
        out_specs=[rows_spec, rows_spec, slot_spec, unit_spec, unit_spec, unit_spec],
        out_shape=[
            rows_shape,
            rows_shape,
            jax.ShapeDtypeStruct((blocks, local, cap, 1), jnp.float32),
            unit_shape,
            unit_shape,
            unit_shape,
        ],
        compiler_params=pltpu.CompilerParams(vmem_limit_bytes=VMEM_BYTES),
        cost_estimate=pl.CostEstimate(flops=flops, bytes_accessed=moved, transcendentals=0),
        name="experts",
    )(row_inputs, gradients, weights, gate_t, up_t, down)


def combine_kernel(
    p_ref, y_ref, dr_ref, dw_ref, x_ref, g_ref, shared_ref, out_ref, ds_ref, grad_ref
):
    picks = p_ref[0]
    row_inputs, cotangent = x_ref[0], g_ref[0]
    gate, up, down = shared_ref[0], shared_ref[1], shared_ref[2]
    gate_pre = matmul_nt(row_inputs, gate)
    up_pre = matmul_nt(row_inputs, up)
    sigmoid_gate, hidden = swiglu(gate_pre, up_pre)
    out_ref[0] = (matmul_tn(picks, y_ref[0]) + matmul(hidden, down)).astype(jnp.bfloat16)
    dhidden = matmul_nt(cotangent, down)
    gate_grad, up_grad = swiglu_back(dhidden, gate_pre, up_pre, sigmoid_gate)
    back = matmul_tn(picks, dr_ref[0]) + matmul(gate_grad, gate) + matmul(up_grad, up)
    width = back.shape[1]
    ds_ref[0, :, :width] = back.astype(jnp.bfloat16)
    ds_ref[0, :, width:] = matmul_tn(picks, dw_ref[0]).astype(jnp.bfloat16)
    first = pl.program_id(0) == 0
    for index, (left, right) in enumerate(
        ((gate_grad, row_inputs), (up_grad, row_inputs), (hidden, cotangent))
    ):
        part = matmul_tn(left, right)

        @pl.when(first)
        def _(index=index, part=part):
            grad_ref[index] = part

        @pl.when(jnp.logical_not(first))
        def _(index=index, part=part):
            grad_ref[index] += part


def combine_stage(picks, produced, back, spread, tokens, gradients, shared):
    blocks, slots, rows = picks.shape
    width = tokens.shape[-1]
    slot_spec = pl.BlockSpec((1, slots, width), lambda b: (b, 0, 0))
    rows_spec = pl.BlockSpec((1, rows, width), lambda b: (b, 0, 0))
    whole = pl.BlockSpec(shared.shape, lambda b: (0, 0, 0))
    lanes = spread.shape[-1]
    units = shared.shape[1]
    flops = 4 * blocks * slots * rows * width + 18 * blocks * rows * width * units
    moved = 4 * blocks * slots * width + 8 * blocks * rows * width
    return pl.pallas_call(
        combine_kernel,
        grid=(blocks,),
        in_specs=[
            pl.BlockSpec((1, slots, rows), lambda b: (b, 0, 0)),
            slot_spec,
            slot_spec,
            pl.BlockSpec((1, slots, lanes), lambda b: (b, 0, 0)),
            rows_spec,
            rows_spec,
            whole,
        ],
        out_specs=[
            rows_spec,
            pl.BlockSpec((1, rows, width + lanes), lambda b: (b, 0, 0)),
            whole,
        ],
        out_shape=[
            jax.ShapeDtypeStruct((blocks, rows, width), jnp.bfloat16),
            jax.ShapeDtypeStruct((blocks, rows, width + lanes), jnp.bfloat16),
            jax.ShapeDtypeStruct(shared.shape, jnp.float32),
        ],
        compiler_params=pltpu.CompilerParams(vmem_limit_bytes=VMEM_BYTES),
        cost_estimate=pl.CostEstimate(flops=flops, bytes_accessed=moved, transcendentals=0),
        name="combine",
    )(picks, produced, back, spread, tokens, gradients, shared)


MESH = pl.DeviceIdType.MESH
PAIR = 2
ANY = pl.BlockSpec(memory_space=pl.ANY)
IN_VMEM = pl.BlockSpec(memory_space=pltpu.VMEM)
DMA = pltpu.SemaphoreType.DMA


def place():
    me, part = lax.axis_index("expert"), lax.axis_index("tensor")
    return (me // PAIR, me % PAIR, part // PAIR, part % PAIR)


def device(z, x, y, c):
    return {"expert": z * PAIR + x, "tensor": y * PAIR + c}


def greet(peers):
    barrier = pltpu.get_barrier_semaphore()
    for peer in peers:
        pl.semaphore_signal(barrier, inc=1, device_id=peer, device_id_type=MESH)
    pl.semaphore_wait(barrier, len(peers))


def push(source, target, send, arrive, peer):
    copy = pltpu.make_async_remote_copy(
        src_ref=source,
        dst_ref=target,
        send_sem=send,
        recv_sem=arrive,
        device_id=peer,
        device_id_type=MESH,
    )
    copy.start()
    return copy


def bring(source, target, done):
    copy = pltpu.make_async_copy(source, target, done)
    copy.start()
    return copy


def arrived(target, done):
    pltpu.make_async_copy(target, target, done).wait()


def slot(ref, axis, index, size):
    start = pl.multiple_of(index * size, size)
    if axis == 0:
        return ref.at[pl.ds(start, size), :]
    return ref.at[:, pl.ds(start, size)]


class Calls:
    def __init__(self):
        self.count = 0

    def params(self):
        self.count += 1
        return pltpu.CompilerParams(
            collective_id=self.count, has_side_effects=True, vmem_limit_bytes=VMEM_BYTES
        )


def gather_expert_kernel(deep, axes, cuts, *refs):
    count = len(axes)
    sources, targets = list(refs[:count]), refs[count : 2 * count]
    held, (send, arrive, own) = refs[2 * count : 3 * count], refs[3 * count :]
    z, x, y, c = place()
    part = y * PAIR + c
    for i, cut in enumerate(cuts):
        if cut is not None:
            sources[i] = slot(sources[i], cut[0], part, cut[1])
    sizes = [h.shape[axis] for h, axis in zip(held, axes)]

    def at(i, from_z, from_x):
        return slot(targets[i], axes[i], from_z * PAIR + from_x, sizes[i])

    others = [device((z + k) % deep, x, y, c) for k in range(1, deep)]
    twin = device(z, 1 - x, y, c)
    greet(others + [twin])
    copies = []
    loads = [bring(sources[i], held[i], own.at[i]) for i in range(count)]
    for i in range(count):
        for k in range(1, deep):
            copies.append(
                push(sources[i], at(i, z, x), send.at[i, k], arrive.at[i, k], others[k - 1])
            )
        copies.append(push(sources[i], at(i, z, x), send.at[i, 0], arrive.at[i, 0], twin))
    stores = []
    for i in range(count):
        loads[i].wait()
        stores.append(bring(held[i], at(i, z, x), own.at[i]))
    for i in range(count):
        for k in range(1, deep):
            piece = at(i, (z + deep - k) % deep, x)
            arrived(piece, arrive.at[i, k])
            copies.append(
                push(piece, piece, send.at[i, deep + k], arrive.at[i, deep + k], twin)
            )
    for i in range(count):
        arrived(at(i, z, 1 - x), arrive.at[i, 0])
        for k in range(1, deep):
            arrived(at(i, (z + deep - k) % deep, 1 - x), arrive.at[i, deep + k])
    for copy in copies:
        copy.wait_send()
    for store in stores:
        store.wait()


def gather_expert(calls, groups, arrays, axes, cuts):
    deep = groups // PAIR
    held, shapes = [], []
    for array, axis, cut in zip(arrays, axes, cuts):
        shape = list(array.shape)
        if cut is not None:
            shape[cut[0]] = cut[1]
        held.append(pltpu.VMEM(tuple(shape), array.dtype))
        shape[axis] *= groups
        shapes.append(jax.ShapeDtypeStruct(tuple(shape), array.dtype))
    count = len(arrays)
    return pl.pallas_call(
        functools.partial(gather_expert_kernel, deep, tuple(axes), tuple(cuts)),
        in_specs=[ANY] * count,
        out_specs=[ANY] * count,
        out_shape=shapes,
        scratch_shapes=held
        + [DMA((count, 2 * deep)), DMA((count, 2 * deep)), DMA((count,))],
        compiler_params=calls.params(),
        name="gather_expert",
    )(*arrays)


def gather_tensor_kernel(axes, *refs):
    count = len(axes)
    sources, targets = refs[:count], refs[count : 2 * count]
    held, (send, arrive, own) = refs[2 * count : 3 * count], refs[3 * count :]
    z, x, y, c = place()
    sizes = [h.shape[axis] for h, axis in zip(held, axes)]

    def at(i, from_y, from_c):
        return slot(targets[i], axes[i], from_y * PAIR + from_c, sizes[i])

    across, beside = device(z, x, 1 - y, c), device(z, x, y, 1 - c)
    greet([across, beside])
    copies = []
    loads = [bring(sources[i], held[i], own.at[i]) for i in range(count)]
    for i in range(count):
        mine = at(i, y, c)
        copies.append(push(sources[i], mine, send.at[i, 0], arrive.at[i, 0], across))
        copies.append(push(sources[i], mine, send.at[i, 1], arrive.at[i, 1], beside))
    stores = []
    for i in range(count):
        loads[i].wait()
        stores.append(bring(held[i], at(i, y, c), own.at[i]))
    for i in range(count):
        piece = at(i, 1 - y, c)
        arrived(piece, arrive.at[i, 0])
        copies.append(push(piece, piece, send.at[i, 2], arrive.at[i, 2], beside))
    for i in range(count):
        arrived(at(i, y, 1 - c), arrive.at[i, 1])
        arrived(at(i, 1 - y, 1 - c), arrive.at[i, 2])
    for copy in copies:
        copy.wait_send()
    for store in stores:
        store.wait()


def gather_tensor(calls, parts, arrays, axes):
    shapes = []
    for array, axis in zip(arrays, axes):
        shape = list(array.shape)
        shape[axis] *= parts
        shapes.append(jax.ShapeDtypeStruct(tuple(shape), array.dtype))
    count = len(arrays)
    return pl.pallas_call(
        functools.partial(gather_tensor_kernel, tuple(axes)),
        in_specs=[ANY] * count,
        out_specs=[ANY] * count,
        out_shape=shapes,
        scratch_shapes=[pltpu.VMEM(a.shape, a.dtype) for a in arrays]
        + [DMA((count, 3)), DMA((count, 3)), DMA((count,))],
        compiler_params=calls.params(),
        name="gather_tensor",
    )(*arrays)


def add_rows(count, store):
    lax.fori_loop(0, count, lambda i, carry: (store(i), carry)[1], 0)


def sum_tensor_kernel(p_ref, o_ref, own_buf, from_beside, out_buf, from_across, send, arrive, own):
    z, x, y, c = place()
    rows = o_ref.shape[0]
    across, beside = device(z, x, 1 - y, c), device(z, x, y, 1 - c)
    greet([across, beside])
    first = push(p_ref.at[:, 1 - c], from_beside, send.at[0], arrive.at[0], beside)
    load = bring(p_ref.at[:, c], own_buf, own.at[0])
    load.wait()
    arrived(from_beside, arrive.at[0])
    step = 16

    def add(at, target, give):
        span = pl.ds(pl.multiple_of(at * step, step), step)
        total = own_buf[give, span, :].astype(jnp.float32) + from_beside[
            give, span, :
        ].astype(jnp.float32)
        target[span, :] = total.astype(target.dtype)

    add_rows(rows // step, lambda i: add(i, out_buf, 1 - y))
    second = push(out_buf, from_across, send.at[1], arrive.at[1], across)
    add_rows(rows // step, lambda i: add(i, o_ref, y))
    arrived(from_across, arrive.at[1])

    def finish(at):
        span = pl.ds(pl.multiple_of(at * step, step), step)
        o_ref[span, :] = o_ref[span, :] + from_across[span, :].astype(jnp.float32)

    add_rows(rows // step, finish)
    first.wait_send()
    second.wait_send()


def sum_tensor(calls, parts, partial):
    rows, width = partial.shape[0] // parts, partial.shape[1]
    half = parts // PAIR
    buf = pltpu.VMEM((half, rows, width), jnp.bfloat16)
    one = pltpu.VMEM((rows, width), jnp.bfloat16)
    return pl.pallas_call(
        sum_tensor_kernel,
        in_specs=[ANY],
        out_specs=IN_VMEM,
        out_shape=jax.ShapeDtypeStruct((rows, width), jnp.float32),
        scratch_shapes=[buf, buf, one, one, DMA((2,)), DMA((2,)), DMA((1,))],
        compiler_params=calls.params(),
        name="sum_tensor",
    )(partial.astype(jnp.bfloat16).reshape(half, PAIR, rows, width))


def gather_all_kernel(deep, streams, count, *refs):
    sources, targets = refs[:count], refs[count : 2 * count]
    held, (send, arrive, own) = refs[2 * count : 3 * count], refs[3 * count :]
    z, x, y, c = place()

    def at(s, from_z, from_x, from_y, from_c):
        i, left, wide, _ = streams[s]
        rows = held[i].shape[0]
        index = ((from_z * PAIR + from_x) * PAIR + from_y) * PAIR + from_c
        start = pl.multiple_of(index * rows, rows)
        return targets[i].at[pl.ds(start, rows), pl.ds(left, wide)]

    others = [device((z + k) % deep, x, y, c) for k in range(1, deep)]
    twin, across, beside = (
        device(z, 1 - x, y, c),
        device(z, x, 1 - y, c),
        device(z, x, y, 1 - c),
    )
    greet(others + [twin, across, beside])
    copies = []
    loads = [bring(sources[i], held[i], own.at[i]) for i in range(count)]

    def forward(s, number, peer, source, target):
        copies.append(push(source, target, send.at[s, number], arrive.at[s, number], peer))

    first = [twin if order == 0 else across for _, _, _, order in streams]
    second = [across if order == 0 else twin for _, _, _, order in streams]

    def piece(s, k, flip_first, flip_second, flip_core):
        order = streams[s][3]
        flip_x, flip_y = (
            (flip_first, flip_second) if order == 0 else (flip_second, flip_first)
        )
        return at(
            s,
            (z + deep - k) % deep,
            1 - x if flip_x else x,
            1 - y if flip_y else y,
            1 - c if flip_core else c,
        )

    for s in range(len(streams)):
        i, left, wide, _ = streams[s]
        source = sources[i].at[:, pl.ds(left, wide)]
        mine = piece(s, 0, False, False, False)
        for k in range(1, deep):
            forward(s, k, others[k - 1], source, mine)
        forward(s, deep, first[s], source, mine)
        forward(s, 2 * deep, second[s], source, mine)
        forward(s, 4 * deep, beside, source, mine)
    for k in range(1, deep):
        for s in range(len(streams)):
            got = piece(s, k, False, False, False)
            arrived(got, arrive.at[s, k])
            forward(s, deep + k, first[s], got, got)
            forward(s, 2 * deep + k, second[s], got, got)
            forward(s, 4 * deep + k, beside, got, got)
    for k in range(deep):
        for s in range(len(streams)):
            got = piece(s, k, True, False, False)
            arrived(got, arrive.at[s, deep + k])
            forward(s, 3 * deep + k, second[s], got, got)
            forward(s, 5 * deep + k, beside, got, got)
    for k in range(deep):
        for s in range(len(streams)):
            got = piece(s, k, False, True, False)
            arrived(got, arrive.at[s, 2 * deep + k])
            forward(s, 6 * deep + k, beside, got, got)
            got = piece(s, k, True, True, False)
            arrived(got, arrive.at[s, 3 * deep + k])
            forward(s, 7 * deep + k, beside, got, got)
    stores = []
    for i in range(count):
        loads[i].wait()
        rows = held[i].shape[0]
        index = ((z * PAIR + x) * PAIR + y) * PAIR + c
        stores.append(bring(held[i], slot(targets[i], 0, index, rows), own.at[i]))
    for k in range(deep):
        for s in range(len(streams)):
            arrived(piece(s, k, False, False, True), arrive.at[s, 4 * deep + k])
            arrived(piece(s, k, True, False, True), arrive.at[s, 5 * deep + k])
            arrived(piece(s, k, False, True, True), arrive.at[s, 6 * deep + k])
            arrived(piece(s, k, True, True, True), arrive.at[s, 7 * deep + k])
    for copy in copies:
        copy.wait_send()
    for store in stores:
        store.wait()


def gather_all(calls, groups, parts, arrays):
    deep = groups // PAIR
    streams = []
    for i, array in enumerate(arrays):
        wide = array.shape[1] // PAIR
        if wide % LANES == 0:
            streams += [(i, 0, wide, 0), (i, wide, wide, 1)]
        else:
            streams.append((i, 0, array.shape[1], 0))
    count = len(arrays)
    shapes = [
        jax.ShapeDtypeStruct((a.shape[0] * groups * parts, a.shape[1]), a.dtype) for a in arrays
    ]
    sems = DMA((len(streams), 8 * deep))
    return pl.pallas_call(
        functools.partial(gather_all_kernel, deep, tuple(streams), count),
        in_specs=[ANY] * count,
        out_specs=[ANY] * count,
        out_shape=shapes,
        scratch_shapes=[pltpu.VMEM(a.shape, a.dtype) for a in arrays]
        + [sems, sems, DMA((count,))],
        compiler_params=calls.params(),
        name="gather_all",
    )(*arrays)


def sum_all_kernel(deep, chunks, count, *refs):
    partials, outs = refs[:count], refs[count : 2 * count]
    total = len(chunks)
    rest = refs[2 * count :]
    own_buf, from_core = rest[:total], rest[total : 2 * total]
    from_first, from_second = rest[2 * total : 3 * total], rest[3 * total : 4 * total]
    from_deep = rest[4 * total : 5 * total]
    send, arrive, own = rest[5 * total :]
    z, x, y, c = place()
    others = [device((z + k) % deep, x, y, c) for k in range(1, deep)]
    twin, across, beside = (
        device(z, 1 - x, y, c),
        device(z, x, 1 - y, c),
        device(z, x, y, 1 - c),
    )
    greet(others + [twin, across, beside])
    copies, loads = [], []
    for n, (i, left, wide, order) in enumerate(chunks):
        span = pl.ds(left, wide)
        copies.append(
            push(
                partials[i].at[:, 1 - c, :, span],
                from_core[n],
                send.at[n, 0],
                arrive.at[n, 0],
                beside,
            )
        )
        loads.append(bring(partials[i].at[:, c, :, span], own_buf[n], own.at[n]))

    def index(order, depth, on_first, on_second):
        on_x, on_y = (on_first, on_second) if order == 0 else (on_second, on_first)
        return (depth * PAIR + on_x) * PAIR + on_y

    def stage_core(n):
        _, _, _, order = chunks[n]
        buf, other = own_buf[n], from_core[n]
        loads[n].wait()
        arrived(other, arrive.at[n, 0])

        def add(k):
            buf[k] = (buf[k].astype(jnp.float32) + other[k].astype(jnp.float32)).astype(
                jnp.bfloat16
            )

        add_rows(deep * PAIR * PAIR, add)
        mine = x if order == 0 else y
        for depth in range(deep):
            for s in range(PAIR):
                number = 1 + depth * PAIR + s
                copies.append(
                    push(
                        buf.at[index(order, depth, 1 - mine, s)],
                        from_first[n].at[depth * PAIR + s],
                        send.at[n, number],
                        arrive.at[n, number],
                        twin if order == 0 else across,
                    )
                )

    def stage_first(n):
        _, _, _, order = chunks[n]
        buf, other = own_buf[n], from_first[n]
        mine, following = (x, y) if order == 0 else (y, x)
        for number in range(1, 1 + PAIR * deep):
            arrived(other.at[number - 1], arrive.at[n, number])

        def add(k):
            at = index(order, k // PAIR, mine, k % PAIR)
            buf[at] = (buf[at].astype(jnp.float32) + other[k].astype(jnp.float32)).astype(
                jnp.bfloat16
            )

        add_rows(deep * PAIR, add)
        for depth in range(deep):
            number = 1 + PAIR * deep + depth
            copies.append(
                push(
                    buf.at[index(order, depth, mine, 1 - following)],
                    from_second[n].at[depth],
                    send.at[n, number],
                    arrive.at[n, number],
                    across if order == 0 else twin,
                )
            )

    def stage_second(n):
        _, _, _, order = chunks[n]
        buf, other = own_buf[n], from_second[n]
        mine, following = (x, y) if order == 0 else (y, x)
        base = 1 + PAIR * deep
        for depth in range(deep):
            arrived(other.at[depth], arrive.at[n, base + depth])

        def add(k):
            at = index(order, k, mine, following)
            buf[at] = (buf[at].astype(jnp.float32) + other[k].astype(jnp.float32)).astype(
                jnp.bfloat16
            )

        add_rows(deep, add)
        for k in range(1, deep):
            number = base + deep + k - 1
            copies.append(
                push(
                    buf.at[index(order, (z + k) % deep, mine, following)],
                    from_deep[n].at[k - 1],
                    send.at[n, number],
                    arrive.at[n, number],
                    others[k - 1],
                )
            )

    def stage_deep(n):
        i, left, wide, order = chunks[n]
        base = 1 + PAIR * deep + deep
        for k in range(1, deep):
            arrived(from_deep[n].at[k - 1], arrive.at[n, base + k - 1])
        mine, following = (x, y) if order == 0 else (y, x)
        result = own_buf[n][index(order, z, mine, following)].astype(jnp.float32)
        for k in range(deep - 1):
            result = result + from_deep[n][k].astype(jnp.float32)
        outs[i][:, pl.ds(left, wide)] = result

    for step in range(total + 3):
        for lag, stage in enumerate((stage_core, stage_first, stage_second, stage_deep)):
            if 0 <= step - lag < total:
                stage(step - lag)
    for copy in copies:
        copy.wait_send()


def sum_all(calls, groups, parts, arrays):
    deep = groups // PAIR
    rows = arrays[0].shape[0] // (groups * parts)
    budget, calls_of, used = 46 * 2**20, [[]], 0
    number = 0
    for i, array in enumerate(arrays):
        left = 0
        while left < array.shape[1]:
            wide = min(512, array.shape[1] - left)
            if 0 < array.shape[1] - left - wide < 512 // 2:
                wide = array.shape[1] - left
            cost = 2 * rows * wide * (4 * deep * 2 + 2 * deep + deep + deep) + 4 * rows * wide
            if used + cost > budget:
                calls_of.append([])
                used = 0
            used += cost
            calls_of[-1].append((i, left, wide, number % 2))
            number += 1
            left += wide
    views = [a.reshape(groups * parts // PAIR, PAIR, rows, a.shape[1]) for a in arrays]
    pieces = [[] for _ in arrays]
    for chunks in calls_of:
        used_arrays = sorted({c[0] for c in chunks})
        bounds = {
            i: (min(c[1] for c in chunks if c[0] == i), sum(c[2] for c in chunks if c[0] == i))
            for i in used_arrays
        }
        local = [(used_arrays.index(i), left, wide, order) for i, left, wide, order in chunks]
        count = len(used_arrays)
        many = deep * PAIR * PAIR

        def bufs(n):
            return [pltpu.VMEM((n, rows, wide), jnp.bfloat16) for _, _, wide, _ in chunks]

        sems = DMA((len(chunks), 1 + PAIR * deep + deep + deep))
        outs = pl.pallas_call(
            functools.partial(
                sum_all_kernel,
                deep,
                tuple(local),
                count,
            ),
            in_specs=[ANY] * count,
            out_specs=[IN_VMEM] * count,
            out_shape=[
                jax.ShapeDtypeStruct((rows, arrays[i].shape[1]), jnp.float32)
                for i in used_arrays
            ],
            scratch_shapes=bufs(many)
            + bufs(many)
            + bufs(PAIR * deep)
            + bufs(deep)
            + bufs(deep - 1)
            + [sems, sems, DMA((len(chunks),))],
            compiler_params=calls.params(),
            name="sum_all",
        )(*[views[i] for i in used_arrays])
        for i, out in zip(used_arrays, outs):
            pieces[i].append(out[:, bounds[i][0] : bounds[i][0] + bounds[i][1]])
    return [p[0] if len(p) == 1 else jnp.concatenate(p, axis=1) for p in pieces]


def sum_expert_kernel(deep, axes, *refs):
    count = len(axes)
    grads, outs = refs[:count], refs[count : 2 * count]
    rest = refs[2 * count :]
    own_buf, from_twin = rest[:count], rest[count : 2 * count]
    from_deep, (send, arrive, own) = rest[2 * count : 3 * count], rest[3 * count :]
    z, x, y, c = place()
    others = [device((z + k) % deep, x, y, c) for k in range(1, deep)]
    twin = device(z, 1 - x, y, c)
    greet(others + [twin])
    sizes = [o.shape[axis] for o, axis in zip(outs, axes)]
    copies, loads = [], []
    for i in range(count):
        loads.append([])
        for k in list(range(1, deep)) + [0]:
            far = (z + k) % deep
            copies.append(
                push(
                    slot(grads[i], axes[i], far * PAIR + 1 - x, sizes[i]),
                    from_twin[i].at[k],
                    send.at[i, k],
                    arrive.at[i, k],
                    twin,
                )
            )
            loads[i].append(
                bring(
                    slot(grads[i], axes[i], far * PAIR + x, sizes[i]),
                    own_buf[i].at[k],
                    own.at[i, k],
                )
            )
    step = 16
    for i in range(count):
        for load in loads[i]:
            load.wait()
        rows = own_buf[i].shape[1]
        for k in list(range(1, deep)) + [0]:
            arrived(from_twin[i].at[k], arrive.at[i, k])
            if k:

                def add(at, i=i, k=k):
                    span = pl.ds(pl.multiple_of(at * step, step), step)
                    own_buf[i][k, span, :] = (
                        own_buf[i][k, span, :].astype(jnp.float32)
                        + from_twin[i][k, span, :].astype(jnp.float32)
                    ).astype(jnp.bfloat16)

                add_rows(rows // step, add)
                copies.append(
                    push(
                        own_buf[i].at[k],
                        from_deep[i].at[k - 1],
                        send.at[i, deep + k],
                        arrive.at[i, deep + k],
                        others[k - 1],
                    )
                )
    for i in range(count):
        for k in range(1, deep):
            arrived(from_deep[i].at[k - 1], arrive.at[i, deep + k])

        def finish(at, i=i):
            span = pl.ds(pl.multiple_of(at * step, step), step)
            result = own_buf[i][0, span, :].astype(jnp.float32)
            result = result + from_twin[i][0, span, :].astype(jnp.float32)
            for k in range(deep - 1):
                result = result + from_deep[i][k, span, :].astype(jnp.float32)
            outs[i][span, :] = result

        add_rows(own_buf[i].shape[1] // step, finish)
    for copy in copies:
        copy.wait_send()


def sum_expert(calls, groups, arrays, axes):
    deep = groups // PAIR
    shapes = []
    for array, axis in zip(arrays, axes):
        shape = list(array.shape)
        shape[axis] //= groups
        shapes.append(tuple(shape))
    count = len(arrays)

    def bufs(n):
        return [pltpu.VMEM((n, *shape), jnp.bfloat16) for shape in shapes]

    sems = DMA((count, 2 * deep))
    return pl.pallas_call(
        functools.partial(sum_expert_kernel, deep, tuple(axes)),
        in_specs=[ANY] * count,
        out_specs=[IN_VMEM] * count,
        out_shape=[jax.ShapeDtypeStruct(shape, jnp.float32) for shape in shapes],
        scratch_shapes=bufs(deep) + bufs(deep) + bufs(deep - 1) + [sems, sems, DMA((count, deep))],
        compiler_params=calls.params(),
        name="sum_expert",
    )(*arrays)


ALL = ("expert", "tensor")


def gather(values, axes, dimension):
    return lax.all_gather(values, axes, axis=dimension, tiled=True)


def scatter_sum(values, axes, dimension):
    return lax.psum_scatter(
        values.astype(jnp.bfloat16), axes, scatter_dimension=dimension, tiled=True
    ).astype(jnp.float32)


def aligned(size, axis):
    return size % LANES == 0 if axis else size % 16 == 0


def gather_experts(calls, groups, part, items):
    taken = [axis == 0 or aligned(array.shape[axis], axis) for array, axis, _ in items]
    given = [item for item, take in zip(items, taken) if take]
    results = iter(gather_expert(calls, groups, *zip(*given)))

    def native(array, axis, cut):
        if cut is not None:
            array = lax.dynamic_slice_in_dim(array, part * cut[1], cut[1], axis=cut[0])
        return gather(array, "expert", axis)

    return [next(results) if take else native(*item) for item, take in zip(items, taken)]


def sum_experts(calls, groups, items):
    items = [(array.astype(jnp.bfloat16), axis) for array, axis in items]
    taken = [aligned(array.shape[axis] // groups, axis) for array, axis in items]
    given = [item for item, take in zip(items, taken) if take]
    results = iter(sum_expert(calls, groups, *zip(*given)))
    return [
        next(results) if take else scatter_sum(item[0], "expert", item[1])
        for item, take in zip(items, taken)
    ]


def part_of(values, index, count, dimension):
    size = values.shape[dimension] // count
    return lax.dynamic_slice_in_dim(values, index * size, size, axis=dimension)


def body(
    calls,
    block_in,
    attention_gain,
    query_down,
    query_gain,
    query_up,
    latent_down,
    latent_gain,
    latent_up,
    out_proj,
    ffn_gain,
    router,
    shared_gate,
    shared_up,
    shared_down,
    expert_gate,
    expert_up,
    expert_down,
    doc_lengths,
    routes,
    out_grad,
):
    groups = lax.axis_size("expert")
    parts = lax.axis_size("tensor")
    me = lax.axis_index("expert")
    part = lax.axis_index("tensor")
    row_count, width = block_in.shape
    top = routes.shape[1]
    local = expert_gate.shape[0]
    experts = local * groups
    latent_rank = latent_gain.shape[0] * groups
    query_rank = query_gain.shape[0] * groups

    all_gains = (attention_gain, ffn_gain, query_gain, latent_gain)
    gain_sizes = [g.shape[0] for g in all_gains]
    gain_room = -(-sum(gain_sizes) // (16 * LANES)) * 16 * LANES
    gains = jnp.concatenate([g.astype(jnp.float32) for g in all_gains])
    gains = jnp.pad(gains, (0, gain_room - sum(gain_sizes))).reshape(-1, LANES)
    routes_pad = jnp.pad(routes.T, ((0, -top % 8), (0, 0)))
    query_cut = query_down.shape[1] // parts
    latent_cut = latent_down.shape[1] // parts
    (
        gains,
        query_down_part,
        latent_down_part,
        query_up_full,
        latent_up_full,
        out_proj_full,
        router_t,
        routes_t,
    ) = gather_experts(
        calls,
        groups,
        part,
        [
            (gains, 0, None),
            (query_down, 0, (1, query_cut)),
            (latent_down.T, 1, (0, latent_cut)),
            (query_up, 0, None),
            (latent_up, 0, None),
            (out_proj, 1, None),
            (router.T, 1, None),
            (routes_pad, 1, None),
        ],
    )
    routes_t = routes_t[:top]
    gains = gains.reshape(groups, gain_room)
    ends = [sum(gain_sizes[: i + 1]) for i in range(len(gain_sizes))]
    attention_full, ffn_full, query_gain_full, latent_gain_full = (
        gains[:, end - size : end].reshape(-1) for size, end in zip(gain_sizes, ends)
    )
    gradient_all = gather(part_of(out_grad, part, parts, 0), ALL, 0)
    shared = jnp.stack([shared_gate.T, shared_up.T, shared_down])
    shared_units = shared.shape[1] // groups
    shared = shared.reshape(3, groups, shared_units, -1).transpose(1, 0, 2, 3)
    shared = lax.all_to_all(shared, "expert", split_axis=0, concat_axis=0, tiled=True)
    shared = shared.transpose(1, 2, 0, 3).reshape(3, shared_units, width)

    residual = block_in.astype(jnp.float32)
    allowed, cosine, sinusoid = layout(doc_lengths[0], row_count)
    first_f, inverse_first = rms_forward(residual, attention_full)
    first_normed = first_f.astype(jnp.bfloat16)
    query_lat = matmul(first_normed, query_down_part).astype(jnp.bfloat16)
    latent_all = matmul_nt(latent_down_part, first_normed).astype(jnp.bfloat16)
    query_lat, latent_all = gather_tensor(calls, parts, (query_lat, latent_all), (1, 0))
    query_lat = query_lat.astype(jnp.float32)
    latent_all = latent_all.T.astype(jnp.float32)
    query_n, inverse_query = rms_forward(query_lat, query_gain_full)
    query_n = query_n.astype(jnp.bfloat16)
    latent = latent_all[:, :latent_rank]
    latent_n, inverse_latent = rms_forward(latent, latent_gain_full)
    latent_n = latent_n.astype(jnp.bfloat16)
    key_rope = rotate(latent_all[:, latent_rank:], cosine, sinusoid)

    attended, logsum, queries, key_rows, value_rows = heads_forward(
        query_n, latent_n, key_rope, query_up_full, latent_up_full, allowed, cosine, sinusoid
    )
    mixed_heads = sum_tensor(calls, parts, matmul(attended, out_proj_full))

    residual_rows = part_of(residual, part, parts, 0)
    gradient_rows = part_of(out_grad, part, parts, 0).astype(jnp.float32)
    middle = residual_rows + mixed_heads
    second_f, inverse_ffn = rms_forward(middle, ffn_full)
    second_normed = second_f.astype(jnp.bfloat16)
    routes_rows = part_of(routes, part, parts, 0)
    expert_ids = jnp.arange(experts, dtype=jnp.int32)
    routed_here = jnp.any(routes_rows[:, :, None] == expert_ids[None, None, :], axis=1)
    chosen = jnp.where(routed_here, jax.nn.sigmoid(matmul_nt(second_normed, router_t)), 0.0)
    totals = jnp.sum(chosen, axis=-1, keepdims=True)
    route_weights = ROUTE_SCALE * chosen / totals

    lane_pad = -experts % LANES
    tokens, weights_all = gather_all(
        calls, groups, parts, (second_normed, jnp.pad(route_weights, ((0, 0), (0, lane_pad))))
    )
    tokens = tokens.reshape(groups, row_count, width)
    gradients = gradient_all.reshape(groups, row_count, width)

    own_ids = me * local + jnp.arange(local, dtype=jnp.int32)
    named = jnp.any(
        routes_t.reshape(top, groups, 1, row_count) == own_ids[None, None, :, None], axis=0
    )
    row_index = jnp.arange(row_count, dtype=jnp.int32)
    earlier = (row_index[:, None] < row_index[None, :]).astype(jnp.bfloat16)
    rank = contract("bjs,st->bjt", named.astype(jnp.bfloat16), earlier)
    slots = jnp.arange(CAP, dtype=jnp.int32).astype(jnp.float32)
    picked = named[:, :, None, :] & (rank[:, :, None, :] == slots[None, None, :, None])
    own_weights = lax.dynamic_slice_in_dim(weights_all, me * local, local, axis=1)
    own_weights = own_weights.reshape(groups, row_count, local).transpose(0, 2, 1)
    slot_weights = jnp.sum(
        jnp.where(picked, own_weights[:, :, None, :], 0.0), axis=-1, keepdims=True
    )
    picks = picked.astype(jnp.bfloat16).reshape(groups, local * CAP, row_count)
    expert_rows = contract("bst,btd->bsd", picks, tokens).astype(jnp.bfloat16)
    expert_grads = contract("bst,btd->bsd", picks, gradients).astype(jnp.bfloat16)
    slot_shape = (groups, local, CAP, width)
    produced, back, slot_dweights, grad_gate, grad_up, grad_down = expert_stage(
        expert_rows.reshape(slot_shape),
        expert_grads.reshape(slot_shape),
        slot_weights,
        expert_gate.transpose(0, 2, 1),
        expert_up.transpose(0, 2, 1),
        expert_down,
    )
    lane_ids = jnp.arange(experts + lane_pad, dtype=jnp.int32)
    spread = jnp.where(
        own_ids[None, :, None, None] == lane_ids[None, None, None, :], slot_dweights, 0.0
    ).astype(jnp.bfloat16)
    mixed_part, dsecond_part, grad_shared = combine_stage(
        picks,
        produced.reshape(groups, local * CAP, width),
        back.reshape(groups, local * CAP, width),
        spread.reshape(groups, local * CAP, experts + lane_pad),
        tokens,
        gradients,
        shared,
    )
    dsecond, mixed = sum_all(
        calls,
        groups,
        parts,
        (
            dsecond_part.reshape(-1, width + experts + lane_pad),
            mixed_part.reshape(-1, width),
        ),
    )
    dweights = dsecond[:, width : width + experts]
    dsecond = dsecond[:, :width]

    dchosen = (
        ROUTE_SCALE
        / totals
        * (dweights - jnp.sum(dweights * chosen, axis=-1, keepdims=True) / totals)
    )
    dlogits = jnp.where(routed_here, dchosen * chosen * (1.0 - chosen), 0.0).astype(jnp.bfloat16)
    dsecond = dsecond + matmul(dlogits, router_t)
    grad_router = matmul_tn(dlogits, second_normed)
    grad_ffn_gain = gain_gradient(middle, inverse_ffn, dsecond)
    middle_grad = gradient_rows + rms_backward(middle, inverse_ffn, ffn_full, dsecond)

    attention_grad, block_out = gather_tensor(
        calls,
        parts,
        (middle_grad.astype(jnp.bfloat16), (middle + mixed).astype(jnp.bfloat16)),
        (0, 0),
    )
    grad_out_proj = matmul_tn(attended, attention_grad)
    attended_grad = matmul_nt(attention_grad, out_proj_full).astype(jnp.bfloat16)
    dquery_n, dlatent_n, dkey_rope, grad_query_up, grad_latent_up = heads_backward(
        attended_grad,
        logsum,
        queries,
        key_rows,
        value_rows,
        query_n,
        latent_n,
        query_up_full,
        latent_up_full,
        allowed,
        cosine,
        sinusoid,
    )
    heads_grad = jnp.concatenate(
        [v.astype(jnp.bfloat16) for v in (dquery_n, dlatent_n, dkey_rope)], axis=1
    )
    heads_wide = heads_grad.shape[1]
    heads_grad = jnp.pad(heads_grad, ((0, 0), (0, -heads_wide % LANES)))
    heads_grad = sum_tensor(calls, parts, heads_grad)
    dquery_n = heads_grad[:, :query_rank]
    dlatent_n = heads_grad[:, query_rank : query_rank + latent_rank]
    dkey_rope = heads_grad[:, query_rank + latent_rank : heads_wide]
    query_lat_rows = part_of(query_lat, part, parts, 0)
    latent_rows = part_of(latent, part, parts, 0)
    inverse_query_rows = part_of(inverse_query, part, parts, 0)
    inverse_latent_rows = part_of(inverse_latent, part, parts, 0)
    dquery_lat = rms_backward(query_lat_rows, inverse_query_rows, query_gain_full, dquery_n)
    grad_query_gain = gain_gradient(query_lat_rows, inverse_query_rows, dquery_n)
    dlatent = rms_backward(latent_rows, inverse_latent_rows, latent_gain_full, dlatent_n)
    grad_latent_gain = gain_gradient(latent_rows, inverse_latent_rows, dlatent_n)
    dlatent_all = jnp.concatenate([dlatent, dkey_rope], axis=-1)
    dquery_lat = lax.all_to_all(
        dquery_lat.astype(jnp.bfloat16), "tensor", split_axis=1, concat_axis=0, tiled=True
    )
    dlatent_all = lax.all_to_all(
        dlatent_all.astype(jnp.bfloat16), "tensor", split_axis=1, concat_axis=0, tiled=True
    )
    grad_query_down = matmul_tn(first_normed, dquery_lat)
    grad_latent_down = matmul_tn(dlatent_all, first_normed)
    dfirst = matmul_nt(dquery_lat, query_down_part) + matmul(dlatent_all, latent_down_part)
    dfirst = sum_tensor(calls, parts, dfirst)
    inverse_rows = part_of(inverse_first, part, parts, 0)
    dresidual = rms_backward(residual_rows, inverse_rows, attention_full, dfirst)
    grad_attention_gain = gain_gradient(residual_rows, inverse_rows, dfirst)

    grad_shared = grad_shared.astype(jnp.bfloat16).reshape(3, shared_units, groups, -1)
    grad_shared = grad_shared.transpose(2, 0, 1, 3)
    grad_shared = lax.all_to_all(grad_shared, "expert", split_axis=0, concat_axis=0, tiled=True)
    grad_shared = grad_shared.transpose(1, 0, 2, 3).astype(jnp.float32)
    grad_shared = grad_shared.reshape(3, groups * shared_units, -1)
    grad_gains = jnp.concatenate(
        [
            g.reshape(groups, -1)
            for g in (grad_attention_gain, grad_ffn_gain, grad_query_gain, grad_latent_gain)
        ],
        axis=1,
    )
    grad_gains = jnp.pad(grad_gains, ((0, 0), (0, gain_room - grad_gains.shape[1])))
    (
        grad_query_up,
        grad_latent_up,
        grad_out_proj,
        grad_query_down,
        grad_latent_down,
        grad_router,
        grad_gains,
    ) = sum_experts(
        calls,
        groups,
        [
            (grad_query_up, 0),
            (grad_latent_up, 0),
            (grad_out_proj, 1),
            (grad_query_down, 0),
            (grad_latent_down, 1),
            (grad_router, 1),
            (grad_gains.reshape(-1, LANES), 0),
        ],
    )
    input_grad, grad_query_down, grad_latent_down, grad_router, grad_gains = gather_tensor(
        calls,
        parts,
        (
            (middle_grad + dresidual).astype(jnp.bfloat16),
            grad_query_down.astype(jnp.bfloat16),
            grad_latent_down.astype(jnp.bfloat16),
            grad_router,
            grad_gains,
        ),
        (0, 1, 0, 0, 0),
    )
    grad_router = jnp.sum(grad_router.reshape(parts, experts, -1), axis=0)
    grad_gains = jnp.sum(grad_gains.reshape(parts, gain_room), axis=0)
    grad_attention_gain, grad_ffn_gain, grad_query_gain, grad_latent_gain = (
        grad_gains[end - size : end] for size, end in zip(gain_sizes, ends)
    )

    return (
        block_out,
        input_grad,
        grad_attention_gain,
        grad_query_down.astype(jnp.float32),
        grad_query_gain,
        grad_query_up,
        grad_latent_down.astype(jnp.float32).T,
        grad_latent_gain,
        grad_latent_up,
        grad_out_proj,
        grad_ffn_gain,
        grad_router.T,
        grad_shared[0].T,
        grad_shared[1].T,
        grad_shared[2],
        grad_gate.transpose(0, 2, 1),
        grad_up.transpose(0, 2, 1),
        grad_down,
    )


def solution(mesh):
    placed = (
        P("expert", None),
        P("expert"),
        P("expert", None),
        P("expert"),
        P("expert", "tensor"),
        P("expert", None),
        P("expert"),
        P("expert", "tensor"),
        P("tensor", "expert"),
        P("expert"),
        P("expert", None),
        P("expert", "tensor"),
        P("expert", "tensor"),
        P("tensor", "expert"),
        P("expert", None, "tensor"),
        P("expert", None, "tensor"),
        P("expert", "tensor", None),
        P("expert", None),
        P("expert", None),
        P("expert", None),
    )
    return jax.shard_map(
        functools.partial(body, Calls()),
        mesh=mesh,
        in_specs=placed,
        out_specs=(
            P("expert", None),
            P("expert", None),
            P("expert"),
            P("expert", None),
            P("expert"),
            P("expert", "tensor"),
            P("expert", None),
            P("expert"),
            P("expert", "tensor"),
            P("tensor", "expert"),
            P("expert"),
            P("expert", None),
            P("expert", "tensor"),
            P("expert", "tensor"),
            P("tensor", "expert"),
            P("expert", None, "tensor"),
            P("expert", None, "tensor"),
            P("expert", "tensor", None),
        ),
        check_vma=False,
    )
```

```python
import functools
import math

import jax
import jax.numpy as jnp
from jax import lax
from jax.experimental import pallas as pl
from jax.experimental.pallas import tpu as pltpu
from jax.sharding import PartitionSpec as P

NOPE = 128
ROPE = 64
VD = 128
CAP = 32
LANES = 128
VMEM_BYTES = 60 * 2**20

EPSILON = 1e-06
ROPE_BASE = 50000.0
ROUTE_SCALE = 2.446

ATTENDED = "attended"
EXPERT = "expert"
FIRST = "first"
GAINS = "gains"
I_PARTIAL = "i_partial"
KEYS = "keys"
LATENT_DOWN = "latent_down"
LATENT_N = "latent_n"
LATENT_T = "latent_t"
LATENT_UP = "latent_up"
OUT_GRAD = "out_grad"
OUT_PROJ = "out_proj"
OWN_SHARED = "own_shared"
QUERIES = "queries"
QUERY_DOWN = "query_down"
QUERY_LAT = "query_lat"
QUERY_N = "query_n"
QUERY_UP = "query_up"
READY = "ready"
ROUTER = "router"
ROUTES = "routes"
SHARED = "shared"
SHUFFLE = "shuffle"
TENSOR = "tensor"
TOKENS = "tokens"
VALUES = "values"
VMEM_ = "vmem"
WEIGHTS = "weights"
ZXYC = "zxyc"


def matmul(left, right):
    return jnp.dot(left, right, preferred_element_type=jnp.float32)


def contract(form, left, right):
    return jnp.einsum(form, left, right, preferred_element_type=jnp.float32)


def matmul_nt(left, right):
    return lax.dot_general(left, right, (((1,), (1,)), ((), ())), preferred_element_type=jnp.float32)


def matmul_tn(left, right):
    return lax.dot_general(left, right, (((0,), (0,)), ((), ())), preferred_element_type=jnp.float32)


def layout(lengths, row_count):
    doc_count = lengths.shape[0]
    doc_ends = jnp.cumsum(lengths)
    starts = doc_ends - lengths
    row_index = jnp.arange(row_count, dtype=jnp.int32)
    doc_ids = jnp.sum((row_index[:, None] >= doc_ends[None, :]).astype(jnp.int32), axis=1)
    owners = doc_ids[:, None] == jnp.arange(doc_count, dtype=jnp.int32)[None, :]
    first_row = jnp.sum(jnp.where(owners, starts[None, :], 0), axis=1)
    positions = (row_index - first_row).astype(jnp.float32)
    allowed = (doc_ids[:, None] == doc_ids[None, :]) & (row_index[None, :] <= row_index[:, None])
    frequency = jnp.exp(
        -math.log(ROPE_BASE) * 2.0 * jnp.arange(ROPE // 2, dtype=jnp.float32) / ROPE
    )
    angles = positions[:, None] * frequency[None, :]
    return (allowed, jnp.cos(angles), jnp.sin(angles))


def swiglu(gate_pre, up_pre):
    sigmoid_gate = jax.nn.sigmoid(gate_pre)
    return (sigmoid_gate, (gate_pre * sigmoid_gate * up_pre).astype(jnp.bfloat16))


def swiglu_back(dhidden, gate_pre, up_pre, sigmoid_gate):
    gate_grad = dhidden * up_pre * sigmoid_gate * (1.0 + gate_pre * (1.0 - sigmoid_gate))
    up_grad = dhidden * gate_pre * sigmoid_gate
    return (gate_grad.astype(jnp.bfloat16), up_grad.astype(jnp.bfloat16))


def expert_kernel(
    x_ref, g_ref, w_ref, gate_ref, up_ref, down_ref, y_ref, dr_ref, dw_ref, gg_ref, gu_ref, gd_ref
):
    blocks, _, cap, width = x_ref.shape
    rows = blocks * cap
    row_inputs = x_ref[...].reshape(rows, width)
    gradient = g_ref[...].reshape(rows, width).astype(jnp.float32)
    weight = w_ref[...].reshape(rows, 1)
    gate, up, down = gate_ref[0], up_ref[0], down_ref[0]
    gate_pre = matmul_nt(row_inputs, gate)
    up_pre = matmul_nt(row_inputs, up)
    sigmoid_gate, hidden = swiglu(gate_pre, up_pre)
    produced = matmul(hidden, down)
    dw_ref[...] = jnp.sum(gradient * produced, axis=1, keepdims=True).reshape(dw_ref.shape)
    y_ref[...] = (weight * produced).astype(jnp.bfloat16).reshape(y_ref.shape)
    cotangent = (weight * gradient).astype(jnp.bfloat16)
    dhidden = matmul_nt(cotangent, down)
    gate_grad, up_grad = swiglu_back(dhidden, gate_pre, up_pre, sigmoid_gate)
    back = matmul(gate_grad, gate) + matmul(up_grad, up)
    dr_ref[...] = back.astype(jnp.bfloat16).reshape(dr_ref.shape)
    first = pl.program_id(1) == 0

    def accumulate(ref, left, right):
        part = matmul_tn(left, right)

        @pl.when(first)
        def _():
            ref[0] = part

        @pl.when(jnp.logical_not(first))
        def _():
            ref[0] += part

    accumulate(gg_ref, gate_grad, row_inputs)
    accumulate(gu_ref, up_grad, row_inputs)
    accumulate(gd_ref, hidden, cotangent)


def expert_stage(row_inputs, gradients, weights, gate_t, up_t, down):
    blocks, local, cap, width = row_inputs.shape
    units = gate_t.shape[1]
    step = min(blocks, 256 // cap)
    rows_spec = pl.BlockSpec((step, 1, cap, width), lambda j, r: (r, j, 0, 0))
    slot_spec = pl.BlockSpec((step, 1, cap, 1), lambda j, r: (r, j, 0, 0))
    unit_spec = pl.BlockSpec((1, units, width), lambda j, r: (j, 0, 0))
    rows_shape = jax.ShapeDtypeStruct(row_inputs.shape, jnp.bfloat16)
    unit_shape = jax.ShapeDtypeStruct((local, units, width), jnp.float32)
    flops = 18 * blocks * local * cap * width * units
    moved = 8 * blocks * local * cap * width + 18 * local * units * width
    return pl.pallas_call(
        expert_kernel,
        grid=(local, blocks // step),
        in_specs=[rows_spec, rows_spec, slot_spec, unit_spec, unit_spec, unit_spec],
        out_specs=[rows_spec, rows_spec, slot_spec, unit_spec, unit_spec, unit_spec],
        out_shape=[
            rows_shape,
            rows_shape,
            jax.ShapeDtypeStruct((blocks, local, cap, 1), jnp.float32),
            unit_shape,
            unit_shape,
            unit_shape,
        ],
        compiler_params=pltpu.CompilerParams(vmem_limit_bytes=VMEM_BYTES),
        cost_estimate=pl.CostEstimate(flops=flops, bytes_accessed=moved, transcendentals=0),
        name="experts",
    )(row_inputs, gradients, weights, gate_t, up_t, down)


def combine_kernel(
    p_ref, y_ref, dr_ref, dw_ref, x_ref, g_ref, shared_ref, out_ref, ds_ref, grad_ref
):
    picks = p_ref[0]
    row_inputs, cotangent = x_ref[0], g_ref[0]
    gate, up, down = shared_ref[0], shared_ref[1], shared_ref[2]
    gate_pre = matmul_nt(row_inputs, gate)
    up_pre = matmul_nt(row_inputs, up)
    sigmoid_gate, hidden = swiglu(gate_pre, up_pre)
    out_ref[0] = (matmul_tn(picks, y_ref[0]) + matmul(hidden, down)).astype(jnp.bfloat16)
    dhidden = matmul_nt(cotangent, down)
    gate_grad, up_grad = swiglu_back(dhidden, gate_pre, up_pre, sigmoid_gate)
    back = matmul_tn(picks, dr_ref[0]) + matmul(gate_grad, gate) + matmul(up_grad, up)
    width = back.shape[1]
    ds_ref[0, :, :width] = back.astype(jnp.bfloat16)
    ds_ref[0, :, width:] = matmul_tn(picks, dw_ref[0]).astype(jnp.bfloat16)
    first = pl.program_id(0) == 0
    for index, (left, right) in enumerate(
        ((gate_grad, row_inputs), (up_grad, row_inputs), (hidden, cotangent))
    ):
        part = matmul_tn(left, right)

        @pl.when(first)
        def _(index=index, part=part):
            grad_ref[index] = part

        @pl.when(jnp.logical_not(first))
        def _(index=index, part=part):
            grad_ref[index] += part


def combine_stage(picks, produced, back, spread, tokens, gradients, shared):
    blocks, slots, rows = picks.shape
    width = tokens.shape[-1]
    slot_spec = pl.BlockSpec((1, slots, width), lambda b: (b, 0, 0))
    rows_spec = pl.BlockSpec((1, rows, width), lambda b: (b, 0, 0))
    whole = pl.BlockSpec(shared.shape, lambda b: (0, 0, 0))
    lanes = spread.shape[-1]
    units = shared.shape[1]
    flops = 4 * blocks * slots * rows * width + 18 * blocks * rows * width * units
    moved = 4 * blocks * slots * width + 8 * blocks * rows * width
    return pl.pallas_call(
        combine_kernel,
        grid=(blocks,),
        in_specs=[
            pl.BlockSpec((1, slots, rows), lambda b: (b, 0, 0)),
            slot_spec,
            slot_spec,
            pl.BlockSpec((1, slots, lanes), lambda b: (b, 0, 0)),
            rows_spec,
            rows_spec,
            whole,
        ],
        out_specs=[
            rows_spec,
            pl.BlockSpec((1, rows, width + lanes), lambda b: (b, 0, 0)),
            whole,
        ],
        out_shape=[
            jax.ShapeDtypeStruct((blocks, rows, width), jnp.bfloat16),
            jax.ShapeDtypeStruct((blocks, rows, width + lanes), jnp.bfloat16),
            jax.ShapeDtypeStruct(shared.shape, jnp.float32),
        ],
        compiler_params=pltpu.CompilerParams(vmem_limit_bytes=VMEM_BYTES),
        cost_estimate=pl.CostEstimate(flops=flops, bytes_accessed=moved, transcendentals=0),
        name="combine",
    )(picks, produced, back, spread, tokens, gradients, shared)


MESH = pl.DeviceIdType.MESH
PAIR = 2
ANY = pl.BlockSpec(memory_space=pl.ANY)
IN_VMEM = pl.BlockSpec(memory_space=pltpu.VMEM)
DMA = pltpu.SemaphoreType.DMA


def place():
    me, part = lax.axis_index(EXPERT), lax.axis_index(TENSOR)
    return (me // PAIR, me % PAIR, part // PAIR, part % PAIR)


def device(z, x, y, c):
    return {EXPERT: z * PAIR + x, TENSOR: y * PAIR + c}


def greet(peers):
    barrier = pltpu.get_barrier_semaphore()
    for peer in peers:
        pl.semaphore_signal(barrier, inc=1, device_id=peer, device_id_type=MESH)
    pl.semaphore_wait(barrier, len(peers))


def push(source, target, send, arrive, peer):
    copy = pltpu.make_async_remote_copy(
        src_ref=source,
        dst_ref=target,
        send_sem=send,
        recv_sem=arrive,
        device_id=peer,
        device_id_type=MESH,
    )
    copy.start()
    return copy


def bring(source, target, done):
    copy = pltpu.make_async_copy(source, target, done)
    copy.start()
    return copy


def arrived(target, done):
    pltpu.make_async_copy(target, target, done).wait()


def slot(ref, axis, index, size):
    start = pl.multiple_of(index * size, size)
    if axis == 0:
        return ref.at[pl.ds(start, size), :]
    return ref.at[:, pl.ds(start, size)]


class Bag(dict):
    __getattr__ = dict.__getitem__
    __setattr__ = dict.__setitem__


class Calls:
    def __init__(self):
        self.count = 0

    def params(self):
        self.count += 1
        return pltpu.CompilerParams(
            collective_id=self.count, has_side_effects=True, vmem_limit_bytes=VMEM_BYTES
        )


def choose(table, index):
    value = table[0]
    for i, entry in enumerate(table[1:], 1):
        if any(entry != other for other in table):
            value = jnp.where(index == i, entry, value)
    return value


class Link:
    def __init__(self, deep):
        me, part = lax.axis_index(EXPERT), lax.axis_index(TENSOR)
        self.deep, self.me, self.part = deep, me, part
        self.z, self.x = me // PAIR, me % PAIR
        self.y, self.c = part // PAIR, part % PAIR
        near = [
            sorted((k for k in range(1, deep)), key=lambda k: abs((z - k) % deep - z))
            for z in range(deep)
        ]
        self.order = [choose([near[z][h] for z in range(deep)], self.z) for h in range(deep - 1)]
        self.drains = []

    def at_z(self, z):
        return device(z, self.x, self.y, self.c)

    def peer(self, axis):
        flip = {name: 1 - getattr(self, name) if name == axis else getattr(self, name) for name in "xyc"}
        return device(self.z, flip["x"], flip["y"], flip["c"])

    def greet(self, groups, axes):
        peers = [{EXPERT: (self.me + j) % groups, TENSOR: self.part} for j in range(1, groups)]
        if "e" not in axes:
            peers = []
        greet(peers + [self.peer(axis) for axis in axes if axis != "e"])

    def emit(self, make, condition=None):
        def start():
            make().start()

        def finish():
            make().wait_send()

        if condition is None:
            start()
            self.drains.append(finish)
        else:
            pl.when(condition)(start)
            self.drains.append(lambda: pl.when(condition)(finish))

    def drain(self):
        for finish in self.drains:
            finish()
        self.drains = []


def spread(link, order, source, at, send, arrive):
    deep, z = link.deep, link.z
    cut = order.find("z")
    before, after = (order[:cut], order[cut + 1 :]) if cut >= 0 else ("", order)
    none = frozenset()

    def piece(k, flips):
        x, y, c = (
            1 - getattr(link, name) if name in flips else getattr(link, name) for name in "xyc"
        )
        return at((z + deep - k) % deep, x, y, c)

    def number(k, flips):
        return k * 8 + sum(1 << "xyc".index(name) for name in flips)

    def forward(k, flips, to_number, peer, condition=None):
        own = isinstance(k, int) and k == 0 and not flips

        def make():
            target = piece(k, flips)
            return pltpu.make_async_remote_copy(
                src_ref=source if own else target,
                dst_ref=target,
                send_sem=send.at[to_number],
                recv_sem=arrive.at[to_number],
                device_id=peer,
                device_id_type=MESH,
            )

        link.emit(make, condition)

    def hand_on(k, flips, axes, along_z):
        if along_z:
            forward(k, flips, number(1, flips), link.at_z(z + 1), z < deep - 1)
            forward(k, flips, number(deep - 1, flips), link.at_z(z - 1), z > 0)
        for axis in axes:
            forward(k, flips, number(k, flips | {axis}), link.peer(axis))

    def take(k, flips):
        arrived(piece(k, flips), arrive.at[number(k, flips)])

    hand_on(0, none, before + after, cut >= 0)
    got = [none]
    for i, axis in enumerate(before):
        for flips in got:
            yield
            take(0, flips | {axis})
            hand_on(0, flips | {axis}, before[i + 1 :] + after, True)
        got = got + [flips | {axis} for flips in got]
    ks = [0]
    if cut >= 0:
        for k in link.order:
            below = z >= k
            onward = jnp.where(below, k + 1, k - 1)
            more = jnp.where(below, z < deep - 1, z > 0)
            following = link.at_z(jnp.where(below, z + 1, z - 1))
            for flips in got:
                yield
                take(k, flips)
                forward(k, flips, number(onward, flips), following, more)
                hand_on(k, flips, after, False)
        ks = ks + link.order
    for i, axis in enumerate(after):
        for k in ks:
            for flips in got:
                yield
                take(k, flips | {axis})
                hand_on(k, flips | {axis}, after[i + 1 :], False)
        got = got + [flips | {axis} for flips in got]


def shuffle(link, groups, source, at, send, arrive):
    def make(j):
        target = (link.me + j) % groups
        return pltpu.make_async_remote_copy(
            src_ref=source(target),
            dst_ref=at(link.me),
            send_sem=send.at[j],
            recv_sem=arrive.at[j],
            device_id={EXPERT: target, TENSOR: link.part},
            device_id_type=MESH,
        )

    for j in range(1, groups):
        link.emit(functools.partial(make, j))
    for j in range(1, groups):
        yield
        arrived(at((link.me + groups - j) % groups), arrive.at[j])


def run(tasks):
    tasks = list(tasks)
    while tasks:
        tasks = [task for task in tasks if next(task, run) is not run]


def add_rows(count, store):
    lax.fori_loop(0, count, lambda i, carry: (store(i), carry)[1], 0)


def sum_all_kernel(deep, chunks, count, *refs):
    partials, outs = refs[:count], refs[count : 2 * count]
    total = len(chunks)
    rest = refs[2 * count :]
    own_buf, from_core = rest[:total], rest[total : 2 * total]
    from_first, from_second = rest[2 * total : 3 * total], rest[3 * total : 4 * total]
    from_deep = rest[4 * total : 5 * total]
    send, arrive, own = rest[5 * total :]
    z, x, y, c = place()
    others = [device((z + k) % deep, x, y, c) for k in range(1, deep)]
    twin, across, beside = (
        device(z, 1 - x, y, c),
        device(z, x, 1 - y, c),
        device(z, x, y, 1 - c),
    )
    greet(others + [twin, across, beside])
    copies, loads = [], []
    for n, (i, left, wide, order) in enumerate(chunks):
        span = pl.ds(left, wide)
        copies.append(
            push(
                partials[i].at[:, 1 - c, :, span],
                from_core[n],
                send.at[n, 0],
                arrive.at[n, 0],
                beside,
            )
        )
        loads.append(bring(partials[i].at[:, c, :, span], own_buf[n], own.at[n]))

    def index(order, depth, on_first, on_second):
        on_x, on_y = (on_first, on_second) if order == 0 else (on_second, on_first)
        return (depth * PAIR + on_x) * PAIR + on_y

    def stage_core(n):
        _, _, _, order = chunks[n]
        buf, other = own_buf[n], from_core[n]
        loads[n].wait()
        arrived(other, arrive.at[n, 0])

        def add(k):
            buf[k] = (buf[k].astype(jnp.float32) + other[k].astype(jnp.float32)).astype(
                jnp.bfloat16
            )

        add_rows(deep * PAIR * PAIR, add)
        mine = x if order == 0 else y
        for depth in range(deep):
            for s in range(PAIR):
                number = 1 + depth * PAIR + s
                copies.append(
                    push(
                        buf.at[index(order, depth, 1 - mine, s)],
                        from_first[n].at[depth * PAIR + s],
                        send.at[n, number],
                        arrive.at[n, number],
                        twin if order == 0 else across,
                    )
                )

    def stage_first(n):
        _, _, _, order = chunks[n]
        buf, other = own_buf[n], from_first[n]
        mine, following = (x, y) if order == 0 else (y, x)
        for number in range(1, 1 + PAIR * deep):
            arrived(other.at[number - 1], arrive.at[n, number])

        def add(k):
            at = index(order, k // PAIR, mine, k % PAIR)
            buf[at] = (buf[at].astype(jnp.float32) + other[k].astype(jnp.float32)).astype(
                jnp.bfloat16
            )

        add_rows(deep * PAIR, add)
        for depth in range(deep):
            number = 1 + PAIR * deep + depth
            copies.append(
                push(
                    buf.at[index(order, depth, mine, 1 - following)],
                    from_second[n].at[depth],
                    send.at[n, number],
                    arrive.at[n, number],
                    across if order == 0 else twin,
                )
            )

    def stage_second(n):
        _, _, _, order = chunks[n]
        buf, other = own_buf[n], from_second[n]
        mine, following = (x, y) if order == 0 else (y, x)
        base = 1 + PAIR * deep
        for depth in range(deep):
            arrived(other.at[depth], arrive.at[n, base + depth])

        def add(k):
            at = index(order, k, mine, following)
            buf[at] = (buf[at].astype(jnp.float32) + other[k].astype(jnp.float32)).astype(
                jnp.bfloat16
            )

        add_rows(deep, add)
        for k in range(1, deep):
            number = base + deep + k - 1
            copies.append(
                push(
                    buf.at[index(order, (z + k) % deep, mine, following)],
                    from_deep[n].at[k - 1],
                    send.at[n, number],
                    arrive.at[n, number],
                    others[k - 1],
                )
            )

    def stage_deep(n):
        i, left, wide, order = chunks[n]
        base = 1 + PAIR * deep + deep
        for k in range(1, deep):
            arrived(from_deep[n].at[k - 1], arrive.at[n, base + k - 1])
        mine, following = (x, y) if order == 0 else (y, x)
        result = own_buf[n][index(order, z, mine, following)].astype(jnp.float32)
        for k in range(deep - 1):
            result = result + from_deep[n][k].astype(jnp.float32)
        outs[i][:, pl.ds(left, wide)] = result

    for step in range(total + 3):
        for lag, stage in enumerate((stage_core, stage_first, stage_second, stage_deep)):
            if 0 <= step - lag < total:
                stage(step - lag)
    for copy in copies:
        copy.wait_send()


def sum_all(calls, groups, parts, arrays):
    deep = groups // PAIR
    rows = arrays[0].shape[0] // (groups * parts)
    budget, calls_of, used = 46 * 2**20, [[]], 0
    number = 0
    for i, array in enumerate(arrays):
        left = 0
        while left < array.shape[1]:
            wide = min(512, array.shape[1] - left)
            if 0 < array.shape[1] - left - wide < 512 // 2:
                wide = array.shape[1] - left
            cost = 2 * rows * wide * (4 * deep * 2 + 2 * deep + deep + deep) + 4 * rows * wide
            if used + cost > budget:
                calls_of.append([])
                used = 0
            used += cost
            calls_of[-1].append((i, left, wide, number % 2))
            number += 1
            left += wide
    views = [a.reshape(groups * parts // PAIR, PAIR, rows, a.shape[1]) for a in arrays]
    pieces = [[] for _ in arrays]
    for chunks in calls_of:
        used_arrays = sorted({c[0] for c in chunks})
        bounds = {
            i: (min(c[1] for c in chunks if c[0] == i), sum(c[2] for c in chunks if c[0] == i))
            for i in used_arrays
        }
        local = [(used_arrays.index(i), left, wide, order) for i, left, wide, order in chunks]
        count = len(used_arrays)
        many = deep * PAIR * PAIR

        def bufs(n):
            return [pltpu.VMEM((n, rows, wide), jnp.bfloat16) for _, _, wide, _ in chunks]

        sems = DMA((len(chunks), 1 + PAIR * deep + deep + deep))
        outs = pl.pallas_call(
            functools.partial(
                sum_all_kernel,
                deep,
                tuple(local),
                count,
            ),
            in_specs=[ANY] * count,
            out_specs=[IN_VMEM] * count,
            out_shape=[
                jax.ShapeDtypeStruct((rows, arrays[i].shape[1]), jnp.float32)
                for i in used_arrays
            ],
            scratch_shapes=bufs(many)
            + bufs(many)
            + bufs(PAIR * deep)
            + bufs(deep)
            + bufs(deep - 1)
            + [sems, sems, DMA((len(chunks),))],
            compiler_params=calls.params(),
            name="sum_all",
        )(*[views[i] for i in used_arrays])
        for i, out in zip(used_arrays, outs):
            pieces[i].append(out[:, bounds[i][0] : bounds[i][0] + bounds[i][1]])
    return [p[0] if len(p) == 1 else jnp.concatenate(p, axis=1) for p in pieces]


def swap_halves(values, half):
    lane = lax.broadcasted_iota(jnp.int32, values.shape, 1)
    wide = values.shape[1]
    return jnp.where(
        lane < half, pltpu.roll(values, wide - half, 1), pltpu.roll(values, half, 1)
    )


def turn(values, cosine, sinusoid):
    return values * cosine + swap_halves(values, ROPE // 2) * sinusoid


def full_gain(gains, row, size, groups):
    total = size * groups
    wide = gains.shape[1]
    result = jnp.zeros((8, total), jnp.float32)
    for e in range(groups):
        share = jnp.broadcast_to(gains[e * 8 + row : e * 8 + row + 1, :], (8, wide))
        if total > wide:
            share = jnp.concatenate([share, jnp.zeros((8, total - wide), jnp.float32)], axis=1)
        result = result + (pltpu.roll(share, e * size, 1) if e else share)
    return result[:1]


def rows_loop(count, step, work):
    def one(i, carry):
        work(pl.ds(pl.multiple_of(i * step, step), step))
        return carry

    lax.fori_loop(0, count // step, one, 0)


def front_kernel(groups, sizes, plan, names, *refs):
    ref = Bag(zip(names, refs))
    deep = groups // PAIR
    link = Link(deep)
    z, x, y, c, part = link.z, link.x, link.y, link.c, link.part
    send, arrive, own, leave = ref.send, ref.arrive, ref.own, ref.leave
    link.greet(groups, "eyc")
    loads, numbers, landing = {}, {}, Bag()
    row_of = {}
    for n, (name, axis, cut, over, orders, home) in enumerate(plan):
        numbers[name] = n
        landing[name] = ref["b_" + name] if home == VMEM_ else ref["o_" + name]

    stream_row = [0]

    def tasks_of(name):
        n = numbers[name]
        _, axis, cut, over, orders, home = plan[n]
        source, target = ref["i_" + name], landing[name]
        if cut is not None:
            source = slot(source, cut[0], part, cut[1])
        if over == READY:
            loads[name] = bring(source, target, own.at[n])
            return []
        if over == SHUFFLE:
            size = source.shape[2]
            keep = ref["k_" + name]
            loads[name] = bring(source.at[link.me], keep, own.at[n])
            row = stream_row[0]
            stream_row[0] += 1
            return [
                shuffle(
                    link,
                    groups,
                    lambda e: source.at[e],
                    lambda e: slot(target, axis, e, size),
                    send.at[row],
                    arrive.at[row],
                )
            ]
        size = cut[1] if cut is not None and cut[0] == axis else source.shape[axis]

        def home_of(sz, sx, sy, sc):
            index = sz * PAIR + sx
            if over == "all":
                index = (index * PAIR + sy) * PAIR + sc
            return slot(target, axis, index, size)

        mine = home_of(z, x, y, c)
        if home == VMEM_:
            loads[name] = bring(source, mine, own.at[n])
        else:
            loads[name] = bring(source, ref["k_" + name], own.at[n])
        return [stream for stream in streams_of(source, home_of, orders)]

    def streams_of(source, home_of, orders):
        result = []
        for i, order in enumerate(orders):
            row = stream_row[0]
            stream_row[0] += 1
            if len(orders) == 1:
                at, part_source = home_of, source
            else:
                wide = source.shape[1] // len(orders)
                span = pl.ds(i * wide, wide)

                def at(*where, span=span):
                    return home_of(*where).at[:, span]

                part_source = source.at[:, span]
            result.append(spread(link, order, part_source, at, send.at[row], arrive.at[row]))
        return result

    def begin(*which):
        found = [task for name in which for task in tasks_of(name)]
        return [task for task in found if next(task, run) is not run]

    gain_tasks = begin(GAINS)
    stem_tasks = begin(QUERY_DOWN, LATENT_DOWN)
    late_tasks = begin(OUT_GRAD)

    def complete(name):
        n = numbers[name]
        loads.pop(name).wait()
        _, axis, cut, over, _, home = plan[n]
        if home == "hbm":
            keep, target = ref["k_" + name], landing[name]
            index = link.me
            if over == "all":
                index = link.me * PAIR * PAIR + part
            move = pltpu.make_async_copy(
                keep, slot(target, axis, index, keep.shape[axis]), own.at[n]
            )
            move.start()
            stores.append(move)

    stores = []

    def keep_out(name, source=None):
        moves = len(stores)
        move = bring(source if source is not None else landing[name], ref["o_" + name], leave.at[len(kept)])
        kept.append(move)

    kept = []
    block_ref = ref.i_block
    first_ref, middle_ref = ref.b_first, ref.b_middle
    width = block_ref.shape[1]
    row_count = block_ref.shape[0]
    sub = row_count // (PAIR * PAIR)

    complete(GAINS)
    run(gain_tasks)
    gains = landing.gains
    attention_gain = full_gain(gains, 0, sizes[0], groups)

    def first_norm(span):
        values = block_ref[span, :].astype(jnp.float32)
        inverse = lax.rsqrt(jnp.mean(values * values, axis=-1, keepdims=True) + EPSILON)
        first_ref[span, :] = (values * inverse * attention_gain).astype(jnp.bfloat16)

    rows_loop(row_count, 32, first_norm)
    for _ in range(deep - 1):
        advance(stem_tasks, 1)
        advance(late_tasks, 1)
    up_tasks = begin(QUERY_UP, LATENT_UP)
    for name in (QUERY_DOWN, LATENT_DOWN):
        complete(name)
    run(stem_tasks)
    ref.b_query_cut[...] = matmul(first_ref[...], landing.query_down[...]).astype(
        jnp.bfloat16
    )
    ref.b_latent_cut[...] = matmul_nt(landing.latent_down[...], first_ref[...]).astype(
        jnp.bfloat16
    )
    query_lat, latent_t = ref.b_query_lat, ref.b_latent_t
    query_cut, latent_cut = ref.b_query_cut, ref.b_latent_cut
    stem_numbers = len(plan)
    stem_tasks = streams_of(
        query_cut, lambda sz, sx, sy, sc: slot(query_lat, 1, sy * PAIR + sc, query_cut.shape[1]), ("yc",)
    ) + streams_of(
        latent_cut, lambda sz, sx, sy, sc: slot(latent_t, 0, sy * PAIR + sc, latent_cut.shape[0]), ("yc",)
    )
    stem_tasks = [task for task in stem_tasks if next(task, run) is not run]
    query_lat[:, pl.ds(pl.multiple_of(part * query_cut.shape[1], LANES), query_cut.shape[1])] = (
        query_cut[...]
    )
    latent_t[pl.ds(pl.multiple_of(part * latent_cut.shape[0], 16), latent_cut.shape[0]), :] = (
        latent_cut[...]
    )
    query_gain = full_gain(gains, 2, sizes[2], groups)
    latent_gain = full_gain(gains, 3, sizes[3], groups)
    cosine, sinusoid = ref.i_cosine, ref.i_sinusoid
    advance(up_tasks, 1)
    run(stem_tasks)
    advance(late_tasks, 2)

    query_n, latent_n, keys = ref.b_query_n, ref.b_latent_n, ref.b_keys

    def query_norm(span):
        values = query_lat[span, :].astype(jnp.float32)
        inverse = lax.rsqrt(jnp.mean(values * values, axis=-1, keepdims=True) + EPSILON)
        query_n[span, :] = (values * inverse * query_gain).astype(jnp.bfloat16)

    rows_loop(row_count, 32, query_norm)
    for _ in range(deep - 2):
        advance(up_tasks, 1)
        advance(late_tasks, 2)
    out_tasks = begin(OUT_PROJ, ROUTER, ROUTES)
    shared_tasks = begin(SHARED)
    latent_rank = latent_n.shape[1]
    latent = latent_t[:latent_rank, :].astype(jnp.float32).T
    inverse = lax.rsqrt(jnp.mean(latent * latent, axis=-1, keepdims=True) + EPSILON)
    latent_n[...] = (latent * inverse * latent_gain).astype(jnp.bfloat16)
    rope_rows = latent_t[latent_rank:, :].astype(jnp.float32).T
    rope_rows = jnp.concatenate(
        [rope_rows, jnp.zeros((row_count, LANES - ROPE), jnp.float32)], axis=1
    )
    key_rope = turn(rope_rows, cosine[...], sinusoid[...])[:, :ROPE].astype(jnp.bfloat16)

    complete(QUERY_UP)
    complete(LATENT_UP)
    run(up_tasks)
    queries, values_ref, attended = ref.b_queries, ref.b_values, ref.b_attended
    heads = queries.shape[0]
    head_width = NOPE + ROPE
    projected = matmul(query_n[...], landing.query_up[...])
    shifted = pltpu.roll(projected, projected.shape[1] - ROPE, 1)
    keyval = matmul(latent_n[...], landing.latent_up[...])
    for h in range(heads):
        start = h * head_width
        base, start = (projected, start) if start % LANES == 0 else (shifted, start - ROPE)
        queries[h, :, :NOPE] = base[:, start : start + NOPE].astype(jnp.bfloat16)
        tail = base[:, start + NOPE : start + NOPE + LANES]
        if tail.shape[1] < LANES:
            tail = jnp.concatenate(
                [tail, jnp.zeros((row_count, LANES - tail.shape[1]), jnp.float32)], axis=1
            )
        queries[h, :, NOPE:] = turn(tail, cosine[...], sinusoid[...])[:, :ROPE].astype(
            jnp.bfloat16
        )
        left = h * (NOPE + VD)
        keys[h, :, :NOPE] = keyval[:, left : left + NOPE].astype(jnp.bfloat16)
        keys[h, :, NOPE:] = key_rope
        values_ref[h] = keyval[:, left + NOPE : left + NOPE + VD].astype(jnp.bfloat16)
        scores = matmul_nt(queries[h], keys[h]) * head_width ** (-0.5)
        scores = jnp.where(ref.i_allowed[...] > 0, scores, -1e30)
        powers = jnp.exp(scores - jnp.max(scores, axis=-1, keepdims=True))
        probs = (powers / jnp.sum(powers, axis=-1, keepdims=True)).astype(jnp.bfloat16)
        attended[:, h * VD : (h + 1) * VD] = matmul(probs, values_ref[h]).astype(jnp.bfloat16)
        if h < deep - 1:
            advance(out_tasks, 1)
        advance(late_tasks, 2)
    advance(out_tasks, max(0, deep - 1 - heads))
    for name in (OUT_PROJ, ROUTER, ROUTES):
        complete(name)
    run(out_tasks)
    for name in (QUERY_DOWN, LATENT_DOWN, QUERY_UP, LATENT_UP, OUT_PROJ, GAINS, ROUTER):
        keep_out(name)
    for name in (FIRST, QUERY_LAT, LATENT_T, QUERY_N, LATENT_N, QUERIES, KEYS, VALUES, ATTENDED):
        keep_out(name, ref["b_" + name])

    partial, from_beside = ref.b_partial, ref.b_from_beside
    give, from_across = ref.b_give, ref.b_from_across
    swap_send, swap_arrive = ref.swap_send, ref.swap_arrive
    for quarter in range(PAIR * PAIR):
        partial[quarter // PAIR, quarter % PAIR] = matmul(
            attended[quarter * sub : (quarter + 1) * sub, :], landing.out_proj[...]
        ).astype(jnp.bfloat16)

    def beside_copy():
        return pltpu.make_async_remote_copy(
            src_ref=partial.at[:, 1 - c],
            dst_ref=from_beside,
            send_sem=swap_send.at[0],
            recv_sem=swap_arrive.at[0],
            device_id=link.peer("c"),
            device_id_type=MESH,
        )

    def across_copy():
        return pltpu.make_async_remote_copy(
            src_ref=give,
            dst_ref=from_across,
            send_sem=swap_send.at[1],
            recv_sem=swap_arrive.at[1],
            device_id=link.peer("y"),
            device_id_type=MESH,
        )

    link.emit(beside_copy)
    advance(late_tasks, 1)
    arrived(from_beside, swap_arrive.at[0])
    give[...] = partial[1 - y, c] + from_beside[1 - y]
    link.emit(across_copy)
    complete(OUT_GRAD)
    complete(SHARED)
    residual = block_ref[pl.ds(pl.multiple_of(part * sub, sub), sub), :].astype(jnp.float32)
    middle_ref[...] = (
        residual + partial[y, c].astype(jnp.float32) + from_beside[y].astype(jnp.float32)
    )
    advance(late_tasks, 1)
    arrived(from_across, swap_arrive.at[1])
    middle = middle_ref[...] + from_across[...].astype(jnp.float32)
    middle_ref[...] = middle
    ffn_gain = full_gain(gains, 1, sizes[1], groups)
    norms = ref.b_norms
    norms[...] = jnp.zeros(norms.shape, jnp.float32)
    for i, gain in enumerate((attention_gain, ffn_gain, query_gain, latent_gain)):
        norms[i : i + 1, : gain.shape[1]] = gain
    keep_out("norms", norms)
    inverse = lax.rsqrt(jnp.mean(middle * middle, axis=-1, keepdims=True) + EPSILON)
    second_ref, weights_ref, chosen_ref = ref.b_second, ref.b_weights, ref.b_chosen
    second_ref[...] = (middle * inverse * ffn_gain).astype(jnp.bfloat16)
    logits = matmul_nt(second_ref[...], landing.router[...])
    experts = logits.shape[1]
    advance(late_tasks, 1)
    routes_rows = ref.i_route_rows[pl.ds(pl.multiple_of(part * sub, sub), sub), :]
    ids = lax.broadcasted_iota(jnp.int32, (sub, experts), 1)
    chosen = jnp.zeros((sub, experts), jnp.float32)
    picked = jax.nn.sigmoid(logits)
    for k in range(routes_rows.shape[1]):
        chosen = jnp.where(routes_rows[:, k : k + 1] == ids, picked, chosen)
    totals = jnp.sum(chosen, axis=-1, keepdims=True)
    weights_ref[...] = jnp.zeros(weights_ref.shape, jnp.float32)
    weights_ref[:, :experts] = ROUTE_SCALE * chosen / totals
    chosen_ref[...] = jnp.zeros(chosen_ref.shape, jnp.float32)
    chosen_ref[:, :experts] = chosen

    def row_home(name):
        def home_of(sz, sx, sy, sc):
            index = ((sz * PAIR + sx) * PAIR + sy) * PAIR + sc
            return slot(ref["o_" + name], 0, index, sub)

        return home_of

    all_tasks = streams_of(weights_ref, row_home(WEIGHTS), (ZXYC,))
    all_tasks += streams_of(second_ref, row_home(TOKENS), (ZXYC, "zyxc") * 2)
    all_tasks = [task for task in all_tasks if next(task, run) is not run]
    mine = link.me * PAIR * PAIR + part
    kept.append(bring(second_ref, slot(ref.o_tokens, 0, mine, sub), leave.at[len(kept)]))
    kept.append(bring(weights_ref, slot(ref.o_weights, 0, mine, sub), leave.at[len(kept)]))
    keep_out("middle", middle_ref)
    keep_out("chosen", chosen_ref)
    run(late_tasks + all_tasks + shared_tasks)
    link.drain()
    for move in stores + kept:
        move.wait()


def front_stage(calls, groups, parts, sizes, items, block, route_rows, allowed, cosine, sinusoid):
    deep = groups // PAIR
    rows, width = block.shape
    sub = rows // parts
    bf16, f32 = jnp.bfloat16, jnp.float32
    names, inputs, in_specs = [], [], []
    out_names, out_shape, plan, scratch = [], [], [], Bag()
    streams = 0
    for name, array, axis, cut, over, orders, home in items:
        names.append("i_" + name)
        inputs.append(array)
        in_specs.append(ANY)
        shape = list(array.shape)
        if over == SHUFFLE:
            shape = shape[1:]
        if cut is not None:
            shape[cut[0]] = cut[1]
        if home == "hbm":
            scratch["k_" + name] = pltpu.VMEM(tuple(shape), array.dtype)
        if over != READY:
            shape[axis] *= groups * parts if over == "all" else groups
            streams += max(1, len(orders))
        if home == VMEM_:
            scratch["b_" + name] = pltpu.VMEM(tuple(shape), array.dtype)
        out_names.append(name)
        out_shape.append(jax.ShapeDtypeStruct(tuple(shape), array.dtype))
        plan.append((name, axis, cut, over, orders, home))
    for name, array in (
        ("block", block),
        ("route_rows", route_rows),
        ("allowed", allowed),
        ("cosine", cosine),
        ("sinusoid", sinusoid),
    ):
        names.append("i_" + name)
        inputs.append(array)
        in_specs.append(IN_VMEM)
    shape_of = Bag((name, shape.shape) for name, shape in zip(out_names, out_shape))
    query_cut, latent_cut = shape_of.query_down[1], shape_of.latent_down[0]
    query_rank, latent_rank = shape_of.query_up[0], shape_of.latent_up[0]
    heads = shape_of.latent_up[1] // (NOPE + VD)
    experts = shape_of.router[0]
    lanes = experts + -experts % LANES
    half = parts // PAIR
    buffers = Bag(
        first=((rows, width), bf16),
        query_lat=((rows, query_cut * parts), bf16),
        latent_t=((latent_cut * parts, rows), bf16),
        query_n=((rows, query_rank), bf16),
        latent_n=((rows, latent_rank), bf16),
        queries=((heads, rows, NOPE + ROPE), bf16),
        keys=((heads, rows, NOPE + ROPE), bf16),
        values=((heads, rows, VD), bf16),
        attended=((rows, heads * VD), bf16),
        middle=((sub, width), f32),
        chosen=((sub, lanes), f32),
        norms=((8, width), f32),
    )
    for name, (shape, dtype) in buffers.items():
        out_names.append(name)
        out_shape.append(jax.ShapeDtypeStruct(shape, dtype))
    inner = Bag(
        query_cut=((rows, query_cut), bf16),
        latent_cut=((latent_cut, rows), bf16),
        partial=((half, PAIR, sub, width), bf16),
        from_beside=((half, sub, width), bf16),
        give=((sub, width), bf16),
        from_across=((sub, width), bf16),
        second=((sub, width), bf16),
        weights=((sub, lanes), f32),
    )
    for name, (shape, dtype) in (buffers | inner).items():
        scratch["b_" + name] = pltpu.VMEM(shape, dtype)
    out_names += [TOKENS, WEIGHTS]
    out_shape += [
        jax.ShapeDtypeStruct((sub * groups * parts, width), bf16),
        jax.ShapeDtypeStruct((sub * groups * parts, lanes), f32),
    ]
    streams += 2 + 1 + 4
    scratch.send = scratch.arrive = DMA((streams, 8 * deep))
    scratch.own = DMA((len(items),))
    scratch.leave = DMA((len(out_names),))
    scratch.swap_send = scratch.swap_arrive = DMA((2,))
    names += ["o_" + name for name in out_names] + list(scratch)
    results = pl.pallas_call(
        functools.partial(front_kernel, groups, tuple(sizes), tuple(plan), tuple(names)),
        in_specs=in_specs,
        out_specs=[ANY] * len(out_names),
        out_shape=out_shape,
        scratch_shapes=list(scratch.values()),
        compiler_params=calls.params(),
        name="front",
    )(*inputs)
    return Bag(zip(out_names, results))


def device_total(link, order, own, give, bufs, result, send, arrive):
    deep, z, x, y = link.deep, link.z, link.x, link.y
    from_core, from_first, from_second, from_deep = bufs
    mine, following = (x, y) if order == 0 else (y, x)
    near, far = (link.peer("x"), link.peer("y")) if order == 0 else (link.peer("y"), link.peer("x"))

    def at(depth, on_first, on_second):
        on_x, on_y = (on_first, on_second) if order == 0 else (on_second, on_first)
        return (depth * PAIR + on_x) * PAIR + on_y

    def hop(number, source, target, peer):
        def make():
            return pltpu.make_async_remote_copy(
                src_ref=source(),
                dst_ref=target,
                send_sem=send.at[number],
                recv_sem=arrive.at[number],
                device_id=peer,
                device_id_type=MESH,
            )

        link.emit(make)

    hop(0, lambda: give, from_core, link.peer("c"))
    yield
    arrived(from_core, arrive.at[0])

    def add_core(k):
        own[k] = own[k] + from_core[k]

    add_rows(deep * PAIR * PAIR, add_core)
    for depth in range(deep):
        for s in range(PAIR):
            n = depth * PAIR + s
            hop(1 + n, lambda d=depth, s=s: own.at[at(d, 1 - mine, s)], from_first.at[n], near)
    yield
    for n in range(PAIR * deep):
        arrived(from_first.at[n], arrive.at[1 + n])

    def add_first(k):
        here = at(k // PAIR, mine, k % PAIR)
        own[here] = own[here] + from_first[k]

    add_rows(deep * PAIR, add_first)
    base = 1 + PAIR * deep
    for depth in range(deep):
        hop(
            base + depth,
            lambda d=depth: own.at[at(d, mine, 1 - following)],
            from_second.at[depth],
            far,
        )
    yield
    for depth in range(deep):
        arrived(from_second.at[depth], arrive.at[base + depth])

    def add_second(k):
        here = at(k, mine, following)
        own[here] = own[here] + from_second[k]

    add_rows(deep, add_second)
    base = base + deep - 1
    for k in range(1, deep):
        hop(
            base + k,
            lambda k=k: own.at[at((z + k) % deep, mine, following)],
            from_deep.at[k - 1],
            link.at_z((z + k) % deep),
        )
    total = own[at(z, mine, following)].astype(jnp.float32)
    yield
    for k in range(1, deep):
        arrived(from_deep.at[k - 1], arrive.at[base + k])
        total = total + from_deep[k - 1].astype(jnp.float32)
    result[...] = total


def total_buffers(deep, rows, wide):
    shapes = (deep * PAIR * PAIR, PAIR * deep, deep, deep - 1)
    return [pltpu.VMEM((n, rows, wide), jnp.bfloat16) for n in shapes]


def total_hops(deep):
    return PAIR * deep + 2 * deep


def route_kernel(ids_ref, routes_ref, x_ref, g_ref, weights_ref, xr_ref, gr_ref, p_ref, w_ref):
    local = ids_ref.shape[0]
    rows = x_ref.shape[0]
    f32, bf16 = jnp.float32, jnp.bfloat16
    ids = ids_ref[...]
    named = jnp.zeros((local, rows), f32)
    for k in range(routes_ref.shape[0]):
        named = jnp.where(routes_ref[k : k + 1, :] == ids, 1.0, named)
    before = lax.broadcasted_iota(jnp.int32, (rows, rows), 0)
    after = lax.broadcasted_iota(jnp.int32, (rows, rows), 1)
    rank = matmul(named.astype(bf16), jnp.where(before < after, 1.0, 0.0).astype(bf16))
    lanes = weights_ref.shape[1]
    mine = jnp.where(lax.broadcasted_iota(jnp.int32, (local, lanes), 1) == ids, 1.0, 0.0)
    weights = lax.dot_general(
        mine,
        weights_ref[...],
        (((1,), (1,)), ((), ())),
        precision=lax.Precision.HIGHEST,
        preferred_element_type=f32,
    )
    slots = lax.broadcasted_iota(jnp.int32, (CAP, rows), 0).astype(f32)
    picks = []
    for j in range(local):
        pick = jnp.where(slots == rank[j : j + 1, :], named[j : j + 1, :], 0.0)
        w_ref[0, j * CAP : (j + 1) * CAP, :] = jnp.sum(
            pick * weights[j : j + 1, :], axis=1, keepdims=True
        )
        picks.append(pick.astype(bf16))
    picks = jnp.concatenate(picks, axis=0)
    p_ref[0] = picks
    xr_ref[0] = matmul(picks, x_ref[...]).astype(bf16)
    gr_ref[0] = matmul(picks, g_ref[...]).astype(bf16)


def route_stage(groups, own_ids, routes_t, tokens, gradients, weights):
    local = own_ids.shape[0]
    rows, width = tokens.shape[0] // groups, tokens.shape[1]
    slots = local * CAP
    row_spec = pl.BlockSpec((rows, width), lambda b: (b, 0))
    slot_spec = pl.BlockSpec((1, slots, width), lambda b: (b, 0, 0))
    slot_shape = jax.ShapeDtypeStruct((groups, slots, width), jnp.bfloat16)
    lanes = weights.shape[1]
    return pl.pallas_call(
        route_kernel,
        grid=(groups,),
        in_specs=[
            pl.BlockSpec((local, 1), lambda b: (0, 0)),
            pl.BlockSpec((routes_t.shape[0], rows), lambda b: (0, b)),
            row_spec,
            row_spec,
            pl.BlockSpec((rows, lanes), lambda b: (b, 0)),
        ],
        out_specs=[
            slot_spec,
            slot_spec,
            pl.BlockSpec((1, slots, rows), lambda b: (b, 0, 0)),
            pl.BlockSpec((1, slots, 1), lambda b: (b, 0, 0)),
        ],
        out_shape=[
            slot_shape,
            slot_shape,
            jax.ShapeDtypeStruct((groups, slots, rows), jnp.bfloat16),
            jax.ShapeDtypeStruct((groups, slots, 1), jnp.float32),
        ],
        compiler_params=pltpu.CompilerParams(vmem_limit_bytes=VMEM_BYTES),
        name="route",
    )(own_ids[:, None], routes_t, tokens, gradients, weights)


def mix_kernel(groups, chunks, names, *refs):
    ref = Bag(zip(names, refs))
    deep = groups // PAIR
    bf16, f32 = jnp.bfloat16, jnp.float32
    link = Link(deep)
    link.greet(groups, "eyc")
    blocks, slots, rows = ref.b_picks.shape
    sub = ref.o_dsecond.shape[0]
    width = ref.i_tokens.shape[1]
    units = ref.i_shared.shape[0] // 3
    loads = [bring(ref.i_picks, ref.b_picks, ref.load.at[0])]
    loads.append(bring(ref.i_shared, ref.b_shared, ref.load.at[1]))

    def fetch(b, at):
        span = pl.ds(pl.multiple_of(b * rows, rows), rows)
        return (
            pltpu.make_async_copy(ref.i_tokens.at[span, :], ref.b_x.at[at], ref.fetch.at[at, 0]),
            pltpu.make_async_copy(ref.i_gradients.at[span, :], ref.b_g.at[at], ref.fetch.at[at, 1]),
        )

    for copy in fetch(0, 0):
        copy.start()
    many = len(chunks)
    work = [(True, *chunk) for chunk in chunks] + [(False, *chunk) for chunk in chunks[:-1]]

    def source_of(n):
        back, left, wide = work[n]
        source = ref.i_back if back else ref.i_produced
        return pltpu.make_async_copy(
            source.at[:, :, pl.ds(left, wide)],
            ref.b_source.at[turn_of[n], :, :, pl.ds(0, wide)],
            ref.pull.at[turn_of[n]],
        )

    has_source = [n != many - 1 for n in range(len(work))]
    order = [many - 1] + [n for n in range(len(work)) if has_source[n]]
    turn_of = {n: i % 2 for i, n in enumerate(order)}
    for load in loads:
        load.wait()
    ref.b_acc[...] = jnp.zeros(ref.b_acc.shape, f32)

    def block(b, carry):
        at = b % 2

        @pl.when(b + 1 < blocks)
        def _():
            for copy in fetch(b + 1, 1 - at):
                copy.start()

        for copy in fetch(b, at):
            copy.wait()
        row_inputs, cotangent = ref.b_x[at], ref.b_g[at]
        pre = matmul_nt(row_inputs, ref.b_shared[: 2 * units, :])
        gate_pre, up_pre = pre[:, :units], pre[:, units:]
        sigmoid_gate, hidden = swiglu(gate_pre, up_pre)
        dhidden = matmul_nt(cotangent, ref.b_shared[2 * units :, :])
        gate_grad, up_grad = swiglu_back(dhidden, gate_pre, up_pre, sigmoid_gate)
        both = jnp.concatenate([gate_grad, up_grad], axis=1)
        ref.b_hidden[b] = hidden
        ref.b_both[b] = both
        ref.b_acc[: 2 * units, :] += matmul_tn(both, row_inputs)
        ref.b_acc[2 * units :, :] += matmul_tn(hidden, cotangent)
        return carry

    source_of(order[1]).start()
    lax.fori_loop(0, blocks, block, 0)
    ref.b_grad[...] = ref.b_acc[...].astype(bf16)
    grad_out = bring(ref.b_grad, ref.o_shared, ref.load.at[0])
    dw_lane = lax.broadcasted_iota(jnp.int32, (slots, chunks[-1][1]), 1)
    tasks, outs = [], []
    pending = [n for n in order if has_source[n]]
    for n in order:
        back, left, wide = work[n]
        if has_source[n]:
            pending.pop(0)
            if pending:
                source_of(pending[0]).start()
            source_of(n).wait()
        staged = None if back else ref.b_stage.at[n % 2]
        if not back and len(outs) >= 2:
            outs[-2].wait()
            outs[-2] = None

        def one(b, carry, n=n, back=back, left=left, wide=wide, staged=staged):
            picks = ref.b_picks[b]
            if not has_source[n]:
                values = matmul_tn(
                    picks, jnp.where(dw_lane == ref.i_lanes[...], ref.i_dweights[b], 0.0).astype(bf16)
                )
            else:
                span = slice(left, left + wide)
                values = matmul_tn(picks, ref.b_source[turn_of[n], b, :, :wide])
                if back:
                    values += matmul(ref.b_both[b], ref.b_shared[: 2 * units, span])
                else:
                    values += matmul(ref.b_hidden[b], ref.b_shared[2 * units :, span])
            values = values.astype(bf16)
            for y in range(PAIR):
                for c in range(PAIR):
                    q = y * PAIR + c
                    piece = values[q * sub : (q + 1) * sub, :]
                    if back:
                        ref["p%d" % n][c, b * PAIR + y] = piece
                    else:
                        staged[b * PAIR + y, c] = piece
            return carry

        lax.fori_loop(0, blocks, one, 0)
        if back:
            task = device_total(
                link,
                n % 2,
                ref["p%d" % n].at[link.c],
                ref["p%d" % n].at[1 - link.c],
                [ref["f%d_%d" % (n, k)] for k in range(4)],
                ref.o_dsecond.at[:, pl.ds(left, wide)],
                ref.send.at[n],
                ref.arrive.at[n],
            )
            advance(tasks)
            tasks += begun([task])
        else:
            outs.append(
                bring(staged, ref.o_mixed.at[:, :, :, pl.ds(left, wide)], ref.push.at[n % 2])
            )
            advance(tasks)
    run(tasks)
    link.drain()
    for copy in outs:
        if copy is not None:
            copy.wait()
    grad_out.wait()


def mix_bytes(groups, rows, slots, width):
    total = groups * rows * width * 2
    return 2 * total + 4 * rows * width * 2 * 2 + 2 * groups * max(rows, slots) * 512 * 2 * 2


def mix_stage(calls, groups, parts, picks, produced, back, dweights, lanes, tokens, gradients, shared):
    deep = groups // PAIR
    blocks, slots, rows = picks.shape
    width = tokens.shape[1]
    sub = rows // parts
    bf16, f32 = jnp.bfloat16, jnp.float32
    experts_wide = lanes[1]
    wide = min(512, width)
    chunks = [(left, wide) for left in range(0, width, wide)] + [(width, experts_wide)]
    inputs = Bag(
        i_picks=picks,
        i_produced=produced,
        i_back=back,
        i_dweights=dweights,
        i_lanes=lanes[0],
        i_tokens=tokens,
        i_gradients=gradients,
        i_shared=shared,
    )
    specs = [IN_VMEM if key in ("i_dweights", "i_lanes") else ANY for key in inputs]
    third = shared.shape[0] // 3
    scratch = Bag(
        b_picks=pltpu.VMEM(picks.shape, bf16),
        b_shared=pltpu.VMEM(shared.shape, bf16),
        b_x=pltpu.VMEM((2, rows, width), bf16),
        b_g=pltpu.VMEM((2, rows, width), bf16),
        b_acc=pltpu.VMEM(shared.shape, f32),
        b_grad=pltpu.VMEM(shared.shape, bf16),
        b_hidden=pltpu.VMEM((blocks, rows, third), bf16),
        b_both=pltpu.VMEM((blocks, rows, 2 * third), bf16),
        b_source=pltpu.VMEM((2, blocks, slots, wide), bf16),
        b_stage=pltpu.VMEM((2, blocks * PAIR, PAIR, sub, wide), bf16),
        load=DMA((2,)),
        fetch=DMA((2, 2)),
        pull=DMA((2,)),
        push=DMA((2,)),
        send=DMA((len(chunks), total_hops(deep))),
        arrive=DMA((len(chunks), total_hops(deep))),
    )
    for n, (_, columns) in enumerate(chunks):
        scratch["p%d" % n] = pltpu.VMEM((PAIR, blocks * PAIR, sub, columns), bf16)
        for k, buffer in enumerate(total_buffers(deep, sub, columns)):
            scratch["f%d_%d" % (n, k)] = buffer
    names = list(inputs) + ["o_dsecond", "o_mixed", "o_shared"] + list(scratch)
    return pl.pallas_call(
        functools.partial(mix_kernel, groups, tuple(chunks), tuple(names)),
        in_specs=specs,
        out_specs=[IN_VMEM, ANY, ANY],
        out_shape=[
            jax.ShapeDtypeStruct((sub, width + experts_wide), f32),
            jax.ShapeDtypeStruct((blocks * PAIR, PAIR, sub, width), bf16),
            jax.ShapeDtypeStruct(shared.shape, bf16),
        ],
        scratch_shapes=list(scratch.values()),
        compiler_params=calls.params(),
        name="mix",
    )(*inputs.values())


def advance(tasks, count=1):
    for _ in range(count):
        for task in tasks:
            next(task, None)


def begun(tasks):
    return [task for task in tasks if next(task, run) is not run]


def tensor_total(link, partial, from_beside, give, from_across, result, send, arrive):
    y, c = link.y, link.c

    def beside():
        return pltpu.make_async_remote_copy(
            src_ref=partial.at[:, 1 - c],
            dst_ref=from_beside,
            send_sem=send.at[0],
            recv_sem=arrive.at[0],
            device_id=link.peer("c"),
            device_id_type=MESH,
        )

    def across():
        return pltpu.make_async_remote_copy(
            src_ref=give,
            dst_ref=from_across,
            send_sem=send.at[1],
            recv_sem=arrive.at[1],
            device_id=link.peer("y"),
            device_id_type=MESH,
        )

    link.emit(beside)
    yield
    arrived(from_beside, arrive.at[0])
    give[...] = partial[1 - y, c] + from_beside[1 - y]
    link.emit(across)
    result[...] = partial[y, c].astype(jnp.float32) + from_beside[y].astype(jnp.float32)
    yield
    arrived(from_across, arrive.at[1])
    result[...] = result[...] + from_across[...].astype(jnp.float32)


def expert_total(link, axis, grad, from_twin, from_deep, result, send, arrive):
    deep, z, x = link.deep, link.z, link.x
    size = result.shape[axis]

    def target(k):
        return (z + k) % deep

    def to_twin(k):
        return pltpu.make_async_remote_copy(
            src_ref=slot(grad, axis, target(k) * PAIR + 1 - x, size),
            dst_ref=from_twin.at[k],
            send_sem=send.at[k],
            recv_sem=arrive.at[k],
            device_id=link.peer("x"),
            device_id_type=MESH,
        )

    def to_deep(k):
        return pltpu.make_async_remote_copy(
            src_ref=from_twin.at[k],
            dst_ref=from_deep.at[k - 1],
            send_sem=send.at[deep + k],
            recv_sem=arrive.at[deep + k],
            device_id=link.at_z(target(k)),
            device_id_type=MESH,
        )

    ks = list(range(1, deep)) + [0]
    for k in ks:
        link.emit(functools.partial(to_twin, k))
    for k in ks[:-1]:
        yield
        arrived(from_twin.at[k], arrive.at[k])
        mine = slot(grad, axis, target(k) * PAIR + x, size)
        from_twin[k] = from_twin[k] + mine[...]
        link.emit(functools.partial(to_deep, k))
    yield
    arrived(from_twin.at[0], arrive.at[0])
    total = slot(grad, axis, z * PAIR + x, size)[...].astype(jnp.float32)
    result[...] = total + from_twin[0].astype(jnp.float32)
    for k in range(1, deep):
        yield
        arrived(from_deep.at[k - 1], arrive.at[deep + k])
        result[...] = result[...] + from_deep[k - 1].astype(jnp.float32)


def back_kernel(groups, sizes, reduced, names, *refs):
    ref = Bag(zip(names, refs))
    deep = groups // PAIR
    parts = PAIR * PAIR
    link = Link(deep)
    part = link.part
    bf16, f32 = jnp.bfloat16, jnp.float32
    link.greet(groups, "eyc")
    loading = {}
    for n, name in enumerate(n[2:] for n in names if n[:2] == "h_"):
        loading[name] = bring(ref["h_" + name], ref["l_" + name], ref.load.at[n])
    left = []

    def leave(name, source=None):
        source = ref["b_" + name] if source is None else source
        left.append(bring(source, ref["o_" + name], ref.leave.at[len(left)]))

    def ready(*which):
        for name in which:
            if name in loading:
                loading.pop(name).wait()
        return [ref["l_" + name] for name in which]

    rows_send, rows_arrive = ref.rows_send, ref.rows_arrive
    used = [0]

    def over_tensor(source, target, axis, size):
        row = used[0]
        used[0] += 1

        def home_of(sz, sx, sy, sc):
            return slot(target, axis, sy * PAIR + sc, size)

        n = len(placed)
        placed.append(bring(source, home_of(link.z, link.x, link.y, link.c), ref.place.at[n]))
        return spread(link, "yc", source, home_of, rows_send.at[row], rows_arrive.at[row])

    placed = []
    totals = {name: i for i, (name, _) in enumerate(reduced)}
    axis_of = dict(reduced)

    def over_expert(name):
        if name not in totals:
            leave(name)
            return []
        i = totals[name]
        return begun(
            [
                expert_total(
                    link,
                    axis_of[name],
                    ref["b_" + name],
                    ref["t_" + name],
                    ref["d_" + name],
                    ref["r_" + name],
                    ref.send.at[i],
                    ref.arrive.at[i],
                )
            ]
        )

    shared_tasks = []
    if SHARED in axis_of:
        wide = ref.o_shared.shape[2]
        source = ref.i_shared
        shared_tasks = begun(
            [
                shuffle(
                    link,
                    groups,
                    lambda e: source.at[:, pl.ds(pl.multiple_of(e * wide, LANES), wide)],
                    lambda e: ref.o_shared.at[e],
                    ref.shared_send,
                    ref.shared_arrive,
                )
            ]
        )
        loading[OWN_SHARED] = bring(
            source.at[:, pl.ds(pl.multiple_of(link.me * wide, LANES), wide)],
            ref.k_shared,
            ref.place.at[len(placed)],
        )
        placed.append(None)

    mixed_parts = len([name for name in names if name[:1] == "m" and name[1:].isdigit()])
    mixed_loads = []
    for n in range(mixed_parts):
        wide = ref.i_block.shape[1] // mixed_parts
        mixed_loads.append(
            bring(
                ref.i_partial.at[:, link.c, :, pl.ds(n * wide, wide)],
                ref["m%d" % n],
                ref.mixed_load.at[n],
            )
        )

    sub, width = ref.i_middle.shape
    experts = ref.i_router.shape[0]
    middle = ref.i_middle[...]
    norms = [ref.i_norms[i : i + 1, : size * groups] for i, size in enumerate(sizes)]
    ffn_gain = norms[1]
    inverse = lax.rsqrt(jnp.mean(middle * middle, axis=-1, keepdims=True) + EPSILON)
    normed = middle * inverse
    chosen = ref.i_chosen[:, :experts]
    dweights = ref.i_dsecond[:, width : width + experts]
    total = jnp.sum(chosen, axis=-1, keepdims=True)
    dchosen = (
        ROUTE_SCALE
        / total
        * (dweights - jnp.sum(dweights * chosen, axis=-1, keepdims=True) / total)
    )
    dlogits = (dchosen * chosen * (1.0 - chosen)).astype(bf16)
    dsecond = ref.i_dsecond[:, :width] + matmul(dlogits, ref.i_router[...])
    scaled = dsecond * ffn_gain
    start = pl.multiple_of(part * sub, sub)
    gradient = ref.i_out_grad[pl.ds(start, sub), :].astype(f32)
    middle_grad = gradient + inverse * (
        scaled - normed * jnp.mean(scaled * normed, axis=-1, keepdims=True)
    )
    ref.b_middle_grad[...] = middle_grad
    ref.b_grad_rows[...] = middle_grad.astype(bf16)
    tensor_tasks = begun([over_tensor(ref.b_grad_rows, ref.b_attention_grad, 0, sub)])
    ref.b_router[...] = matmul_tn(dlogits, (normed * ffn_gain).astype(bf16)).astype(bf16)
    expert_tasks = over_expert(ROUTER)
    gain_sums = {1: jnp.sum(dsecond * normed, axis=0, keepdims=True)}

    run(tensor_tasks)
    placed[1 if SHARED in axis_of else 0].wait()
    placed[1 if SHARED in axis_of else 0] = None

    attended, out_proj = ready(ATTENDED, OUT_PROJ)
    attention_grad = ref.b_attention_grad
    for at in range(0, attended.shape[1], 256):
        ref.b_out_proj[at : at + 256, :] = matmul_tn(
            attended[:, at : at + 256], attention_grad[...]
        ).astype(bf16)
    expert_tasks += over_expert(OUT_PROJ)
    mixed_tasks = []
    if I_PARTIAL in ref:
        partial = ref.i_partial
        for load in mixed_loads:
            load.wait()
        for n in range(mixed_parts):
            wide = width // mixed_parts
            span = pl.ds(n * wide, wide)
            mixed_tasks.append(
                device_total(
                    link,
                    1,
                    ref["m%d" % n],
                    partial.at[:, 1 - link.c, :, span],
                    [ref["m%d_%d" % (n, k)] for k in range(4)],
                    ref.b_mixed.at[:, span],
                    ref.mixed_send.at[n],
                    ref.mixed_arrive.at[n],
                )
            )
        mixed_tasks = begun(mixed_tasks)
    ref.b_attended_grad[...] = matmul_nt(attention_grad[...], out_proj[...]).astype(bf16)

    queries, keys, values = ready(QUERIES, KEYS, VALUES)
    heads, row_count, head_width = queries.shape
    cosine, sinusoid = ref.i_cosine[...], ref.i_sinusoid[...]
    dkey_rope = jnp.zeros((row_count, LANES), f32)
    scale = head_width ** (-0.5)
    filler = jnp.zeros((row_count, LANES - ROPE), f32)
    for h in range(heads):
        scores = matmul_nt(queries[h], keys[h]) * scale
        scores = jnp.where(ref.i_allowed[...] > 0, scores, -1e30)
        powers = jnp.exp(scores - jnp.max(scores, axis=-1, keepdims=True))
        probs = powers / jnp.sum(powers, axis=-1, keepdims=True)
        attended_grad = ref.b_attended_grad[:, h * VD : (h + 1) * VD]
        dvalues = matmul_tn(probs.astype(bf16), attended_grad)
        dprobs = matmul_nt(attended_grad, values[h])
        delta = jnp.sum(probs * dprobs, axis=-1, keepdims=True)
        dscores = (probs * (dprobs - delta) * scale).astype(bf16)
        dquery = matmul(dscores, keys[h])
        dkeys = matmul_tn(dscores, queries[h])
        rope = turn(jnp.concatenate([dquery[:, NOPE:], filler], axis=1), cosine, -sinusoid)
        pair = jnp.concatenate(
            [dquery[:, :NOPE], rope, jnp.zeros((row_count, LANES), f32)], axis=1
        )
        if h % 2 == 0:
            held = pair
        else:
            held = held + pltpu.roll(pair, head_width, 1)
            ref.b_dquery[:, (h - 1) * head_width : (h + 1) * head_width] = held.astype(bf16)
        dkey_rope = dkey_rope + jnp.concatenate([dkeys[:, NOPE:], filler], axis=1)
        base = h * (NOPE + VD)
        ref.b_dkeyval[:, base : base + NOPE] = dkeys[:, :NOPE].astype(bf16)
        ref.b_dkeyval[:, base + NOPE : base + NOPE + VD] = dvalues.astype(bf16)
        advance(expert_tasks)
        advance(mixed_tasks[h % max(1, len(mixed_tasks)) :][:1])
    dkey_rope = turn(dkey_rope, cosine, -sinusoid)

    query_n, latent_n, query_up, latent_up = ready(QUERY_N, LATENT_N, QUERY_UP, LATENT_UP)
    query_rank, latent_rank = query_n.shape[1], latent_n.shape[1]
    for at in range(0, query_rank, 256):
        ref.b_query_up[at : at + 256, :] = matmul_tn(
            query_n[:, at : at + 256], ref.b_dquery[...]
        ).astype(bf16)
    expert_tasks += over_expert(QUERY_UP)
    for at in range(0, latent_rank, 256):
        ref.b_latent_up[at : at + 256, :] = matmul_tn(
            latent_n[:, at : at + 256], ref.b_dkeyval[...]
        ).astype(bf16)
    expert_tasks += over_expert(LATENT_UP)
    partial = ref.b_heads_partial
    lead = query_rank + latent_rank
    for quarter in range(parts):
        span = slice(quarter * sub, (quarter + 1) * sub)
        at = (quarter // PAIR, quarter % PAIR)
        partial[(*at, slice(None), slice(0, query_rank))] = matmul_nt(
            ref.b_dquery[span, :], query_up[...]
        ).astype(bf16)
        partial[(*at, slice(None), slice(query_rank, lead))] = matmul_nt(
            ref.b_dkeyval[span, :], latent_up[...]
        ).astype(bf16)
        partial[(*at, slice(None), slice(lead, lead + LANES))] = dkey_rope[span, :].astype(bf16)
    sum_tasks = begun(
        [
            tensor_total(
                link,
                partial,
                ref.b_heads_beside,
                ref.b_heads_give,
                ref.b_heads_across,
                ref.b_heads_rows,
                ref.sum_send.at[0],
                ref.sum_arrive.at[0],
            )
        ]
    )
    advance(expert_tasks)
    advance(mixed_tasks)
    run(sum_tasks)

    heads_rows = ref.b_heads_rows
    (query_lat, latent_t) = ready(QUERY_LAT, LATENT_T)

    def norm_back(values, gain, cotangent):
        inverse = lax.rsqrt(jnp.mean(values * values, axis=-1, keepdims=True) + EPSILON)
        normed = values * inverse
        scaled = cotangent * gain
        back = inverse * (scaled - normed * jnp.mean(scaled * normed, axis=-1, keepdims=True))
        return (back, jnp.sum(cotangent * normed, axis=0, keepdims=True))

    query_rows = query_lat[pl.ds(start, sub), :].astype(f32)
    back, gain_sums[2] = norm_back(query_rows, norms[2], heads_rows[:, :query_rank])
    ref.b_query_rows[...] = back.astype(bf16)
    ref.b_latent_block[...] = latent_t[:latent_rank, :].astype(f32).T
    latent_rows = ref.b_latent_block[pl.ds(start, sub), :]
    back, gain_sums[3] = norm_back(
        latent_rows, norms[3], heads_rows[:, query_rank:lead]
    )
    ref.b_latent_rows[:, :latent_rank] = back.astype(bf16)
    ref.b_latent_rows[:, latent_rank:] = heads_rows[:, lead:].astype(bf16)
    own = len(placed)
    tensor_tasks = begun(
        [
            over_tensor(ref.b_query_rows, ref.b_dquery_lat, 0, sub),
            over_tensor(ref.b_latent_rows, ref.b_dlatent_all, 0, sub),
        ]
    )
    advance(expert_tasks)
    advance(mixed_tasks)
    run(tensor_tasks)
    for n in (own, own + 1):
        placed[n].wait()
        placed[n] = None

    first, query_down, latent_down = ready(FIRST, QUERY_DOWN, LATENT_DOWN)
    query_cut, latent_cut = query_down.shape[1], latent_down.shape[0]
    dquery_lat = ref.b_dquery_lat[
        :, pl.ds(pl.multiple_of(part * query_cut, LANES), query_cut)
    ]
    ref.b_dlatent_t[...] = ref.b_dlatent_all[...].astype(f32).T
    dlatent_t = ref.b_dlatent_t[
        pl.ds(pl.multiple_of(part * latent_cut, 8), latent_cut), :
    ].astype(bf16)
    for at in range(0, width, 256):
        ref.b_query_down[at : at + 256, :] = matmul_tn(
            first[:, at : at + 256], dquery_lat
        ).astype(bf16)
    expert_tasks += over_expert(QUERY_DOWN)
    for at in range(0, width, 512):
        ref.b_latent_down[:, at : at + 512] = matmul(dlatent_t, first[:, at : at + 512]).astype(
            bf16
        )
    expert_tasks += over_expert(LATENT_DOWN)
    advance(expert_tasks)
    partial = ref.b_first_partial
    for quarter in range(parts):
        span = slice(quarter * sub, (quarter + 1) * sub)
        partial[quarter // PAIR, quarter % PAIR] = (
            matmul_nt(dquery_lat[span], query_down[...])
            + matmul_tn(dlatent_t[:, span], latent_down[...])
        ).astype(bf16)
    sum_tasks = begun(
        [
            tensor_total(
                link,
                partial,
                ref.b_first_beside,
                ref.b_first_give,
                ref.b_first_across,
                ref.b_first_rows,
                ref.sum_send.at[1],
                ref.sum_arrive.at[1],
            )
        ]
    )
    advance(expert_tasks)
    run(sum_tasks)
    residual = ref.i_block[pl.ds(start, sub), :].astype(f32)
    back, gain_sums[0] = norm_back(
        residual, norms[0], ref.b_first_rows[...]
    )
    ref.b_input_rows[...] = (ref.b_middle_grad[...] + back).astype(bf16)
    input_tasks = begun([over_tensor(ref.b_input_rows, ref.o_input_grad, 0, sub)])
    wide = ref.b_gains.shape[1]
    for i, size in enumerate(sizes):
        sums = jnp.broadcast_to(gain_sums[i], (8, gain_sums[i].shape[1]))
        span = sums.shape[1]
        if span < wide:
            sums = jnp.concatenate([sums, jnp.zeros((8, wide - span), f32)], axis=1)
            span = wide
        for e in range(groups):
            moved = pltpu.roll(sums, span - e * size, 1) if e else sums
            ref.b_gains[e * 8 + i : e * 8 + i + 1, :] = moved[:1, :wide]
    for e in range(groups):
        ref.b_gains[e * 8 + len(sizes) : e * 8 + 8, :] = jnp.zeros((8 - len(sizes), wide), f32)
    expert_tasks += over_expert(GAINS)
    advance(expert_tasks)
    run(mixed_tasks)
    mixed = ref.b_mixed if I_PARTIAL in ref else ref.i_mixed
    ref.b_block_rows[...] = (middle + mixed[...]).astype(bf16)
    block_tasks = begun([over_tensor(ref.b_block_rows, ref.o_block_out, 0, sub)])
    run(expert_tasks)

    finished = ("o_query_down", "o_latent_down")
    finals = []
    for name, axis in ((QUERY_DOWN, 1), (LATENT_DOWN, 0), (ROUTER, 0), (GAINS, 0)):
        if name not in totals:
            continue
        share = ref["s_" + name]
        whole = ref["o_" + name] if "o_" + name in finished else ref["g_" + name]
        share[...] = ref["r_" + name][...].astype(share.dtype)
        finals.append(over_tensor(share, whole, axis, share.shape[axis]))
    finals = begun(finals)
    for name in (OUT_PROJ, QUERY_UP, LATENT_UP):
        if name in totals:
            leave(name, ref["r_" + name])
    if SHARED in axis_of:
        loading.pop(OWN_SHARED).wait()
        left.append(
            bring(ref.k_shared, ref.o_shared.at[link.me], ref.leave.at[len(left)])
        )
    run(finals)
    for move in placed:
        if move is not None:
            move.wait()
    for name in (ROUTER, GAINS):
        if name in totals:
            size = ref["s_" + name].shape[0]
            total = ref["g_" + name][:size, :]
            for t in range(1, parts):
                total = total + ref["g_" + name][t * size : (t + 1) * size, :]
            ref["f_" + name][...] = total
            leave(name, ref["f_" + name])
    run(block_tasks + input_tasks + shared_tasks)
    link.drain()
    for move in left:
        move.wait()


def back_stage(calls, groups, parts, sizes, held, small, grad_shared, partial):
    deep = groups // PAIR
    bf16, f32 = jnp.bfloat16, jnp.float32
    rows, width = small.block.shape
    sub = rows // parts
    query_rank, latent_rank = held.query_n.shape[1], held.latent_n.shape[1]
    heads, _, head_width = held.queries.shape
    query_cut, latent_cut = held.query_down.shape[1], held.latent_down.shape[0]
    experts = small.router.shape[0]
    gain_wide = -(-max(sizes) // LANES) * LANES
    lead = query_rank + latent_rank + LANES
    half = parts // PAIR
    full = Bag(
        out_proj=(held.out_proj.shape, 1, bf16),
        query_up=(held.query_up.shape, 0, bf16),
        latent_up=(held.latent_up.shape, 0, bf16),
        query_down=((width, query_cut), 0, bf16),
        latent_down=((latent_cut, width), 1, bf16),
        router=((experts, width), 1, bf16),
        gains=((groups * 8, gain_wide), 0, f32),
    )
    reduced, pieces = [], {}
    for name, (shape, axis, dtype) in full.items():
        piece = list(shape)
        piece[axis] //= groups
        if aligned(piece[axis], 1) or axis == 0:
            reduced.append((name, axis))
            pieces[name] = tuple(piece)
    buffers = Bag(
        middle_grad=((sub, width), f32),
        grad_rows=((sub, width), bf16),
        block_rows=((sub, width), bf16),
        attention_grad=((rows, width), bf16),
        attended_grad=(held.attended.shape, bf16),
        dquery=((rows, heads * head_width), bf16),
        dkeyval=((rows, heads * (NOPE + VD)), bf16),
        heads_partial=((half, PAIR, sub, lead), bf16),
        heads_beside=((half, sub, lead), bf16),
        heads_give=((sub, lead), bf16),
        heads_across=((sub, lead), bf16),
        heads_rows=((sub, lead), f32),
        query_rows=((sub, query_rank), bf16),
        latent_rows=((sub, latent_rank + LANES), bf16),
        latent_block=((rows, latent_rank), f32),
        dquery_lat=((rows, query_rank), bf16),
        dlatent_all=((rows, latent_rank + LANES), bf16),
        dlatent_t=((latent_rank + LANES, rows), f32),
        first_partial=((half, PAIR, sub, width), bf16),
        first_beside=((half, sub, width), bf16),
        first_give=((sub, width), bf16),
        first_across=((sub, width), bf16),
        first_rows=((sub, width), f32),
        input_rows=((sub, width), bf16),
    )
    for name, (shape, _, dtype) in full.items():
        buffers[name] = (shape, dtype)
    scratch = Bag(("b_" + name, pltpu.VMEM(*spec)) for name, spec in buffers.items())
    for name, array in held.items():
        scratch["l_" + name] = pltpu.VMEM(array.shape, array.dtype)
    outs = Bag(block_out=((rows, width), bf16), input_grad=((rows, width), bf16))
    for name, (shape, axis, dtype) in full.items():
        if name not in pieces:
            outs[name] = (shape, dtype)
            continue
        piece = pieces[name]
        scratch["t_" + name] = pltpu.VMEM((deep, *piece), dtype)
        scratch["d_" + name] = pltpu.VMEM((deep - 1, *piece), dtype)
        scratch["r_" + name] = pltpu.VMEM(piece, f32)
        outs[name] = (piece, f32)
        if name in (QUERY_DOWN, LATENT_DOWN, ROUTER, GAINS):
            kind = bf16 if name in (QUERY_DOWN, LATENT_DOWN) else f32
            along = 1 if name == QUERY_DOWN else 0
            whole = list(piece)
            whole[along] *= parts
            scratch["s_" + name] = pltpu.VMEM(piece, kind)
            if name in (QUERY_DOWN, LATENT_DOWN):
                outs[name] = (tuple(whole), bf16)
            else:
                scratch["g_" + name] = pltpu.VMEM(tuple(whole), kind)
                scratch["f_" + name] = pltpu.VMEM(piece, f32)
    share = grad_shared.shape[1] // groups
    inputs = {"i_" + name: array for name, array in small.items()}
    specs = [IN_VMEM] * len(small)
    if aligned(share, 1):
        reduced.append((SHARED, 1))
        inputs["i_shared"] = grad_shared
        specs.append(ANY)
        outs.shared = ((groups, grad_shared.shape[0], share), bf16)
        scratch.k_shared = pltpu.VMEM((grad_shared.shape[0], share), bf16)
        scratch.shared_send = scratch.shared_arrive = DMA((groups,))
    inputs |= {"h_" + name: array for name, array in held.items()}
    specs += [ANY] * len(held)
    if partial is not None:
        inputs[I_PARTIAL] = partial
        specs.append(ANY)
        mixed_parts = max(1, width // 512)
        wide = width // mixed_parts
        for n in range(mixed_parts):
            scratch["m%d" % n] = pltpu.VMEM((groups * half, sub, wide), bf16)
            for k, buffer in enumerate(total_buffers(deep, sub, wide)):
                scratch["m%d_%d" % (n, k)] = buffer
        scratch.b_mixed = pltpu.VMEM((sub, width), f32)
        scratch.mixed_load = DMA((mixed_parts,))
        scratch.mixed_send = scratch.mixed_arrive = DMA((mixed_parts, total_hops(deep)))
    scratch.load = DMA((len(held),))
    scratch.leave = DMA((len(outs) + 1,))
    scratch.place = DMA((12,))
    scratch.rows_send = scratch.rows_arrive = DMA((12, 8))
    scratch.send = scratch.arrive = DMA((len(full), 2 * deep))
    scratch.sum_send = scratch.sum_arrive = DMA((2, 2))
    names = list(inputs) + ["o_" + name for name in outs] + list(scratch)
    reduced = [entry for entry in reduced]
    results = pl.pallas_call(
        functools.partial(back_kernel, groups, tuple(sizes), tuple(reduced), tuple(names)),
        in_specs=specs,
        out_specs=[ANY] * len(outs),
        out_shape=[jax.ShapeDtypeStruct(*spec) for spec in outs.values()],
        scratch_shapes=list(scratch.values()),
        compiler_params=calls.params(),
        name="back",
    )(*inputs.values())
    results = Bag(zip(outs, results))
    for name, (shape, axis, dtype) in full.items():
        if name not in pieces:
            results[name] = scatter_sum(results[name], EXPERT, axis)
            if name == LATENT_DOWN:
                results[name] = gather(results[name].astype(bf16), TENSOR, 0).astype(f32)
            if name == ROUTER:
                results[name] = lax.psum(results[name].astype(bf16), TENSOR).astype(f32)
    if SHARED not in results:
        split = grad_shared.reshape(grad_shared.shape[0], groups, share).transpose(1, 0, 2)
        results.shared = lax.all_to_all(
            split, EXPERT, split_axis=0, concat_axis=0, tiled=True
        )
    return results


ALL = (EXPERT, TENSOR)


def gather(values, axes, dimension):
    return lax.all_gather(values, axes, axis=dimension, tiled=True)


def scatter_sum(values, axes, dimension):
    return lax.psum_scatter(
        values.astype(jnp.bfloat16), axes, scatter_dimension=dimension, tiled=True
    ).astype(jnp.float32)


def aligned(size, axis):
    return size % LANES == 0 if axis else size % 16 == 0


def ready_items(items, part):
    result = []
    for name, array, axis, cut, over, orders, home in items:
        if axis == 1 and array.shape[-1] % LANES:
            if over == SHUFFLE:
                array = lax.all_to_all(array, EXPERT, split_axis=0, concat_axis=0, tiled=True)
                array = array.transpose(1, 0, 2).reshape(array.shape[1], -1)
            else:
                if cut is not None:
                    array = lax.dynamic_slice_in_dim(array, part * cut[1], cut[1], axis=cut[0])
                array = gather(array, EXPERT, axis)
            cut, over, orders, home = None, READY, (), VMEM_
        result.append((name, array, axis, cut, over, orders, home))
    return result


def body(
    calls,
    block_in,
    attention_gain,
    query_down,
    query_gain,
    query_up,
    latent_down,
    latent_gain,
    latent_up,
    out_proj,
    ffn_gain,
    router,
    shared_gate,
    shared_up,
    shared_down,
    expert_gate,
    expert_up,
    expert_down,
    doc_lengths,
    routes,
    out_grad,
):
    groups = lax.axis_size(EXPERT)
    parts = lax.axis_size(TENSOR)
    me = lax.axis_index(EXPERT)
    part = lax.axis_index(TENSOR)
    row_count, width = block_in.shape
    top = routes.shape[1]
    local = expert_gate.shape[0]
    experts = local * groups

    all_gains = (attention_gain, ffn_gain, query_gain, latent_gain)
    gain_sizes = [g.shape[0] for g in all_gains]
    gain_wide = -(-max(gain_sizes) // LANES) * LANES
    gains = jnp.stack(
        [jnp.pad(g.astype(jnp.float32), (0, gain_wide - g.shape[0])) for g in all_gains]
    )
    gains = jnp.pad(gains, ((0, 8 - len(all_gains)), (0, 0)))
    routes_pad = jnp.pad(routes.T, ((0, -top % 8), (0, 0)), constant_values=-1)
    shared = jnp.stack([shared_gate.T, shared_up.T, shared_down])
    shared_units = shared.shape[1] // groups
    shared = shared.reshape(3, groups, shared_units, -1).transpose(1, 0, 2, 3)
    shared = shared.reshape(groups, 3 * shared_units, -1)
    query_cut = query_down.shape[1] // parts
    latent_cut = latent_down.shape[1] // parts
    allowed, cosine, sinusoid = layout(doc_lengths[0], row_count)
    allowed = allowed.astype(jnp.float32)
    tables = [
        jnp.pad(jnp.concatenate(pair, axis=1), ((0, 0), (0, LANES - ROPE)))
        for pair in ((cosine, cosine), (-sinusoid, sinusoid))
    ]
    items = [
        (GAINS, gains, 0, None, EXPERT, ("zx",), VMEM_),
        (QUERY_DOWN, query_down, 0, (1, query_cut), EXPERT, ("zx",), VMEM_),
        (LATENT_DOWN, latent_down.T, 1, (0, latent_cut), EXPERT, ("zx",), VMEM_),
        (QUERY_UP, query_up, 0, None, EXPERT, ("zx",), VMEM_),
        (LATENT_UP, latent_up, 0, None, EXPERT, ("zx",), VMEM_),
        (OUT_PROJ, out_proj, 1, None, EXPERT, ("zx",), VMEM_),
        (ROUTER, router.T, 1, None, EXPERT, ("zx",), VMEM_),
        (ROUTES, routes_pad, 1, None, EXPERT, ("zx",), "hbm"),
        (SHARED, shared, 1, None, SHUFFLE, (), "hbm"),
        (OUT_GRAD, out_grad, 0, (0, row_count // parts), "all", (ZXYC, "xzyc"), "hbm"),
    ]
    front = front_stage(
        calls,
        groups,
        parts,
        gain_sizes,
        ready_items(items, part),
        block_in,
        routes,
        allowed,
        *tables,
    )
    router_t = front.router
    shared = front.shared
    tokens, gradients = front.tokens, front.out_grad
    lane_pad = -experts % LANES
    own_ids = me * local + jnp.arange(local, dtype=jnp.int32)
    expert_rows, expert_grads, picks, slot_weights = route_stage(
        groups, own_ids, front.routes, tokens, gradients, front.weights
    )
    slot_shape = (groups, local, CAP)
    produced, back_rows, slot_dweights, grad_gate, grad_up, grad_down = expert_stage(
        expert_rows.reshape(*slot_shape, width),
        expert_grads.reshape(*slot_shape, width),
        slot_weights.reshape(*slot_shape, 1),
        expert_gate.transpose(0, 2, 1),
        expert_up.transpose(0, 2, 1),
        expert_down,
    )
    slots = local * CAP
    produced = produced.reshape(groups, slots, width)
    back_rows = back_rows.reshape(groups, slots, width)
    slot_dweights = slot_dweights.reshape(groups, slots, 1)
    slot_lanes = jnp.repeat(own_ids, CAP)[:, None]
    if mix_bytes(groups, row_count, slots, width) < 40 * 2**20:
        mixed = None
        dsecond, partial, grad_shared = mix_stage(
            calls,
            groups,
            parts,
            picks,
            produced,
            back_rows,
            slot_dweights,
            (slot_lanes, experts + lane_pad),
            tokens,
            gradients,
            shared,
        )
    else:
        partial = None
        lane_ids = jnp.arange(experts + lane_pad, dtype=jnp.int32)
        spread_out = jnp.where(slot_lanes == lane_ids[None, :], slot_dweights, 0.0)
        mixed_part, dsecond_part, grad_shared = combine_stage(
            picks,
            produced,
            back_rows,
            spread_out.astype(jnp.bfloat16),
            tokens.reshape(groups, row_count, width),
            gradients.reshape(groups, row_count, width),
            shared.reshape(3, shared_units, width),
        )
        grad_shared = grad_shared.astype(jnp.bfloat16).reshape(3 * shared_units, width)
        dsecond, mixed = sum_all(
            calls,
            groups,
            parts,
            (
                dsecond_part.reshape(-1, width + experts + lane_pad),
                mixed_part.reshape(-1, width),
            ),
        )
    held = Bag(
        (name, front[name])
        for name in (
            ATTENDED,
            OUT_PROJ,
            QUERIES,
            KEYS,
            VALUES,
            QUERY_N,
            LATENT_N,
            QUERY_UP,
            LATENT_UP,
            QUERY_LAT,
            LATENT_T,
            FIRST,
            QUERY_DOWN,
            LATENT_DOWN,
        )
    )
    small = Bag(
        dsecond=dsecond,
        middle=front.middle,
        chosen=front.chosen,
        router=router_t,
        out_grad=out_grad,
        block=block_in,
        allowed=allowed,
        cosine=tables[0],
        sinusoid=tables[1],
        norms=front.norms,
    )
    if partial is None:
        small.mixed = mixed
    back = back_stage(calls, groups, parts, gain_sizes, held, small, grad_shared, partial)
    grad_shared = back.shared.reshape(groups, 3, shared_units, -1).transpose(1, 0, 2, 3)
    grad_shared = grad_shared.astype(jnp.float32).reshape(3, groups * shared_units, -1)
    grad_gains = [back.gains[i, :size] for i, size in enumerate(gain_sizes)]

    return (
        back.block_out,
        back.input_grad,
        grad_gains[0],
        back.query_down.astype(jnp.float32),
        grad_gains[2],
        back.query_up,
        back.latent_down.T.astype(jnp.float32),
        grad_gains[3],
        back.latent_up,
        back.out_proj,
        grad_gains[1],
        back.router.T,
        grad_shared[0].T,
        grad_shared[1].T,
        grad_shared[2],
        grad_gate.transpose(0, 2, 1),
        grad_up.transpose(0, 2, 1),
        grad_down,
    )


def solution(mesh):
    placed = (
        P(EXPERT, None),
        P(EXPERT),
        P(EXPERT, None),
        P(EXPERT),
        P(EXPERT, TENSOR),
        P(EXPERT, None),
        P(EXPERT),
        P(EXPERT, TENSOR),
        P(TENSOR, EXPERT),
        P(EXPERT),
        P(EXPERT, None),
        P(EXPERT, TENSOR),
        P(EXPERT, TENSOR),
        P(TENSOR, EXPERT),
        P(EXPERT, None, TENSOR),
        P(EXPERT, None, TENSOR),
        P(EXPERT, TENSOR, None),
        P(EXPERT, None),
        P(EXPERT, None),
        P(EXPERT, None),
    )
    return jax.shard_map(
        functools.partial(body, Calls()),
        mesh=mesh,
        in_specs=placed,
        out_specs=(
            P(EXPERT, None),
            P(EXPERT, None),
            P(EXPERT),
            P(EXPERT, None),
            P(EXPERT),
            P(EXPERT, TENSOR),
            P(EXPERT, None),
            P(EXPERT),
            P(EXPERT, TENSOR),
            P(TENSOR, EXPERT),
            P(EXPERT),
            P(EXPERT, None),
            P(EXPERT, TENSOR),
            P(EXPERT, TENSOR),
            P(TENSOR, EXPERT),
            P(EXPERT, None, TENSOR),
            P(EXPERT, None, TENSOR),
            P(EXPERT, TENSOR, None),
        ),
        check_vma=False,
    )
```

```python
import functools
import math

import jax
import jax.numpy as jnp
from jax import lax
from jax.experimental import pallas as pl
from jax.experimental.pallas import tpu as pltpu
from jax.sharding import PartitionSpec as P

NOPE = 128
ROPE = 64
VD = 128
CAP = 32
LANES = 128
VMEM_BYTES = 60 * 2**20

EPSILON = 1e-06
ROPE_BASE = 50000.0
ROUTE_SCALE = 2.446

ATTENDED = "attended"
EXPERT = "expert"
FIRST = "first"
GAINS = "gains"
KEYS = "keys"
LATENT_DOWN = "latent_down"
LATENT_N = "latent_n"
LATENT_T = "latent_t"
LATENT_UP = "latent_up"
OUT_GRAD = "out_grad"
OUT_PROJ = "out_proj"
OWN_SHARED = "own_shared"
QUERIES = "queries"
QUERY_DOWN = "query_down"
QUERY_LAT = "query_lat"
QUERY_N = "query_n"
QUERY_UP = "query_up"
READY = "ready"
ROUTER = "router"
ROUTES = "routes"
SHARED = "shared"
SHUFFLE = "shuffle"
TENSOR = "tensor"
TOKENS = "tokens"
VALUES = "values"
VMEM_ = "vmem"
WEIGHTS = "weights"
ZXYC = "zxyc"


def matmul(left, right):
    return jnp.dot(left, right, preferred_element_type=jnp.float32)


def contract(form, left, right):
    return jnp.einsum(form, left, right, preferred_element_type=jnp.float32)


def matmul_nt(left, right):
    return lax.dot_general(left, right, (((1,), (1,)), ((), ())), preferred_element_type=jnp.float32)


def matmul_tn(left, right):
    return lax.dot_general(left, right, (((0,), (0,)), ((), ())), preferred_element_type=jnp.float32)


def layout(lengths, row_count):
    doc_count = lengths.shape[0]
    doc_ends = jnp.cumsum(lengths)
    starts = doc_ends - lengths
    row_index = jnp.arange(row_count, dtype=jnp.int32)
    doc_ids = jnp.sum((row_index[:, None] >= doc_ends[None, :]).astype(jnp.int32), axis=1)
    owners = doc_ids[:, None] == jnp.arange(doc_count, dtype=jnp.int32)[None, :]
    first_row = jnp.sum(jnp.where(owners, starts[None, :], 0), axis=1)
    positions = (row_index - first_row).astype(jnp.float32)
    allowed = (doc_ids[:, None] == doc_ids[None, :]) & (row_index[None, :] <= row_index[:, None])
    frequency = jnp.exp(
        -math.log(ROPE_BASE) * 2.0 * jnp.arange(ROPE // 2, dtype=jnp.float32) / ROPE
    )
    angles = positions[:, None] * frequency[None, :]
    return (allowed, jnp.cos(angles), jnp.sin(angles))


def swiglu(gate_pre, up_pre):
    sigmoid_gate = jax.nn.sigmoid(gate_pre)
    return (sigmoid_gate, (gate_pre * sigmoid_gate * up_pre).astype(jnp.bfloat16))


def swiglu_back(dhidden, gate_pre, up_pre, sigmoid_gate):
    gate_grad = dhidden * up_pre * sigmoid_gate * (1.0 + gate_pre * (1.0 - sigmoid_gate))
    up_grad = dhidden * gate_pre * sigmoid_gate
    return (gate_grad.astype(jnp.bfloat16), up_grad.astype(jnp.bfloat16))


def expert_kernel(
    x_ref, g_ref, w_ref, gate_ref, up_ref, down_ref, y_ref, dr_ref, dw_ref, gg_ref, gu_ref, gd_ref
):
    blocks, _, cap, width = x_ref.shape
    rows = blocks * cap
    row_inputs = x_ref[...].reshape(rows, width)
    gradient = g_ref[...].reshape(rows, width).astype(jnp.float32)
    weight = w_ref[...].reshape(rows, 1)
    gate, up, down = gate_ref[0], up_ref[0], down_ref[0]
    gate_pre = matmul_nt(row_inputs, gate)
    up_pre = matmul_nt(row_inputs, up)
    sigmoid_gate, hidden = swiglu(gate_pre, up_pre)
    produced = matmul(hidden, down)
    dw_ref[...] = jnp.sum(gradient * produced, axis=1, keepdims=True).reshape(dw_ref.shape)
    y_ref[...] = (weight * produced).astype(jnp.bfloat16).reshape(y_ref.shape)
    cotangent = (weight * gradient).astype(jnp.bfloat16)
    dhidden = matmul_nt(cotangent, down)
    gate_grad, up_grad = swiglu_back(dhidden, gate_pre, up_pre, sigmoid_gate)
    back = matmul(gate_grad, gate) + matmul(up_grad, up)
    dr_ref[...] = back.astype(jnp.bfloat16).reshape(dr_ref.shape)
    first = pl.program_id(1) == 0

    def accumulate(ref, left, right):
        part = matmul_tn(left, right)

        @pl.when(first)
        def _():
            ref[0] = part

        @pl.when(jnp.logical_not(first))
        def _():
            ref[0] += part

    accumulate(gg_ref, gate_grad, row_inputs)
    accumulate(gu_ref, up_grad, row_inputs)
    accumulate(gd_ref, hidden, cotangent)


def expert_stage(row_inputs, gradients, weights, gate_t, up_t, down):
    blocks, local, cap, width = row_inputs.shape
    units = gate_t.shape[1]
    step = min(blocks, 256 // cap)
    rows_spec = pl.BlockSpec((step, 1, cap, width), lambda j, r: (r, j, 0, 0))
    slot_spec = pl.BlockSpec((step, 1, cap, 1), lambda j, r: (r, j, 0, 0))
    unit_spec = pl.BlockSpec((1, units, width), lambda j, r: (j, 0, 0))
    rows_shape = jax.ShapeDtypeStruct(row_inputs.shape, jnp.bfloat16)
    unit_shape = jax.ShapeDtypeStruct((local, units, width), jnp.float32)
    flops = 18 * blocks * local * cap * width * units
    moved = 8 * blocks * local * cap * width + 18 * local * units * width
    return pl.pallas_call(
        expert_kernel,
        grid=(local, blocks // step),
        in_specs=[rows_spec, rows_spec, slot_spec, unit_spec, unit_spec, unit_spec],
        out_specs=[rows_spec, rows_spec, slot_spec, unit_spec, unit_spec, unit_spec],
        out_shape=[
            rows_shape,
            rows_shape,
            jax.ShapeDtypeStruct((blocks, local, cap, 1), jnp.float32),
            unit_shape,
            unit_shape,
            unit_shape,
        ],
        compiler_params=pltpu.CompilerParams(vmem_limit_bytes=VMEM_BYTES),
        cost_estimate=pl.CostEstimate(flops=flops, bytes_accessed=moved, transcendentals=0),
        name="experts",
    )(row_inputs, gradients, weights, gate_t, up_t, down)


def combine_kernel(
    p_ref, y_ref, dr_ref, dw_ref, x_ref, g_ref, shared_ref, out_ref, ds_ref, grad_ref
):
    picks = p_ref[0]
    row_inputs, cotangent = x_ref[0], g_ref[0]
    gate, up, down = shared_ref[0], shared_ref[1], shared_ref[2]
    gate_pre = matmul_nt(row_inputs, gate)
    up_pre = matmul_nt(row_inputs, up)
    sigmoid_gate, hidden = swiglu(gate_pre, up_pre)
    out_ref[0] = (matmul_tn(picks, y_ref[0]) + matmul(hidden, down)).astype(jnp.bfloat16)
    dhidden = matmul_nt(cotangent, down)
    gate_grad, up_grad = swiglu_back(dhidden, gate_pre, up_pre, sigmoid_gate)
    back = matmul_tn(picks, dr_ref[0]) + matmul(gate_grad, gate) + matmul(up_grad, up)
    width = back.shape[1]
    ds_ref[0, :, :width] = back.astype(jnp.bfloat16)
    ds_ref[0, :, width:] = matmul_tn(picks, dw_ref[0]).astype(jnp.bfloat16)
    first = pl.program_id(0) == 0
    for index, (left, right) in enumerate(
        ((gate_grad, row_inputs), (up_grad, row_inputs), (hidden, cotangent))
    ):
        part = matmul_tn(left, right)

        @pl.when(first)
        def _(index=index, part=part):
            grad_ref[index] = part

        @pl.when(jnp.logical_not(first))
        def _(index=index, part=part):
            grad_ref[index] += part


def combine_stage(picks, produced, back, spread, tokens, gradients, shared):
    blocks, slots, rows = picks.shape
    width = tokens.shape[-1]
    slot_spec = pl.BlockSpec((1, slots, width), lambda b: (b, 0, 0))
    rows_spec = pl.BlockSpec((1, rows, width), lambda b: (b, 0, 0))
    whole = pl.BlockSpec(shared.shape, lambda b: (0, 0, 0))
    lanes = spread.shape[-1]
    units = shared.shape[1]
    flops = 4 * blocks * slots * rows * width + 18 * blocks * rows * width * units
    moved = 4 * blocks * slots * width + 8 * blocks * rows * width
    return pl.pallas_call(
        combine_kernel,
        grid=(blocks,),
        in_specs=[
            pl.BlockSpec((1, slots, rows), lambda b: (b, 0, 0)),
            slot_spec,
            slot_spec,
            pl.BlockSpec((1, slots, lanes), lambda b: (b, 0, 0)),
            rows_spec,
            rows_spec,
            whole,
        ],
        out_specs=[
            rows_spec,
            pl.BlockSpec((1, rows, width + lanes), lambda b: (b, 0, 0)),
            whole,
        ],
        out_shape=[
            jax.ShapeDtypeStruct((blocks, rows, width), jnp.bfloat16),
            jax.ShapeDtypeStruct((blocks, rows, width + lanes), jnp.bfloat16),
            jax.ShapeDtypeStruct(shared.shape, jnp.float32),
        ],
        compiler_params=pltpu.CompilerParams(vmem_limit_bytes=VMEM_BYTES),
        cost_estimate=pl.CostEstimate(flops=flops, bytes_accessed=moved, transcendentals=0),
        name="combine",
    )(picks, produced, back, spread, tokens, gradients, shared)


MESH = pl.DeviceIdType.MESH
PAIR = 2
ANY = pl.BlockSpec(memory_space=pl.ANY)
IN_VMEM = pl.BlockSpec(memory_space=pltpu.VMEM)
DMA = pltpu.SemaphoreType.DMA


def place():
    me, part = lax.axis_index(EXPERT), lax.axis_index(TENSOR)
    return (me // PAIR, me % PAIR, part // PAIR, part % PAIR)


def device(z, x, y, c):
    return {EXPERT: z * PAIR + x, TENSOR: y * PAIR + c}


def greet(peers):
    barrier = pltpu.get_barrier_semaphore()
    for peer in peers:
        pl.semaphore_signal(barrier, inc=1, device_id=peer, device_id_type=MESH)
    pl.semaphore_wait(barrier, len(peers))


def push(source, target, send, arrive, peer):
    copy = pltpu.make_async_remote_copy(
        src_ref=source,
        dst_ref=target,
        send_sem=send,
        recv_sem=arrive,
        device_id=peer,
        device_id_type=MESH,
    )
    copy.start()
    return copy


def bring(source, target, done):
    copy = pltpu.make_async_copy(source, target, done)
    copy.start()
    return copy


def arrived(target, done):
    pltpu.make_async_copy(target, target, done).wait()


def slot(ref, axis, index, size):
    start = pl.multiple_of(index * size, size)
    if axis == 0:
        return ref.at[pl.ds(start, size), :]
    return ref.at[:, pl.ds(start, size)]


class Bag(dict):
    __getattr__ = dict.__getitem__
    __setattr__ = dict.__setitem__


class Calls:
    def __init__(self):
        self.count = 0

    def params(self):
        self.count += 1
        return pltpu.CompilerParams(
            collective_id=self.count, has_side_effects=True, vmem_limit_bytes=VMEM_BYTES
        )


def choose(table, index):
    value = table[0]
    for i, entry in enumerate(table[1:], 1):
        if any(entry != other for other in table):
            value = jnp.where(index == i, entry, value)
    return value


class Link:
    def __init__(self, deep):
        me, part = lax.axis_index(EXPERT), lax.axis_index(TENSOR)
        self.deep, self.me, self.part = deep, me, part
        self.z, self.x = me // PAIR, me % PAIR
        self.y, self.c = part // PAIR, part % PAIR
        near = [
            sorted((k for k in range(1, deep)), key=lambda k: abs((z - k) % deep - z))
            for z in range(deep)
        ]
        self.order = [choose([near[z][h] for z in range(deep)], self.z) for h in range(deep - 1)]
        self.drains = []

    def at_z(self, z):
        return device(z, self.x, self.y, self.c)

    def peer(self, axis):
        flip = {name: 1 - getattr(self, name) if name == axis else getattr(self, name) for name in "xyc"}
        return device(self.z, flip["x"], flip["y"], flip["c"])

    def greet(self, groups, axes):
        peers = [{EXPERT: (self.me + j) % groups, TENSOR: self.part} for j in range(1, groups)]
        if "e" not in axes:
            peers = []
        greet(peers + [self.peer(axis) for axis in axes if axis != "e"])

    def emit(self, make, condition=None):
        def start():
            make().start()

        def finish():
            make().wait_send()

        if condition is None:
            start()
            self.drains.append(finish)
        else:
            pl.when(condition)(start)
            self.drains.append(lambda: pl.when(condition)(finish))

    def drain(self):
        for finish in self.drains:
            finish()
        self.drains = []


def spread(link, order, source, at, send, arrive):
    deep, z = link.deep, link.z
    cut = order.find("z")
    before, after = (order[:cut], order[cut + 1 :]) if cut >= 0 else ("", order)
    none = frozenset()

    def piece(k, flips):
        x, y, c = (
            1 - getattr(link, name) if name in flips else getattr(link, name) for name in "xyc"
        )
        return at((z + deep - k) % deep, x, y, c)

    def number(k, flips):
        return k * 8 + sum(1 << "xyc".index(name) for name in flips)

    def forward(k, flips, to_number, peer, condition=None):
        own = isinstance(k, int) and k == 0 and not flips

        def make():
            target = piece(k, flips)
            return pltpu.make_async_remote_copy(
                src_ref=source if own else target,
                dst_ref=target,
                send_sem=send.at[to_number],
                recv_sem=arrive.at[to_number],
                device_id=peer,
                device_id_type=MESH,
            )

        link.emit(make, condition)

    def hand_on(k, flips, axes, along_z):
        if along_z:
            forward(k, flips, number(1, flips), link.at_z(z + 1), z < deep - 1)
            forward(k, flips, number(deep - 1, flips), link.at_z(z - 1), z > 0)
        for axis in axes:
            forward(k, flips, number(k, flips | {axis}), link.peer(axis))

    def take(k, flips):
        arrived(piece(k, flips), arrive.at[number(k, flips)])

    hand_on(0, none, before + after, cut >= 0)
    got = [none]
    for i, axis in enumerate(before):
        for flips in got:
            yield
            take(0, flips | {axis})
            hand_on(0, flips | {axis}, before[i + 1 :] + after, True)
        got = got + [flips | {axis} for flips in got]
    ks = [0]
    if cut >= 0:
        for k in link.order:
            below = z >= k
            onward = jnp.where(below, k + 1, k - 1)
            more = jnp.where(below, z < deep - 1, z > 0)
            following = link.at_z(jnp.where(below, z + 1, z - 1))
            for flips in got:
                yield
                take(k, flips)
                forward(k, flips, number(onward, flips), following, more)
                hand_on(k, flips, after, False)
        ks = ks + link.order
    for i, axis in enumerate(after):
        for k in ks:
            for flips in got:
                yield
                take(k, flips | {axis})
                hand_on(k, flips | {axis}, after[i + 1 :], False)
        got = got + [flips | {axis} for flips in got]


def shuffle(link, groups, source, at, send, arrive):
    def make(j):
        target = (link.me + j) % groups
        return pltpu.make_async_remote_copy(
            src_ref=source(target),
            dst_ref=at(link.me),
            send_sem=send.at[j],
            recv_sem=arrive.at[j],
            device_id={EXPERT: target, TENSOR: link.part},
            device_id_type=MESH,
        )

    for j in range(1, groups):
        link.emit(functools.partial(make, j))
    for j in range(1, groups):
        yield
        arrived(at((link.me + groups - j) % groups), arrive.at[j])


def run(tasks):
    tasks = list(tasks)
    while tasks:
        tasks = [task for task in tasks if next(task, run) is not run]


def add_rows(count, store):
    lax.fori_loop(0, count, lambda i, carry: (store(i), carry)[1], 0)


def sum_all_kernel(deep, chunks, count, *refs):
    partials, outs = refs[:count], refs[count : 2 * count]
    total = len(chunks)
    rest = refs[2 * count :]
    own_buf, from_core = rest[:total], rest[total : 2 * total]
    from_first, from_second = rest[2 * total : 3 * total], rest[3 * total : 4 * total]
    from_deep = rest[4 * total : 5 * total]
    send, arrive, own = rest[5 * total :]
    z, x, y, c = place()
    others = [device((z + k) % deep, x, y, c) for k in range(1, deep)]
    twin, across, beside = (
        device(z, 1 - x, y, c),
        device(z, x, 1 - y, c),
        device(z, x, y, 1 - c),
    )
    greet(others + [twin, across, beside])
    copies, loads = [], []
    for n, (i, left, wide, order) in enumerate(chunks):
        span = pl.ds(left, wide)
        copies.append(
            push(
                partials[i].at[:, 1 - c, :, span],
                from_core[n],
                send.at[n, 0],
                arrive.at[n, 0],
                beside,
            )
        )
        loads.append(bring(partials[i].at[:, c, :, span], own_buf[n], own.at[n]))

    def index(order, depth, on_first, on_second):
        on_x, on_y = (on_first, on_second) if order == 0 else (on_second, on_first)
        return (depth * PAIR + on_x) * PAIR + on_y

    def stage_core(n):
        _, _, _, order = chunks[n]
        buf, other = own_buf[n], from_core[n]
        loads[n].wait()
        arrived(other, arrive.at[n, 0])

        def add(k):
            buf[k] = (buf[k].astype(jnp.float32) + other[k].astype(jnp.float32)).astype(
                jnp.bfloat16
            )

        add_rows(deep * PAIR * PAIR, add)
        mine = x if order == 0 else y
        for depth in range(deep):
            for s in range(PAIR):
                number = 1 + depth * PAIR + s
                copies.append(
                    push(
                        buf.at[index(order, depth, 1 - mine, s)],
                        from_first[n].at[depth * PAIR + s],
                        send.at[n, number],
                        arrive.at[n, number],
                        twin if order == 0 else across,
                    )
                )

    def stage_first(n):
        _, _, _, order = chunks[n]
        buf, other = own_buf[n], from_first[n]
        mine, following = (x, y) if order == 0 else (y, x)
        for number in range(1, 1 + PAIR * deep):
            arrived(other.at[number - 1], arrive.at[n, number])

        def add(k):
            at = index(order, k // PAIR, mine, k % PAIR)
            buf[at] = (buf[at].astype(jnp.float32) + other[k].astype(jnp.float32)).astype(
                jnp.bfloat16
            )

        add_rows(deep * PAIR, add)
        for depth in range(deep):
            number = 1 + PAIR * deep + depth
            copies.append(
                push(
                    buf.at[index(order, depth, mine, 1 - following)],
                    from_second[n].at[depth],
                    send.at[n, number],
                    arrive.at[n, number],
                    across if order == 0 else twin,
                )
            )

    def stage_second(n):
        _, _, _, order = chunks[n]
        buf, other = own_buf[n], from_second[n]
        mine, following = (x, y) if order == 0 else (y, x)
        base = 1 + PAIR * deep
        for depth in range(deep):
            arrived(other.at[depth], arrive.at[n, base + depth])

        def add(k):
            at = index(order, k, mine, following)
            buf[at] = (buf[at].astype(jnp.float32) + other[k].astype(jnp.float32)).astype(
                jnp.bfloat16
            )

        add_rows(deep, add)
        for k in range(1, deep):
            number = base + deep + k - 1
            copies.append(
                push(
                    buf.at[index(order, (z + k) % deep, mine, following)],
                    from_deep[n].at[k - 1],
                    send.at[n, number],
                    arrive.at[n, number],
                    others[k - 1],
                )
            )

    def stage_deep(n):
        i, left, wide, order = chunks[n]
        base = 1 + PAIR * deep + deep
        for k in range(1, deep):
            arrived(from_deep[n].at[k - 1], arrive.at[n, base + k - 1])
        mine, following = (x, y) if order == 0 else (y, x)
        result = own_buf[n][index(order, z, mine, following)].astype(jnp.float32)
        for k in range(deep - 1):
            result = result + from_deep[n][k].astype(jnp.float32)
        outs[i][:, pl.ds(left, wide)] = result

    for step in range(total + 3):
        for lag, stage in enumerate((stage_core, stage_first, stage_second, stage_deep)):
            if 0 <= step - lag < total:
                stage(step - lag)
    for copy in copies:
        copy.wait_send()


def sum_all(calls, groups, parts, arrays):
    deep = groups // PAIR
    rows = arrays[0].shape[0] // (groups * parts)
    budget, calls_of, used = 46 * 2**20, [[]], 0
    number = 0
    for i, array in enumerate(arrays):
        left = 0
        while left < array.shape[1]:
            wide = min(512, array.shape[1] - left)
            if 0 < array.shape[1] - left - wide < 512 // 2:
                wide = array.shape[1] - left
            cost = 2 * rows * wide * (4 * deep * 2 + 2 * deep + deep + deep) + 4 * rows * wide
            if used + cost > budget:
                calls_of.append([])
                used = 0
            used += cost
            calls_of[-1].append((i, left, wide, number % 2))
            number += 1
            left += wide
    views = [a.reshape(groups * parts // PAIR, PAIR, rows, a.shape[1]) for a in arrays]
    pieces = [[] for _ in arrays]
    for chunks in calls_of:
        used_arrays = sorted({c[0] for c in chunks})
        bounds = {
            i: (min(c[1] for c in chunks if c[0] == i), sum(c[2] for c in chunks if c[0] == i))
            for i in used_arrays
        }
        local = [(used_arrays.index(i), left, wide, order) for i, left, wide, order in chunks]
        count = len(used_arrays)
        many = deep * PAIR * PAIR

        def bufs(n):
            return [pltpu.VMEM((n, rows, wide), jnp.bfloat16) for _, _, wide, _ in chunks]

        sems = DMA((len(chunks), 1 + PAIR * deep + deep + deep))
        outs = pl.pallas_call(
            functools.partial(
                sum_all_kernel,
                deep,
                tuple(local),
                count,
            ),
            in_specs=[ANY] * count,
            out_specs=[IN_VMEM] * count,
            out_shape=[
                jax.ShapeDtypeStruct((rows, arrays[i].shape[1]), jnp.float32)
                for i in used_arrays
            ],
            scratch_shapes=bufs(many)
            + bufs(many)
            + bufs(PAIR * deep)
            + bufs(deep)
            + bufs(deep - 1)
            + [sems, sems, DMA((len(chunks),))],
            compiler_params=calls.params(),
            name="sum_all",
        )(*[views[i] for i in used_arrays])
        for i, out in zip(used_arrays, outs):
            pieces[i].append(out[:, bounds[i][0] : bounds[i][0] + bounds[i][1]])
    return [p[0] if len(p) == 1 else jnp.concatenate(p, axis=1) for p in pieces]


def swap_halves(values, half):
    lane = lax.broadcasted_iota(jnp.int32, values.shape, 1)
    wide = values.shape[1]
    return jnp.where(
        lane < half, pltpu.roll(values, wide - half, 1), pltpu.roll(values, half, 1)
    )


def turn(values, cosine, sinusoid):
    return values * cosine + swap_halves(values, ROPE // 2) * sinusoid


def full_gain(gains, row, size, groups):
    total = size * groups
    wide = gains.shape[1]
    result = jnp.zeros((8, total), jnp.float32)
    for e in range(groups):
        share = jnp.broadcast_to(gains[e * 8 + row : e * 8 + row + 1, :], (8, wide))
        if total > wide:
            share = jnp.concatenate([share, jnp.zeros((8, total - wide), jnp.float32)], axis=1)
        result = result + (pltpu.roll(share, e * size, 1) if e else share)
    return result[:1]


def rows_loop(count, step, work):
    def one(i, carry):
        work(pl.ds(pl.multiple_of(i * step, step), step))
        return carry

    lax.fori_loop(0, count // step, one, 0)


def front_kernel(groups, sizes, plan, names, *refs):
    ref = Bag(zip(names, refs))
    deep = groups // PAIR
    link = Link(deep)
    z, x, y, c, part = link.z, link.x, link.y, link.c, link.part
    send, arrive, own, leave = ref.send, ref.arrive, ref.own, ref.leave
    link.greet(groups, "eyc")
    loads, numbers, landing = {}, {}, Bag()
    row_of = {}
    for n, (name, axis, cut, over, orders, home) in enumerate(plan):
        numbers[name] = n
        landing[name] = ref["b_" + name] if home == VMEM_ else ref["o_" + name]

    stream_row = [0]

    def tasks_of(name):
        n = numbers[name]
        _, axis, cut, over, orders, home = plan[n]
        source, target = ref["i_" + name], landing[name]
        if cut is not None:
            source = slot(source, cut[0], part, cut[1])
        if over == READY:
            loads[name] = bring(source, target, own.at[n])
            return []
        if over == SHUFFLE:
            size = source.shape[2]
            keep = ref["k_" + name]
            loads[name] = bring(source.at[link.me], keep, own.at[n])
            row = stream_row[0]
            stream_row[0] += 1
            return [
                shuffle(
                    link,
                    groups,
                    lambda e: source.at[e],
                    lambda e: slot(target, axis, e, size),
                    send.at[row],
                    arrive.at[row],
                )
            ]
        size = cut[1] if cut is not None and cut[0] == axis else source.shape[axis]

        def home_of(sz, sx, sy, sc):
            index = sz * PAIR + sx
            if over == "all":
                index = (index * PAIR + sy) * PAIR + sc
            return slot(target, axis, index, size)

        mine = home_of(z, x, y, c)
        if home == VMEM_:
            loads[name] = bring(source, mine, own.at[n])
        else:
            loads[name] = bring(source, ref["k_" + name], own.at[n])
        if orders == ("e",):
            row = stream_row[0]
            stream_row[0] += 1
            return [
                shuffle(
                    link,
                    groups,
                    lambda e: source,
                    lambda e: slot(target, axis, e, size),
                    send.at[row],
                    arrive.at[row],
                )
            ]
        return streams_of(source, home_of, orders)

    def streams_of(source, home_of, orders):
        result = []
        for i, order in enumerate(orders):
            row = stream_row[0]
            stream_row[0] += 1
            if len(orders) == 1:
                at, part_source = home_of, source
            else:
                wide = source.shape[1] // len(orders)
                span = pl.ds(i * wide, wide)

                def at(*where, span=span):
                    return home_of(*where).at[:, span]

                part_source = source.at[:, span]
            result.append(spread(link, order, part_source, at, send.at[row], arrive.at[row]))
        return result

    def begin(*which):
        found = [task for name in which for task in tasks_of(name)]
        return [task for task in found if next(task, run) is not run]

    gain_tasks = begin(GAINS, ROUTES)
    stem_tasks = begin(QUERY_DOWN, LATENT_DOWN)
    late_tasks = begin(OUT_GRAD)

    def complete(name):
        n = numbers[name]
        loads.pop(name).wait()
        _, axis, cut, over, _, home = plan[n]
        if home == "hbm":
            keep, target = ref["k_" + name], landing[name]
            index = link.me
            if over == "all":
                index = link.me * PAIR * PAIR + part
            move = pltpu.make_async_copy(
                keep, slot(target, axis, index, keep.shape[axis]), own.at[n]
            )
            move.start()
            stores.append(move)

    stores = []

    def keep_out(name, source=None):
        moves = len(stores)
        move = bring(source if source is not None else landing[name], ref["o_" + name], leave.at[len(kept)])
        kept.append(move)

    kept = []
    block_ref = ref.i_block
    first_ref, middle_ref = ref.b_first, ref.b_middle
    width = block_ref.shape[1]
    row_count = block_ref.shape[0]
    sub = row_count // (PAIR * PAIR)

    complete(GAINS)
    complete(ROUTES)
    run(gain_tasks)
    gains = landing.gains
    attention_gain = full_gain(gains, 0, sizes[0], groups)

    def first_norm(span):
        values = block_ref[span, :].astype(jnp.float32)
        inverse = lax.rsqrt(jnp.mean(values * values, axis=-1, keepdims=True) + EPSILON)
        first_ref[span, :] = (values * inverse * attention_gain).astype(jnp.bfloat16)

    rows_loop(row_count, 32, first_norm)
    for _ in range(deep - 1):
        advance(stem_tasks, 1)
        advance(late_tasks, 1)
    up_tasks = begin(QUERY_UP, LATENT_UP)
    for name in (QUERY_DOWN, LATENT_DOWN):
        complete(name)
    run(stem_tasks)
    ref.b_query_cut[...] = matmul(first_ref[...], landing.query_down[...]).astype(
        jnp.bfloat16
    )
    ref.b_latent_cut[...] = matmul_nt(landing.latent_down[...], first_ref[...]).astype(
        jnp.bfloat16
    )
    query_lat, latent_t = ref.b_query_lat, ref.b_latent_t
    query_cut, latent_cut = ref.b_query_cut, ref.b_latent_cut
    stem_numbers = len(plan)
    stem_tasks = streams_of(
        query_cut, lambda sz, sx, sy, sc: slot(query_lat, 1, sy * PAIR + sc, query_cut.shape[1]), ("yc",)
    ) + streams_of(
        latent_cut, lambda sz, sx, sy, sc: slot(latent_t, 0, sy * PAIR + sc, latent_cut.shape[0]), ("yc",)
    )
    stem_tasks = [task for task in stem_tasks if next(task, run) is not run]
    query_lat[:, pl.ds(pl.multiple_of(part * query_cut.shape[1], LANES), query_cut.shape[1])] = (
        query_cut[...]
    )
    latent_t[pl.ds(pl.multiple_of(part * latent_cut.shape[0], 16), latent_cut.shape[0]), :] = (
        latent_cut[...]
    )
    query_gain = full_gain(gains, 2, sizes[2], groups)
    latent_gain = full_gain(gains, 3, sizes[3], groups)
    cosine, sinusoid = ref.i_cosine, ref.i_sinusoid
    advance(up_tasks, 1)
    run(stem_tasks)
    advance(late_tasks, 2)

    query_n, latent_n, keys = ref.b_query_n, ref.b_latent_n, ref.b_keys

    def query_norm(span):
        values = query_lat[span, :].astype(jnp.float32)
        inverse = lax.rsqrt(jnp.mean(values * values, axis=-1, keepdims=True) + EPSILON)
        query_n[span, :] = (values * inverse * query_gain).astype(jnp.bfloat16)

    rows_loop(row_count, 32, query_norm)
    for _ in range(deep - 2):
        advance(up_tasks, 1)
        advance(late_tasks, 2)
    out_tasks = begin(OUT_PROJ, ROUTER)
    latent_rank = latent_n.shape[1]
    latent = latent_t[:latent_rank, :].astype(jnp.float32).T
    inverse = lax.rsqrt(jnp.mean(latent * latent, axis=-1, keepdims=True) + EPSILON)
    latent_n[...] = (latent * inverse * latent_gain).astype(jnp.bfloat16)
    rope_rows = latent_t[latent_rank:, :].astype(jnp.float32).T
    rope_rows = jnp.concatenate(
        [rope_rows, jnp.zeros((row_count, LANES - ROPE), jnp.float32)], axis=1
    )
    key_rope = turn(rope_rows, cosine[...], sinusoid[...])[:, :ROPE].astype(jnp.bfloat16)

    complete(QUERY_UP)
    complete(LATENT_UP)
    run(up_tasks)
    queries, values_ref, attended = ref.b_queries, ref.b_values, ref.b_attended
    heads = queries.shape[0]
    head_width = NOPE + ROPE
    projected = matmul(query_n[...], landing.query_up[...])
    shifted = pltpu.roll(projected, projected.shape[1] - ROPE, 1)
    keyval = matmul(latent_n[...], landing.latent_up[...])
    for h in range(heads):
        start = h * head_width
        base, start = (projected, start) if start % LANES == 0 else (shifted, start - ROPE)
        queries[h, :, :NOPE] = base[:, start : start + NOPE].astype(jnp.bfloat16)
        tail = base[:, start + NOPE : start + NOPE + LANES]
        if tail.shape[1] < LANES:
            tail = jnp.concatenate(
                [tail, jnp.zeros((row_count, LANES - tail.shape[1]), jnp.float32)], axis=1
            )
        queries[h, :, NOPE:] = turn(tail, cosine[...], sinusoid[...])[:, :ROPE].astype(
            jnp.bfloat16
        )
        left = h * (NOPE + VD)
        keys[h, :, :NOPE] = keyval[:, left : left + NOPE].astype(jnp.bfloat16)
        keys[h, :, NOPE:] = key_rope
        values_ref[h] = keyval[:, left + NOPE : left + NOPE + VD].astype(jnp.bfloat16)
        scores = matmul_nt(queries[h], keys[h]) * head_width ** (-0.5)
        scores = jnp.where(ref.i_allowed[...] > 0, scores, -1e30)
        powers = jnp.exp(scores - jnp.max(scores, axis=-1, keepdims=True))
        probs = (powers / jnp.sum(powers, axis=-1, keepdims=True)).astype(jnp.bfloat16)
        attended[:, h * VD : (h + 1) * VD] = matmul(probs, values_ref[h]).astype(jnp.bfloat16)
        if h < deep - 1:
            advance(out_tasks, 1)
        advance(late_tasks, 2)
    advance(out_tasks, max(0, deep - 1 - heads))
    shared_tasks = begin(SHARED)
    for name in (OUT_PROJ, ROUTER):
        complete(name)
    run(out_tasks)
    for name in (QUERY_DOWN, LATENT_DOWN, QUERY_UP, LATENT_UP, OUT_PROJ, GAINS, ROUTER):
        keep_out(name)
    for name in (FIRST, QUERY_LAT, LATENT_T, QUERY_N, LATENT_N, QUERIES, KEYS, VALUES, ATTENDED):
        keep_out(name, ref["b_" + name])

    partial, from_beside = ref.b_partial, ref.b_from_beside
    give, from_across = ref.b_give, ref.b_from_across
    swap_send, swap_arrive = ref.swap_send, ref.swap_arrive
    for quarter in range(PAIR * PAIR):
        partial[quarter // PAIR, quarter % PAIR] = matmul(
            attended[quarter * sub : (quarter + 1) * sub, :], landing.out_proj[...]
        ).astype(jnp.bfloat16)

    def beside_copy():
        return pltpu.make_async_remote_copy(
            src_ref=partial.at[:, 1 - c],
            dst_ref=from_beside,
            send_sem=swap_send.at[0],
            recv_sem=swap_arrive.at[0],
            device_id=link.peer("c"),
            device_id_type=MESH,
        )

    def across_copy():
        return pltpu.make_async_remote_copy(
            src_ref=give,
            dst_ref=from_across,
            send_sem=swap_send.at[1],
            recv_sem=swap_arrive.at[1],
            device_id=link.peer("y"),
            device_id_type=MESH,
        )

    link.emit(beside_copy)
    advance(late_tasks, 1)
    arrived(from_beside, swap_arrive.at[0])
    give[...] = partial[1 - y, c] + from_beside[1 - y]
    link.emit(across_copy)
    complete(OUT_GRAD)
    complete(SHARED)
    residual = block_ref[pl.ds(pl.multiple_of(part * sub, sub), sub), :].astype(jnp.float32)
    middle_ref[...] = (
        residual + partial[y, c].astype(jnp.float32) + from_beside[y].astype(jnp.float32)
    )
    advance(late_tasks, 1)
    arrived(from_across, swap_arrive.at[1])
    middle = middle_ref[...] + from_across[...].astype(jnp.float32)
    middle_ref[...] = middle
    ffn_gain = full_gain(gains, 1, sizes[1], groups)
    norms = ref.b_norms
    norms[...] = jnp.zeros(norms.shape, jnp.float32)
    for i, gain in enumerate((attention_gain, ffn_gain, query_gain, latent_gain)):
        norms[i : i + 1, : gain.shape[1]] = gain
    keep_out("norms", norms)
    inverse = lax.rsqrt(jnp.mean(middle * middle, axis=-1, keepdims=True) + EPSILON)
    second_ref, weights_ref, chosen_ref = ref.b_second, ref.b_weights, ref.b_chosen
    second_ref[...] = (middle * inverse * ffn_gain).astype(jnp.bfloat16)
    logits = matmul_nt(second_ref[...], landing.router[...])
    experts = logits.shape[1]
    advance(late_tasks, 1)
    routes_rows = ref.i_route_rows[pl.ds(pl.multiple_of(part * sub, sub), sub), :]
    ids = lax.broadcasted_iota(jnp.int32, (sub, experts), 1)
    chosen = jnp.zeros((sub, experts), jnp.float32)
    picked = jax.nn.sigmoid(logits)
    for k in range(routes_rows.shape[1]):
        chosen = jnp.where(routes_rows[:, k : k + 1] == ids, picked, chosen)
    totals = jnp.sum(chosen, axis=-1, keepdims=True)
    weights_ref[...] = jnp.zeros(weights_ref.shape, jnp.float32)
    weights_ref[:, :experts] = ROUTE_SCALE * chosen / totals
    chosen_ref[...] = jnp.zeros(chosen_ref.shape, jnp.float32)
    chosen_ref[:, :experts] = chosen

    def row_home(name):
        def home_of(sz, sx, sy, sc):
            index = ((sz * PAIR + sx) * PAIR + sy) * PAIR + sc
            return slot(ref["o_" + name], 0, index, sub)

        return home_of

    all_tasks = streams_of(weights_ref, row_home(WEIGHTS), (ZXYC,))
    all_tasks += streams_of(second_ref, row_home(TOKENS), (ZXYC, "zyxc") * 2)
    all_tasks = [task for task in all_tasks if next(task, run) is not run]
    mine = link.me * PAIR * PAIR + part
    kept.append(bring(second_ref, slot(ref.o_tokens, 0, mine, sub), leave.at[len(kept)]))
    kept.append(bring(weights_ref, slot(ref.o_weights, 0, mine, sub), leave.at[len(kept)]))
    keep_out("middle", middle_ref)
    keep_out("chosen", chosen_ref)
    run(late_tasks + all_tasks + shared_tasks)
    link.drain()
    for move in stores + kept:
        move.wait()


def front_stage(calls, groups, parts, sizes, items, block, route_rows, allowed, cosine, sinusoid):
    deep = groups // PAIR
    rows, width = block.shape
    sub = rows // parts
    bf16, f32 = jnp.bfloat16, jnp.float32
    names, inputs, in_specs = [], [], []
    out_names, out_shape, plan, scratch = [], [], [], Bag()
    streams = 0
    for name, array, axis, cut, over, orders, home in items:
        names.append("i_" + name)
        inputs.append(array)
        in_specs.append(ANY)
        shape = list(array.shape)
        if over == SHUFFLE:
            shape = shape[1:]
        if cut is not None:
            shape[cut[0]] = cut[1]
        if home == "hbm":
            scratch["k_" + name] = pltpu.VMEM(tuple(shape), array.dtype)
        if over != READY:
            shape[axis] *= groups * parts if over == "all" else groups
            streams += max(1, len(orders))
        if home == VMEM_:
            scratch["b_" + name] = pltpu.VMEM(tuple(shape), array.dtype)
        out_names.append(name)
        out_shape.append(jax.ShapeDtypeStruct(tuple(shape), array.dtype))
        plan.append((name, axis, cut, over, orders, home))
    for name, array in (
        ("block", block),
        ("route_rows", route_rows),
        ("allowed", allowed),
        ("cosine", cosine),
        ("sinusoid", sinusoid),
    ):
        names.append("i_" + name)
        inputs.append(array)
        in_specs.append(IN_VMEM)
    shape_of = Bag((name, shape.shape) for name, shape in zip(out_names, out_shape))
    query_cut, latent_cut = shape_of.query_down[1], shape_of.latent_down[0]
    query_rank, latent_rank = shape_of.query_up[0], shape_of.latent_up[0]
    heads = shape_of.latent_up[1] // (NOPE + VD)
    experts = shape_of.router[0]
    lanes = experts + -experts % LANES
    half = parts // PAIR
    buffers = Bag(
        first=((rows, width), bf16),
        query_lat=((rows, query_cut * parts), bf16),
        latent_t=((latent_cut * parts, rows), bf16),
        query_n=((rows, query_rank), bf16),
        latent_n=((rows, latent_rank), bf16),
        queries=((heads, rows, NOPE + ROPE), bf16),
        keys=((heads, rows, NOPE + ROPE), bf16),
        values=((heads, rows, VD), bf16),
        attended=((rows, heads * VD), bf16),
        middle=((sub, width), f32),
        chosen=((sub, lanes), f32),
        norms=((8, width), f32),
    )
    for name, (shape, dtype) in buffers.items():
        out_names.append(name)
        out_shape.append(jax.ShapeDtypeStruct(shape, dtype))
    inner = Bag(
        query_cut=((rows, query_cut), bf16),
        latent_cut=((latent_cut, rows), bf16),
        partial=((half, PAIR, sub, width), bf16),
        from_beside=((half, sub, width), bf16),
        give=((sub, width), bf16),
        from_across=((sub, width), bf16),
        second=((sub, width), bf16),
        weights=((sub, lanes), f32),
    )
    for name, (shape, dtype) in (buffers | inner).items():
        scratch["b_" + name] = pltpu.VMEM(shape, dtype)
    out_names += [TOKENS, WEIGHTS]
    out_shape += [
        jax.ShapeDtypeStruct((sub * groups * parts, width), bf16),
        jax.ShapeDtypeStruct((sub * groups * parts, lanes), f32),
    ]
    streams += 2 + 1 + 4
    scratch.send = scratch.arrive = DMA((streams, 8 * deep))
    scratch.own = DMA((len(items),))
    scratch.leave = DMA((len(out_names),))
    scratch.swap_send = scratch.swap_arrive = DMA((2,))
    names += ["o_" + name for name in out_names] + list(scratch)
    results = pl.pallas_call(
        functools.partial(front_kernel, groups, tuple(sizes), tuple(plan), tuple(names)),
        in_specs=in_specs,
        out_specs=[ANY] * len(out_names),
        out_shape=out_shape,
        scratch_shapes=list(scratch.values()),
        compiler_params=calls.params(),
        name="front",
    )(*inputs)
    return Bag(zip(out_names, results))


def device_total(link, order, own, give, bufs, result, send, arrive):
    deep, z, x, y = link.deep, link.z, link.x, link.y
    from_core, from_first, from_second, from_deep = bufs
    mine, following = (x, y) if order == 0 else (y, x)
    near, far = (link.peer("x"), link.peer("y")) if order == 0 else (link.peer("y"), link.peer("x"))

    def at(depth, on_first, on_second):
        on_x, on_y = (on_first, on_second) if order == 0 else (on_second, on_first)
        return (depth * PAIR + on_x) * PAIR + on_y

    def hop(number, source, target, peer):
        def make():
            return pltpu.make_async_remote_copy(
                src_ref=source(),
                dst_ref=target,
                send_sem=send.at[number],
                recv_sem=arrive.at[number],
                device_id=peer,
                device_id_type=MESH,
            )

        link.emit(make)

    hop(0, lambda: give, from_core, link.peer("c"))
    yield
    arrived(from_core, arrive.at[0])

    def add_core(k):
        own[k] = own[k] + from_core[k]

    add_rows(deep * PAIR * PAIR, add_core)
    for depth in range(deep):
        for s in range(PAIR):
            n = depth * PAIR + s
            hop(1 + n, lambda d=depth, s=s: own.at[at(d, 1 - mine, s)], from_first.at[n], near)
    yield
    for n in range(PAIR * deep):
        arrived(from_first.at[n], arrive.at[1 + n])

    def add_first(k):
        here = at(k // PAIR, mine, k % PAIR)
        own[here] = own[here] + from_first[k]

    add_rows(deep * PAIR, add_first)
    base = 1 + PAIR * deep
    for depth in range(deep):
        hop(
            base + depth,
            lambda d=depth: own.at[at(d, mine, 1 - following)],
            from_second.at[depth],
            far,
        )
    yield
    for depth in range(deep):
        arrived(from_second.at[depth], arrive.at[base + depth])

    def add_second(k):
        here = at(k, mine, following)
        own[here] = own[here] + from_second[k]

    add_rows(deep, add_second)
    base = base + deep - 1
    for k in range(1, deep):
        hop(
            base + k,
            lambda k=k: own.at[at((z + k) % deep, mine, following)],
            from_deep.at[k - 1],
            link.at_z((z + k) % deep),
        )
    total = own[at(z, mine, following)].astype(jnp.float32)
    yield
    for k in range(1, deep):
        arrived(from_deep.at[k - 1], arrive.at[base + k])
        total = total + from_deep[k - 1].astype(jnp.float32)
    result[...] = total


def total_buffers(deep, rows, wide):
    shapes = (deep * PAIR * PAIR, PAIR * deep, deep, deep - 1)
    return [pltpu.VMEM((n, rows, wide), jnp.bfloat16) for n in shapes]


def total_hops(deep):
    return PAIR * deep + 2 * deep


def route_kernel(ids_ref, routes_ref, x_ref, g_ref, weights_ref, xr_ref, gr_ref, p_ref, w_ref):
    local = ids_ref.shape[0]
    rows = x_ref.shape[0]
    f32, bf16 = jnp.float32, jnp.bfloat16
    ids = ids_ref[...]
    named = jnp.zeros((local, rows), f32)
    for k in range(routes_ref.shape[0]):
        named = jnp.where(routes_ref[k : k + 1, :] == ids, 1.0, named)
    before = lax.broadcasted_iota(jnp.int32, (rows, rows), 0)
    after = lax.broadcasted_iota(jnp.int32, (rows, rows), 1)
    rank = matmul(named.astype(bf16), jnp.where(before < after, 1.0, 0.0).astype(bf16))
    lanes = weights_ref.shape[1]
    mine = jnp.where(lax.broadcasted_iota(jnp.int32, (local, lanes), 1) == ids, 1.0, 0.0)
    weights = lax.dot_general(
        mine,
        weights_ref[...],
        (((1,), (1,)), ((), ())),
        precision=lax.Precision.HIGHEST,
        preferred_element_type=f32,
    )
    slots = lax.broadcasted_iota(jnp.int32, (CAP, rows), 0).astype(f32)
    picks = []
    for j in range(local):
        pick = jnp.where(slots == rank[j : j + 1, :], named[j : j + 1, :], 0.0)
        w_ref[0, j * CAP : (j + 1) * CAP, :] = jnp.sum(
            pick * weights[j : j + 1, :], axis=1, keepdims=True
        )
        picks.append(pick.astype(bf16))
    picks = jnp.concatenate(picks, axis=0)
    p_ref[0] = picks
    xr_ref[0] = matmul(picks, x_ref[...]).astype(bf16)
    gr_ref[0] = matmul(picks, g_ref[...]).astype(bf16)


def route_stage(groups, own_ids, routes_t, tokens, gradients, weights):
    local = own_ids.shape[0]
    rows, width = tokens.shape[0] // groups, tokens.shape[1]
    slots = local * CAP
    row_spec = pl.BlockSpec((rows, width), lambda b: (b, 0))
    slot_spec = pl.BlockSpec((1, slots, width), lambda b: (b, 0, 0))
    slot_shape = jax.ShapeDtypeStruct((groups, slots, width), jnp.bfloat16)
    lanes = weights.shape[1]
    return pl.pallas_call(
        route_kernel,
        grid=(groups,),
        in_specs=[
            pl.BlockSpec((local, 1), lambda b: (0, 0)),
            pl.BlockSpec((routes_t.shape[0], rows), lambda b: (0, b)),
            row_spec,
            row_spec,
            pl.BlockSpec((rows, lanes), lambda b: (b, 0)),
        ],
        out_specs=[
            slot_spec,
            slot_spec,
            pl.BlockSpec((1, slots, rows), lambda b: (b, 0, 0)),
            pl.BlockSpec((1, slots, 1), lambda b: (b, 0, 0)),
        ],
        out_shape=[
            slot_shape,
            slot_shape,
            jax.ShapeDtypeStruct((groups, slots, rows), jnp.bfloat16),
            jax.ShapeDtypeStruct((groups, slots, 1), jnp.float32),
        ],
        compiler_params=pltpu.CompilerParams(vmem_limit_bytes=VMEM_BYTES),
        name="route",
    )(own_ids[:, None], routes_t, tokens, gradients, weights)


MIX_LAGS = (1, 3, 5, 7)


def mix_kernel(groups, chunks, names, *refs):
    ref = Bag(zip(names, refs))
    deep = groups // PAIR
    bf16, f32 = jnp.bfloat16, jnp.float32
    link = Link(deep)
    link.greet(groups, "eyc")
    blocks, slots, rows = ref.b_picks.shape
    sub = ref.o_dsecond.shape[0]
    width = ref.i_tokens.shape[1]
    units = ref.i_shared.shape[0] // 3
    loads = [bring(ref.i_picks, ref.b_picks, ref.load.at[0])]
    loads.append(bring(ref.i_shared, ref.b_shared, ref.load.at[1]))

    def fetch(b, at):
        span = pl.ds(pl.multiple_of(b * rows, rows), rows)
        return (
            pltpu.make_async_copy(ref.i_tokens.at[span, :], ref.b_x.at[at], ref.fetch.at[at, 0]),
            pltpu.make_async_copy(ref.i_gradients.at[span, :], ref.b_g.at[at], ref.fetch.at[at, 1]),
        )

    for copy in fetch(0, 0):
        copy.start()
    many = len(chunks)
    work = [(True, *chunk) for chunk in chunks] + [(False, *chunk) for chunk in chunks[:-1]]

    def source_of(n):
        back, left, wide = work[n]
        source = ref.i_back if back else ref.i_produced
        return pltpu.make_async_copy(
            source.at[:, :, pl.ds(left, wide)],
            ref.b_source.at[turn_of[n], :, :, pl.ds(0, wide)],
            ref.pull.at[turn_of[n]],
        )

    has_source = [n != many - 1 for n in range(len(work))]
    order = [many - 1] + [n for n in range(len(work)) if has_source[n]]
    turn_of = {n: i % 2 for i, n in enumerate(order)}
    for load in loads:
        load.wait()
    ref.b_acc[...] = jnp.zeros(ref.b_acc.shape, f32)

    def block(b, carry):
        at = b % 2

        @pl.when(b + 1 < blocks)
        def _():
            for copy in fetch(b + 1, 1 - at):
                copy.start()

        for copy in fetch(b, at):
            copy.wait()
        row_inputs, cotangent = ref.b_x[at], ref.b_g[at]
        pre = matmul_nt(row_inputs, ref.b_shared[: 2 * units, :])
        gate_pre, up_pre = pre[:, :units], pre[:, units:]
        sigmoid_gate, hidden = swiglu(gate_pre, up_pre)
        dhidden = matmul_nt(cotangent, ref.b_shared[2 * units :, :])
        gate_grad, up_grad = swiglu_back(dhidden, gate_pre, up_pre, sigmoid_gate)
        both = jnp.concatenate([gate_grad, up_grad], axis=1)
        ref.b_hidden[b] = hidden
        ref.b_both[b] = both
        return carry

    def shared_gradients(b):
        at = b % 2
        if b + 1 < blocks:
            for copy in fetch(b + 1, 1 - at):
                copy.start()
        for copy in fetch(b, at):
            copy.wait()
        ref.b_acc[: 2 * units, :] += matmul_tn(ref.b_both[b], ref.b_x[at])
        ref.b_acc[2 * units :, :] += matmul_tn(ref.b_hidden[b], ref.b_g[at])

    source_of(order[1]).start()
    lax.fori_loop(0, blocks, block, 0)
    for copy in fetch(0, 0):
        copy.start()
    dw_lane = lax.broadcasted_iota(jnp.int32, (slots, chunks[-1][1]), 1)
    tasks = []

    def step_at(moment):
        for lag in MIX_LAGS:
            if 0 <= moment - lag < len(tasks):
                next(tasks[moment - lag], None)

    pending = [n for n in order if has_source[n]]
    for n in order:
        back, left, wide = work[n]
        if has_source[n]:
            pending.pop(0)
            if pending:
                source_of(pending[0]).start()
            source_of(n).wait()

        def one(b, carry, n=n, back=back, left=left, wide=wide):
            picks = ref.b_picks[b]
            if not has_source[n]:
                values = matmul_tn(
                    picks, jnp.where(dw_lane == ref.i_lanes[...], ref.i_dweights[b], 0.0).astype(bf16)
                )
            else:
                span = slice(left, left + wide)
                values = matmul_tn(picks, ref.b_source[turn_of[n], b, :, :wide])
                if back:
                    values += matmul(ref.b_both[b], ref.b_shared[: 2 * units, span])
                else:
                    values += matmul(ref.b_hidden[b], ref.b_shared[2 * units :, span])
            values = values.astype(bf16)
            for y in range(PAIR):
                for c in range(PAIR):
                    q = y * PAIR + c
                    piece = values[q * sub : (q + 1) * sub, :]
                    ref["p%d" % n][c, b * PAIR + y] = piece
            return carry

        lax.fori_loop(0, blocks, one, 0)
        result = ref.o_dsecond if back else ref.o_mixed
        task = device_total(
            link,
            n % 2,
            ref["p%d" % n].at[link.c],
            ref["p%d" % n].at[1 - link.c],
            [ref["f%d_%d" % (n, k)] for k in range(4)],
            result.at[:, pl.ds(left, wide)],
            ref.send.at[n],
            ref.arrive.at[n],
        )
        tasks += begun([task])
        step_at(len(tasks) - 1)
    share = -(-blocks // 4)
    for late in range(MIX_LAGS[-1]):
        step_at(len(order) + late)
        for b in range(late * share, min(blocks, (late + 1) * share)):
            shared_gradients(b)
        if late == 3:
            ref.b_grad[...] = ref.b_acc[...].astype(bf16)
            grad_out = bring(ref.b_grad, ref.o_shared, ref.load.at[0])
    link.drain()
    grad_out.wait()


def mix_bytes(groups, rows, slots, width):
    total = groups * rows * width * 2
    return 2 * total + 4 * rows * width * 2 * 2 + 2 * groups * max(rows, slots) * 512 * 2 * 2


def mix_stage(calls, groups, parts, picks, produced, back, dweights, lanes, tokens, gradients, shared):
    deep = groups // PAIR
    blocks, slots, rows = picks.shape
    width = tokens.shape[1]
    sub = rows // parts
    bf16, f32 = jnp.bfloat16, jnp.float32
    experts_wide = lanes[1]
    wide = min(512, width)
    chunks = [(left, wide) for left in range(0, width, wide)] + [(width, experts_wide)]
    inputs = Bag(
        i_picks=picks,
        i_produced=produced,
        i_back=back,
        i_dweights=dweights,
        i_lanes=lanes[0],
        i_tokens=tokens,
        i_gradients=gradients,
        i_shared=shared,
    )
    specs = [IN_VMEM if key in ("i_dweights", "i_lanes") else ANY for key in inputs]
    third = shared.shape[0] // 3
    scratch = Bag(
        b_picks=pltpu.VMEM(picks.shape, bf16),
        b_shared=pltpu.VMEM(shared.shape, bf16),
        b_x=pltpu.VMEM((2, rows, width), bf16),
        b_g=pltpu.VMEM((2, rows, width), bf16),
        b_acc=pltpu.VMEM(shared.shape, f32),
        b_grad=pltpu.VMEM(shared.shape, bf16),
        b_hidden=pltpu.VMEM((blocks, rows, third), bf16),
        b_both=pltpu.VMEM((blocks, rows, 2 * third), bf16),
        b_source=pltpu.VMEM((2, blocks, slots, wide), bf16),
        load=DMA((2,)),
        fetch=DMA((2, 2)),
        pull=DMA((2,)),
        send=DMA((2 * len(chunks), total_hops(deep))),
        arrive=DMA((2 * len(chunks), total_hops(deep))),
    )
    for n, (_, columns) in enumerate(chunks + chunks[:-1]):
        scratch["p%d" % n] = pltpu.VMEM((PAIR, blocks * PAIR, sub, columns), bf16)
        for k, buffer in enumerate(total_buffers(deep, sub, columns)):
            scratch["f%d_%d" % (n, k)] = buffer
    names = list(inputs) + ["o_dsecond", "o_mixed", "o_shared"] + list(scratch)
    return pl.pallas_call(
        functools.partial(mix_kernel, groups, tuple(chunks), tuple(names)),
        in_specs=specs,
        out_specs=[IN_VMEM, IN_VMEM, ANY],
        out_shape=[
            jax.ShapeDtypeStruct((sub, width + experts_wide), f32),
            jax.ShapeDtypeStruct((sub, width), f32),
            jax.ShapeDtypeStruct(shared.shape, bf16),
        ],
        scratch_shapes=list(scratch.values()),
        compiler_params=calls.params(),
        name="mix",
    )(*inputs.values())


def advance(tasks, count=1):
    for _ in range(count):
        for task in tasks:
            next(task, None)


def begun(tasks):
    return [task for task in tasks if next(task, run) is not run]


def tensor_total(link, partial, from_beside, give, from_across, result, send, arrive):
    y, c = link.y, link.c

    def beside():
        return pltpu.make_async_remote_copy(
            src_ref=partial.at[:, 1 - c],
            dst_ref=from_beside,
            send_sem=send.at[0],
            recv_sem=arrive.at[0],
            device_id=link.peer("c"),
            device_id_type=MESH,
        )

    def across():
        return pltpu.make_async_remote_copy(
            src_ref=give,
            dst_ref=from_across,
            send_sem=send.at[1],
            recv_sem=arrive.at[1],
            device_id=link.peer("y"),
            device_id_type=MESH,
        )

    link.emit(beside)
    yield
    arrived(from_beside, arrive.at[0])
    give[...] = partial[1 - y, c] + from_beside[1 - y]
    link.emit(across)
    result[...] = partial[y, c].astype(jnp.float32) + from_beside[y].astype(jnp.float32)
    yield
    arrived(from_across, arrive.at[1])
    result[...] = result[...] + from_across[...].astype(jnp.float32)


def expert_total(link, axis, grad, from_twin, from_deep, result, send, arrive):
    deep, z, x = link.deep, link.z, link.x
    size = result.shape[axis]

    def target(k):
        return (z + k) % deep

    def to_twin(k):
        return pltpu.make_async_remote_copy(
            src_ref=slot(grad, axis, target(k) * PAIR + 1 - x, size),
            dst_ref=from_twin.at[k],
            send_sem=send.at[k],
            recv_sem=arrive.at[k],
            device_id=link.peer("x"),
            device_id_type=MESH,
        )

    def to_deep(k):
        return pltpu.make_async_remote_copy(
            src_ref=from_twin.at[k],
            dst_ref=from_deep.at[k - 1],
            send_sem=send.at[deep + k],
            recv_sem=arrive.at[deep + k],
            device_id=link.at_z(target(k)),
            device_id_type=MESH,
        )

    ks = list(range(1, deep)) + [0]
    for k in ks:
        link.emit(functools.partial(to_twin, k))
    for k in ks[:-1]:
        yield
        arrived(from_twin.at[k], arrive.at[k])
        mine = slot(grad, axis, target(k) * PAIR + x, size)
        from_twin[k] = from_twin[k] + mine[...]
        link.emit(functools.partial(to_deep, k))
    yield
    arrived(from_twin.at[0], arrive.at[0])
    total = slot(grad, axis, z * PAIR + x, size)[...].astype(jnp.float32)
    result[...] = total + from_twin[0].astype(jnp.float32)
    for k in range(1, deep):
        yield
        arrived(from_deep.at[k - 1], arrive.at[deep + k])
        result[...] = result[...] + from_deep[k - 1].astype(jnp.float32)


def back_kernel(groups, sizes, reduced, names, *refs):
    ref = Bag(zip(names, refs))
    deep = groups // PAIR
    parts = PAIR * PAIR
    link = Link(deep)
    part = link.part
    bf16, f32 = jnp.bfloat16, jnp.float32
    link.greet(groups, "eyc")
    loading = {}
    for n, name in enumerate(n[2:] for n in names if n[:2] == "h_"):
        loading[name] = bring(ref["h_" + name], ref["l_" + name], ref.load.at[n])
    left = []

    def leave(name, source=None):
        source = ref["b_" + name] if source is None else source
        left.append(bring(source, ref["o_" + name], ref.leave.at[len(left)]))

    def ready(*which):
        for name in which:
            if name in loading:
                loading.pop(name).wait()
        return [ref["l_" + name] for name in which]

    rows_send, rows_arrive = ref.rows_send, ref.rows_arrive
    used = [0]

    def over_tensor(source, target, axis, size):
        row = used[0]
        used[0] += 1

        def home_of(sz, sx, sy, sc):
            return slot(target, axis, sy * PAIR + sc, size)

        n = len(placed)
        placed.append(bring(source, home_of(link.z, link.x, link.y, link.c), ref.place.at[n]))
        return spread(link, "yc", source, home_of, rows_send.at[row], rows_arrive.at[row])

    placed = []
    totals = {name: i for i, (name, _) in enumerate(reduced)}
    axis_of = dict(reduced)

    def over_expert(name):
        if name not in totals:
            leave(name)
            return
        i = totals[name]
        tasks = begun(
            [
                expert_total(
                    link,
                    axis_of[name],
                    ref["b_" + name],
                    ref["t_" + name],
                    ref["d_" + name],
                    ref["r_" + name],
                    ref.send.at[i],
                    ref.arrive.at[i],
                )
            ]
        )
        queue.extend([task, deep - 1] for task in tasks)

    queue, finishing = [], []

    def pump(count):
        while count and queue:
            entry = queue[0]
            next(entry[0], None)
            entry[1] -= 1
            count -= 1
            if not entry[1]:
                finishing.append(queue.pop(0)[0])

    shared_tasks = []
    if SHARED in axis_of:
        wide = ref.o_shared.shape[2]
        source = ref.i_shared
        shared_tasks = begun(
            [
                shuffle(
                    link,
                    groups,
                    lambda e: source.at[:, pl.ds(pl.multiple_of(e * wide, LANES), wide)],
                    lambda e: ref.o_shared.at[e],
                    ref.shared_send,
                    ref.shared_arrive,
                )
            ]
        )
        loading[OWN_SHARED] = bring(
            source.at[:, pl.ds(pl.multiple_of(link.me * wide, LANES), wide)],
            ref.k_shared,
            ref.place.at[len(placed)],
        )
        placed.append(None)

    sub, width = ref.i_middle.shape
    experts = ref.i_router.shape[0]
    middle = ref.i_middle[...]
    norms = [ref.i_norms[i : i + 1, : size * groups] for i, size in enumerate(sizes)]
    ffn_gain = norms[1]
    inverse = lax.rsqrt(jnp.mean(middle * middle, axis=-1, keepdims=True) + EPSILON)
    normed = middle * inverse
    chosen = ref.i_chosen[:, :experts]
    dweights = ref.i_dsecond[:, width : width + experts]
    total = jnp.sum(chosen, axis=-1, keepdims=True)
    dchosen = (
        ROUTE_SCALE
        / total
        * (dweights - jnp.sum(dweights * chosen, axis=-1, keepdims=True) / total)
    )
    dlogits = (dchosen * chosen * (1.0 - chosen)).astype(bf16)
    dsecond = ref.i_dsecond[:, :width] + matmul(dlogits, ref.i_router[...])
    scaled = dsecond * ffn_gain
    start = pl.multiple_of(part * sub, sub)
    gradient = ref.i_out_grad[pl.ds(start, sub), :].astype(f32)
    middle_grad = gradient + inverse * (
        scaled - normed * jnp.mean(scaled * normed, axis=-1, keepdims=True)
    )
    ref.b_middle_grad[...] = middle_grad
    ref.b_grad_rows[...] = middle_grad.astype(bf16)
    tensor_tasks = begun([over_tensor(ref.b_grad_rows, ref.b_attention_grad, 0, sub)])
    ref.b_block_rows[...] = (middle + ref.i_mixed[...]).astype(bf16)
    ref.b_router[...] = matmul_tn(dlogits, (normed * ffn_gain).astype(bf16)).astype(bf16)
    over_expert(ROUTER)
    gain_sums = {1: jnp.sum(dsecond * normed, axis=0, keepdims=True)}

    run(tensor_tasks)
    block_tasks = begun([over_tensor(ref.b_block_rows, ref.o_block_out, 0, sub)])
    placed[1 if SHARED in axis_of else 0].wait()
    placed[1 if SHARED in axis_of else 0] = None

    attended, out_proj = ready(ATTENDED, OUT_PROJ)
    attention_grad = ref.b_attention_grad
    for at in range(0, attended.shape[1], 256):
        ref.b_out_proj[at : at + 256, :] = matmul_tn(
            attended[:, at : at + 256], attention_grad[...]
        ).astype(bf16)
    over_expert(OUT_PROJ)
    ref.b_attended_grad[...] = matmul_nt(attention_grad[...], out_proj[...]).astype(bf16)

    queries, keys, values = ready(QUERIES, KEYS, VALUES)
    heads, row_count, head_width = queries.shape
    cosine, sinusoid = ref.i_cosine[...], ref.i_sinusoid[...]
    dkey_rope = jnp.zeros((row_count, LANES), f32)
    scale = head_width ** (-0.5)
    filler = jnp.zeros((row_count, LANES - ROPE), f32)
    for h in range(heads):
        scores = matmul_nt(queries[h], keys[h]) * scale
        scores = jnp.where(ref.i_allowed[...] > 0, scores, -1e30)
        powers = jnp.exp(scores - jnp.max(scores, axis=-1, keepdims=True))
        probs = powers / jnp.sum(powers, axis=-1, keepdims=True)
        attended_grad = ref.b_attended_grad[:, h * VD : (h + 1) * VD]
        dvalues = matmul_tn(probs.astype(bf16), attended_grad)
        dprobs = matmul_nt(attended_grad, values[h])
        delta = jnp.sum(probs * dprobs, axis=-1, keepdims=True)
        dscores = (probs * (dprobs - delta) * scale).astype(bf16)
        dquery = matmul(dscores, keys[h])
        dkeys = matmul_tn(dscores, queries[h])
        rope = turn(jnp.concatenate([dquery[:, NOPE:], filler], axis=1), cosine, -sinusoid)
        pair = jnp.concatenate(
            [dquery[:, :NOPE], rope, jnp.zeros((row_count, LANES), f32)], axis=1
        )
        if h % 2 == 0:
            held = pair
        else:
            held = held + pltpu.roll(pair, head_width, 1)
            ref.b_dquery[:, (h - 1) * head_width : (h + 1) * head_width] = held.astype(bf16)
        dkey_rope = dkey_rope + jnp.concatenate([dkeys[:, NOPE:], filler], axis=1)
        base = h * (NOPE + VD)
        ref.b_dkeyval[:, base : base + NOPE] = dkeys[:, :NOPE].astype(bf16)
        ref.b_dkeyval[:, base + NOPE : base + NOPE + VD] = dvalues.astype(bf16)
        if h:
            pump(1)
    dkey_rope = turn(dkey_rope, cosine, -sinusoid)

    query_n, latent_n, query_up, latent_up = ready(QUERY_N, LATENT_N, QUERY_UP, LATENT_UP)
    query_rank, latent_rank = query_n.shape[1], latent_n.shape[1]
    for at in range(0, query_rank, 256):
        ref.b_query_up[at : at + 256, :] = matmul_tn(
            query_n[:, at : at + 256], ref.b_dquery[...]
        ).astype(bf16)
    over_expert(QUERY_UP)
    for at in range(0, latent_rank, 256):
        ref.b_latent_up[at : at + 256, :] = matmul_tn(
            latent_n[:, at : at + 256], ref.b_dkeyval[...]
        ).astype(bf16)
    over_expert(LATENT_UP)
    partial = ref.b_heads_partial
    lead = query_rank + latent_rank
    for quarter in range(parts):
        span = slice(quarter * sub, (quarter + 1) * sub)
        at = (quarter // PAIR, quarter % PAIR)
        partial[(*at, slice(None), slice(0, query_rank))] = matmul_nt(
            ref.b_dquery[span, :], query_up[...]
        ).astype(bf16)
        partial[(*at, slice(None), slice(query_rank, lead))] = matmul_nt(
            ref.b_dkeyval[span, :], latent_up[...]
        ).astype(bf16)
        partial[(*at, slice(None), slice(lead, lead + LANES))] = dkey_rope[span, :].astype(bf16)
    sum_tasks = begun(
        [
            tensor_total(
                link,
                partial,
                ref.b_heads_beside,
                ref.b_heads_give,
                ref.b_heads_across,
                ref.b_heads_rows,
                ref.sum_send.at[0],
                ref.sum_arrive.at[0],
            )
        ]
    )
    pump(1)
    run(sum_tasks)

    heads_rows = ref.b_heads_rows
    (query_lat, latent_t) = ready(QUERY_LAT, LATENT_T)

    def norm_back(values, gain, cotangent):
        inverse = lax.rsqrt(jnp.mean(values * values, axis=-1, keepdims=True) + EPSILON)
        normed = values * inverse
        scaled = cotangent * gain
        back = inverse * (scaled - normed * jnp.mean(scaled * normed, axis=-1, keepdims=True))
        return (back, jnp.sum(cotangent * normed, axis=0, keepdims=True))

    query_rows = query_lat[pl.ds(start, sub), :].astype(f32)
    back, gain_sums[2] = norm_back(query_rows, norms[2], heads_rows[:, :query_rank])
    ref.b_query_rows[...] = back.astype(bf16)
    ref.b_latent_block[...] = latent_t[:latent_rank, :].astype(f32).T
    latent_rows = ref.b_latent_block[pl.ds(start, sub), :]
    back, gain_sums[3] = norm_back(
        latent_rows, norms[3], heads_rows[:, query_rank:lead]
    )
    ref.b_latent_rows[:, :latent_rank] = back.astype(bf16)
    ref.b_latent_rows[:, latent_rank:] = heads_rows[:, lead:].astype(bf16)
    own = len(placed)
    tensor_tasks = begun(
        [
            over_tensor(ref.b_query_rows, ref.b_dquery_lat, 0, sub),
            over_tensor(ref.b_latent_rows, ref.b_dlatent_all, 0, sub),
        ]
    )
    pump(1)
    run(tensor_tasks)
    for n in (own, own + 1):
        placed[n].wait()
        placed[n] = None

    first, query_down, latent_down = ready(FIRST, QUERY_DOWN, LATENT_DOWN)
    query_cut, latent_cut = query_down.shape[1], latent_down.shape[0]
    dquery_lat = ref.b_dquery_lat[
        :, pl.ds(pl.multiple_of(part * query_cut, LANES), query_cut)
    ]
    ref.b_dlatent_t[...] = ref.b_dlatent_all[...].astype(f32).T
    dlatent_t = ref.b_dlatent_t[
        pl.ds(pl.multiple_of(part * latent_cut, 8), latent_cut), :
    ].astype(bf16)
    for at in range(0, width, 256):
        ref.b_query_down[at : at + 256, :] = matmul_tn(
            first[:, at : at + 256], dquery_lat
        ).astype(bf16)
    over_expert(QUERY_DOWN)
    for at in range(0, width, 512):
        ref.b_latent_down[:, at : at + 512] = matmul(dlatent_t, first[:, at : at + 512]).astype(
            bf16
        )
    over_expert(LATENT_DOWN)
    pump(1)
    partial = ref.b_first_partial
    for quarter in range(parts):
        span = slice(quarter * sub, (quarter + 1) * sub)
        partial[quarter // PAIR, quarter % PAIR] = (
            matmul_nt(dquery_lat[span], query_down[...])
            + matmul_tn(dlatent_t[:, span], latent_down[...])
        ).astype(bf16)
    sum_tasks = begun(
        [
            tensor_total(
                link,
                partial,
                ref.b_first_beside,
                ref.b_first_give,
                ref.b_first_across,
                ref.b_first_rows,
                ref.sum_send.at[1],
                ref.sum_arrive.at[1],
            )
        ]
    )
    pump(1)
    run(sum_tasks)
    residual = ref.i_block[pl.ds(start, sub), :].astype(f32)
    back, gain_sums[0] = norm_back(
        residual, norms[0], ref.b_first_rows[...]
    )
    ref.b_input_rows[...] = (ref.b_middle_grad[...] + back).astype(bf16)
    input_tasks = begun([over_tensor(ref.b_input_rows, ref.o_input_grad, 0, sub)])
    wide = ref.b_gains.shape[1]
    for i, size in enumerate(sizes):
        sums = jnp.broadcast_to(gain_sums[i], (8, gain_sums[i].shape[1]))
        span = sums.shape[1]
        if span < wide:
            sums = jnp.concatenate([sums, jnp.zeros((8, wide - span), f32)], axis=1)
            span = wide
        for e in range(groups):
            moved = pltpu.roll(sums, span - e * size, 1) if e else sums
            ref.b_gains[e * 8 + i : e * 8 + i + 1, :] = moved[:1, :wide]
    for e in range(groups):
        ref.b_gains[e * 8 + len(sizes) : e * 8 + 8, :] = jnp.zeros((8 - len(sizes), wide), f32)
    over_expert(GAINS)
    pump(len(queue) * deep)
    run(finishing)

    finished = ("o_query_down", "o_latent_down")
    finals = []
    for name, axis in ((QUERY_DOWN, 1), (LATENT_DOWN, 0), (ROUTER, 0), (GAINS, 0)):
        if name not in totals:
            continue
        share = ref["s_" + name]
        whole = ref["o_" + name] if "o_" + name in finished else ref["g_" + name]
        share[...] = ref["r_" + name][...].astype(share.dtype)
        finals.append(over_tensor(share, whole, axis, share.shape[axis]))
    finals = begun(finals)
    for name in (OUT_PROJ, QUERY_UP, LATENT_UP):
        if name in totals:
            leave(name, ref["r_" + name])
    if SHARED in axis_of:
        loading.pop(OWN_SHARED).wait()
        left.append(
            bring(ref.k_shared, ref.o_shared.at[link.me], ref.leave.at[len(left)])
        )
    run(finals)
    for move in placed:
        if move is not None:
            move.wait()
    for name in (ROUTER, GAINS):
        if name in totals:
            size = ref["s_" + name].shape[0]
            total = ref["g_" + name][:size, :]
            for t in range(1, parts):
                total = total + ref["g_" + name][t * size : (t + 1) * size, :]
            ref["f_" + name][...] = total
            leave(name, ref["f_" + name])
    run(block_tasks + input_tasks + shared_tasks)
    link.drain()
    for move in left:
        move.wait()


def back_stage(calls, groups, parts, sizes, held, small, grad_shared):
    deep = groups // PAIR
    bf16, f32 = jnp.bfloat16, jnp.float32
    rows, width = small.block.shape
    sub = rows // parts
    query_rank, latent_rank = held.query_n.shape[1], held.latent_n.shape[1]
    heads, _, head_width = held.queries.shape
    query_cut, latent_cut = held.query_down.shape[1], held.latent_down.shape[0]
    experts = small.router.shape[0]
    gain_wide = -(-max(sizes) // LANES) * LANES
    lead = query_rank + latent_rank + LANES
    half = parts // PAIR
    full = Bag(
        out_proj=(held.out_proj.shape, 1, bf16),
        query_up=(held.query_up.shape, 0, bf16),
        latent_up=(held.latent_up.shape, 0, bf16),
        query_down=((width, query_cut), 0, bf16),
        latent_down=((latent_cut, width), 1, bf16),
        router=((experts, width), 1, bf16),
        gains=((groups * 8, gain_wide), 0, f32),
    )
    reduced, pieces = [], {}
    for name, (shape, axis, dtype) in full.items():
        piece = list(shape)
        piece[axis] //= groups
        if aligned(piece[axis], 1) or axis == 0:
            reduced.append((name, axis))
            pieces[name] = tuple(piece)
    buffers = Bag(
        middle_grad=((sub, width), f32),
        grad_rows=((sub, width), bf16),
        block_rows=((sub, width), bf16),
        attention_grad=((rows, width), bf16),
        attended_grad=(held.attended.shape, bf16),
        dquery=((rows, heads * head_width), bf16),
        dkeyval=((rows, heads * (NOPE + VD)), bf16),
        heads_partial=((half, PAIR, sub, lead), bf16),
        heads_beside=((half, sub, lead), bf16),
        heads_give=((sub, lead), bf16),
        heads_across=((sub, lead), bf16),
        heads_rows=((sub, lead), f32),
        query_rows=((sub, query_rank), bf16),
        latent_rows=((sub, latent_rank + LANES), bf16),
        latent_block=((rows, latent_rank), f32),
        dquery_lat=((rows, query_rank), bf16),
        dlatent_all=((rows, latent_rank + LANES), bf16),
        dlatent_t=((latent_rank + LANES, rows), f32),
        first_partial=((half, PAIR, sub, width), bf16),
        first_beside=((half, sub, width), bf16),
        first_give=((sub, width), bf16),
        first_across=((sub, width), bf16),
        first_rows=((sub, width), f32),
        input_rows=((sub, width), bf16),
    )
    for name, (shape, _, dtype) in full.items():
        buffers[name] = (shape, dtype)
    scratch = Bag(("b_" + name, pltpu.VMEM(*spec)) for name, spec in buffers.items())
    for name, array in held.items():
        scratch["l_" + name] = pltpu.VMEM(array.shape, array.dtype)
    outs = Bag(block_out=((rows, width), bf16), input_grad=((rows, width), bf16))
    for name, (shape, axis, dtype) in full.items():
        if name not in pieces:
            outs[name] = (shape, dtype)
            continue
        piece = pieces[name]
        scratch["t_" + name] = pltpu.VMEM((deep, *piece), dtype)
        scratch["d_" + name] = pltpu.VMEM((deep - 1, *piece), dtype)
        scratch["r_" + name] = pltpu.VMEM(piece, f32)
        outs[name] = (piece, f32)
        if name in (QUERY_DOWN, LATENT_DOWN, ROUTER, GAINS):
            kind = bf16 if name in (QUERY_DOWN, LATENT_DOWN) else f32
            along = 1 if name == QUERY_DOWN else 0
            whole = list(piece)
            whole[along] *= parts
            scratch["s_" + name] = pltpu.VMEM(piece, kind)
            if name in (QUERY_DOWN, LATENT_DOWN):
                outs[name] = (tuple(whole), bf16)
            else:
                scratch["g_" + name] = pltpu.VMEM(tuple(whole), kind)
                scratch["f_" + name] = pltpu.VMEM(piece, f32)
    share = grad_shared.shape[1] // groups
    inputs = {"i_" + name: array for name, array in small.items()}
    specs = [IN_VMEM] * len(small)
    if aligned(share, 1):
        reduced.append((SHARED, 1))
        inputs["i_shared"] = grad_shared
        specs.append(ANY)
        outs.shared = ((groups, grad_shared.shape[0], share), bf16)
        scratch.k_shared = pltpu.VMEM((grad_shared.shape[0], share), bf16)
        scratch.shared_send = scratch.shared_arrive = DMA((groups,))
    inputs |= {"h_" + name: array for name, array in held.items()}
    specs += [ANY] * len(held)
    scratch.load = DMA((len(held),))
    scratch.leave = DMA((len(outs) + 1,))
    scratch.place = DMA((12,))
    scratch.rows_send = scratch.rows_arrive = DMA((12, 8))
    scratch.send = scratch.arrive = DMA((len(full), 2 * deep))
    scratch.sum_send = scratch.sum_arrive = DMA((2, 2))
    names = list(inputs) + ["o_" + name for name in outs] + list(scratch)
    reduced = [entry for entry in reduced]
    results = pl.pallas_call(
        functools.partial(back_kernel, groups, tuple(sizes), tuple(reduced), tuple(names)),
        in_specs=specs,
        out_specs=[ANY] * len(outs),
        out_shape=[jax.ShapeDtypeStruct(*spec) for spec in outs.values()],
        scratch_shapes=list(scratch.values()),
        compiler_params=calls.params(),
        name="back",
    )(*inputs.values())
    results = Bag(zip(outs, results))
    for name, (shape, axis, dtype) in full.items():
        if name not in pieces:
            results[name] = scatter_sum(results[name], EXPERT, axis)
            if name == LATENT_DOWN:
                results[name] = gather(results[name].astype(bf16), TENSOR, 0).astype(f32)
            if name == ROUTER:
                results[name] = lax.psum(results[name].astype(bf16), TENSOR).astype(f32)
    if SHARED not in results:
        split = grad_shared.reshape(grad_shared.shape[0], groups, share).transpose(1, 0, 2)
        results.shared = lax.all_to_all(
            split, EXPERT, split_axis=0, concat_axis=0, tiled=True
        )
    return results


ALL = (EXPERT, TENSOR)


def gather(values, axes, dimension):
    return lax.all_gather(values, axes, axis=dimension, tiled=True)


def scatter_sum(values, axes, dimension):
    return lax.psum_scatter(
        values.astype(jnp.bfloat16), axes, scatter_dimension=dimension, tiled=True
    ).astype(jnp.float32)


def aligned(size, axis):
    return size % LANES == 0 if axis else size % 16 == 0


def ready_items(items, part):
    result = []
    for name, array, axis, cut, over, orders, home in items:
        if axis == 1 and array.shape[-1] % LANES:
            if over == SHUFFLE:
                array = lax.all_to_all(array, EXPERT, split_axis=0, concat_axis=0, tiled=True)
                array = array.transpose(1, 0, 2).reshape(array.shape[1], -1)
            else:
                if cut is not None:
                    array = lax.dynamic_slice_in_dim(array, part * cut[1], cut[1], axis=cut[0])
                array = gather(array, EXPERT, axis)
            cut, over, orders, home = None, READY, (), VMEM_
        result.append((name, array, axis, cut, over, orders, home))
    return result


def body(
    calls,
    block_in,
    attention_gain,
    query_down,
    query_gain,
    query_up,
    latent_down,
    latent_gain,
    latent_up,
    out_proj,
    ffn_gain,
    router,
    shared_gate,
    shared_up,
    shared_down,
    expert_gate,
    expert_up,
    expert_down,
    doc_lengths,
    routes,
    out_grad,
):
    groups = lax.axis_size(EXPERT)
    parts = lax.axis_size(TENSOR)
    me = lax.axis_index(EXPERT)
    part = lax.axis_index(TENSOR)
    row_count, width = block_in.shape
    top = routes.shape[1]
    local = expert_gate.shape[0]
    experts = local * groups

    all_gains = (attention_gain, ffn_gain, query_gain, latent_gain)
    gain_sizes = [g.shape[0] for g in all_gains]
    gain_wide = -(-max(gain_sizes) // LANES) * LANES
    gains = jnp.stack(
        [jnp.pad(g.astype(jnp.float32), (0, gain_wide - g.shape[0])) for g in all_gains]
    )
    gains = jnp.pad(gains, ((0, 8 - len(all_gains)), (0, 0)))
    routes_pad = jnp.pad(routes.T, ((0, -top % 8), (0, 0)), constant_values=-1)
    shared = jnp.stack([shared_gate.T, shared_up.T, shared_down])
    shared_units = shared.shape[1] // groups
    shared = shared.reshape(3, groups, shared_units, -1).transpose(1, 0, 2, 3)
    shared = shared.reshape(groups, 3 * shared_units, -1)
    query_cut = query_down.shape[1] // parts
    latent_cut = latent_down.shape[1] // parts
    allowed, cosine, sinusoid = layout(doc_lengths[0], row_count)
    allowed = allowed.astype(jnp.float32)
    tables = [
        jnp.pad(jnp.concatenate(pair, axis=1), ((0, 0), (0, LANES - ROPE)))
        for pair in ((cosine, cosine), (-sinusoid, sinusoid))
    ]
    items = [
        (GAINS, gains, 0, None, EXPERT, ("e",), VMEM_),
        (QUERY_DOWN, query_down, 0, (1, query_cut), EXPERT, ("zx",), VMEM_),
        (LATENT_DOWN, latent_down.T, 1, (0, latent_cut), EXPERT, ("zx",), VMEM_),
        (QUERY_UP, query_up, 0, None, EXPERT, ("zx",), VMEM_),
        (LATENT_UP, latent_up, 0, None, EXPERT, ("zx",), VMEM_),
        (OUT_PROJ, out_proj, 1, None, EXPERT, ("zx",), VMEM_),
        (ROUTER, router.T, 1, None, EXPERT, ("zx",), VMEM_),
        (ROUTES, routes_pad, 1, None, EXPERT, ("e",), "hbm"),
        (SHARED, shared, 1, None, SHUFFLE, (), "hbm"),
        (OUT_GRAD, out_grad, 0, (0, row_count // parts), "all", (ZXYC, "xzyc"), "hbm"),
    ]
    front = front_stage(
        calls,
        groups,
        parts,
        gain_sizes,
        ready_items(items, part),
        block_in,
        routes,
        allowed,
        *tables,
    )
    router_t = front.router
    shared = front.shared
    tokens, gradients = front.tokens, front.out_grad
    lane_pad = -experts % LANES
    own_ids = me * local + jnp.arange(local, dtype=jnp.int32)
    expert_rows, expert_grads, picks, slot_weights = route_stage(
        groups, own_ids, front.routes, tokens, gradients, front.weights
    )
    slot_shape = (groups, local, CAP)
    produced, back_rows, slot_dweights, grad_gate, grad_up, grad_down = expert_stage(
        expert_rows.reshape(*slot_shape, width),
        expert_grads.reshape(*slot_shape, width),
        slot_weights.reshape(*slot_shape, 1),
        expert_gate.transpose(0, 2, 1),
        expert_up.transpose(0, 2, 1),
        expert_down,
    )
    slots = local * CAP
    produced = produced.reshape(groups, slots, width)
    back_rows = back_rows.reshape(groups, slots, width)
    slot_dweights = slot_dweights.reshape(groups, slots, 1)
    slot_lanes = jnp.repeat(own_ids, CAP)[:, None]
    if mix_bytes(groups, row_count, slots, width) < 40 * 2**20:
        dsecond, mixed, grad_shared = mix_stage(
            calls,
            groups,
            parts,
            picks,
            produced,
            back_rows,
            slot_dweights,
            (slot_lanes, experts + lane_pad),
            tokens,
            gradients,
            shared,
        )
    else:
        lane_ids = jnp.arange(experts + lane_pad, dtype=jnp.int32)
        spread_out = jnp.where(slot_lanes == lane_ids[None, :], slot_dweights, 0.0)
        mixed_part, dsecond_part, grad_shared = combine_stage(
            picks,
            produced,
            back_rows,
            spread_out.astype(jnp.bfloat16),
            tokens.reshape(groups, row_count, width),
            gradients.reshape(groups, row_count, width),
            shared.reshape(3, shared_units, width),
        )
        grad_shared = grad_shared.astype(jnp.bfloat16).reshape(3 * shared_units, width)
        dsecond, mixed = sum_all(
            calls,
            groups,
            parts,
            (
                dsecond_part.reshape(-1, width + experts + lane_pad),
                mixed_part.reshape(-1, width),
            ),
        )
    held = Bag(
        (name, front[name])
        for name in (
            ATTENDED,
            OUT_PROJ,
            QUERIES,
            KEYS,
            VALUES,
            QUERY_N,
            LATENT_N,
            QUERY_UP,
            LATENT_UP,
            QUERY_LAT,
            LATENT_T,
            FIRST,
            QUERY_DOWN,
            LATENT_DOWN,
        )
    )
    small = Bag(
        dsecond=dsecond,
        mixed=mixed,
        middle=front.middle,
        chosen=front.chosen,
        router=router_t,
        out_grad=out_grad,
        block=block_in,
        allowed=allowed,
        cosine=tables[0],
        sinusoid=tables[1],
        norms=front.norms,
    )
    back = back_stage(calls, groups, parts, gain_sizes, held, small, grad_shared)
    grad_shared = back.shared.reshape(groups, 3, shared_units, -1).transpose(1, 0, 2, 3)
    grad_shared = grad_shared.astype(jnp.float32).reshape(3, groups * shared_units, -1)
    grad_gains = [back.gains[i, :size] for i, size in enumerate(gain_sizes)]

    return (
        back.block_out,
        back.input_grad,
        grad_gains[0],
        back.query_down.astype(jnp.float32),
        grad_gains[2],
        back.query_up,
        back.latent_down.T.astype(jnp.float32),
        grad_gains[3],
        back.latent_up,
        back.out_proj,
        grad_gains[1],
        back.router.T,
        grad_shared[0].T,
        grad_shared[1].T,
        grad_shared[2],
        grad_gate.transpose(0, 2, 1),
        grad_up.transpose(0, 2, 1),
        grad_down,
    )


def solution(mesh):
    placed = (
        P(EXPERT, None),
        P(EXPERT),
        P(EXPERT, None),
        P(EXPERT),
        P(EXPERT, TENSOR),
        P(EXPERT, None),
        P(EXPERT),
        P(EXPERT, TENSOR),
        P(TENSOR, EXPERT),
        P(EXPERT),
        P(EXPERT, None),
        P(EXPERT, TENSOR),
        P(EXPERT, TENSOR),
        P(TENSOR, EXPERT),
        P(EXPERT, None, TENSOR),
        P(EXPERT, None, TENSOR),
        P(EXPERT, TENSOR, None),
        P(EXPERT, None),
        P(EXPERT, None),
        P(EXPERT, None),
    )
    return jax.shard_map(
        functools.partial(body, Calls()),
        mesh=mesh,
        in_specs=placed,
        out_specs=(
            P(EXPERT, None),
            P(EXPERT, None),
            P(EXPERT),
            P(EXPERT, None),
            P(EXPERT),
            P(EXPERT, TENSOR),
            P(EXPERT, None),
            P(EXPERT),
            P(EXPERT, TENSOR),
            P(TENSOR, EXPERT),
            P(EXPERT),
            P(EXPERT, None),
            P(EXPERT, TENSOR),
            P(EXPERT, TENSOR),
            P(TENSOR, EXPERT),
            P(EXPERT, None, TENSOR),
            P(EXPERT, None, TENSOR),
            P(EXPERT, TENSOR, None),
        ),
        check_vma=False,
    )
```

```python
import functools
import math

import jax
import jax.numpy as jnp
from jax import lax
from jax.experimental import pallas as pl
from jax.experimental.pallas import tpu as pltpu
from jax.sharding import PartitionSpec as P

NOPE = 128
ROPE = 64
VD = 128
CAP = 32
LANES = 128
VMEM_BYTES = 60 * 2**20

EPSILON = 1e-06
ROPE_BASE = 50000.0
ROUTE_SCALE = 2.446

ATTENDED = "attended"
EXPERT = "expert"
FIRST = "first"
GAINS = "gains"
KEYS = "keys"
LATENT_DOWN = "latent_down"
LATENT_N = "latent_n"
LATENT_T = "latent_t"
LATENT_UP = "latent_up"
OUT_GRAD = "out_grad"
OUT_PROJ = "out_proj"
OWN_SHARED = "own_shared"
QUERIES = "queries"
QUERY_DOWN = "query_down"
QUERY_LAT = "query_lat"
QUERY_N = "query_n"
QUERY_UP = "query_up"
READY = "ready"
ROUTER = "router"
ROUTES = "routes"
SHARED = "shared"
SHUFFLE = "shuffle"
TENSOR = "tensor"
TOKENS = "tokens"
VALUES = "values"
VMEM_ = "vmem"
WEIGHTS = "weights"
ZXYC = "zxyc"


def matmul(left, right):
    return jnp.dot(left, right, preferred_element_type=jnp.float32)


def contract(form, left, right):
    return jnp.einsum(form, left, right, preferred_element_type=jnp.float32)


def matmul_nt(left, right):
    return lax.dot_general(left, right, (((1,), (1,)), ((), ())), preferred_element_type=jnp.float32)


def matmul_tn(left, right):
    return lax.dot_general(left, right, (((0,), (0,)), ((), ())), preferred_element_type=jnp.float32)


def layout(lengths, row_count):
    doc_count = lengths.shape[0]
    doc_ends = jnp.cumsum(lengths)
    starts = doc_ends - lengths
    row_index = jnp.arange(row_count, dtype=jnp.int32)
    doc_ids = jnp.sum((row_index[:, None] >= doc_ends[None, :]).astype(jnp.int32), axis=1)
    owners = doc_ids[:, None] == jnp.arange(doc_count, dtype=jnp.int32)[None, :]
    first_row = jnp.sum(jnp.where(owners, starts[None, :], 0), axis=1)
    positions = (row_index - first_row).astype(jnp.float32)
    allowed = (doc_ids[:, None] == doc_ids[None, :]) & (row_index[None, :] <= row_index[:, None])
    frequency = jnp.exp(
        -math.log(ROPE_BASE) * 2.0 * jnp.arange(ROPE // 2, dtype=jnp.float32) / ROPE
    )
    angles = positions[:, None] * frequency[None, :]
    return (allowed, jnp.cos(angles), jnp.sin(angles))


def swiglu(gate_pre, up_pre):
    sigmoid_gate = jax.nn.sigmoid(gate_pre)
    return (sigmoid_gate, (gate_pre * sigmoid_gate * up_pre).astype(jnp.bfloat16))


def swiglu_back(dhidden, gate_pre, up_pre, sigmoid_gate):
    gate_grad = dhidden * up_pre * sigmoid_gate * (1.0 + gate_pre * (1.0 - sigmoid_gate))
    up_grad = dhidden * gate_pre * sigmoid_gate
    return (gate_grad.astype(jnp.bfloat16), up_grad.astype(jnp.bfloat16))


def expert_kernel(
    x_ref, g_ref, w_ref, gate_ref, up_ref, down_ref, y_ref, dr_ref, dw_ref, gg_ref, gu_ref, gd_ref
):
    blocks, _, cap, width = x_ref.shape
    rows = blocks * cap
    row_inputs = x_ref[...].reshape(rows, width)
    gradient = g_ref[...].reshape(rows, width).astype(jnp.float32)
    weight = w_ref[...].reshape(rows, 1)
    gate, up, down = gate_ref[0], up_ref[0], down_ref[0]
    gate_pre = matmul_nt(row_inputs, gate)
    up_pre = matmul_nt(row_inputs, up)
    sigmoid_gate, hidden = swiglu(gate_pre, up_pre)
    produced = matmul(hidden, down)
    dw_ref[...] = jnp.sum(gradient * produced, axis=1, keepdims=True).reshape(dw_ref.shape)
    y_ref[...] = (weight * produced).astype(jnp.bfloat16).reshape(y_ref.shape)
    cotangent = (weight * gradient).astype(jnp.bfloat16)
    dhidden = matmul_nt(cotangent, down)
    gate_grad, up_grad = swiglu_back(dhidden, gate_pre, up_pre, sigmoid_gate)
    back = matmul(gate_grad, gate) + matmul(up_grad, up)
    dr_ref[...] = back.astype(jnp.bfloat16).reshape(dr_ref.shape)
    first = pl.program_id(1) == 0

    def accumulate(ref, left, right):
        part = matmul_tn(left, right)

        @pl.when(first)
        def _():
            ref[0] = part

        @pl.when(jnp.logical_not(first))
        def _():
            ref[0] += part

    accumulate(gg_ref, gate_grad, row_inputs)
    accumulate(gu_ref, up_grad, row_inputs)
    accumulate(gd_ref, hidden, cotangent)


def expert_stage(row_inputs, gradients, weights, gate_t, up_t, down):
    blocks, local, cap, width = row_inputs.shape
    units = gate_t.shape[1]
    step = min(blocks, 256 // cap)
    rows_spec = pl.BlockSpec((step, 1, cap, width), lambda j, r: (r, j, 0, 0))
    slot_spec = pl.BlockSpec((step, 1, cap, 1), lambda j, r: (r, j, 0, 0))
    unit_spec = pl.BlockSpec((1, units, width), lambda j, r: (j, 0, 0))
    rows_shape = jax.ShapeDtypeStruct(row_inputs.shape, jnp.bfloat16)
    unit_shape = jax.ShapeDtypeStruct((local, units, width), jnp.float32)
    flops = 18 * blocks * local * cap * width * units
    moved = 8 * blocks * local * cap * width + 18 * local * units * width
    return pl.pallas_call(
        expert_kernel,
        grid=(local, blocks // step),
        in_specs=[rows_spec, rows_spec, slot_spec, unit_spec, unit_spec, unit_spec],
        out_specs=[rows_spec, rows_spec, slot_spec, unit_spec, unit_spec, unit_spec],
        out_shape=[
            rows_shape,
            rows_shape,
            jax.ShapeDtypeStruct((blocks, local, cap, 1), jnp.float32),
            unit_shape,
            unit_shape,
            unit_shape,
        ],
        compiler_params=pltpu.CompilerParams(vmem_limit_bytes=VMEM_BYTES),
        cost_estimate=pl.CostEstimate(flops=flops, bytes_accessed=moved, transcendentals=0),
        name="experts",
    )(row_inputs, gradients, weights, gate_t, up_t, down)


def combine_kernel(
    p_ref, y_ref, dr_ref, dw_ref, x_ref, g_ref, shared_ref, out_ref, ds_ref, grad_ref
):
    picks = p_ref[0]
    row_inputs, cotangent = x_ref[0], g_ref[0]
    gate, up, down = shared_ref[0], shared_ref[1], shared_ref[2]
    gate_pre = matmul_nt(row_inputs, gate)
    up_pre = matmul_nt(row_inputs, up)
    sigmoid_gate, hidden = swiglu(gate_pre, up_pre)
    out_ref[0] = (matmul_tn(picks, y_ref[0]) + matmul(hidden, down)).astype(jnp.bfloat16)
    dhidden = matmul_nt(cotangent, down)
    gate_grad, up_grad = swiglu_back(dhidden, gate_pre, up_pre, sigmoid_gate)
    back = matmul_tn(picks, dr_ref[0]) + matmul(gate_grad, gate) + matmul(up_grad, up)
    width = back.shape[1]
    ds_ref[0, :, :width] = back.astype(jnp.bfloat16)
    ds_ref[0, :, width:] = matmul_tn(picks, dw_ref[0]).astype(jnp.bfloat16)
    first = pl.program_id(0) == 0
    for index, (left, right) in enumerate(
        ((gate_grad, row_inputs), (up_grad, row_inputs), (hidden, cotangent))
    ):
        part = matmul_tn(left, right)

        @pl.when(first)
        def _(index=index, part=part):
            grad_ref[index] = part

        @pl.when(jnp.logical_not(first))
        def _(index=index, part=part):
            grad_ref[index] += part


def combine_stage(picks, produced, back, spread, tokens, gradients, shared):
    blocks, slots, rows = picks.shape
    width = tokens.shape[-1]
    slot_spec = pl.BlockSpec((1, slots, width), lambda b: (b, 0, 0))
    rows_spec = pl.BlockSpec((1, rows, width), lambda b: (b, 0, 0))
    whole = pl.BlockSpec(shared.shape, lambda b: (0, 0, 0))
    lanes = spread.shape[-1]
    units = shared.shape[1]
    flops = 4 * blocks * slots * rows * width + 18 * blocks * rows * width * units
    moved = 4 * blocks * slots * width + 8 * blocks * rows * width
    return pl.pallas_call(
        combine_kernel,
        grid=(blocks,),
        in_specs=[
            pl.BlockSpec((1, slots, rows), lambda b: (b, 0, 0)),
            slot_spec,
            slot_spec,
            pl.BlockSpec((1, slots, lanes), lambda b: (b, 0, 0)),
            rows_spec,
            rows_spec,
            whole,
        ],
        out_specs=[
            rows_spec,
            pl.BlockSpec((1, rows, width + lanes), lambda b: (b, 0, 0)),
            whole,
        ],
        out_shape=[
            jax.ShapeDtypeStruct((blocks, rows, width), jnp.bfloat16),
            jax.ShapeDtypeStruct((blocks, rows, width + lanes), jnp.bfloat16),
            jax.ShapeDtypeStruct(shared.shape, jnp.float32),
        ],
        compiler_params=pltpu.CompilerParams(vmem_limit_bytes=VMEM_BYTES),
        cost_estimate=pl.CostEstimate(flops=flops, bytes_accessed=moved, transcendentals=0),
        name="combine",
    )(picks, produced, back, spread, tokens, gradients, shared)


MESH = pl.DeviceIdType.MESH
PAIR = 2
ANY = pl.BlockSpec(memory_space=pl.ANY)
IN_VMEM = pl.BlockSpec(memory_space=pltpu.VMEM)
DMA = pltpu.SemaphoreType.DMA


def place():
    me, part = lax.axis_index(EXPERT), lax.axis_index(TENSOR)
    return (me // PAIR, me % PAIR, part // PAIR, part % PAIR)


def device(z, x, y, c):
    return {EXPERT: z * PAIR + x, TENSOR: y * PAIR + c}


def greet(peers):
    barrier = pltpu.get_barrier_semaphore()
    for peer in peers:
        pl.semaphore_signal(barrier, inc=1, device_id=peer, device_id_type=MESH)
    pl.semaphore_wait(barrier, len(peers))


def push(source, target, send, arrive, peer):
    copy = pltpu.make_async_remote_copy(
        src_ref=source,
        dst_ref=target,
        send_sem=send,
        recv_sem=arrive,
        device_id=peer,
        device_id_type=MESH,
    )
    copy.start()
    return copy


def bring(source, target, done):
    copy = pltpu.make_async_copy(source, target, done)
    copy.start()
    return copy


def arrived(target, done):
    pltpu.make_async_copy(target, target, done).wait()


def slot(ref, axis, index, size):
    start = pl.multiple_of(index * size, size)
    if axis == 0:
        return ref.at[pl.ds(start, size), :]
    return ref.at[:, pl.ds(start, size)]


class Bag(dict):
    __getattr__ = dict.__getitem__
    __setattr__ = dict.__setitem__


class Calls:
    def __init__(self):
        self.count = 0

    def params(self):
        self.count += 1
        return pltpu.CompilerParams(
            collective_id=self.count, has_side_effects=True, vmem_limit_bytes=VMEM_BYTES
        )


def choose(table, index):
    value = table[0]
    for i, entry in enumerate(table[1:], 1):
        if any(entry != other for other in table):
            value = jnp.where(index == i, entry, value)
    return value


class Link:
    def __init__(self, deep):
        me, part = lax.axis_index(EXPERT), lax.axis_index(TENSOR)
        self.deep, self.me, self.part = deep, me, part
        self.z, self.x = me // PAIR, me % PAIR
        self.y, self.c = part // PAIR, part % PAIR
        near = [
            sorted((k for k in range(1, deep)), key=lambda k: abs((z - k) % deep - z))
            for z in range(deep)
        ]
        self.order = [choose([near[z][h] for z in range(deep)], self.z) for h in range(deep - 1)]
        self.drains = []

    def at_z(self, z):
        return device(z, self.x, self.y, self.c)

    def peer(self, axis):
        flip = {name: 1 - getattr(self, name) if name == axis else getattr(self, name) for name in "xyc"}
        return device(self.z, flip["x"], flip["y"], flip["c"])

    def greet(self, groups, axes):
        peers = [{EXPERT: (self.me + j) % groups, TENSOR: self.part} for j in range(1, groups)]
        if "e" not in axes:
            peers = []
        greet(peers + [self.peer(axis) for axis in axes if axis != "e"])

    def emit(self, make, condition=None):
        def start():
            make().start()

        def finish():
            make().wait_send()

        if condition is None:
            start()
            self.drains.append(finish)
        else:
            pl.when(condition)(start)
            self.drains.append(lambda: pl.when(condition)(finish))

    def drain(self):
        for finish in self.drains:
            finish()
        self.drains = []


def spread(link, order, source, at, send, arrive):
    deep, z = link.deep, link.z
    cut = order.find("z")
    before, after = (order[:cut], order[cut + 1 :]) if cut >= 0 else ("", order)
    none = frozenset()

    def piece(k, flips):
        x, y, c = (
            1 - getattr(link, name) if name in flips else getattr(link, name) for name in "xyc"
        )
        return at((z + deep - k) % deep, x, y, c)

    def number(k, flips):
        return k * 8 + sum(1 << "xyc".index(name) for name in flips)

    def forward(k, flips, to_number, peer, condition=None):
        own = isinstance(k, int) and k == 0 and not flips

        def make():
            target = piece(k, flips)
            return pltpu.make_async_remote_copy(
                src_ref=source if own else target,
                dst_ref=target,
                send_sem=send.at[to_number],
                recv_sem=arrive.at[to_number],
                device_id=peer,
                device_id_type=MESH,
            )

        link.emit(make, condition)

    def hand_on(k, flips, axes, along_z):
        if along_z:
            forward(k, flips, number(1, flips), link.at_z(z + 1), z < deep - 1)
            forward(k, flips, number(deep - 1, flips), link.at_z(z - 1), z > 0)
        for axis in axes:
            forward(k, flips, number(k, flips | {axis}), link.peer(axis))

    def take(k, flips):
        arrived(piece(k, flips), arrive.at[number(k, flips)])

    hand_on(0, none, before + after, cut >= 0)
    got = [none]
    for i, axis in enumerate(before):
        for flips in got:
            yield
            take(0, flips | {axis})
            hand_on(0, flips | {axis}, before[i + 1 :] + after, True)
        got = got + [flips | {axis} for flips in got]
    ks = [0]
    if cut >= 0:
        for k in link.order:
            below = z >= k
            onward = jnp.where(below, k + 1, k - 1)
            more = jnp.where(below, z < deep - 1, z > 0)
            following = link.at_z(jnp.where(below, z + 1, z - 1))
            for flips in got:
                yield
                take(k, flips)
                forward(k, flips, number(onward, flips), following, more)
                hand_on(k, flips, after, False)
        ks = ks + link.order
    for i, axis in enumerate(after):
        for k in ks:
            for flips in got:
                yield
                take(k, flips | {axis})
                hand_on(k, flips | {axis}, after[i + 1 :], False)
        got = got + [flips | {axis} for flips in got]


def shuffle(link, groups, source, at, send, arrive):
    def make(j):
        target = (link.me + j) % groups
        return pltpu.make_async_remote_copy(
            src_ref=source(target),
            dst_ref=at(link.me),
            send_sem=send.at[j],
            recv_sem=arrive.at[j],
            device_id={EXPERT: target, TENSOR: link.part},
            device_id_type=MESH,
        )

    for j in range(1, groups):
        link.emit(functools.partial(make, j))
    for j in range(1, groups):
        yield
        arrived(at((link.me + groups - j) % groups), arrive.at[j])


def run(tasks):
    tasks = list(tasks)
    while tasks:
        tasks = [task for task in tasks if next(task, run) is not run]


def add_rows(count, store):
    lax.fori_loop(0, count, lambda i, carry: (store(i), carry)[1], 0)


def sum_all_kernel(deep, chunks, count, *refs):
    partials, outs = refs[:count], refs[count : 2 * count]
    total = len(chunks)
    rest = refs[2 * count :]
    own_buf, from_core = rest[:total], rest[total : 2 * total]
    from_first, from_second = rest[2 * total : 3 * total], rest[3 * total : 4 * total]
    from_deep = rest[4 * total : 5 * total]
    send, arrive, own = rest[5 * total :]
    z, x, y, c = place()
    others = [device((z + k) % deep, x, y, c) for k in range(1, deep)]
    twin, across, beside = (
        device(z, 1 - x, y, c),
        device(z, x, 1 - y, c),
        device(z, x, y, 1 - c),
    )
    greet(others + [twin, across, beside])
    copies, loads = [], []
    for n, (i, left, wide, order) in enumerate(chunks):
        span = pl.ds(left, wide)
        copies.append(
            push(
                partials[i].at[:, 1 - c, :, span],
                from_core[n],
                send.at[n, 0],
                arrive.at[n, 0],
                beside,
            )
        )
        loads.append(bring(partials[i].at[:, c, :, span], own_buf[n], own.at[n]))

    def index(order, depth, on_first, on_second):
        on_x, on_y = (on_first, on_second) if order == 0 else (on_second, on_first)
        return (depth * PAIR + on_x) * PAIR + on_y

    def stage_core(n):
        _, _, _, order = chunks[n]
        buf, other = own_buf[n], from_core[n]
        loads[n].wait()
        arrived(other, arrive.at[n, 0])

        def add(k):
            buf[k] = (buf[k].astype(jnp.float32) + other[k].astype(jnp.float32)).astype(
                jnp.bfloat16
            )

        add_rows(deep * PAIR * PAIR, add)
        mine = x if order == 0 else y
        for depth in range(deep):
            for s in range(PAIR):
                number = 1 + depth * PAIR + s
                copies.append(
                    push(
                        buf.at[index(order, depth, 1 - mine, s)],
                        from_first[n].at[depth * PAIR + s],
                        send.at[n, number],
                        arrive.at[n, number],
                        twin if order == 0 else across,
                    )
                )

    def stage_first(n):
        _, _, _, order = chunks[n]
        buf, other = own_buf[n], from_first[n]
        mine, following = (x, y) if order == 0 else (y, x)
        for number in range(1, 1 + PAIR * deep):
            arrived(other.at[number - 1], arrive.at[n, number])

        def add(k):
            at = index(order, k // PAIR, mine, k % PAIR)
            buf[at] = (buf[at].astype(jnp.float32) + other[k].astype(jnp.float32)).astype(
                jnp.bfloat16
            )

        add_rows(deep * PAIR, add)
        for depth in range(deep):
            number = 1 + PAIR * deep + depth
            copies.append(
                push(
                    buf.at[index(order, depth, mine, 1 - following)],
                    from_second[n].at[depth],
                    send.at[n, number],
                    arrive.at[n, number],
                    across if order == 0 else twin,
                )
            )

    def stage_second(n):
        _, _, _, order = chunks[n]
        buf, other = own_buf[n], from_second[n]
        mine, following = (x, y) if order == 0 else (y, x)
        base = 1 + PAIR * deep
        for depth in range(deep):
            arrived(other.at[depth], arrive.at[n, base + depth])

        def add(k):
            at = index(order, k, mine, following)
            buf[at] = (buf[at].astype(jnp.float32) + other[k].astype(jnp.float32)).astype(
                jnp.bfloat16
            )

        add_rows(deep, add)
        for k in range(1, deep):
            number = base + deep + k - 1
            copies.append(
                push(
                    buf.at[index(order, (z + k) % deep, mine, following)],
                    from_deep[n].at[k - 1],
                    send.at[n, number],
                    arrive.at[n, number],
                    others[k - 1],
                )
            )

    def stage_deep(n):
        i, left, wide, order = chunks[n]
        base = 1 + PAIR * deep + deep
        for k in range(1, deep):
            arrived(from_deep[n].at[k - 1], arrive.at[n, base + k - 1])
        mine, following = (x, y) if order == 0 else (y, x)
        result = own_buf[n][index(order, z, mine, following)].astype(jnp.float32)
        for k in range(deep - 1):
            result = result + from_deep[n][k].astype(jnp.float32)
        outs[i][:, pl.ds(left, wide)] = result

    for step in range(total + 3):
        for lag, stage in enumerate((stage_core, stage_first, stage_second, stage_deep)):
            if 0 <= step - lag < total:
                stage(step - lag)
    for copy in copies:
        copy.wait_send()


def sum_all(calls, groups, parts, arrays):
    deep = groups // PAIR
    rows = arrays[0].shape[0] // (groups * parts)
    budget, calls_of, used = 46 * 2**20, [[]], 0
    number = 0
    for i, array in enumerate(arrays):
        left = 0
        while left < array.shape[1]:
            wide = min(512, array.shape[1] - left)
            if 0 < array.shape[1] - left - wide < 512 // 2:
                wide = array.shape[1] - left
            cost = 2 * rows * wide * (4 * deep * 2 + 2 * deep + deep + deep) + 4 * rows * wide
            if used + cost > budget:
                calls_of.append([])
                used = 0
            used += cost
            calls_of[-1].append((i, left, wide, number % 2))
            number += 1
            left += wide
    views = [a.reshape(groups * parts // PAIR, PAIR, rows, a.shape[1]) for a in arrays]
    pieces = [[] for _ in arrays]
    for chunks in calls_of:
        used_arrays = sorted({c[0] for c in chunks})
        bounds = {
            i: (min(c[1] for c in chunks if c[0] == i), sum(c[2] for c in chunks if c[0] == i))
            for i in used_arrays
        }
        local = [(used_arrays.index(i), left, wide, order) for i, left, wide, order in chunks]
        count = len(used_arrays)
        many = deep * PAIR * PAIR

        def bufs(n):
            return [pltpu.VMEM((n, rows, wide), jnp.bfloat16) for _, _, wide, _ in chunks]

        sems = DMA((len(chunks), 1 + PAIR * deep + deep + deep))
        outs = pl.pallas_call(
            functools.partial(
                sum_all_kernel,
                deep,
                tuple(local),
                count,
            ),
            in_specs=[ANY] * count,
            out_specs=[IN_VMEM] * count,
            out_shape=[
                jax.ShapeDtypeStruct((rows, arrays[i].shape[1]), jnp.float32)
                for i in used_arrays
            ],
            scratch_shapes=bufs(many)
            + bufs(many)
            + bufs(PAIR * deep)
            + bufs(deep)
            + bufs(deep - 1)
            + [sems, sems, DMA((len(chunks),))],
            compiler_params=calls.params(),
            name="sum_all",
        )(*[views[i] for i in used_arrays])
        for i, out in zip(used_arrays, outs):
            pieces[i].append(out[:, bounds[i][0] : bounds[i][0] + bounds[i][1]])
    return [p[0] if len(p) == 1 else jnp.concatenate(p, axis=1) for p in pieces]


def swap_halves(values, half):
    lane = lax.broadcasted_iota(jnp.int32, values.shape, 1)
    wide = values.shape[1]
    return jnp.where(
        lane < half, pltpu.roll(values, wide - half, 1), pltpu.roll(values, half, 1)
    )


def turn(values, cosine, sinusoid):
    return values * cosine + swap_halves(values, ROPE // 2) * sinusoid


def full_gain(gains, row, size, groups):
    total = size * groups
    wide = gains.shape[1]
    if size % LANES == 0:
        shares = [gains[e * 8 + row : e * 8 + row + 1, :size] for e in range(groups)]
        return jnp.concatenate(shares, axis=1)
    result = jnp.zeros((8, total), jnp.float32)
    for e in range(groups):
        share = jnp.broadcast_to(gains[e * 8 + row : e * 8 + row + 1, :], (8, wide))
        if total > wide:
            share = jnp.concatenate([share, jnp.zeros((8, total - wide), jnp.float32)], axis=1)
        result = result + (pltpu.roll(share, e * size, 1) if e else share)
    return result[:1]


def rows_loop(count, step, work):
    def one(i, carry):
        work(pl.ds(pl.multiple_of(i * step, step), step))
        return carry

    lax.fori_loop(0, count // step, one, 0)


def by_rows(count, work):
    rows_loop(count, 16 if count % 16 == 0 else count, work)


def front_kernel(groups, sizes, plan, names, *refs):
    ref = Bag(zip(names, refs))
    deep = groups // PAIR
    link = Link(deep)
    z, x, y, c, part = link.z, link.x, link.y, link.c, link.part
    send, arrive, own, leave = ref.send, ref.arrive, ref.own, ref.leave
    link.greet(groups, "eyc")
    loads, numbers, landing = {}, {}, Bag()
    row_of = {}
    for n, (name, axis, cut, over, orders, home) in enumerate(plan):
        numbers[name] = n
        landing[name] = ref["b_" + name] if home == VMEM_ else ref["o_" + name]

    stream_row = [0]

    def tasks_of(name):
        n = numbers[name]
        _, axis, cut, over, orders, home = plan[n]
        source, target = ref["i_" + name], landing[name]
        if cut is not None:
            source = slot(source, cut[0], part, cut[1])
        if over == READY:
            loads[name] = bring(source, target, own.at[n])
            return []
        if over == SHUFFLE:
            size = source.shape[2]
            keep = ref["k_" + name]
            loads[name] = bring(source.at[link.me], keep, own.at[n])
            row = stream_row[0]
            stream_row[0] += 1
            return [
                shuffle(
                    link,
                    groups,
                    lambda e: source.at[e],
                    lambda e: slot(target, axis, e, size),
                    send.at[row],
                    arrive.at[row],
                )
            ]
        size = cut[1] if cut is not None and cut[0] == axis else source.shape[axis]

        def home_of(sz, sx, sy, sc):
            index = sz * PAIR + sx
            if over == "all":
                index = (index * PAIR + sy) * PAIR + sc
            return slot(target, axis, index, size)

        mine = home_of(z, x, y, c)
        if home == VMEM_:
            loads[name] = bring(source, mine, own.at[n])
        else:
            loads[name] = bring(source, ref["k_" + name], own.at[n])
        if orders == ("e",):
            row = stream_row[0]
            stream_row[0] += 1
            return [
                shuffle(
                    link,
                    groups,
                    lambda e: source,
                    lambda e: slot(target, axis, e, size),
                    send.at[row],
                    arrive.at[row],
                )
            ]
        return streams_of(source, home_of, orders)

    def streams_of(source, home_of, orders):
        result = []
        for i, order in enumerate(orders):
            row = stream_row[0]
            stream_row[0] += 1
            if len(orders) == 1:
                at, part_source = home_of, source
            else:
                wide = source.shape[1] // len(orders)
                span = pl.ds(i * wide, wide)

                def at(*where, span=span):
                    return home_of(*where).at[:, span]

                part_source = source.at[:, span]
            result.append(spread(link, order, part_source, at, send.at[row], arrive.at[row]))
        return result

    def begin(*which):
        found = [task for name in which for task in tasks_of(name)]
        return [task for task in found if next(task, run) is not run]

    gain_tasks = begin(GAINS, ROUTES)
    stem_tasks = begin(QUERY_DOWN, LATENT_DOWN)
    late_tasks = begin(OUT_GRAD)

    def complete(name):
        n = numbers[name]
        loads.pop(name).wait()
        _, axis, cut, over, _, home = plan[n]
        if home == "hbm":
            keep, target = ref["k_" + name], landing[name]
            index = link.me
            if over == "all":
                index = link.me * PAIR * PAIR + part
            move = pltpu.make_async_copy(
                keep, slot(target, axis, index, keep.shape[axis]), own.at[n]
            )
            move.start()
            stores.append(move)

    stores = []

    def keep_out(name, source=None):
        moves = len(stores)
        move = bring(source if source is not None else landing[name], ref["o_" + name], leave.at[len(kept)])
        kept.append(move)

    kept = []
    block_ref = ref.i_block
    first_ref, middle_ref = ref.b_first, ref.b_middle
    width = block_ref.shape[1]
    row_count = block_ref.shape[0]
    sub = row_count // (PAIR * PAIR)

    complete(GAINS)
    complete(ROUTES)
    run(gain_tasks)
    gains = landing.gains
    attention_gain = full_gain(gains, 0, sizes[0], groups)

    def first_norm(span):
        values = block_ref[span, :].astype(jnp.float32)
        inverse = lax.rsqrt(jnp.mean(values * values, axis=-1, keepdims=True) + EPSILON)
        first_ref[span, :] = (values * inverse * attention_gain).astype(jnp.bfloat16)

    rows_loop(row_count, 32, first_norm)
    for _ in range(deep - 1):
        advance(stem_tasks, 1)
        advance(late_tasks, 1)
    up_tasks = begin(QUERY_UP, LATENT_UP)
    for name in (QUERY_DOWN, LATENT_DOWN):
        complete(name)
    run(stem_tasks)
    ref.b_query_cut[...] = matmul(first_ref[...], landing.query_down[...]).astype(
        jnp.bfloat16
    )
    ref.b_latent_cut[...] = matmul_nt(landing.latent_down[...], first_ref[...]).astype(
        jnp.bfloat16
    )
    query_lat, latent_t = ref.b_query_lat, ref.b_latent_t
    query_cut, latent_cut = ref.b_query_cut, ref.b_latent_cut
    stem_numbers = len(plan)
    stem_tasks = streams_of(
        query_cut, lambda sz, sx, sy, sc: slot(query_lat, 1, sy * PAIR + sc, query_cut.shape[1]), ("yc",)
    ) + streams_of(
        latent_cut, lambda sz, sx, sy, sc: slot(latent_t, 0, sy * PAIR + sc, latent_cut.shape[0]), ("yc",)
    )
    stem_tasks = [task for task in stem_tasks if next(task, run) is not run]
    query_lat[:, pl.ds(pl.multiple_of(part * query_cut.shape[1], LANES), query_cut.shape[1])] = (
        query_cut[...]
    )
    latent_t[pl.ds(pl.multiple_of(part * latent_cut.shape[0], 16), latent_cut.shape[0]), :] = (
        latent_cut[...]
    )
    query_gain = full_gain(gains, 2, sizes[2], groups)
    latent_gain = full_gain(gains, 3, sizes[3], groups)
    cosine, sinusoid = ref.i_cosine, ref.i_sinusoid
    advance(up_tasks, 1)
    run(stem_tasks)
    advance(late_tasks, 2)

    query_n, latent_n, keys = ref.b_query_n, ref.b_latent_n, ref.b_keys

    def query_norm(span):
        values = query_lat[span, :].astype(jnp.float32)
        inverse = lax.rsqrt(jnp.mean(values * values, axis=-1, keepdims=True) + EPSILON)
        query_n[span, :] = (values * inverse * query_gain).astype(jnp.bfloat16)

    rows_loop(row_count, 32, query_norm)
    for _ in range(deep - 2):
        advance(up_tasks, 1)
        advance(late_tasks, 2)
    out_tasks = begin(OUT_PROJ, ROUTER)
    latent_rank = latent_n.shape[1]
    latent = latent_t[:latent_rank, :].astype(jnp.float32).T
    inverse = lax.rsqrt(jnp.mean(latent * latent, axis=-1, keepdims=True) + EPSILON)
    latent_n[...] = (latent * inverse * latent_gain).astype(jnp.bfloat16)
    rope_rows = latent_t[latent_rank:, :].astype(jnp.float32).T
    rope_rows = jnp.concatenate(
        [rope_rows, jnp.zeros((row_count, LANES - ROPE), jnp.float32)], axis=1
    )
    key_rope = turn(rope_rows, cosine[...], sinusoid[...])[:, :ROPE].astype(jnp.bfloat16)

    complete(QUERY_UP)
    complete(LATENT_UP)
    run(up_tasks)
    queries, values_ref, attended = ref.b_queries, ref.b_values, ref.b_attended
    heads = queries.shape[0]
    head_width = NOPE + ROPE
    projected = matmul(query_n[...], landing.query_up[...])
    shifted = pltpu.roll(projected, projected.shape[1] - ROPE, 1)
    keyval = matmul(latent_n[...], landing.latent_up[...])
    for h in range(heads):
        start = h * head_width
        base, start = (projected, start) if start % LANES == 0 else (shifted, start - ROPE)
        queries[h, :, :NOPE] = base[:, start : start + NOPE].astype(jnp.bfloat16)
        tail = base[:, start + NOPE : start + NOPE + LANES]
        if tail.shape[1] < LANES:
            tail = jnp.concatenate(
                [tail, jnp.zeros((row_count, LANES - tail.shape[1]), jnp.float32)], axis=1
            )
        queries[h, :, NOPE:] = turn(tail, cosine[...], sinusoid[...])[:, :ROPE].astype(
            jnp.bfloat16
        )
        left = h * (NOPE + VD)
        keys[h, :, :NOPE] = keyval[:, left : left + NOPE].astype(jnp.bfloat16)
        keys[h, :, NOPE:] = key_rope
        values_ref[h] = keyval[:, left + NOPE : left + NOPE + VD].astype(jnp.bfloat16)
        scores = matmul_nt(queries[h], keys[h]) * head_width ** (-0.5)
        scores = jnp.where(ref.i_allowed[...] > 0, scores, -1e30)
        powers = jnp.exp(scores - jnp.max(scores, axis=-1, keepdims=True))
        probs = (powers / jnp.sum(powers, axis=-1, keepdims=True)).astype(jnp.bfloat16)
        attended[:, h * VD : (h + 1) * VD] = matmul(probs, values_ref[h]).astype(jnp.bfloat16)
        if h < deep - 1:
            advance(out_tasks, 1)
        advance(late_tasks, 2)
    advance(out_tasks, max(0, deep - 1 - heads))
    shared_tasks = begin(SHARED)
    for name in (OUT_PROJ, ROUTER):
        complete(name)
    run(out_tasks)
    for name in (QUERY_DOWN, LATENT_DOWN, QUERY_UP, LATENT_UP, OUT_PROJ, GAINS, ROUTER):
        keep_out(name)
    for name in (FIRST, QUERY_LAT, LATENT_T, QUERY_N, LATENT_N, QUERIES, KEYS, VALUES, ATTENDED):
        keep_out(name, ref["b_" + name])

    partial, from_beside = ref.b_partial, ref.b_from_beside
    give, from_across = ref.b_give, ref.b_from_across
    swap_send, swap_arrive = ref.swap_send, ref.swap_arrive
    for quarter in range(PAIR * PAIR):
        partial[quarter // PAIR, quarter % PAIR] = matmul(
            attended[quarter * sub : (quarter + 1) * sub, :], landing.out_proj[...]
        ).astype(jnp.bfloat16)

    sum_task = tensor_total(
        link, partial, from_beside, give, from_across, middle_ref, swap_send, swap_arrive
    )
    next(sum_task, None)
    advance(late_tasks, 1)
    next(sum_task, None)
    complete(OUT_GRAD)
    complete(SHARED)
    advance(late_tasks, 1)
    next(sum_task, None)
    ffn_gain = full_gain(gains, 1, sizes[1], groups)
    norms = ref.b_norms
    norms[...] = jnp.zeros(norms.shape, jnp.float32)
    for i, gain in enumerate((attention_gain, ffn_gain, query_gain, latent_gain)):
        norms[i : i + 1, : gain.shape[1]] = gain
    keep_out("norms", norms)
    second_ref, weights_ref, chosen_ref = ref.b_second, ref.b_weights, ref.b_chosen
    start = pl.multiple_of(part * sub, sub)

    def middle_norm(span):
        mine = pl.ds(pl.multiple_of(start + span.start, 16), span.size)
        middle = middle_ref[span, :] + block_ref[mine, :].astype(jnp.float32)
        middle_ref[span, :] = middle
        inverse = lax.rsqrt(jnp.mean(middle * middle, axis=-1, keepdims=True) + EPSILON)
        second_ref[span, :] = (middle * inverse * ffn_gain).astype(jnp.bfloat16)

    by_rows(sub, middle_norm)
    logits = matmul_nt(second_ref[...], landing.router[...])
    experts = logits.shape[1]
    advance(late_tasks, 1)
    routes_rows = ref.i_route_rows[pl.ds(pl.multiple_of(part * sub, sub), sub), :]
    ids = lax.broadcasted_iota(jnp.int32, (sub, experts), 1)
    chosen = jnp.zeros((sub, experts), jnp.float32)
    picked = jax.nn.sigmoid(logits)
    for k in range(routes_rows.shape[1]):
        chosen = jnp.where(routes_rows[:, k : k + 1] == ids, picked, chosen)
    totals = jnp.sum(chosen, axis=-1, keepdims=True)
    weights_ref[...] = jnp.zeros(weights_ref.shape, jnp.float32)
    weights_ref[:, :experts] = ROUTE_SCALE * chosen / totals
    chosen_ref[...] = jnp.zeros(chosen_ref.shape, jnp.float32)
    chosen_ref[:, :experts] = chosen

    def row_home(name):
        def home_of(sz, sx, sy, sc):
            index = ((sz * PAIR + sx) * PAIR + sy) * PAIR + sc
            return slot(ref["o_" + name], 0, index, sub)

        return home_of

    all_tasks = streams_of(weights_ref, row_home(WEIGHTS), (ZXYC,))
    all_tasks += streams_of(second_ref, row_home(TOKENS), (ZXYC, "zyxc"))
    all_tasks = [task for task in all_tasks if next(task, run) is not run]
    mine = link.me * PAIR * PAIR + part
    kept.append(bring(second_ref, slot(ref.o_tokens, 0, mine, sub), leave.at[len(kept)]))
    kept.append(bring(weights_ref, slot(ref.o_weights, 0, mine, sub), leave.at[len(kept)]))
    keep_out("middle", middle_ref)
    keep_out("chosen", chosen_ref)
    run(late_tasks + all_tasks + shared_tasks)
    link.drain()
    for move in stores + kept:
        move.wait()


def front_stage(calls, groups, parts, sizes, items, block, route_rows, allowed, cosine, sinusoid):
    deep = groups // PAIR
    rows, width = block.shape
    sub = rows // parts
    bf16, f32 = jnp.bfloat16, jnp.float32
    names, inputs, in_specs = [], [], []
    out_names, out_shape, plan, scratch = [], [], [], Bag()
    streams = 0
    for name, array, axis, cut, over, orders, home in items:
        names.append("i_" + name)
        inputs.append(array)
        in_specs.append(ANY)
        shape = list(array.shape)
        if over == SHUFFLE:
            shape = shape[1:]
        if cut is not None:
            shape[cut[0]] = cut[1]
        if home == "hbm":
            scratch["k_" + name] = pltpu.VMEM(tuple(shape), array.dtype)
        if over != READY:
            shape[axis] *= groups * parts if over == "all" else groups
            streams += max(1, len(orders))
        if home == VMEM_:
            scratch["b_" + name] = pltpu.VMEM(tuple(shape), array.dtype)
        out_names.append(name)
        out_shape.append(jax.ShapeDtypeStruct(tuple(shape), array.dtype))
        plan.append((name, axis, cut, over, orders, home))
    for name, array in (
        ("block", block),
        ("route_rows", route_rows),
        ("allowed", allowed),
        ("cosine", cosine),
        ("sinusoid", sinusoid),
    ):
        names.append("i_" + name)
        inputs.append(array)
        in_specs.append(IN_VMEM)
    shape_of = Bag((name, shape.shape) for name, shape in zip(out_names, out_shape))
    query_cut, latent_cut = shape_of.query_down[1], shape_of.latent_down[0]
    query_rank, latent_rank = shape_of.query_up[0], shape_of.latent_up[0]
    heads = shape_of.latent_up[1] // (NOPE + VD)
    experts = shape_of.router[0]
    lanes = experts + -experts % LANES
    half = parts // PAIR
    buffers = Bag(
        first=((rows, width), bf16),
        query_lat=((rows, query_cut * parts), bf16),
        latent_t=((latent_cut * parts, rows), bf16),
        query_n=((rows, query_rank), bf16),
        latent_n=((rows, latent_rank), bf16),
        queries=((heads, rows, NOPE + ROPE), bf16),
        keys=((heads, rows, NOPE + ROPE), bf16),
        values=((heads, rows, VD), bf16),
        attended=((rows, heads * VD), bf16),
        middle=((sub, width), f32),
        chosen=((sub, lanes), f32),
        norms=((8, width), f32),
    )
    for name, (shape, dtype) in buffers.items():
        out_names.append(name)
        out_shape.append(jax.ShapeDtypeStruct(shape, dtype))
    inner = Bag(
        query_cut=((rows, query_cut), bf16),
        latent_cut=((latent_cut, rows), bf16),
        partial=((half, PAIR, sub, width), bf16),
        from_beside=((half, sub, width), bf16),
        give=((sub, width), bf16),
        from_across=((sub, width), bf16),
        second=((sub, width), bf16),
        weights=((sub, lanes), f32),
    )
    for name, (shape, dtype) in (buffers | inner).items():
        scratch["b_" + name] = pltpu.VMEM(shape, dtype)
    out_names += [TOKENS, WEIGHTS]
    out_shape += [
        jax.ShapeDtypeStruct((sub * groups * parts, width), bf16),
        jax.ShapeDtypeStruct((sub * groups * parts, lanes), f32),
    ]
    streams += 2 + 1 + 2
    scratch.send = scratch.arrive = DMA((streams, 8 * deep))
    scratch.own = DMA((len(items),))
    scratch.leave = DMA((len(out_names),))
    scratch.swap_send = scratch.swap_arrive = DMA((2,))
    names += ["o_" + name for name in out_names] + list(scratch)
    results = pl.pallas_call(
        functools.partial(front_kernel, groups, tuple(sizes), tuple(plan), tuple(names)),
        in_specs=in_specs,
        out_specs=[ANY] * len(out_names),
        out_shape=out_shape,
        scratch_shapes=list(scratch.values()),
        compiler_params=calls.params(),
        name="front",
    )(*inputs)
    return Bag(zip(out_names, results))


def device_total(link, order, own, give, bufs, result, send, arrive):
    deep, z, x, y = link.deep, link.z, link.x, link.y
    from_core, from_first, from_second, from_deep = bufs
    mine, following = (x, y) if order == 0 else (y, x)
    near, far = (link.peer("x"), link.peer("y")) if order == 0 else (link.peer("y"), link.peer("x"))

    def at(depth, on_first, on_second):
        on_x, on_y = (on_first, on_second) if order == 0 else (on_second, on_first)
        return (depth * PAIR + on_x) * PAIR + on_y

    def hop(number, source, target, peer):
        def make():
            return pltpu.make_async_remote_copy(
                src_ref=source(),
                dst_ref=target,
                send_sem=send.at[number],
                recv_sem=arrive.at[number],
                device_id=peer,
                device_id_type=MESH,
            )

        link.emit(make)

    hop(0, lambda: give, from_core, link.peer("c"))
    yield
    arrived(from_core, arrive.at[0])

    def add_core(k):
        own[k] = own[k] + from_core[k]

    add_rows(deep * PAIR * PAIR, add_core)
    for depth in range(deep):
        for s in range(PAIR):
            n = depth * PAIR + s
            hop(1 + n, lambda d=depth, s=s: own.at[at(d, 1 - mine, s)], from_first.at[n], near)
    yield
    for n in range(PAIR * deep):
        arrived(from_first.at[n], arrive.at[1 + n])

    def add_first(k):
        here = at(k // PAIR, mine, k % PAIR)
        own[here] = own[here] + from_first[k]

    add_rows(deep * PAIR, add_first)
    base = 1 + PAIR * deep
    for depth in range(deep):
        hop(
            base + depth,
            lambda d=depth: own.at[at(d, mine, 1 - following)],
            from_second.at[depth],
            far,
        )
    yield
    for depth in range(deep):
        arrived(from_second.at[depth], arrive.at[base + depth])

    def add_second(k):
        here = at(k, mine, following)
        own[here] = own[here] + from_second[k]

    add_rows(deep, add_second)
    base = base + deep - 1
    for k in range(1, deep):
        hop(
            base + k,
            lambda k=k: own.at[at((z + k) % deep, mine, following)],
            from_deep.at[k - 1],
            link.at_z((z + k) % deep),
        )
    yield
    for k in range(1, deep):
        arrived(from_deep.at[k - 1], arrive.at[base + k])

    def finish(span):
        total = own[at(z, mine, following), span, :].astype(jnp.float32)
        for k in range(1, deep):
            total = total + from_deep[k - 1, span, :].astype(jnp.float32)
        result[span, :] = total

    by_rows(result.shape[0], finish)


def total_buffers(deep, rows, wide):
    shapes = (deep * PAIR * PAIR, PAIR * deep, deep, deep - 1)
    return [pltpu.VMEM((n, rows, wide), jnp.bfloat16) for n in shapes]


def total_hops(deep):
    return PAIR * deep + 2 * deep


def route_kernel(ids_ref, routes_ref, x_ref, g_ref, weights_ref, xr_ref, gr_ref, p_ref, w_ref):
    local = ids_ref.shape[0]
    rows = x_ref.shape[0]
    f32, bf16 = jnp.float32, jnp.bfloat16
    ids = ids_ref[...]
    named = jnp.zeros((local, rows), f32)
    for k in range(routes_ref.shape[0]):
        named = jnp.where(routes_ref[k : k + 1, :] == ids, 1.0, named)
    before = lax.broadcasted_iota(jnp.int32, (rows, rows), 0)
    after = lax.broadcasted_iota(jnp.int32, (rows, rows), 1)
    rank = matmul(named.astype(bf16), jnp.where(before < after, 1.0, 0.0).astype(bf16))
    lanes = weights_ref.shape[1]
    mine = jnp.where(lax.broadcasted_iota(jnp.int32, (local, lanes), 1) == ids, 1.0, 0.0)
    weights = lax.dot_general(
        mine,
        weights_ref[...],
        (((1,), (1,)), ((), ())),
        precision=lax.Precision.HIGHEST,
        preferred_element_type=f32,
    )
    slots = lax.broadcasted_iota(jnp.int32, (CAP, rows), 0).astype(f32)
    picks = []
    for j in range(local):
        pick = jnp.where(slots == rank[j : j + 1, :], named[j : j + 1, :], 0.0)
        w_ref[0, j * CAP : (j + 1) * CAP, :] = jnp.sum(
            pick * weights[j : j + 1, :], axis=1, keepdims=True
        )
        picks.append(pick.astype(bf16))
    picks = jnp.concatenate(picks, axis=0)
    p_ref[0] = picks
    xr_ref[0] = matmul(picks, x_ref[...]).astype(bf16)
    gr_ref[0] = matmul(picks, g_ref[...]).astype(bf16)


def route_stage(groups, own_ids, routes_t, tokens, gradients, weights):
    local = own_ids.shape[0]
    rows, width = tokens.shape[0] // groups, tokens.shape[1]
    slots = local * CAP
    row_spec = pl.BlockSpec((rows, width), lambda b: (b, 0))
    slot_spec = pl.BlockSpec((1, slots, width), lambda b: (b, 0, 0))
    slot_shape = jax.ShapeDtypeStruct((groups, slots, width), jnp.bfloat16)
    lanes = weights.shape[1]
    return pl.pallas_call(
        route_kernel,
        grid=(groups,),
        in_specs=[
            pl.BlockSpec((local, 1), lambda b: (0, 0)),
            pl.BlockSpec((routes_t.shape[0], rows), lambda b: (0, b)),
            row_spec,
            row_spec,
            pl.BlockSpec((rows, lanes), lambda b: (b, 0)),
        ],
        out_specs=[
            slot_spec,
            slot_spec,
            pl.BlockSpec((1, slots, rows), lambda b: (b, 0, 0)),
            pl.BlockSpec((1, slots, 1), lambda b: (b, 0, 0)),
        ],
        out_shape=[
            slot_shape,
            slot_shape,
            jax.ShapeDtypeStruct((groups, slots, rows), jnp.bfloat16),
            jax.ShapeDtypeStruct((groups, slots, 1), jnp.float32),
        ],
        compiler_params=pltpu.CompilerParams(vmem_limit_bytes=VMEM_BYTES),
        name="route",
    )(own_ids[:, None], routes_t, tokens, gradients, weights)


MIX_LAGS = (1, 3, 5, 7)


def mix_kernel(groups, chunks, names, *refs):
    ref = Bag(zip(names, refs))
    deep = groups // PAIR
    bf16, f32 = jnp.bfloat16, jnp.float32
    link = Link(deep)
    link.greet(groups, "eyc")
    blocks, slots, rows = ref.b_picks.shape
    sub = ref.o_dsecond.shape[0]
    width = ref.i_tokens.shape[1]
    units = ref.i_shared.shape[0] // 3
    loads = [bring(ref.i_picks, ref.b_picks, ref.load.at[0])]
    loads.append(bring(ref.i_shared, ref.b_shared, ref.load.at[1]))

    def fetch(b, at):
        span = pl.ds(pl.multiple_of(b * rows, rows), rows)
        return (
            pltpu.make_async_copy(ref.i_tokens.at[span, :], ref.b_x.at[at], ref.fetch.at[at, 0]),
            pltpu.make_async_copy(ref.i_gradients.at[span, :], ref.b_g.at[at], ref.fetch.at[at, 1]),
        )

    many = len(chunks)
    work = [(True, *chunk) for chunk in chunks] + [(False, *chunk) for chunk in chunks[:-1]]

    def source_of(n):
        back, left, wide = work[n]
        source = ref.i_back if back else ref.i_produced
        return pltpu.make_async_copy(
            source.at[:, :, pl.ds(left, wide)],
            ref.b_source.at[turn_of[n], :, :, pl.ds(0, wide)],
            ref.pull.at[turn_of[n]],
        )

    has_source = [n != many - 1 for n in range(len(work))]
    order = [n for n in range(many, len(work))] + [many - 1] + list(range(many - 1))
    turn_of = {n: i % 2 for i, n in enumerate(n for n in order if has_source[n])}
    for load in loads:
        load.wait()
    ref.b_acc[...] = jnp.zeros(ref.b_acc.shape, f32)

    def fetch_one(which, b, at):
        source, target, column = (
            (ref.i_tokens, ref.b_x, 0) if which == 0 else (ref.i_gradients, ref.b_g, 1)
        )
        span = pl.ds(pl.multiple_of(b * rows, rows), rows)
        return pltpu.make_async_copy(source.at[span, :], target.at[at], ref.fetch.at[at, column])

    def over_blocks(which, work):
        fetch_one(which, 0, 0).start()

        def one(b, carry):
            at = b % 2

            @pl.when(b + 1 < blocks)
            def _():
                fetch_one(which, b + 1, 1 - at).start()

            fetch_one(which, b, at).wait()
            work(b, at)
            return carry

        lax.fori_loop(0, blocks, one, 0)

    def forward_block(b, at):
        pre = matmul_nt(ref.b_x[at], ref.b_shared[: 2 * units, :])
        ref.b_pre[b] = pre
        ref.b_hidden[b] = swiglu(pre[:, :units], pre[:, units:])[1]

    def backward_block(b, at):
        pre = ref.b_pre[b]
        gate_pre, up_pre = pre[:, :units], pre[:, units:]
        dhidden = matmul_nt(ref.b_g[at], ref.b_shared[2 * units :, :])
        grads = swiglu_back(dhidden, gate_pre, up_pre, jax.nn.sigmoid(gate_pre))
        ref.b_both[b] = jnp.concatenate(grads, axis=1)

    def shared_gradients(b):
        at = b % 2
        if b + 1 < blocks:
            for copy in fetch(b + 1, 1 - at):
                copy.start()
        for copy in fetch(b, at):
            copy.wait()
        ref.b_acc[: 2 * units, :] += matmul_tn(ref.b_both[b], ref.b_x[at])
        ref.b_acc[2 * units :, :] += matmul_tn(ref.b_hidden[b], ref.b_g[at])

    source_of(order[0]).start()
    over_blocks(0, forward_block)
    dw_lane = lax.broadcasted_iota(jnp.int32, (slots, chunks[-1][1]), 1)
    tasks = []

    def step_at(moment):
        for lag in MIX_LAGS:
            if 0 <= moment - lag < len(tasks):
                next(tasks[moment - lag], None)

    pending = [n for n in order if has_source[n]]
    for n in order:
        back, left, wide = work[n]
        if has_source[n]:
            pending.pop(0)
            if pending:
                source_of(pending[0]).start()
            source_of(n).wait()

        def one(b, carry, n=n, back=back, left=left, wide=wide):
            picks = ref.b_picks[b]
            if not has_source[n]:
                values = matmul_tn(
                    picks, jnp.where(dw_lane == ref.i_lanes[...], ref.i_dweights[b], 0.0).astype(bf16)
                )
            else:
                span = slice(left, left + wide)
                values = matmul_tn(picks, ref.b_source[turn_of[n], b, :, :wide])
                if back:
                    values += matmul(ref.b_both[b], ref.b_shared[: 2 * units, span])
                else:
                    values += matmul(ref.b_hidden[b], ref.b_shared[2 * units :, span])
            values = values.astype(bf16)
            for y in range(PAIR):
                for c in range(PAIR):
                    q = y * PAIR + c
                    piece = values[q * sub : (q + 1) * sub, :]
                    ref["p%d" % n][c, b * PAIR + y] = piece
            return carry

        lax.fori_loop(0, blocks, one, 0)
        result = ref.o_dsecond if back else ref.o_mixed
        task = device_total(
            link,
            n % 2,
            ref["p%d" % n].at[link.c],
            ref["p%d" % n].at[1 - link.c],
            [ref["f%d_%d" % (n, k)] for k in range(4)],
            result.at[:, pl.ds(left, wide)],
            ref.send.at[n],
            ref.arrive.at[n],
        )
        tasks += begun([task])
        step_at(len(tasks) - 1)
        if n == many + 2:
            over_blocks(1, backward_block)
    for copy in fetch(0, 0):
        copy.start()
    share = -(-blocks // 4)
    for late in range(MIX_LAGS[-1]):
        step_at(len(order) + late)
        for b in range(late * share, min(blocks, (late + 1) * share)):
            shared_gradients(b)
        if late == 3:
            ref.b_grad[...] = ref.b_acc[...].astype(bf16)
            grad_out = bring(ref.b_grad, ref.o_shared, ref.load.at[0])
    link.drain()
    grad_out.wait()


def mix_bytes(groups, rows, slots, width):
    total = groups * rows * width * 2
    return 2 * total + 4 * rows * width * 2 * 2 + 2 * groups * max(rows, slots) * 512 * 2 * 2


def mix_stage(calls, groups, parts, picks, produced, back, dweights, lanes, tokens, gradients, shared):
    deep = groups // PAIR
    blocks, slots, rows = picks.shape
    width = tokens.shape[1]
    sub = rows // parts
    bf16, f32 = jnp.bfloat16, jnp.float32
    experts_wide = lanes[1]
    wide = min(512, width)
    chunks = [(left, wide) for left in range(0, width, wide)] + [(width, experts_wide)]
    inputs = Bag(
        i_picks=picks,
        i_produced=produced,
        i_back=back,
        i_dweights=dweights,
        i_lanes=lanes[0],
        i_tokens=tokens,
        i_gradients=gradients,
        i_shared=shared,
    )
    specs = [IN_VMEM if key in ("i_dweights", "i_lanes") else ANY for key in inputs]
    third = shared.shape[0] // 3
    scratch = Bag(
        b_picks=pltpu.VMEM(picks.shape, bf16),
        b_shared=pltpu.VMEM(shared.shape, bf16),
        b_x=pltpu.VMEM((2, rows, width), bf16),
        b_g=pltpu.VMEM((2, rows, width), bf16),
        b_acc=pltpu.VMEM(shared.shape, f32),
        b_grad=pltpu.VMEM(shared.shape, bf16),
        b_pre=pltpu.VMEM((blocks, rows, 2 * third), f32),
        b_hidden=pltpu.VMEM((blocks, rows, third), bf16),
        b_both=pltpu.VMEM((blocks, rows, 2 * third), bf16),
        b_source=pltpu.VMEM((2, blocks, slots, wide), bf16),
        load=DMA((2,)),
        fetch=DMA((2, 2)),
        pull=DMA((2,)),
        send=DMA((2 * len(chunks), total_hops(deep))),
        arrive=DMA((2 * len(chunks), total_hops(deep))),
    )
    for n, (_, columns) in enumerate(chunks + chunks[:-1]):
        scratch["p%d" % n] = pltpu.VMEM((PAIR, blocks * PAIR, sub, columns), bf16)
        for k, buffer in enumerate(total_buffers(deep, sub, columns)):
            scratch["f%d_%d" % (n, k)] = buffer
    names = list(inputs) + ["o_dsecond", "o_mixed", "o_shared"] + list(scratch)
    return pl.pallas_call(
        functools.partial(mix_kernel, groups, tuple(chunks), tuple(names)),
        in_specs=specs,
        out_specs=[IN_VMEM, IN_VMEM, ANY],
        out_shape=[
            jax.ShapeDtypeStruct((sub, width + experts_wide), f32),
            jax.ShapeDtypeStruct((sub, width), f32),
            jax.ShapeDtypeStruct(shared.shape, bf16),
        ],
        scratch_shapes=list(scratch.values()),
        compiler_params=calls.params(),
        name="mix",
    )(*inputs.values())


def advance(tasks, count=1):
    for _ in range(count):
        for task in tasks:
            next(task, None)


def begun(tasks):
    return [task for task in tasks if next(task, run) is not run]


def tensor_total(link, partial, from_beside, give, from_across, result, send, arrive):
    y, c = link.y, link.c

    def beside():
        return pltpu.make_async_remote_copy(
            src_ref=partial.at[:, 1 - c],
            dst_ref=from_beside,
            send_sem=send.at[0],
            recv_sem=arrive.at[0],
            device_id=link.peer("c"),
            device_id_type=MESH,
        )

    def across():
        return pltpu.make_async_remote_copy(
            src_ref=give,
            dst_ref=from_across,
            send_sem=send.at[1],
            recv_sem=arrive.at[1],
            device_id=link.peer("y"),
            device_id_type=MESH,
        )

    link.emit(beside)
    yield
    arrived(from_beside, arrive.at[0])
    rows = result.shape[0]

    def add_given(span):
        give[span, :] = partial[1 - y, c, span, :] + from_beside[1 - y, span, :]

    def add_kept(span):
        kept = partial[y, c, span, :].astype(jnp.float32)
        result[span, :] = kept + from_beside[y, span, :].astype(jnp.float32)

    def add_last(span):
        result[span, :] = result[span, :] + from_across[span, :].astype(jnp.float32)

    by_rows(rows, add_given)
    link.emit(across)
    by_rows(rows, add_kept)
    yield
    arrived(from_across, arrive.at[1])
    by_rows(rows, add_last)


def expert_total(link, axis, grad, from_twin, from_deep, result, send, arrive):
    deep, z, x = link.deep, link.z, link.x
    size = result.shape[axis]

    def target(k):
        return (z + k) % deep

    def to_twin(k):
        return pltpu.make_async_remote_copy(
            src_ref=slot(grad, axis, target(k) * PAIR + 1 - x, size),
            dst_ref=from_twin.at[k],
            send_sem=send.at[k],
            recv_sem=arrive.at[k],
            device_id=link.peer("x"),
            device_id_type=MESH,
        )

    def to_deep(k):
        return pltpu.make_async_remote_copy(
            src_ref=from_twin.at[k],
            dst_ref=from_deep.at[k - 1],
            send_sem=send.at[deep + k],
            recv_sem=arrive.at[deep + k],
            device_id=link.at_z(target(k)),
            device_id_type=MESH,
        )

    ks = list(range(1, deep)) + [0]
    for k in ks:
        link.emit(functools.partial(to_twin, k))
    for k in ks[:-1]:
        yield
        arrived(from_twin.at[k], arrive.at[k])
        mine = slot(grad, axis, target(k) * PAIR + x, size)

        def add(span, mine=mine, k=k):
            from_twin[k, span, :] = from_twin[k, span, :] + mine[span, :]

        by_rows(result.shape[0], add)
        link.emit(functools.partial(to_deep, k))
    yield
    arrived(from_twin.at[0], arrive.at[0])
    mine = slot(grad, axis, z * PAIR + x, size)

    def finish(span):
        total = mine[span, :].astype(jnp.float32) + from_twin[0, span, :].astype(jnp.float32)
        for k in range(1, deep):
            total = total + from_deep[k - 1, span, :].astype(jnp.float32)
        result[span, :] = total

    for k in range(1, deep):
        yield
        arrived(from_deep.at[k - 1], arrive.at[deep + k])
    by_rows(result.shape[0], finish)


def back_kernel(groups, sizes, reduced, names, *refs):
    ref = Bag(zip(names, refs))
    deep = groups // PAIR
    parts = PAIR * PAIR
    link = Link(deep)
    part = link.part
    bf16, f32 = jnp.bfloat16, jnp.float32
    link.greet(groups, "eyc")
    loading = {}
    for n, name in enumerate(n[2:] for n in names if n[:2] == "h_"):
        loading[name] = bring(ref["h_" + name], ref["l_" + name], ref.load.at[n])
    left = []

    def leave(name, source=None):
        source = ref["b_" + name] if source is None else source
        left.append(bring(source, ref["o_" + name], ref.leave.at[len(left)]))

    def ready(*which):
        for name in which:
            if name in loading:
                loading.pop(name).wait()
        return [ref["l_" + name] for name in which]

    rows_send, rows_arrive = ref.rows_send, ref.rows_arrive
    used = [0]

    def over_tensor(source, target, axis, size):
        row = used[0]
        used[0] += 1

        def home_of(sz, sx, sy, sc):
            return slot(target, axis, sy * PAIR + sc, size)

        n = len(placed)
        placed.append(bring(source, home_of(link.z, link.x, link.y, link.c), ref.place.at[n]))
        return spread(link, "yc", source, home_of, rows_send.at[row], rows_arrive.at[row])

    placed = []
    totals = {name: i for i, (name, _) in enumerate(reduced)}
    axis_of = dict(reduced)

    def over_expert(name):
        if name not in totals:
            leave(name)
            return
        i = totals[name]
        tasks = begun(
            [
                expert_total(
                    link,
                    axis_of[name],
                    ref["b_" + name],
                    ref["t_" + name],
                    ref["d_" + name],
                    ref["r_" + name],
                    ref.send.at[i],
                    ref.arrive.at[i],
                )
            ]
        )
        queue.extend([task, deep - 1] for task in tasks)

    queue, finishing = [], []

    def pump(count):
        while count and queue:
            entry = queue[0]
            next(entry[0], None)
            entry[1] -= 1
            count -= 1
            if not entry[1]:
                finishing.append(queue.pop(0)[0])

    shared_tasks = []
    if SHARED in axis_of:
        wide = ref.o_shared.shape[2]
        source = ref.i_shared
        shared_tasks = begun(
            [
                shuffle(
                    link,
                    groups,
                    lambda e: source.at[:, pl.ds(pl.multiple_of(e * wide, LANES), wide)],
                    lambda e: ref.o_shared.at[e],
                    ref.shared_send,
                    ref.shared_arrive,
                )
            ]
        )
        loading[OWN_SHARED] = bring(
            source.at[:, pl.ds(pl.multiple_of(link.me * wide, LANES), wide)],
            ref.k_shared,
            ref.place.at[len(placed)],
        )
        placed.append(None)

    sub, width = ref.i_middle.shape
    experts = ref.i_router.shape[0]
    norms = [ref.i_norms[i : i + 1, : size * groups] for i, size in enumerate(sizes)]
    sums = ref.b_sums
    sums[...] = jnp.zeros(sums.shape, f32)
    start = pl.multiple_of(part * sub, sub)

    def norm_back(which, values, cotangent):
        inverse = lax.rsqrt(jnp.mean(values * values, axis=-1, keepdims=True) + EPSILON)
        normed = values * inverse
        scaled = cotangent * norms[which]
        sums[which : which + 1, : values.shape[1]] += jnp.sum(
            cotangent * normed, axis=0, keepdims=True
        )
        back = inverse * (scaled - normed * jnp.mean(scaled * normed, axis=-1, keepdims=True))
        return (back, normed)

    def own_rows(span):
        return pl.ds(pl.multiple_of(start + span.start, 16), span.size)

    chosen = ref.i_chosen[:, :experts]
    dweights = ref.i_dsecond[:, width : width + experts]
    total = jnp.sum(chosen, axis=-1, keepdims=True)
    dchosen = (
        ROUTE_SCALE
        / total
        * (dweights - jnp.sum(dweights * chosen, axis=-1, keepdims=True) / total)
    )
    dlogits = (dchosen * chosen * (1.0 - chosen)).astype(bf16)
    ref.b_first_rows[...] = matmul(dlogits, ref.i_router[...])

    def middle_back(span):
        middle = ref.i_middle[span, :]
        dsecond = ref.i_dsecond[span, :width] + ref.b_first_rows[span, :]
        back, normed = norm_back(1, middle, dsecond)
        middle_grad = ref.i_out_grad[own_rows(span), :].astype(f32) + back
        ref.b_middle_grad[span, :] = middle_grad
        ref.b_grad_rows[span, :] = middle_grad.astype(bf16)
        ref.b_block_rows[span, :] = (middle + ref.i_mixed[span, :]).astype(bf16)
        ref.b_input_rows[span, :] = (normed * norms[1]).astype(bf16)

    by_rows(sub, middle_back)
    tensor_tasks = begun([over_tensor(ref.b_grad_rows, ref.b_attention_grad, 0, sub)])
    ref.b_router[...] = matmul_tn(dlogits, ref.b_input_rows[...]).astype(bf16)
    over_expert(ROUTER)
    run(tensor_tasks)
    block_tasks = begun([over_tensor(ref.b_block_rows, ref.o_block_out, 0, sub)])
    placed[1 if SHARED in axis_of else 0].wait()
    placed[1 if SHARED in axis_of else 0] = None

    attended, out_proj = ready(ATTENDED, OUT_PROJ)
    attention_grad = ref.b_attention_grad
    for at in range(0, attended.shape[1], 256):
        ref.b_out_proj[at : at + 256, :] = matmul_tn(
            attended[:, at : at + 256], attention_grad[...]
        ).astype(bf16)
    over_expert(OUT_PROJ)
    ref.b_attended_grad[...] = matmul_nt(attention_grad[...], out_proj[...]).astype(bf16)

    queries, keys, values = ready(QUERIES, KEYS, VALUES)
    heads, row_count, head_width = queries.shape
    cosine, sinusoid = ref.i_cosine[...], ref.i_sinusoid[...]
    dkey_rope = jnp.zeros((row_count, LANES), f32)
    scale = head_width ** (-0.5)
    filler = jnp.zeros((row_count, LANES - ROPE), f32)
    for h in range(heads):
        scores = matmul_nt(queries[h], keys[h]) * scale
        scores = jnp.where(ref.i_allowed[...] > 0, scores, -1e30)
        powers = jnp.exp(scores - jnp.max(scores, axis=-1, keepdims=True))
        probs = powers / jnp.sum(powers, axis=-1, keepdims=True)
        attended_grad = ref.b_attended_grad[:, h * VD : (h + 1) * VD]
        dvalues = matmul_tn(probs.astype(bf16), attended_grad)
        dprobs = matmul_nt(attended_grad, values[h])
        delta = jnp.sum(probs * dprobs, axis=-1, keepdims=True)
        dscores = (probs * (dprobs - delta) * scale).astype(bf16)
        dquery = matmul(dscores, keys[h])
        dkeys = matmul_tn(dscores, queries[h])
        rope = turn(jnp.concatenate([dquery[:, NOPE:], filler], axis=1), cosine, -sinusoid)
        pair = jnp.concatenate(
            [dquery[:, :NOPE], rope, jnp.zeros((row_count, LANES), f32)], axis=1
        )
        if h % 2 == 0:
            held = pair
        else:
            held = held + pltpu.roll(pair, head_width, 1)
            ref.b_dquery[:, (h - 1) * head_width : (h + 1) * head_width] = held.astype(bf16)
        dkey_rope = dkey_rope + jnp.concatenate([dkeys[:, NOPE:], filler], axis=1)
        base = h * (NOPE + VD)
        ref.b_dkeyval[:, base : base + NOPE] = dkeys[:, :NOPE].astype(bf16)
        ref.b_dkeyval[:, base + NOPE : base + NOPE + VD] = dvalues.astype(bf16)
        if h:
            pump(1)
    dkey_rope = turn(dkey_rope, cosine, -sinusoid)

    query_n, latent_n, query_up, latent_up = ready(QUERY_N, LATENT_N, QUERY_UP, LATENT_UP)
    query_rank, latent_rank = query_n.shape[1], latent_n.shape[1]

    def query_up_rows(span):
        ref.b_query_up[span, :] = matmul_tn(query_n[:, span], ref.b_dquery[...]).astype(bf16)

    rows_loop(query_rank, 256, query_up_rows)
    over_expert(QUERY_UP)
    for at in range(0, latent_rank, 256):
        ref.b_latent_up[at : at + 256, :] = matmul_tn(
            latent_n[:, at : at + 256], ref.b_dkeyval[...]
        ).astype(bf16)
    over_expert(LATENT_UP)
    partial = ref.b_heads_partial
    lead = query_rank + latent_rank
    for quarter in range(parts):
        span = slice(quarter * sub, (quarter + 1) * sub)
        at = (quarter // PAIR, quarter % PAIR)
        partial[(*at, slice(None), slice(0, query_rank))] = matmul_nt(
            ref.b_dquery[span, :], query_up[...]
        ).astype(bf16)
        partial[(*at, slice(None), slice(query_rank, lead))] = matmul_nt(
            ref.b_dkeyval[span, :], latent_up[...]
        ).astype(bf16)
        partial[(*at, slice(None), slice(lead, lead + LANES))] = dkey_rope[span, :].astype(bf16)
    sum_tasks = begun(
        [
            tensor_total(
                link,
                partial,
                ref.b_heads_beside,
                ref.b_heads_give,
                ref.b_heads_across,
                ref.b_heads_rows,
                ref.sum_send.at[0],
                ref.sum_arrive.at[0],
            )
        ]
    )
    pump(1)
    run(sum_tasks)

    heads_rows = ref.b_heads_rows
    (query_lat, latent_t) = ready(QUERY_LAT, LATENT_T)

    ref.b_latent_block[...] = latent_t[:latent_rank, :].astype(f32).T

    def latents_back(span):
        mine = own_rows(span)
        back, _ = norm_back(2, query_lat[mine, :].astype(f32), heads_rows[span, :query_rank])
        ref.b_query_rows[span, :] = back.astype(bf16)
        back, _ = norm_back(3, ref.b_latent_block[mine, :], heads_rows[span, query_rank:lead])
        ref.b_latent_rows[span, :latent_rank] = back.astype(bf16)
        ref.b_latent_rows[span, latent_rank:] = heads_rows[span, lead:].astype(bf16)

    by_rows(sub, latents_back)
    own = len(placed)
    tensor_tasks = begun(
        [
            over_tensor(ref.b_query_rows, ref.b_dquery_lat, 0, sub),
            over_tensor(ref.b_latent_rows, ref.b_dlatent_all, 0, sub),
        ]
    )
    pump(1)
    run(tensor_tasks)
    for n in (own, own + 1):
        placed[n].wait()
        placed[n] = None

    first, query_down, latent_down = ready(FIRST, QUERY_DOWN, LATENT_DOWN)
    query_cut, latent_cut = query_down.shape[1], latent_down.shape[0]
    dquery_lat = ref.b_dquery_lat[
        :, pl.ds(pl.multiple_of(part * query_cut, LANES), query_cut)
    ]
    ref.b_dlatent_t[...] = ref.b_dlatent_all[...].astype(f32).T
    dlatent_t = ref.b_dlatent_t[
        pl.ds(pl.multiple_of(part * latent_cut, 8), latent_cut), :
    ].astype(bf16)
    ref.b_dquery_cut[...] = dquery_lat

    def query_down_rows(span):
        ref.b_query_down[span, :] = matmul_tn(first[:, span], ref.b_dquery_cut[...]).astype(
            bf16
        )

    rows_loop(width, 256, query_down_rows)
    over_expert(QUERY_DOWN)
    for at in range(0, width, 512):
        ref.b_latent_down[:, at : at + 512] = matmul(dlatent_t, first[:, at : at + 512]).astype(
            bf16
        )
    over_expert(LATENT_DOWN)
    pump(1)
    partial = ref.b_first_partial
    for quarter in range(parts):
        span = slice(quarter * sub, (quarter + 1) * sub)
        partial[quarter // PAIR, quarter % PAIR] = (
            matmul_nt(dquery_lat[span], query_down[...])
            + matmul_tn(dlatent_t[:, span], latent_down[...])
        ).astype(bf16)
    sum_tasks = begun(
        [
            tensor_total(
                link,
                partial,
                ref.b_first_beside,
                ref.b_first_give,
                ref.b_first_across,
                ref.b_first_rows,
                ref.sum_send.at[1],
                ref.sum_arrive.at[1],
            )
        ]
    )
    pump(1)
    run(sum_tasks)

    def first_back(span):
        residual = ref.i_block[own_rows(span), :].astype(f32)
        back, _ = norm_back(0, residual, ref.b_first_rows[span, :])
        ref.b_input_rows[span, :] = (ref.b_middle_grad[span, :] + back).astype(bf16)

    by_rows(sub, first_back)
    input_tasks = begun([over_tensor(ref.b_input_rows, ref.o_input_grad, 0, sub)])
    wide = ref.b_gains.shape[1]
    for i, size in enumerate(sizes):
        span = size * groups
        total = jnp.broadcast_to(sums[i : i + 1, :span], (8, span))
        if span < wide:
            total = jnp.concatenate([total, jnp.zeros((8, wide - span), f32)], axis=1)
            span = wide
        for e in range(groups):
            if size % LANES == 0:
                moved = total[:1, e * size : (e + 1) * size]
                if size < wide:
                    moved = jnp.concatenate([moved, jnp.zeros((1, wide - size), f32)], axis=1)
            else:
                moved = (pltpu.roll(total, span - e * size, 1) if e else total)[:1, :wide]
            ref.b_gains[e * 8 + i : e * 8 + i + 1, :] = moved
    for e in range(groups):
        ref.b_gains[e * 8 + len(sizes) : e * 8 + 8, :] = jnp.zeros((8 - len(sizes), wide), f32)
    over_expert(GAINS)
    pump(len(queue) * deep)
    run(finishing)

    finished = ("o_query_down", "o_latent_down")
    finals = []
    for name, axis in ((QUERY_DOWN, 1), (LATENT_DOWN, 0), (ROUTER, 0), (GAINS, 0)):
        if name not in totals:
            continue
        share = ref["s_" + name]
        whole = ref["o_" + name] if "o_" + name in finished else ref["g_" + name]
        share[...] = ref["r_" + name][...].astype(share.dtype)
        finals.append(over_tensor(share, whole, axis, share.shape[axis]))
    finals = begun(finals)
    for name in (OUT_PROJ, QUERY_UP, LATENT_UP):
        if name in totals:
            leave(name, ref["r_" + name])
    if SHARED in axis_of:
        loading.pop(OWN_SHARED).wait()
        left.append(
            bring(ref.k_shared, ref.o_shared.at[link.me], ref.leave.at[len(left)])
        )
    run(finals)
    for move in placed:
        if move is not None:
            move.wait()
    for name in (ROUTER, GAINS):
        if name in totals:
            size = ref["s_" + name].shape[0]
            total = ref["g_" + name][:size, :]
            for t in range(1, parts):
                total = total + ref["g_" + name][t * size : (t + 1) * size, :]
            ref["f_" + name][...] = total
            leave(name, ref["f_" + name])
    run(block_tasks + input_tasks + shared_tasks)
    link.drain()
    for move in left:
        move.wait()


def back_stage(calls, groups, parts, sizes, held, small, grad_shared):
    deep = groups // PAIR
    bf16, f32 = jnp.bfloat16, jnp.float32
    rows, width = small.block.shape
    sub = rows // parts
    query_rank, latent_rank = held.query_n.shape[1], held.latent_n.shape[1]
    heads, _, head_width = held.queries.shape
    query_cut, latent_cut = held.query_down.shape[1], held.latent_down.shape[0]
    experts = small.router.shape[0]
    gain_wide = -(-max(sizes) // LANES) * LANES
    lead = query_rank + latent_rank + LANES
    half = parts // PAIR
    full = Bag(
        out_proj=(held.out_proj.shape, 1, bf16),
        query_up=(held.query_up.shape, 0, bf16),
        latent_up=(held.latent_up.shape, 0, bf16),
        query_down=((width, query_cut), 0, bf16),
        latent_down=((latent_cut, width), 1, bf16),
        router=((experts, width), 1, bf16),
        gains=((groups * 8, gain_wide), 0, f32),
    )
    reduced, pieces = [], {}
    for name, (shape, axis, dtype) in full.items():
        piece = list(shape)
        piece[axis] //= groups
        if aligned(piece[axis], 1) or axis == 0:
            reduced.append((name, axis))
            pieces[name] = tuple(piece)
    buffers = Bag(
        middle_grad=((sub, width), f32),
        sums=((8, width), f32),
        grad_rows=((sub, width), bf16),
        block_rows=((sub, width), bf16),
        attention_grad=((rows, width), bf16),
        attended_grad=(held.attended.shape, bf16),
        dquery=((rows, heads * head_width), bf16),
        dkeyval=((rows, heads * (NOPE + VD)), bf16),
        heads_partial=((half, PAIR, sub, lead), bf16),
        heads_beside=((half, sub, lead), bf16),
        heads_give=((sub, lead), bf16),
        heads_across=((sub, lead), bf16),
        heads_rows=((sub, lead), f32),
        query_rows=((sub, query_rank), bf16),
        latent_rows=((sub, latent_rank + LANES), bf16),
        latent_block=((rows, latent_rank), f32),
        dquery_lat=((rows, query_rank), bf16),
        dquery_cut=((rows, query_cut), bf16),
        dlatent_all=((rows, latent_rank + LANES), bf16),
        dlatent_t=((latent_rank + LANES, rows), f32),
        first_partial=((half, PAIR, sub, width), bf16),
        first_beside=((half, sub, width), bf16),
        first_give=((sub, width), bf16),
        first_across=((sub, width), bf16),
        first_rows=((sub, width), f32),
        input_rows=((sub, width), bf16),
    )
    for name, (shape, _, dtype) in full.items():
        buffers[name] = (shape, dtype)
    scratch = Bag(("b_" + name, pltpu.VMEM(*spec)) for name, spec in buffers.items())
    for name, array in held.items():
        scratch["l_" + name] = pltpu.VMEM(array.shape, array.dtype)
    outs = Bag(block_out=((rows, width), bf16), input_grad=((rows, width), bf16))
    for name, (shape, axis, dtype) in full.items():
        if name not in pieces:
            outs[name] = (shape, dtype)
            continue
        piece = pieces[name]
        scratch["t_" + name] = pltpu.VMEM((deep, *piece), dtype)
        scratch["d_" + name] = pltpu.VMEM((deep - 1, *piece), dtype)
        scratch["r_" + name] = pltpu.VMEM(piece, f32)
        outs[name] = (piece, f32)
        if name in (QUERY_DOWN, LATENT_DOWN, ROUTER, GAINS):
            kind = bf16 if name in (QUERY_DOWN, LATENT_DOWN) else f32
            along = 1 if name == QUERY_DOWN else 0
            whole = list(piece)
            whole[along] *= parts
            scratch["s_" + name] = pltpu.VMEM(piece, kind)
            if name in (QUERY_DOWN, LATENT_DOWN):
                outs[name] = (tuple(whole), bf16)
            else:
                scratch["g_" + name] = pltpu.VMEM(tuple(whole), kind)
                scratch["f_" + name] = pltpu.VMEM(piece, f32)
    share = grad_shared.shape[1] // groups
    inputs = {"i_" + name: array for name, array in small.items()}
    specs = [IN_VMEM] * len(small)
    if aligned(share, 1):
        reduced.append((SHARED, 1))
        inputs["i_shared"] = grad_shared
        specs.append(ANY)
        outs.shared = ((groups, grad_shared.shape[0], share), bf16)
        scratch.k_shared = pltpu.VMEM((grad_shared.shape[0], share), bf16)
        scratch.shared_send = scratch.shared_arrive = DMA((groups,))
    inputs |= {"h_" + name: array for name, array in held.items()}
    specs += [ANY] * len(held)
    scratch.load = DMA((len(held),))
    scratch.leave = DMA((len(outs) + 1,))
    scratch.place = DMA((12,))
    scratch.rows_send = scratch.rows_arrive = DMA((12, 8))
    scratch.send = scratch.arrive = DMA((len(full), 2 * deep))
    scratch.sum_send = scratch.sum_arrive = DMA((2, 2))
    names = list(inputs) + ["o_" + name for name in outs] + list(scratch)
    reduced = [entry for entry in reduced]
    results = pl.pallas_call(
        functools.partial(back_kernel, groups, tuple(sizes), tuple(reduced), tuple(names)),
        in_specs=specs,
        out_specs=[ANY] * len(outs),
        out_shape=[jax.ShapeDtypeStruct(*spec) for spec in outs.values()],
        scratch_shapes=list(scratch.values()),
        compiler_params=calls.params(),
        name="back",
    )(*inputs.values())
    results = Bag(zip(outs, results))
    for name, (shape, axis, dtype) in full.items():
        if name not in pieces:
            results[name] = scatter_sum(results[name], EXPERT, axis)
            if name == LATENT_DOWN:
                results[name] = gather(results[name].astype(bf16), TENSOR, 0).astype(f32)
            if name == ROUTER:
                results[name] = lax.psum(results[name].astype(bf16), TENSOR).astype(f32)
    if SHARED not in results:
        split = grad_shared.reshape(grad_shared.shape[0], groups, share).transpose(1, 0, 2)
        results.shared = lax.all_to_all(
            split, EXPERT, split_axis=0, concat_axis=0, tiled=True
        )
    return results


ALL = (EXPERT, TENSOR)


def gather(values, axes, dimension):
    return lax.all_gather(values, axes, axis=dimension, tiled=True)


def scatter_sum(values, axes, dimension):
    return lax.psum_scatter(
        values.astype(jnp.bfloat16), axes, scatter_dimension=dimension, tiled=True
    ).astype(jnp.float32)


def aligned(size, axis):
    return size % LANES == 0 if axis else size % 16 == 0


def ready_items(items, part):
    result = []
    for name, array, axis, cut, over, orders, home in items:
        if axis == 1 and array.shape[-1] % LANES:
            if over == SHUFFLE:
                array = lax.all_to_all(array, EXPERT, split_axis=0, concat_axis=0, tiled=True)
                array = array.transpose(1, 0, 2).reshape(array.shape[1], -1)
            else:
                if cut is not None:
                    array = lax.dynamic_slice_in_dim(array, part * cut[1], cut[1], axis=cut[0])
                array = gather(array, EXPERT, axis)
            cut, over, orders, home = None, READY, (), VMEM_
        result.append((name, array, axis, cut, over, orders, home))
    return result


def body(
    calls,
    block_in,
    attention_gain,
    query_down,
    query_gain,
    query_up,
    latent_down,
    latent_gain,
    latent_up,
    out_proj,
    ffn_gain,
    router,
    shared_gate,
    shared_up,
    shared_down,
    expert_gate,
    expert_up,
    expert_down,
    doc_lengths,
    routes,
    out_grad,
):
    groups = lax.axis_size(EXPERT)
    parts = lax.axis_size(TENSOR)
    me = lax.axis_index(EXPERT)
    part = lax.axis_index(TENSOR)
    row_count, width = block_in.shape
    top = routes.shape[1]
    local = expert_gate.shape[0]
    experts = local * groups

    all_gains = (attention_gain, ffn_gain, query_gain, latent_gain)
    gain_sizes = [g.shape[0] for g in all_gains]
    gain_wide = -(-max(gain_sizes) // LANES) * LANES
    gains = jnp.stack(
        [jnp.pad(g.astype(jnp.float32), (0, gain_wide - g.shape[0])) for g in all_gains]
    )
    gains = jnp.pad(gains, ((0, 8 - len(all_gains)), (0, 0)))
    routes_pad = jnp.pad(routes.T, ((0, -top % 8), (0, 0)), constant_values=-1)
    shared = jnp.stack([shared_gate.T, shared_up.T, shared_down])
    shared_units = shared.shape[1] // groups
    shared = shared.reshape(3, groups, shared_units, -1).transpose(1, 0, 2, 3)
    shared = shared.reshape(groups, 3 * shared_units, -1)
    query_cut = query_down.shape[1] // parts
    latent_cut = latent_down.shape[1] // parts
    allowed, cosine, sinusoid = layout(doc_lengths[0], row_count)
    allowed = allowed.astype(jnp.float32)
    tables = [
        jnp.pad(jnp.concatenate(pair, axis=1), ((0, 0), (0, LANES - ROPE)))
        for pair in ((cosine, cosine), (-sinusoid, sinusoid))
    ]
    items = [
        (GAINS, gains, 0, None, EXPERT, ("e",), VMEM_),
        (QUERY_DOWN, query_down, 0, (1, query_cut), EXPERT, ("zx",), VMEM_),
        (LATENT_DOWN, latent_down.T, 1, (0, latent_cut), EXPERT, ("zx",), VMEM_),
        (QUERY_UP, query_up, 0, None, EXPERT, ("zx",), VMEM_),
        (LATENT_UP, latent_up, 0, None, EXPERT, ("zx",), VMEM_),
        (OUT_PROJ, out_proj, 1, None, EXPERT, ("zx",), VMEM_),
        (ROUTER, router.T, 1, None, EXPERT, ("zx",), VMEM_),
        (ROUTES, routes_pad, 1, None, EXPERT, ("e",), "hbm"),
        (SHARED, shared, 1, None, SHUFFLE, (), "hbm"),
        (OUT_GRAD, out_grad, 0, (0, row_count // parts), "all", (ZXYC, "xzyc"), "hbm"),
    ]
    front = front_stage(
        calls,
        groups,
        parts,
        gain_sizes,
        ready_items(items, part),
        block_in,
        routes,
        allowed,
        *tables,
    )
    router_t = front.router
    shared = front.shared
    tokens, gradients = front.tokens, front.out_grad
    lane_pad = -experts % LANES
    own_ids = me * local + jnp.arange(local, dtype=jnp.int32)
    expert_rows, expert_grads, picks, slot_weights = route_stage(
        groups, own_ids, front.routes, tokens, gradients, front.weights
    )
    slot_shape = (groups, local, CAP)
    produced, back_rows, slot_dweights, grad_gate, grad_up, grad_down = expert_stage(
        expert_rows.reshape(*slot_shape, width),
        expert_grads.reshape(*slot_shape, width),
        slot_weights.reshape(*slot_shape, 1),
        expert_gate.transpose(0, 2, 1),
        expert_up.transpose(0, 2, 1),
        expert_down,
    )
    slots = local * CAP
    produced = produced.reshape(groups, slots, width)
    back_rows = back_rows.reshape(groups, slots, width)
    slot_dweights = slot_dweights.reshape(groups, slots, 1)
    slot_lanes = jnp.repeat(own_ids, CAP)[:, None]
    if mix_bytes(groups, row_count, slots, width) < 40 * 2**20:
        dsecond, mixed, grad_shared = mix_stage(
            calls,
            groups,
            parts,
            picks,
            produced,
            back_rows,
            slot_dweights,
            (slot_lanes, experts + lane_pad),
            tokens,
            gradients,
            shared,
        )
    else:
        lane_ids = jnp.arange(experts + lane_pad, dtype=jnp.int32)
        spread_out = jnp.where(slot_lanes == lane_ids[None, :], slot_dweights, 0.0)
        mixed_part, dsecond_part, grad_shared = combine_stage(
            picks,
            produced,
            back_rows,
            spread_out.astype(jnp.bfloat16),
            tokens.reshape(groups, row_count, width),
            gradients.reshape(groups, row_count, width),
            shared.reshape(3, shared_units, width),
        )
        grad_shared = grad_shared.astype(jnp.bfloat16).reshape(3 * shared_units, width)
        dsecond, mixed = sum_all(
            calls,
            groups,
            parts,
            (
                dsecond_part.reshape(-1, width + experts + lane_pad),
                mixed_part.reshape(-1, width),
            ),
        )
    held = Bag(
        (name, front[name])
        for name in (
            ATTENDED,
            OUT_PROJ,
            QUERIES,
            KEYS,
            VALUES,
            QUERY_N,
            LATENT_N,
            QUERY_UP,
            LATENT_UP,
            QUERY_LAT,
            LATENT_T,
            FIRST,
            QUERY_DOWN,
            LATENT_DOWN,
        )
    )
    small = Bag(
        dsecond=dsecond,
        mixed=mixed,
        middle=front.middle,
        chosen=front.chosen,
        router=router_t,
        out_grad=out_grad,
        block=block_in,
        allowed=allowed,
        cosine=tables[0],
        sinusoid=tables[1],
        norms=front.norms,
    )
    back = back_stage(calls, groups, parts, gain_sizes, held, small, grad_shared)
    grad_shared = back.shared.reshape(groups, 3, shared_units, -1).transpose(1, 0, 2, 3)
    grad_shared = grad_shared.astype(jnp.float32).reshape(3, groups * shared_units, -1)
    grad_gains = [back.gains[i, :size] for i, size in enumerate(gain_sizes)]

    return (
        back.block_out,
        back.input_grad,
        grad_gains[0],
        back.query_down.astype(jnp.float32),
        grad_gains[2],
        back.query_up,
        back.latent_down.T.astype(jnp.float32),
        grad_gains[3],
        back.latent_up,
        back.out_proj,
        grad_gains[1],
        back.router.T,
        grad_shared[0].T,
        grad_shared[1].T,
        grad_shared[2],
        grad_gate.transpose(0, 2, 1),
        grad_up.transpose(0, 2, 1),
        grad_down,
    )


def solution(mesh):
    placed = (
        P(EXPERT, None),
        P(EXPERT),
        P(EXPERT, None),
        P(EXPERT),
        P(EXPERT, TENSOR),
        P(EXPERT, None),
        P(EXPERT),
        P(EXPERT, TENSOR),
        P(TENSOR, EXPERT),
        P(EXPERT),
        P(EXPERT, None),
        P(EXPERT, TENSOR),
        P(EXPERT, TENSOR),
        P(TENSOR, EXPERT),
        P(EXPERT, None, TENSOR),
        P(EXPERT, None, TENSOR),
        P(EXPERT, TENSOR, None),
        P(EXPERT, None),
        P(EXPERT, None),
        P(EXPERT, None),
    )
    return jax.shard_map(
        functools.partial(body, Calls()),
        mesh=mesh,
        in_specs=placed,
        out_specs=(
            P(EXPERT, None),
            P(EXPERT, None),
            P(EXPERT),
            P(EXPERT, None),
            P(EXPERT),
            P(EXPERT, TENSOR),
            P(EXPERT, None),
            P(EXPERT),
            P(EXPERT, TENSOR),
            P(TENSOR, EXPERT),
            P(EXPERT),
            P(EXPERT, None),
            P(EXPERT, TENSOR),
            P(EXPERT, TENSOR),
            P(TENSOR, EXPERT),
            P(EXPERT, None, TENSOR),
            P(EXPERT, None, TENSOR),
            P(EXPERT, TENSOR, None),
        ),
        check_vma=False,
    )
```

```python
import functools
import math

import jax
import jax.numpy as jnp
from jax import lax
from jax.experimental import pallas as pl
from jax.experimental.pallas import tpu as pltpu
from jax.sharding import PartitionSpec as P

NOPE = 128
ROPE = 64
VD = 128
CAP = 32
LANES = 128
VMEM_BYTES = 60 * 2**20

EPSILON = 1e-06
ROPE_BASE = 50000.0
ROUTE_SCALE = 2.446

ATTENDED = "attended"
EXPERT = "expert"
FIRST = "first"
GAINS = "gains"
KEYS = "keys"
LATENT_DOWN = "latent_down"
LATENT_N = "latent_n"
LATENT_T = "latent_t"
LATENT_UP = "latent_up"
OUT_GRAD = "out_grad"
OUT_PROJ = "out_proj"
OWN_SHARED = "own_shared"
QUERIES = "queries"
QUERY_DOWN = "query_down"
QUERY_LAT = "query_lat"
QUERY_N = "query_n"
QUERY_UP = "query_up"
READY = "ready"
ROUTER = "router"
ROUTES = "routes"
SHARED = "shared"
SHUFFLE = "shuffle"
TENSOR = "tensor"
TOKENS = "tokens"
VALUES = "values"
VMEM_ = "vmem"
WEIGHTS = "weights"
ZXYC = "zxyc"


def matmul(left, right):
    return jnp.dot(left, right, preferred_element_type=jnp.float32)


def contract(form, left, right):
    return jnp.einsum(form, left, right, preferred_element_type=jnp.float32)


def matmul_nt(left, right):
    return lax.dot_general(left, right, (((1,), (1,)), ((), ())), preferred_element_type=jnp.float32)


def matmul_tn(left, right):
    return lax.dot_general(left, right, (((0,), (0,)), ((), ())), preferred_element_type=jnp.float32)


def layout(lengths, row_count):
    doc_count = lengths.shape[0]
    doc_ends = jnp.cumsum(lengths)
    starts = doc_ends - lengths
    row_index = jnp.arange(row_count, dtype=jnp.int32)
    doc_ids = jnp.sum((row_index[:, None] >= doc_ends[None, :]).astype(jnp.int32), axis=1)
    owners = doc_ids[:, None] == jnp.arange(doc_count, dtype=jnp.int32)[None, :]
    first_row = jnp.sum(jnp.where(owners, starts[None, :], 0), axis=1)
    positions = (row_index - first_row).astype(jnp.float32)
    allowed = (doc_ids[:, None] == doc_ids[None, :]) & (row_index[None, :] <= row_index[:, None])
    frequency = jnp.exp(
        -math.log(ROPE_BASE) * 2.0 * jnp.arange(ROPE // 2, dtype=jnp.float32) / ROPE
    )
    angles = positions[:, None] * frequency[None, :]
    return (allowed, jnp.cos(angles), jnp.sin(angles))


def swiglu(gate_pre, up_pre):
    sigmoid_gate = jax.nn.sigmoid(gate_pre)
    return (sigmoid_gate, (gate_pre * sigmoid_gate * up_pre).astype(jnp.bfloat16))


def swiglu_back(dhidden, gate_pre, up_pre, sigmoid_gate):
    gate_grad = dhidden * up_pre * sigmoid_gate * (1.0 + gate_pre * (1.0 - sigmoid_gate))
    up_grad = dhidden * gate_pre * sigmoid_gate
    return (gate_grad.astype(jnp.bfloat16), up_grad.astype(jnp.bfloat16))


def expert_kernel(
    x_ref, g_ref, w_ref, gate_ref, up_ref, down_ref, y_ref, dr_ref, dw_ref, gg_ref, gu_ref, gd_ref
):
    blocks, _, cap, width = x_ref.shape
    rows = blocks * cap
    row_inputs = x_ref[...].reshape(rows, width)
    gradient = g_ref[...].reshape(rows, width).astype(jnp.float32)
    weight = w_ref[...].reshape(rows, 1)
    gate, up, down = gate_ref[0], up_ref[0], down_ref[0]
    gate_pre = matmul_nt(row_inputs, gate)
    up_pre = matmul_nt(row_inputs, up)
    sigmoid_gate, hidden = swiglu(gate_pre, up_pre)
    produced = matmul(hidden, down)
    dw_ref[...] = jnp.sum(gradient * produced, axis=1, keepdims=True).reshape(dw_ref.shape)
    y_ref[...] = (weight * produced).astype(jnp.bfloat16).reshape(y_ref.shape)
    cotangent = (weight * gradient).astype(jnp.bfloat16)
    dhidden = matmul_nt(cotangent, down)
    gate_grad, up_grad = swiglu_back(dhidden, gate_pre, up_pre, sigmoid_gate)
    back = matmul(gate_grad, gate) + matmul(up_grad, up)
    dr_ref[...] = back.astype(jnp.bfloat16).reshape(dr_ref.shape)
    first = pl.program_id(1) == 0

    def accumulate(ref, left, right):
        part = matmul_tn(left, right)

        @pl.when(first)
        def _():
            ref[0] = part

        @pl.when(jnp.logical_not(first))
        def _():
            ref[0] += part

    accumulate(gg_ref, gate_grad, row_inputs)
    accumulate(gu_ref, up_grad, row_inputs)
    accumulate(gd_ref, hidden, cotangent)


def expert_stage(row_inputs, gradients, weights, gate_t, up_t, down):
    blocks, local, cap, width = row_inputs.shape
    units = gate_t.shape[1]
    step = min(blocks, 256 // cap)
    rows_spec = pl.BlockSpec((step, 1, cap, width), lambda j, r: (r, j, 0, 0))
    slot_spec = pl.BlockSpec((step, 1, cap, 1), lambda j, r: (r, j, 0, 0))
    unit_spec = pl.BlockSpec((1, units, width), lambda j, r: (j, 0, 0))
    rows_shape = jax.ShapeDtypeStruct(row_inputs.shape, jnp.bfloat16)
    unit_shape = jax.ShapeDtypeStruct((local, units, width), jnp.float32)
    flops = 18 * blocks * local * cap * width * units
    moved = 8 * blocks * local * cap * width + 18 * local * units * width
    return pl.pallas_call(
        expert_kernel,
        grid=(local, blocks // step),
        in_specs=[rows_spec, rows_spec, slot_spec, unit_spec, unit_spec, unit_spec],
        out_specs=[rows_spec, rows_spec, slot_spec, unit_spec, unit_spec, unit_spec],
        out_shape=[
            rows_shape,
            rows_shape,
            jax.ShapeDtypeStruct((blocks, local, cap, 1), jnp.float32),
            unit_shape,
            unit_shape,
            unit_shape,
        ],
        compiler_params=pltpu.CompilerParams(vmem_limit_bytes=VMEM_BYTES),
        cost_estimate=pl.CostEstimate(flops=flops, bytes_accessed=moved, transcendentals=0),
        name="experts",
    )(row_inputs, gradients, weights, gate_t, up_t, down)


def combine_kernel(
    p_ref, y_ref, dr_ref, dw_ref, x_ref, g_ref, shared_ref, out_ref, ds_ref, grad_ref
):
    picks = p_ref[0]
    row_inputs, cotangent = x_ref[0], g_ref[0]
    gate, up, down = shared_ref[0], shared_ref[1], shared_ref[2]
    gate_pre = matmul_nt(row_inputs, gate)
    up_pre = matmul_nt(row_inputs, up)
    sigmoid_gate, hidden = swiglu(gate_pre, up_pre)
    out_ref[0] = (matmul_tn(picks, y_ref[0]) + matmul(hidden, down)).astype(jnp.bfloat16)
    dhidden = matmul_nt(cotangent, down)
    gate_grad, up_grad = swiglu_back(dhidden, gate_pre, up_pre, sigmoid_gate)
    back = matmul_tn(picks, dr_ref[0]) + matmul(gate_grad, gate) + matmul(up_grad, up)
    width = back.shape[1]
    ds_ref[0, :, :width] = back.astype(jnp.bfloat16)
    ds_ref[0, :, width:] = matmul_tn(picks, dw_ref[0]).astype(jnp.bfloat16)
    first = pl.program_id(0) == 0
    for index, (left, right) in enumerate(
        ((gate_grad, row_inputs), (up_grad, row_inputs), (hidden, cotangent))
    ):
        part = matmul_tn(left, right)

        @pl.when(first)
        def _(index=index, part=part):
            grad_ref[index] = part

        @pl.when(jnp.logical_not(first))
        def _(index=index, part=part):
            grad_ref[index] += part


def combine_stage(picks, produced, back, spread, tokens, gradients, shared):
    blocks, slots, rows = picks.shape
    width = tokens.shape[-1]
    slot_spec = pl.BlockSpec((1, slots, width), lambda b: (b, 0, 0))
    rows_spec = pl.BlockSpec((1, rows, width), lambda b: (b, 0, 0))
    whole = pl.BlockSpec(shared.shape, lambda b: (0, 0, 0))
    lanes = spread.shape[-1]
    units = shared.shape[1]
    flops = 4 * blocks * slots * rows * width + 18 * blocks * rows * width * units
    moved = 4 * blocks * slots * width + 8 * blocks * rows * width
    return pl.pallas_call(
        combine_kernel,
        grid=(blocks,),
        in_specs=[
            pl.BlockSpec((1, slots, rows), lambda b: (b, 0, 0)),
            slot_spec,
            slot_spec,
            pl.BlockSpec((1, slots, lanes), lambda b: (b, 0, 0)),
            rows_spec,
            rows_spec,
            whole,
        ],
        out_specs=[
            rows_spec,
            pl.BlockSpec((1, rows, width + lanes), lambda b: (b, 0, 0)),
            whole,
        ],
        out_shape=[
            jax.ShapeDtypeStruct((blocks, rows, width), jnp.bfloat16),
            jax.ShapeDtypeStruct((blocks, rows, width + lanes), jnp.bfloat16),
            jax.ShapeDtypeStruct(shared.shape, jnp.float32),
        ],
        compiler_params=pltpu.CompilerParams(vmem_limit_bytes=VMEM_BYTES),
        cost_estimate=pl.CostEstimate(flops=flops, bytes_accessed=moved, transcendentals=0),
        name="combine",
    )(picks, produced, back, spread, tokens, gradients, shared)


MESH = pl.DeviceIdType.MESH
PAIR = 2
ANY = pl.BlockSpec(memory_space=pl.ANY)
IN_VMEM = pl.BlockSpec(memory_space=pltpu.VMEM)
DMA = pltpu.SemaphoreType.DMA


def place():
    me, part = lax.axis_index(EXPERT), lax.axis_index(TENSOR)
    return (me // PAIR, me % PAIR, part // PAIR, part % PAIR)


def device(z, x, y, c):
    return {EXPERT: z * PAIR + x, TENSOR: y * PAIR + c}


def greet(peers):
    barrier = pltpu.get_barrier_semaphore()
    for peer in peers:
        pl.semaphore_signal(barrier, inc=1, device_id=peer, device_id_type=MESH)
    pl.semaphore_wait(barrier, len(peers))


def push(source, target, send, arrive, peer):
    copy = pltpu.make_async_remote_copy(
        src_ref=source,
        dst_ref=target,
        send_sem=send,
        recv_sem=arrive,
        device_id=peer,
        device_id_type=MESH,
    )
    copy.start()
    return copy


def bring(source, target, done):
    copy = pltpu.make_async_copy(source, target, done)
    copy.start()
    return copy


def arrived(target, done):
    pltpu.make_async_copy(target, target, done).wait()


def slot(ref, axis, index, size):
    start = pl.multiple_of(index * size, size)
    if axis == 0:
        return ref.at[pl.ds(start, size), :]
    return ref.at[:, pl.ds(start, size)]


class Bag(dict):
    __getattr__ = dict.__getitem__
    __setattr__ = dict.__setitem__


class Calls:
    def __init__(self):
        self.count = 0

    def params(self):
        self.count += 1
        return pltpu.CompilerParams(
            collective_id=self.count, has_side_effects=True, vmem_limit_bytes=VMEM_BYTES
        )


def choose(table, index):
    value = table[0]
    for i, entry in enumerate(table[1:], 1):
        if any(entry != other for other in table):
            value = jnp.where(index == i, entry, value)
    return value


class Link:
    def __init__(self, deep):
        me, part = lax.axis_index(EXPERT), lax.axis_index(TENSOR)
        self.deep, self.me, self.part = deep, me, part
        self.z, self.x = me // PAIR, me % PAIR
        self.y, self.c = part // PAIR, part % PAIR
        near = [
            sorted((k for k in range(1, deep)), key=lambda k: abs((z - k) % deep - z))
            for z in range(deep)
        ]
        self.order = [choose([near[z][h] for z in range(deep)], self.z) for h in range(deep - 1)]
        self.drains = []

    def at_z(self, z):
        return device(z, self.x, self.y, self.c)

    def peer(self, axis):
        flip = {name: 1 - getattr(self, name) if name == axis else getattr(self, name) for name in "xyc"}
        return device(self.z, flip["x"], flip["y"], flip["c"])

    def greet(self, groups, axes):
        peers = [{EXPERT: (self.me + j) % groups, TENSOR: self.part} for j in range(1, groups)]
        if "e" not in axes:
            peers = []
        greet(peers + [self.peer(axis) for axis in axes if axis != "e"])

    def emit(self, make, condition=None):
        def start():
            make().start()

        def finish():
            make().wait_send()

        if condition is None:
            start()
            self.drains.append(finish)
        else:
            pl.when(condition)(start)
            self.drains.append(lambda: pl.when(condition)(finish))

    def drain(self):
        for finish in self.drains:
            finish()
        self.drains = []


def spread(link, order, source, at, send, arrive):
    deep, z = link.deep, link.z
    cut = order.find("z")
    before, after = (order[:cut], order[cut + 1 :]) if cut >= 0 else ("", order)
    none = frozenset()

    def piece(k, flips):
        x, y, c = (
            1 - getattr(link, name) if name in flips else getattr(link, name) for name in "xyc"
        )
        return at((z + deep - k) % deep, x, y, c)

    def number(k, flips):
        return k * 8 + sum(1 << "xyc".index(name) for name in flips)

    def forward(k, flips, to_number, peer, condition=None):
        own = isinstance(k, int) and k == 0 and not flips

        def make():
            target = piece(k, flips)
            return pltpu.make_async_remote_copy(
                src_ref=source if own else target,
                dst_ref=target,
                send_sem=send.at[to_number],
                recv_sem=arrive.at[to_number],
                device_id=peer,
                device_id_type=MESH,
            )

        link.emit(make, condition)

    def hand_on(k, flips, axes, along_z):
        if along_z:
            forward(k, flips, number(1, flips), link.at_z(z + 1), z < deep - 1)
            forward(k, flips, number(deep - 1, flips), link.at_z(z - 1), z > 0)
        for axis in axes:
            forward(k, flips, number(k, flips | {axis}), link.peer(axis))

    def take(k, flips):
        arrived(piece(k, flips), arrive.at[number(k, flips)])

    hand_on(0, none, before + after, cut >= 0)
    got = [none]
    for i, axis in enumerate(before):
        for flips in got:
            yield
            take(0, flips | {axis})
            hand_on(0, flips | {axis}, before[i + 1 :] + after, True)
        got = got + [flips | {axis} for flips in got]
    ks = [0]
    if cut >= 0:
        for k in link.order:
            below = z >= k
            onward = jnp.where(below, k + 1, k - 1)
            more = jnp.where(below, z < deep - 1, z > 0)
            following = link.at_z(jnp.where(below, z + 1, z - 1))
            for flips in got:
                yield
                take(k, flips)
                forward(k, flips, number(onward, flips), following, more)
                hand_on(k, flips, after, False)
        ks = ks + link.order
    for i, axis in enumerate(after):
        for k in ks:
            for flips in got:
                yield
                take(k, flips | {axis})
                hand_on(k, flips | {axis}, after[i + 1 :], False)
        got = got + [flips | {axis} for flips in got]


def shuffle(link, groups, source, at, send, arrive):
    def make(j):
        target = (link.me + j) % groups
        return pltpu.make_async_remote_copy(
            src_ref=source(target),
            dst_ref=at(link.me),
            send_sem=send.at[j],
            recv_sem=arrive.at[j],
            device_id={EXPERT: target, TENSOR: link.part},
            device_id_type=MESH,
        )

    for j in range(1, groups):
        link.emit(functools.partial(make, j))
    for j in range(1, groups):
        yield
        arrived(at((link.me + groups - j) % groups), arrive.at[j])


def run(tasks):
    tasks = list(tasks)
    while tasks:
        tasks = [task for task in tasks if next(task, run) is not run]


def add_rows(count, store):
    lax.fori_loop(0, count, lambda i, carry: (store(i), carry)[1], 0)


def sum_all_kernel(deep, chunks, count, *refs):
    partials, outs = refs[:count], refs[count : 2 * count]
    total = len(chunks)
    rest = refs[2 * count :]
    own_buf, from_core = rest[:total], rest[total : 2 * total]
    from_first, from_second = rest[2 * total : 3 * total], rest[3 * total : 4 * total]
    from_deep = rest[4 * total : 5 * total]
    send, arrive, own = rest[5 * total :]
    z, x, y, c = place()
    others = [device((z + k) % deep, x, y, c) for k in range(1, deep)]
    twin, across, beside = (
        device(z, 1 - x, y, c),
        device(z, x, 1 - y, c),
        device(z, x, y, 1 - c),
    )
    greet(others + [twin, across, beside])
    copies, loads = [], []
    for n, (i, left, wide, order) in enumerate(chunks):
        span = pl.ds(left, wide)
        copies.append(
            push(
                partials[i].at[:, 1 - c, :, span],
                from_core[n],
                send.at[n, 0],
                arrive.at[n, 0],
                beside,
            )
        )
        loads.append(bring(partials[i].at[:, c, :, span], own_buf[n], own.at[n]))

    def index(order, depth, on_first, on_second):
        on_x, on_y = (on_first, on_second) if order == 0 else (on_second, on_first)
        return (depth * PAIR + on_x) * PAIR + on_y

    def stage_core(n):
        _, _, _, order = chunks[n]
        buf, other = own_buf[n], from_core[n]
        loads[n].wait()
        arrived(other, arrive.at[n, 0])

        def add(k):
            buf[k] = (buf[k].astype(jnp.float32) + other[k].astype(jnp.float32)).astype(
                jnp.bfloat16
            )

        add_rows(deep * PAIR * PAIR, add)
        mine = x if order == 0 else y
        for depth in range(deep):
            for s in range(PAIR):
                number = 1 + depth * PAIR + s
                copies.append(
                    push(
                        buf.at[index(order, depth, 1 - mine, s)],
                        from_first[n].at[depth * PAIR + s],
                        send.at[n, number],
                        arrive.at[n, number],
                        twin if order == 0 else across,
                    )
                )

    def stage_first(n):
        _, _, _, order = chunks[n]
        buf, other = own_buf[n], from_first[n]
        mine, following = (x, y) if order == 0 else (y, x)
        for number in range(1, 1 + PAIR * deep):
            arrived(other.at[number - 1], arrive.at[n, number])

        def add(k):
            at = index(order, k // PAIR, mine, k % PAIR)
            buf[at] = (buf[at].astype(jnp.float32) + other[k].astype(jnp.float32)).astype(
                jnp.bfloat16
            )

        add_rows(deep * PAIR, add)
        for depth in range(deep):
            number = 1 + PAIR * deep + depth
            copies.append(
                push(
                    buf.at[index(order, depth, mine, 1 - following)],
                    from_second[n].at[depth],
                    send.at[n, number],
                    arrive.at[n, number],
                    across if order == 0 else twin,
                )
            )

    def stage_second(n):
        _, _, _, order = chunks[n]
        buf, other = own_buf[n], from_second[n]
        mine, following = (x, y) if order == 0 else (y, x)
        base = 1 + PAIR * deep
        for depth in range(deep):
            arrived(other.at[depth], arrive.at[n, base + depth])

        def add(k):
            at = index(order, k, mine, following)
            buf[at] = (buf[at].astype(jnp.float32) + other[k].astype(jnp.float32)).astype(
                jnp.bfloat16
            )

        add_rows(deep, add)
        for k in range(1, deep):
            number = base + deep + k - 1
            copies.append(
                push(
                    buf.at[index(order, (z + k) % deep, mine, following)],
                    from_deep[n].at[k - 1],
                    send.at[n, number],
                    arrive.at[n, number],
                    others[k - 1],
                )
            )

    def stage_deep(n):
        i, left, wide, order = chunks[n]
        base = 1 + PAIR * deep + deep
        for k in range(1, deep):
            arrived(from_deep[n].at[k - 1], arrive.at[n, base + k - 1])
        mine, following = (x, y) if order == 0 else (y, x)
        result = own_buf[n][index(order, z, mine, following)].astype(jnp.float32)
        for k in range(deep - 1):
            result = result + from_deep[n][k].astype(jnp.float32)
        outs[i][:, pl.ds(left, wide)] = result

    for step in range(total + 3):
        for lag, stage in enumerate((stage_core, stage_first, stage_second, stage_deep)):
            if 0 <= step - lag < total:
                stage(step - lag)
    for copy in copies:
        copy.wait_send()


def sum_all(calls, groups, parts, arrays):
    deep = groups // PAIR
    rows = arrays[0].shape[0] // (groups * parts)
    budget, calls_of, used = 46 * 2**20, [[]], 0
    number = 0
    for i, array in enumerate(arrays):
        left = 0
        while left < array.shape[1]:
            wide = min(512, array.shape[1] - left)
            if 0 < array.shape[1] - left - wide < 512 // 2:
                wide = array.shape[1] - left
            cost = 2 * rows * wide * (4 * deep * 2 + 2 * deep + deep + deep) + 4 * rows * wide
            if used + cost > budget:
                calls_of.append([])
                used = 0
            used += cost
            calls_of[-1].append((i, left, wide, number % 2))
            number += 1
            left += wide
    views = [a.reshape(groups * parts // PAIR, PAIR, rows, a.shape[1]) for a in arrays]
    pieces = [[] for _ in arrays]
    for chunks in calls_of:
        used_arrays = sorted({c[0] for c in chunks})
        bounds = {
            i: (min(c[1] for c in chunks if c[0] == i), sum(c[2] for c in chunks if c[0] == i))
            for i in used_arrays
        }
        local = [(used_arrays.index(i), left, wide, order) for i, left, wide, order in chunks]
        count = len(used_arrays)
        many = deep * PAIR * PAIR

        def bufs(n):
            return [pltpu.VMEM((n, rows, wide), jnp.bfloat16) for _, _, wide, _ in chunks]

        sems = DMA((len(chunks), 1 + PAIR * deep + deep + deep))
        outs = pl.pallas_call(
            functools.partial(
                sum_all_kernel,
                deep,
                tuple(local),
                count,
            ),
            in_specs=[ANY] * count,
            out_specs=[IN_VMEM] * count,
            out_shape=[
                jax.ShapeDtypeStruct((rows, arrays[i].shape[1]), jnp.float32)
                for i in used_arrays
            ],
            scratch_shapes=bufs(many)
            + bufs(many)
            + bufs(PAIR * deep)
            + bufs(deep)
            + bufs(deep - 1)
            + [sems, sems, DMA((len(chunks),))],
            compiler_params=calls.params(),
            name="sum_all",
        )(*[views[i] for i in used_arrays])
        for i, out in zip(used_arrays, outs):
            pieces[i].append(out[:, bounds[i][0] : bounds[i][0] + bounds[i][1]])
    return [p[0] if len(p) == 1 else jnp.concatenate(p, axis=1) for p in pieces]


def swap_halves(values, half):
    lane = lax.broadcasted_iota(jnp.int32, values.shape, 1)
    wide = values.shape[1]
    return jnp.where(
        lane < half, pltpu.roll(values, wide - half, 1), pltpu.roll(values, half, 1)
    )


def turn(values, cosine, sinusoid):
    return values * cosine + swap_halves(values, ROPE // 2) * sinusoid


def full_gain(gains, row, size, groups):
    total = size * groups
    wide = gains.shape[1]
    if size % LANES == 0:
        shares = [gains[e * 8 + row : e * 8 + row + 1, :size] for e in range(groups)]
        return jnp.concatenate(shares, axis=1)
    result = jnp.zeros((8, total), jnp.float32)
    for e in range(groups):
        share = jnp.broadcast_to(gains[e * 8 + row : e * 8 + row + 1, :], (8, wide))
        if total > wide:
            share = jnp.concatenate([share, jnp.zeros((8, total - wide), jnp.float32)], axis=1)
        result = result + (pltpu.roll(share, e * size, 1) if e else share)
    return result[:1]


def rows_loop(count, step, work):
    def one(i, carry):
        work(pl.ds(pl.multiple_of(i * step, step), step))
        return carry

    lax.fori_loop(0, count // step, one, 0)


def by_rows(count, work):
    rows_loop(count, 16 if count % 16 == 0 else count, work)


def front_kernel(groups, sizes, plan, names, *refs):
    ref = Bag(zip(names, refs))
    deep = groups // PAIR
    link = Link(deep)
    z, x, y, c, part = link.z, link.x, link.y, link.c, link.part
    send, arrive, own, leave = ref.send, ref.arrive, ref.own, ref.leave
    link.greet(groups, "eyc")
    loads, numbers, landing = {}, {}, Bag()
    row_of = {}
    for n, (name, axis, cut, over, orders, home) in enumerate(plan):
        numbers[name] = n
        landing[name] = ref["b_" + name] if home == VMEM_ else ref["o_" + name]

    stream_row = [0]

    def tasks_of(name):
        n = numbers[name]
        _, axis, cut, over, orders, home = plan[n]
        source, target = ref["i_" + name], landing[name]
        if cut is not None:
            source = slot(source, cut[0], part, cut[1])
        if over == READY:
            loads[name] = bring(source, target, own.at[n])
            return []
        if over == SHUFFLE:
            size = source.shape[2]
            keep = ref["k_" + name]
            loads[name] = bring(source.at[link.me], keep, own.at[n])
            row = stream_row[0]
            stream_row[0] += 1
            return [
                shuffle(
                    link,
                    groups,
                    lambda e: source.at[e],
                    lambda e: slot(target, axis, e, size),
                    send.at[row],
                    arrive.at[row],
                )
            ]
        size = cut[1] if cut is not None and cut[0] == axis else source.shape[axis]

        def home_of(sz, sx, sy, sc):
            index = sz * PAIR + sx
            if over == "all":
                index = (index * PAIR + sy) * PAIR + sc
            return slot(target, axis, index, size)

        mine = home_of(z, x, y, c)
        if home == VMEM_:
            loads[name] = bring(source, mine, own.at[n])
        else:
            loads[name] = bring(source, ref["k_" + name], own.at[n])
        if orders == ("e",):
            row = stream_row[0]
            stream_row[0] += 1
            return [
                shuffle(
                    link,
                    groups,
                    lambda e: source,
                    lambda e: slot(target, axis, e, size),
                    send.at[row],
                    arrive.at[row],
                )
            ]
        return streams_of(source, home_of, orders)

    def streams_of(source, home_of, orders):
        result = []
        for i, order in enumerate(orders):
            row = stream_row[0]
            stream_row[0] += 1
            if len(orders) == 1:
                at, part_source = home_of, source
            else:
                wide = source.shape[1] // len(orders)
                span = pl.ds(i * wide, wide)

                def at(*where, span=span):
                    return home_of(*where).at[:, span]

                part_source = source.at[:, span]
            result.append(spread(link, order, part_source, at, send.at[row], arrive.at[row]))
        return result

    def begin(*which):
        found = [task for name in which for task in tasks_of(name)]
        return [task for task in found if next(task, run) is not run]

    gain_tasks = begin(GAINS, ROUTES)
    stem_tasks = begin(QUERY_DOWN, LATENT_DOWN)
    late_tasks = begin(OUT_GRAD)

    def complete(name):
        n = numbers[name]
        loads.pop(name).wait()
        _, axis, cut, over, _, home = plan[n]
        if home == "hbm":
            keep, target = ref["k_" + name], landing[name]
            index = link.me
            if over == "all":
                index = link.me * PAIR * PAIR + part
            move = pltpu.make_async_copy(
                keep, slot(target, axis, index, keep.shape[axis]), own.at[n]
            )
            move.start()
            stores.append(move)

    stores = []

    def keep_out(name, source=None):
        moves = len(stores)
        move = bring(source if source is not None else landing[name], ref["o_" + name], leave.at[len(kept)])
        kept.append(move)

    kept = []
    block_ref = ref.i_block
    first_ref, middle_ref = ref.b_first, ref.b_middle
    width = block_ref.shape[1]
    row_count = block_ref.shape[0]
    sub = row_count // (PAIR * PAIR)

    complete(GAINS)
    complete(ROUTES)
    run(gain_tasks)
    gains = landing.gains
    attention_gain = full_gain(gains, 0, sizes[0], groups)

    def first_norm(span):
        values = block_ref[span, :].astype(jnp.float32)
        inverse = lax.rsqrt(jnp.mean(values * values, axis=-1, keepdims=True) + EPSILON)
        first_ref[span, :] = (values * inverse * attention_gain).astype(jnp.bfloat16)

    rows_loop(row_count, 32, first_norm)
    for _ in range(deep - 1):
        advance(stem_tasks, 1)
        advance(late_tasks, 1)
    up_tasks = begin(QUERY_UP, LATENT_UP)
    for name in (QUERY_DOWN, LATENT_DOWN):
        complete(name)
    run(stem_tasks)
    ref.b_query_cut[...] = matmul(first_ref[...], landing.query_down[...]).astype(
        jnp.bfloat16
    )
    ref.b_latent_cut[...] = matmul_nt(landing.latent_down[...], first_ref[...]).astype(
        jnp.bfloat16
    )
    query_lat, latent_t = ref.b_query_lat, ref.b_latent_t
    query_cut, latent_cut = ref.b_query_cut, ref.b_latent_cut
    stem_numbers = len(plan)
    stem_tasks = streams_of(
        query_cut, lambda sz, sx, sy, sc: slot(query_lat, 1, sy * PAIR + sc, query_cut.shape[1]), ("yc",)
    ) + streams_of(
        latent_cut, lambda sz, sx, sy, sc: slot(latent_t, 0, sy * PAIR + sc, latent_cut.shape[0]), ("yc",)
    )
    stem_tasks = [task for task in stem_tasks if next(task, run) is not run]
    query_lat[:, pl.ds(pl.multiple_of(part * query_cut.shape[1], LANES), query_cut.shape[1])] = (
        query_cut[...]
    )
    latent_t[pl.ds(pl.multiple_of(part * latent_cut.shape[0], 16), latent_cut.shape[0]), :] = (
        latent_cut[...]
    )
    query_gain = full_gain(gains, 2, sizes[2], groups)
    latent_gain = full_gain(gains, 3, sizes[3], groups)
    cosine, sinusoid = ref.i_cosine, ref.i_sinusoid
    advance(up_tasks, 1)
    run(stem_tasks)
    advance(late_tasks, 2)

    query_n, latent_n, keys = ref.b_query_n, ref.b_latent_n, ref.b_keys

    def query_norm(span):
        values = query_lat[span, :].astype(jnp.float32)
        inverse = lax.rsqrt(jnp.mean(values * values, axis=-1, keepdims=True) + EPSILON)
        query_n[span, :] = (values * inverse * query_gain).astype(jnp.bfloat16)

    rows_loop(row_count, 32, query_norm)
    for _ in range(deep - 2):
        advance(up_tasks, 1)
        advance(late_tasks, 2)
    out_tasks = begin(OUT_PROJ, ROUTER)
    latent_rank = latent_n.shape[1]
    latent = latent_t[:latent_rank, :].astype(jnp.float32).T
    inverse = lax.rsqrt(jnp.mean(latent * latent, axis=-1, keepdims=True) + EPSILON)
    latent_n[...] = (latent * inverse * latent_gain).astype(jnp.bfloat16)
    rope_rows = latent_t[latent_rank:, :].astype(jnp.float32).T
    rope_rows = jnp.concatenate(
        [rope_rows, jnp.zeros((row_count, LANES - ROPE), jnp.float32)], axis=1
    )
    key_rope = turn(rope_rows, cosine[...], sinusoid[...])[:, :ROPE].astype(jnp.bfloat16)

    complete(QUERY_UP)
    complete(LATENT_UP)
    run(up_tasks)
    queries, values_ref, attended = ref.b_queries, ref.b_values, ref.b_attended
    heads = queries.shape[0]
    head_width = NOPE + ROPE
    projected = matmul(query_n[...], landing.query_up[...])
    shifted = pltpu.roll(projected, projected.shape[1] - ROPE, 1)
    keyval = matmul(latent_n[...], landing.latent_up[...])
    for h in range(heads):
        start = h * head_width
        base, start = (projected, start) if start % LANES == 0 else (shifted, start - ROPE)
        queries[h, :, :NOPE] = base[:, start : start + NOPE].astype(jnp.bfloat16)
        tail = base[:, start + NOPE : start + NOPE + LANES]
        if tail.shape[1] < LANES:
            tail = jnp.concatenate(
                [tail, jnp.zeros((row_count, LANES - tail.shape[1]), jnp.float32)], axis=1
            )
        queries[h, :, NOPE:] = turn(tail, cosine[...], sinusoid[...])[:, :ROPE].astype(
            jnp.bfloat16
        )
        left = h * (NOPE + VD)
        keys[h, :, :NOPE] = keyval[:, left : left + NOPE].astype(jnp.bfloat16)
        keys[h, :, NOPE:] = key_rope
        values_ref[h] = keyval[:, left + NOPE : left + NOPE + VD].astype(jnp.bfloat16)
        scores = matmul_nt(queries[h], keys[h]) * head_width ** (-0.5)
        scores = jnp.where(ref.i_allowed[...] > 0, scores, -1e30)
        powers = jnp.exp(scores - jnp.max(scores, axis=-1, keepdims=True))
        probs = (powers / jnp.sum(powers, axis=-1, keepdims=True)).astype(jnp.bfloat16)
        attended[:, h * VD : (h + 1) * VD] = matmul(probs, values_ref[h]).astype(jnp.bfloat16)
        if h < deep - 1:
            advance(out_tasks, 1)
        advance(late_tasks, 2)
    advance(out_tasks, max(0, deep - 1 - heads))
    shared_tasks = begin(SHARED)
    for name in (OUT_PROJ, ROUTER):
        complete(name)
    run(out_tasks)
    for name in (QUERY_DOWN, LATENT_DOWN, QUERY_UP, LATENT_UP, OUT_PROJ, GAINS, ROUTER):
        keep_out(name)
    for name in (FIRST, QUERY_LAT, LATENT_T, QUERY_N, LATENT_N, QUERIES, KEYS, VALUES, ATTENDED):
        keep_out(name, ref["b_" + name])

    partial, from_beside = ref.b_partial, ref.b_from_beside
    give, from_across = ref.b_give, ref.b_from_across
    swap_send, swap_arrive = ref.swap_send, ref.swap_arrive
    for quarter in range(PAIR * PAIR):
        partial[quarter // PAIR, quarter % PAIR] = matmul(
            attended[quarter * sub : (quarter + 1) * sub, :], landing.out_proj[...]
        ).astype(jnp.bfloat16)

    sum_task = tensor_total(
        link, partial, from_beside, give, from_across, middle_ref, swap_send, swap_arrive
    )
    next(sum_task, None)
    advance(late_tasks, 1)
    next(sum_task, None)
    complete(OUT_GRAD)
    complete(SHARED)
    advance(late_tasks, 1)
    next(sum_task, None)
    ffn_gain = full_gain(gains, 1, sizes[1], groups)
    norms = ref.b_norms
    norms[...] = jnp.zeros(norms.shape, jnp.float32)
    for i, gain in enumerate((attention_gain, ffn_gain, query_gain, latent_gain)):
        norms[i : i + 1, : gain.shape[1]] = gain
    keep_out("norms", norms)
    second_ref, weights_ref, chosen_ref = ref.b_second, ref.b_weights, ref.b_chosen
    start = pl.multiple_of(part * sub, sub)

    def middle_norm(span):
        mine = pl.ds(pl.multiple_of(start + span.start, 16), span.size)
        middle = middle_ref[span, :] + block_ref[mine, :].astype(jnp.float32)
        middle_ref[span, :] = middle
        inverse = lax.rsqrt(jnp.mean(middle * middle, axis=-1, keepdims=True) + EPSILON)
        second_ref[span, :] = (middle * inverse * ffn_gain).astype(jnp.bfloat16)

    by_rows(sub, middle_norm)
    logits = matmul_nt(second_ref[...], landing.router[...])
    experts = logits.shape[1]
    advance(late_tasks, 1)
    routes_rows = ref.i_route_rows[pl.ds(pl.multiple_of(part * sub, sub), sub), :]
    ids = lax.broadcasted_iota(jnp.int32, (sub, experts), 1)
    chosen = jnp.zeros((sub, experts), jnp.float32)
    picked = jax.nn.sigmoid(logits)
    for k in range(routes_rows.shape[1]):
        chosen = jnp.where(routes_rows[:, k : k + 1] == ids, picked, chosen)
    totals = jnp.sum(chosen, axis=-1, keepdims=True)
    weights_ref[...] = jnp.zeros(weights_ref.shape, jnp.float32)
    weights_ref[:, :experts] = ROUTE_SCALE * chosen / totals
    chosen_ref[...] = jnp.zeros(chosen_ref.shape, jnp.float32)
    chosen_ref[:, :experts] = chosen

    def row_home(name):
        def home_of(sz, sx, sy, sc):
            index = ((sz * PAIR + sx) * PAIR + sy) * PAIR + sc
            return slot(ref["o_" + name], 0, index, sub)

        return home_of

    all_tasks = streams_of(weights_ref, row_home(WEIGHTS), (ZXYC,))
    all_tasks += streams_of(second_ref, row_home(TOKENS), (ZXYC, "zyxc"))
    all_tasks = [task for task in all_tasks if next(task, run) is not run]
    mine = link.me * PAIR * PAIR + part
    kept.append(bring(second_ref, slot(ref.o_tokens, 0, mine, sub), leave.at[len(kept)]))
    kept.append(bring(weights_ref, slot(ref.o_weights, 0, mine, sub), leave.at[len(kept)]))
    keep_out("middle", middle_ref)
    keep_out("chosen", chosen_ref)
    run(late_tasks + all_tasks + shared_tasks)
    link.drain()
    for move in stores + kept:
        move.wait()


def front_stage(calls, groups, parts, sizes, items, block, route_rows, allowed, cosine, sinusoid):
    deep = groups // PAIR
    rows, width = block.shape
    sub = rows // parts
    bf16, f32 = jnp.bfloat16, jnp.float32
    names, inputs, in_specs = [], [], []
    out_names, out_shape, plan, scratch = [], [], [], Bag()
    streams = 0
    for name, array, axis, cut, over, orders, home in items:
        names.append("i_" + name)
        inputs.append(array)
        in_specs.append(ANY)
        shape = list(array.shape)
        if over == SHUFFLE:
            shape = shape[1:]
        if cut is not None:
            shape[cut[0]] = cut[1]
        if home == "hbm":
            scratch["k_" + name] = pltpu.VMEM(tuple(shape), array.dtype)
        if over != READY:
            shape[axis] *= groups * parts if over == "all" else groups
            streams += max(1, len(orders))
        if home == VMEM_:
            scratch["b_" + name] = pltpu.VMEM(tuple(shape), array.dtype)
        out_names.append(name)
        out_shape.append(jax.ShapeDtypeStruct(tuple(shape), array.dtype))
        plan.append((name, axis, cut, over, orders, home))
    for name, array in (
        ("block", block),
        ("route_rows", route_rows),
        ("allowed", allowed),
        ("cosine", cosine),
        ("sinusoid", sinusoid),
    ):
        names.append("i_" + name)
        inputs.append(array)
        in_specs.append(IN_VMEM)
    shape_of = Bag((name, shape.shape) for name, shape in zip(out_names, out_shape))
    query_cut, latent_cut = shape_of.query_down[1], shape_of.latent_down[0]
    query_rank, latent_rank = shape_of.query_up[0], shape_of.latent_up[0]
    heads = shape_of.latent_up[1] // (NOPE + VD)
    experts = shape_of.router[0]
    lanes = experts + -experts % LANES
    half = parts // PAIR
    buffers = Bag(
        first=((rows, width), bf16),
        query_lat=((rows, query_cut * parts), bf16),
        latent_t=((latent_cut * parts, rows), bf16),
        query_n=((rows, query_rank), bf16),
        latent_n=((rows, latent_rank), bf16),
        queries=((heads, rows, NOPE + ROPE), bf16),
        keys=((heads, rows, NOPE + ROPE), bf16),
        values=((heads, rows, VD), bf16),
        attended=((rows, heads * VD), bf16),
        middle=((sub, width), f32),
        chosen=((sub, lanes), f32),
        norms=((8, width), f32),
    )
    for name, (shape, dtype) in buffers.items():
        out_names.append(name)
        out_shape.append(jax.ShapeDtypeStruct(shape, dtype))
    inner = Bag(
        query_cut=((rows, query_cut), bf16),
        latent_cut=((latent_cut, rows), bf16),
        partial=((half, PAIR, sub, width), bf16),
        from_beside=((half, sub, width), bf16),
        give=((sub, width), bf16),
        from_across=((sub, width), bf16),
        second=((sub, width), bf16),
        weights=((sub, lanes), f32),
    )
    for name, (shape, dtype) in (buffers | inner).items():
        scratch["b_" + name] = pltpu.VMEM(shape, dtype)
    out_names += [TOKENS, WEIGHTS]
    out_shape += [
        jax.ShapeDtypeStruct((sub * groups * parts, width), bf16),
        jax.ShapeDtypeStruct((sub * groups * parts, lanes), f32),
    ]
    streams += 2 + 1 + 2
    scratch.send = scratch.arrive = DMA((streams, 8 * deep))
    scratch.own = DMA((len(items),))
    scratch.leave = DMA((len(out_names),))
    scratch.swap_send = scratch.swap_arrive = DMA((2,))
    names += ["o_" + name for name in out_names] + list(scratch)
    results = pl.pallas_call(
        functools.partial(front_kernel, groups, tuple(sizes), tuple(plan), tuple(names)),
        in_specs=in_specs,
        out_specs=[ANY] * len(out_names),
        out_shape=out_shape,
        scratch_shapes=list(scratch.values()),
        compiler_params=calls.params(),
        name="front",
    )(*inputs)
    return Bag(zip(out_names, results))


def device_total(link, order, own, give, bufs, result, send, arrive):
    deep, z, x, y = link.deep, link.z, link.x, link.y
    from_core, from_first, from_second, from_deep = bufs
    mine, following = (x, y) if order == 0 else (y, x)
    near, far = (link.peer("x"), link.peer("y")) if order == 0 else (link.peer("y"), link.peer("x"))

    def at(depth, on_first, on_second):
        on_x, on_y = (on_first, on_second) if order == 0 else (on_second, on_first)
        return (depth * PAIR + on_x) * PAIR + on_y

    def hop(number, source, target, peer):
        def make():
            return pltpu.make_async_remote_copy(
                src_ref=source(),
                dst_ref=target,
                send_sem=send.at[number],
                recv_sem=arrive.at[number],
                device_id=peer,
                device_id_type=MESH,
            )

        link.emit(make)

    hop(0, lambda: give, from_core, link.peer("c"))
    yield
    arrived(from_core, arrive.at[0])

    def add_core(k):
        own[k] = own[k] + from_core[k]

    add_rows(deep * PAIR * PAIR, add_core)
    for depth in range(deep):
        for s in range(PAIR):
            n = depth * PAIR + s
            hop(1 + n, lambda d=depth, s=s: own.at[at(d, 1 - mine, s)], from_first.at[n], near)
    yield
    for n in range(PAIR * deep):
        arrived(from_first.at[n], arrive.at[1 + n])

    def add_first(k):
        here = at(k // PAIR, mine, k % PAIR)
        own[here] = own[here] + from_first[k]

    add_rows(deep * PAIR, add_first)
    base = 1 + PAIR * deep
    for depth in range(deep):
        hop(
            base + depth,
            lambda d=depth: own.at[at(d, mine, 1 - following)],
            from_second.at[depth],
            far,
        )
    yield
    for depth in range(deep):
        arrived(from_second.at[depth], arrive.at[base + depth])

    def add_second(k):
        here = at(k, mine, following)
        own[here] = own[here] + from_second[k]

    add_rows(deep, add_second)
    base = base + deep - 1
    for k in range(1, deep):
        hop(
            base + k,
            lambda k=k: own.at[at((z + k) % deep, mine, following)],
            from_deep.at[k - 1],
            link.at_z((z + k) % deep),
        )
    yield
    for k in range(1, deep):
        arrived(from_deep.at[k - 1], arrive.at[base + k])

    def finish(span):
        total = own[at(z, mine, following), span, :].astype(jnp.float32)
        for k in range(1, deep):
            total = total + from_deep[k - 1, span, :].astype(jnp.float32)
        result[span, :] = total

    by_rows(result.shape[0], finish)


def total_buffers(deep, rows, wide):
    shapes = (deep * PAIR * PAIR, PAIR * deep, deep, deep - 1)
    return [pltpu.VMEM((n, rows, wide), jnp.bfloat16) for n in shapes]


def total_hops(deep):
    return PAIR * deep + 2 * deep


def route_kernel(ids_ref, routes_ref, x_ref, g_ref, weights_ref, xr_ref, gr_ref, p_ref, w_ref):
    local = ids_ref.shape[0]
    rows = x_ref.shape[0]
    f32, bf16 = jnp.float32, jnp.bfloat16
    ids = ids_ref[...]
    named = jnp.zeros((local, rows), f32)
    for k in range(routes_ref.shape[0]):
        named = jnp.where(routes_ref[k : k + 1, :] == ids, 1.0, named)
    before = lax.broadcasted_iota(jnp.int32, (rows, rows), 0)
    after = lax.broadcasted_iota(jnp.int32, (rows, rows), 1)
    rank = matmul(named.astype(bf16), jnp.where(before < after, 1.0, 0.0).astype(bf16))
    lanes = weights_ref.shape[1]
    mine = jnp.where(lax.broadcasted_iota(jnp.int32, (local, lanes), 1) == ids, 1.0, 0.0)
    weights = lax.dot_general(
        mine,
        weights_ref[...],
        (((1,), (1,)), ((), ())),
        precision=lax.Precision.HIGHEST,
        preferred_element_type=f32,
    )
    slots = lax.broadcasted_iota(jnp.int32, (CAP, rows), 0).astype(f32)
    picks = []
    for j in range(local):
        pick = jnp.where(slots == rank[j : j + 1, :], named[j : j + 1, :], 0.0)
        w_ref[0, j * CAP : (j + 1) * CAP, :] = jnp.sum(
            pick * weights[j : j + 1, :], axis=1, keepdims=True
        )
        picks.append(pick.astype(bf16))
    picks = jnp.concatenate(picks, axis=0)
    p_ref[0] = picks
    xr_ref[0] = matmul(picks, x_ref[...]).astype(bf16)
    gr_ref[0] = matmul(picks, g_ref[...]).astype(bf16)


def route_stage(groups, own_ids, routes_t, tokens, gradients, weights):
    local = own_ids.shape[0]
    rows, width = tokens.shape[0] // groups, tokens.shape[1]
    slots = local * CAP
    row_spec = pl.BlockSpec((rows, width), lambda b: (b, 0))
    slot_spec = pl.BlockSpec((1, slots, width), lambda b: (b, 0, 0))
    slot_shape = jax.ShapeDtypeStruct((groups, slots, width), jnp.bfloat16)
    lanes = weights.shape[1]
    return pl.pallas_call(
        route_kernel,
        grid=(groups,),
        in_specs=[
            pl.BlockSpec((local, 1), lambda b: (0, 0)),
            pl.BlockSpec((routes_t.shape[0], rows), lambda b: (0, b)),
            row_spec,
            row_spec,
            pl.BlockSpec((rows, lanes), lambda b: (b, 0)),
        ],
        out_specs=[
            slot_spec,
            slot_spec,
            pl.BlockSpec((1, slots, rows), lambda b: (b, 0, 0)),
            pl.BlockSpec((1, slots, 1), lambda b: (b, 0, 0)),
        ],
        out_shape=[
            slot_shape,
            slot_shape,
            jax.ShapeDtypeStruct((groups, slots, rows), jnp.bfloat16),
            jax.ShapeDtypeStruct((groups, slots, 1), jnp.float32),
        ],
        compiler_params=pltpu.CompilerParams(vmem_limit_bytes=VMEM_BYTES),
        name="route",
    )(own_ids[:, None], routes_t, tokens, gradients, weights)


MIX_LAGS = (1, 3, 5, 7)


def mix_kernel(groups, chunks, names, *refs):
    ref = Bag(zip(names, refs))
    deep = groups // PAIR
    bf16, f32 = jnp.bfloat16, jnp.float32
    link = Link(deep)
    link.greet(groups, "eyc")
    blocks, slots, rows = ref.b_picks.shape
    sub = ref.o_dsecond.shape[0]
    width = ref.i_tokens.shape[1]
    units = ref.i_shared.shape[0] // 3
    loads = [bring(ref.i_picks, ref.b_picks, ref.load.at[0])]
    loads.append(bring(ref.i_shared, ref.b_shared, ref.load.at[1]))

    def fetch(b, at):
        span = pl.ds(pl.multiple_of(b * rows, rows), rows)
        return (
            pltpu.make_async_copy(ref.i_tokens.at[span, :], ref.b_x.at[at], ref.fetch.at[at, 0]),
            pltpu.make_async_copy(ref.i_gradients.at[span, :], ref.b_g.at[at], ref.fetch.at[at, 1]),
        )

    many = len(chunks)
    work = [(True, *chunk) for chunk in chunks] + [(False, *chunk) for chunk in chunks[:-1]]

    def source_of(n):
        back, left, wide = work[n]
        source = ref.i_back if back else ref.i_produced
        return pltpu.make_async_copy(
            source.at[:, :, pl.ds(left, wide)],
            ref.b_source.at[turn_of[n], :, :, pl.ds(0, wide)],
            ref.pull.at[turn_of[n]],
        )

    has_source = [n != many - 1 for n in range(len(work))]
    order = [n for n in range(many, len(work))] + [many - 1] + list(range(many - 1))
    turn_of = {n: i % 2 for i, n in enumerate(n for n in order if has_source[n])}
    for load in loads:
        load.wait()
    ref.b_acc[...] = jnp.zeros(ref.b_acc.shape, f32)

    def fetch_one(which, b, at):
        source, target, column = (
            (ref.i_tokens, ref.b_x, 0) if which == 0 else (ref.i_gradients, ref.b_g, 1)
        )
        span = pl.ds(pl.multiple_of(b * rows, rows), rows)
        return pltpu.make_async_copy(source.at[span, :], target.at[at], ref.fetch.at[at, column])

    def over_blocks(which, work):
        fetch_one(which, 0, 0).start()

        def one(b, carry):
            at = b % 2

            @pl.when(b + 1 < blocks)
            def _():
                fetch_one(which, b + 1, 1 - at).start()

            fetch_one(which, b, at).wait()
            work(b, at)
            return carry

        lax.fori_loop(0, blocks, one, 0)

    def forward_block(b, at):
        pre = matmul_nt(ref.b_x[at], ref.b_shared[: 2 * units, :])
        ref.b_pre[b] = pre
        ref.b_hidden[b] = swiglu(pre[:, :units], pre[:, units:])[1]

    def backward_block(b, at):
        pre = ref.b_pre[b]
        gate_pre, up_pre = pre[:, :units], pre[:, units:]
        dhidden = matmul_nt(ref.b_g[at], ref.b_shared[2 * units :, :])
        grads = swiglu_back(dhidden, gate_pre, up_pre, jax.nn.sigmoid(gate_pre))
        ref.b_both[b] = jnp.concatenate(grads, axis=1)

    def shared_gradients(b):
        at = b % 2
        if b + 1 < blocks:
            for copy in fetch(b + 1, 1 - at):
                copy.start()
        for copy in fetch(b, at):
            copy.wait()
        ref.b_acc[: 2 * units, :] += matmul_tn(ref.b_both[b], ref.b_x[at])
        ref.b_acc[2 * units :, :] += matmul_tn(ref.b_hidden[b], ref.b_g[at])

    source_of(order[0]).start()
    over_blocks(0, forward_block)
    dw_lane = lax.broadcasted_iota(jnp.int32, (slots, chunks[-1][1]), 1)
    tasks = []

    def step_at(moment):
        for lag in MIX_LAGS:
            if 0 <= moment - lag < len(tasks):
                next(tasks[moment - lag], None)

    pending = [n for n in order if has_source[n]]
    for n in order:
        back, left, wide = work[n]
        if has_source[n]:
            pending.pop(0)
            if pending:
                source_of(pending[0]).start()
            source_of(n).wait()

        def one(b, carry, n=n, back=back, left=left, wide=wide):
            picks = ref.b_picks[b]
            if not has_source[n]:
                values = matmul_tn(
                    picks, jnp.where(dw_lane == ref.i_lanes[...], ref.i_dweights[b], 0.0).astype(bf16)
                )
            else:
                span = slice(left, left + wide)
                values = matmul_tn(picks, ref.b_source[turn_of[n], b, :, :wide])
                if back:
                    values += matmul(ref.b_both[b], ref.b_shared[: 2 * units, span])
                else:
                    values += matmul(ref.b_hidden[b], ref.b_shared[2 * units :, span])
            values = values.astype(bf16)
            for y in range(PAIR):
                for c in range(PAIR):
                    q = y * PAIR + c
                    piece = values[q * sub : (q + 1) * sub, :]
                    ref["p%d" % n][c, b * PAIR + y] = piece
            return carry

        lax.fori_loop(0, blocks, one, 0)
        result = ref.o_dsecond if back else ref.o_mixed
        task = device_total(
            link,
            n % 2,
            ref["p%d" % n].at[link.c],
            ref["p%d" % n].at[1 - link.c],
            [ref["f%d_%d" % (n, k)] for k in range(4)],
            result.at[:, pl.ds(left, wide)],
            ref.send.at[n],
            ref.arrive.at[n],
        )
        tasks += begun([task])
        step_at(len(tasks) - 1)
        if n == many + 2:
            over_blocks(1, backward_block)
    for copy in fetch(0, 0):
        copy.start()
    share = -(-blocks // 4)
    for late in range(MIX_LAGS[-1]):
        step_at(len(order) + late)
        for b in range(late * share, min(blocks, (late + 1) * share)):
            shared_gradients(b)
        if late == 3:
            ref.b_grad[...] = ref.b_acc[...].astype(bf16)
            grad_out = bring(ref.b_grad, ref.o_shared, ref.load.at[0])
    link.drain()
    grad_out.wait()


def mix_bytes(groups, rows, slots, width):
    total = groups * rows * width * 2
    return 2 * total + 4 * rows * width * 2 * 2 + 2 * groups * max(rows, slots) * 512 * 2 * 2


def mix_stage(calls, groups, parts, picks, produced, back, dweights, lanes, tokens, gradients, shared):
    deep = groups // PAIR
    blocks, slots, rows = picks.shape
    width = tokens.shape[1]
    sub = rows // parts
    bf16, f32 = jnp.bfloat16, jnp.float32
    experts_wide = lanes[1]
    wide = min(512, width)
    chunks = [(left, wide) for left in range(0, width, wide)] + [(width, experts_wide)]
    inputs = Bag(
        i_picks=picks,
        i_produced=produced,
        i_back=back,
        i_dweights=dweights,
        i_lanes=lanes[0],
        i_tokens=tokens,
        i_gradients=gradients,
        i_shared=shared,
    )
    specs = [IN_VMEM if key in ("i_dweights", "i_lanes") else ANY for key in inputs]
    third = shared.shape[0] // 3
    scratch = Bag(
        b_picks=pltpu.VMEM(picks.shape, bf16),
        b_shared=pltpu.VMEM(shared.shape, bf16),
        b_x=pltpu.VMEM((2, rows, width), bf16),
        b_g=pltpu.VMEM((2, rows, width), bf16),
        b_acc=pltpu.VMEM(shared.shape, f32),
        b_grad=pltpu.VMEM(shared.shape, bf16),
        b_pre=pltpu.VMEM((blocks, rows, 2 * third), f32),
        b_hidden=pltpu.VMEM((blocks, rows, third), bf16),
        b_both=pltpu.VMEM((blocks, rows, 2 * third), bf16),
        b_source=pltpu.VMEM((2, blocks, slots, wide), bf16),
        load=DMA((2,)),
        fetch=DMA((2, 2)),
        pull=DMA((2,)),
        send=DMA((2 * len(chunks), total_hops(deep))),
        arrive=DMA((2 * len(chunks), total_hops(deep))),
    )
    for n, (_, columns) in enumerate(chunks + chunks[:-1]):
        scratch["p%d" % n] = pltpu.VMEM((PAIR, blocks * PAIR, sub, columns), bf16)
        for k, buffer in enumerate(total_buffers(deep, sub, columns)):
            scratch["f%d_%d" % (n, k)] = buffer
    names = list(inputs) + ["o_dsecond", "o_mixed", "o_shared"] + list(scratch)
    return pl.pallas_call(
        functools.partial(mix_kernel, groups, tuple(chunks), tuple(names)),
        in_specs=specs,
        out_specs=[IN_VMEM, IN_VMEM, ANY],
        out_shape=[
            jax.ShapeDtypeStruct((sub, width + experts_wide), f32),
            jax.ShapeDtypeStruct((sub, width), f32),
            jax.ShapeDtypeStruct(shared.shape, bf16),
        ],
        scratch_shapes=list(scratch.values()),
        compiler_params=calls.params(),
        name="mix",
    )(*inputs.values())


def advance(tasks, count=1):
    for _ in range(count):
        for task in tasks:
            next(task, None)


def begun(tasks):
    return [task for task in tasks if next(task, run) is not run]


def tensor_total(link, partial, from_beside, give, from_across, result, send, arrive):
    y, c = link.y, link.c

    def beside():
        return pltpu.make_async_remote_copy(
            src_ref=partial.at[:, 1 - c],
            dst_ref=from_beside,
            send_sem=send.at[0],
            recv_sem=arrive.at[0],
            device_id=link.peer("c"),
            device_id_type=MESH,
        )

    def across():
        return pltpu.make_async_remote_copy(
            src_ref=give,
            dst_ref=from_across,
            send_sem=send.at[1],
            recv_sem=arrive.at[1],
            device_id=link.peer("y"),
            device_id_type=MESH,
        )

    link.emit(beside)
    yield
    arrived(from_beside, arrive.at[0])
    rows = result.shape[0]

    def add_given(span):
        give[span, :] = partial[1 - y, c, span, :] + from_beside[1 - y, span, :]

    def add_kept(span):
        kept = partial[y, c, span, :].astype(jnp.float32)
        result[span, :] = kept + from_beside[y, span, :].astype(jnp.float32)

    def add_last(span):
        result[span, :] = result[span, :] + from_across[span, :].astype(jnp.float32)

    by_rows(rows, add_given)
    link.emit(across)
    by_rows(rows, add_kept)
    yield
    arrived(from_across, arrive.at[1])
    by_rows(rows, add_last)


def expert_total(link, axis, grad, from_twin, from_deep, result, send, arrive):
    deep, z, x = link.deep, link.z, link.x
    size = result.shape[axis]

    def target(k):
        return (z + k) % deep

    def to_twin(k):
        return pltpu.make_async_remote_copy(
            src_ref=slot(grad, axis, target(k) * PAIR + 1 - x, size),
            dst_ref=from_twin.at[k],
            send_sem=send.at[k],
            recv_sem=arrive.at[k],
            device_id=link.peer("x"),
            device_id_type=MESH,
        )

    def to_deep(k):
        return pltpu.make_async_remote_copy(
            src_ref=from_twin.at[k],
            dst_ref=from_deep.at[k - 1],
            send_sem=send.at[deep + k],
            recv_sem=arrive.at[deep + k],
            device_id=link.at_z(target(k)),
            device_id_type=MESH,
        )

    ks = list(range(1, deep)) + [0]
    for k in ks:
        link.emit(functools.partial(to_twin, k))
    for k in ks[:-1]:
        yield
        arrived(from_twin.at[k], arrive.at[k])
        mine = slot(grad, axis, target(k) * PAIR + x, size)

        def add(span, mine=mine, k=k):
            from_twin[k, span, :] = from_twin[k, span, :] + mine[span, :]

        by_rows(result.shape[0], add)
        link.emit(functools.partial(to_deep, k))
    yield
    arrived(from_twin.at[0], arrive.at[0])
    mine = slot(grad, axis, z * PAIR + x, size)

    def finish(span):
        total = mine[span, :].astype(jnp.float32) + from_twin[0, span, :].astype(jnp.float32)
        for k in range(1, deep):
            total = total + from_deep[k - 1, span, :].astype(jnp.float32)
        result[span, :] = total

    for k in range(1, deep):
        yield
        arrived(from_deep.at[k - 1], arrive.at[deep + k])
    by_rows(result.shape[0], finish)


def back_kernel(groups, sizes, reduced, names, *refs):
    ref = Bag(zip(names, refs))
    deep = groups // PAIR
    parts = PAIR * PAIR
    link = Link(deep)
    part = link.part
    bf16, f32 = jnp.bfloat16, jnp.float32
    link.greet(groups, "eyc")
    loading = {}
    for n, name in enumerate(n[2:] for n in names if n[:2] == "h_"):
        loading[name] = bring(ref["h_" + name], ref["l_" + name], ref.load.at[n])
    left = []

    def leave(name, source=None):
        source = ref["b_" + name] if source is None else source
        left.append(bring(source, ref["o_" + name], ref.leave.at[len(left)]))

    def ready(*which):
        for name in which:
            if name in loading:
                loading.pop(name).wait()
        return [ref["l_" + name] for name in which]

    rows_send, rows_arrive = ref.rows_send, ref.rows_arrive
    used = [0]

    def over_tensor(source, target, axis, size):
        row = used[0]
        used[0] += 1

        def home_of(sz, sx, sy, sc):
            return slot(target, axis, sy * PAIR + sc, size)

        n = len(placed)
        placed.append(bring(source, home_of(link.z, link.x, link.y, link.c), ref.place.at[n]))
        return spread(link, "yc", source, home_of, rows_send.at[row], rows_arrive.at[row])

    placed = []
    totals = {name: i for i, (name, _) in enumerate(reduced)}
    axis_of = dict(reduced)

    def over_expert(name):
        if name not in totals:
            leave(name)
            return
        i = totals[name]
        tasks = begun(
            [
                expert_total(
                    link,
                    axis_of[name],
                    ref["b_" + name],
                    ref["t_" + name],
                    ref["d_" + name],
                    ref["r_" + name],
                    ref.send.at[i],
                    ref.arrive.at[i],
                )
            ]
        )
        queue.extend([task, deep - 1] for task in tasks)

    queue, finishing = [], []

    def pump(count):
        while count and queue:
            entry = queue[0]
            next(entry[0], None)
            entry[1] -= 1
            count -= 1
            if not entry[1]:
                finishing.append(queue.pop(0)[0])

    shared_tasks = []
    if SHARED in axis_of:
        wide = ref.o_shared.shape[2]
        source = ref.i_shared
        shared_tasks = begun(
            [
                shuffle(
                    link,
                    groups,
                    lambda e: source.at[:, pl.ds(pl.multiple_of(e * wide, LANES), wide)],
                    lambda e: ref.o_shared.at[e],
                    ref.shared_send,
                    ref.shared_arrive,
                )
            ]
        )
        loading[OWN_SHARED] = bring(
            source.at[:, pl.ds(pl.multiple_of(link.me * wide, LANES), wide)],
            ref.k_shared,
            ref.place.at[len(placed)],
        )
        placed.append(None)

    sub, width = ref.i_middle.shape
    experts = ref.i_router.shape[0]
    norms = [ref.i_norms[i : i + 1, : size * groups] for i, size in enumerate(sizes)]
    sums = ref.b_sums
    sums[...] = jnp.zeros(sums.shape, f32)
    start = pl.multiple_of(part * sub, sub)

    def norm_back(which, values, cotangent):
        inverse = lax.rsqrt(jnp.mean(values * values, axis=-1, keepdims=True) + EPSILON)
        normed = values * inverse
        scaled = cotangent * norms[which]
        sums[which : which + 1, : values.shape[1]] += jnp.sum(
            cotangent * normed, axis=0, keepdims=True
        )
        back = inverse * (scaled - normed * jnp.mean(scaled * normed, axis=-1, keepdims=True))
        return (back, normed)

    def own_rows(span):
        return pl.ds(pl.multiple_of(start + span.start, 16), span.size)

    chosen = ref.i_chosen[:, :experts]
    dweights = ref.i_dsecond[:, width : width + experts]
    total = jnp.sum(chosen, axis=-1, keepdims=True)
    dchosen = (
        ROUTE_SCALE
        / total
        * (dweights - jnp.sum(dweights * chosen, axis=-1, keepdims=True) / total)
    )
    dlogits = (dchosen * chosen * (1.0 - chosen)).astype(bf16)
    ref.b_first_rows[...] = matmul(dlogits, ref.i_router[...])

    def middle_back(span):
        middle = ref.i_middle[span, :]
        dsecond = ref.i_dsecond[span, :width] + ref.b_first_rows[span, :]
        back, normed = norm_back(1, middle, dsecond)
        middle_grad = ref.i_out_grad[own_rows(span), :].astype(f32) + back
        ref.b_middle_grad[span, :] = middle_grad
        ref.b_grad_rows[span, :] = middle_grad.astype(bf16)
        ref.b_block_rows[span, :] = (middle + ref.i_mixed[span, :]).astype(bf16)
        ref.b_input_rows[span, :] = (normed * norms[1]).astype(bf16)

    by_rows(sub, middle_back)
    tensor_tasks = begun([over_tensor(ref.b_grad_rows, ref.b_attention_grad, 0, sub)])
    ref.b_router[...] = matmul_tn(dlogits, ref.b_input_rows[...]).astype(bf16)
    over_expert(ROUTER)
    run(tensor_tasks)
    block_tasks = begun([over_tensor(ref.b_block_rows, ref.o_block_out, 0, sub)])
    placed[1 if SHARED in axis_of else 0].wait()
    placed[1 if SHARED in axis_of else 0] = None

    attended, out_proj = ready(ATTENDED, OUT_PROJ)
    attention_grad = ref.b_attention_grad
    for at in range(0, attended.shape[1], 256):
        ref.b_out_proj[at : at + 256, :] = matmul_tn(
            attended[:, at : at + 256], attention_grad[...]
        ).astype(bf16)
    over_expert(OUT_PROJ)
    ref.b_attended_grad[...] = matmul_nt(attention_grad[...], out_proj[...]).astype(bf16)

    queries, keys, values = ready(QUERIES, KEYS, VALUES)
    heads, row_count, head_width = queries.shape
    cosine, sinusoid = ref.i_cosine[...], ref.i_sinusoid[...]
    dkey_rope = jnp.zeros((row_count, LANES), f32)
    scale = head_width ** (-0.5)
    filler = jnp.zeros((row_count, LANES - ROPE), f32)
    for h in range(heads):
        scores = matmul_nt(queries[h], keys[h]) * scale
        scores = jnp.where(ref.i_allowed[...] > 0, scores, -1e30)
        powers = jnp.exp(scores - jnp.max(scores, axis=-1, keepdims=True))
        probs = powers / jnp.sum(powers, axis=-1, keepdims=True)
        attended_grad = ref.b_attended_grad[:, h * VD : (h + 1) * VD]
        dvalues = matmul_tn(probs.astype(bf16), attended_grad)
        dprobs = matmul_nt(attended_grad, values[h])
        delta = jnp.sum(probs * dprobs, axis=-1, keepdims=True)
        dscores = (probs * (dprobs - delta) * scale).astype(bf16)
        dquery = matmul(dscores, keys[h])
        dkeys = matmul_tn(dscores, queries[h])
        rope = turn(jnp.concatenate([dquery[:, NOPE:], filler], axis=1), cosine, -sinusoid)
        pair = jnp.concatenate(
            [dquery[:, :NOPE], rope, jnp.zeros((row_count, LANES), f32)], axis=1
        )
        if h % 2 == 0:
            held = pair
        else:
            held = held + pltpu.roll(pair, head_width, 1)
            ref.b_dquery[:, (h - 1) * head_width : (h + 1) * head_width] = held.astype(bf16)
        dkey_rope = dkey_rope + jnp.concatenate([dkeys[:, NOPE:], filler], axis=1)
        base = h * (NOPE + VD)
        ref.b_dkeyval[:, base : base + NOPE] = dkeys[:, :NOPE].astype(bf16)
        ref.b_dkeyval[:, base + NOPE : base + NOPE + VD] = dvalues.astype(bf16)
        if h:
            pump(1)
    dkey_rope = turn(dkey_rope, cosine, -sinusoid)

    query_n, latent_n, query_up, latent_up = ready(QUERY_N, LATENT_N, QUERY_UP, LATENT_UP)
    query_rank, latent_rank = query_n.shape[1], latent_n.shape[1]

    def query_up_rows(span):
        ref.b_query_up[span, :] = matmul_tn(query_n[:, span], ref.b_dquery[...]).astype(bf16)

    rows_loop(query_rank, 256, query_up_rows)
    over_expert(QUERY_UP)
    for at in range(0, latent_rank, 256):
        ref.b_latent_up[at : at + 256, :] = matmul_tn(
            latent_n[:, at : at + 256], ref.b_dkeyval[...]
        ).astype(bf16)
    over_expert(LATENT_UP)
    partial = ref.b_heads_partial
    lead = query_rank + latent_rank
    for quarter in range(parts):
        span = slice(quarter * sub, (quarter + 1) * sub)
        at = (quarter // PAIR, quarter % PAIR)
        partial[(*at, slice(None), slice(0, query_rank))] = matmul_nt(
            ref.b_dquery[span, :], query_up[...]
        ).astype(bf16)
        partial[(*at, slice(None), slice(query_rank, lead))] = matmul_nt(
            ref.b_dkeyval[span, :], latent_up[...]
        ).astype(bf16)
        partial[(*at, slice(None), slice(lead, lead + LANES))] = dkey_rope[span, :].astype(bf16)
    sum_tasks = begun(
        [
            tensor_total(
                link,
                partial,
                ref.b_heads_beside,
                ref.b_heads_give,
                ref.b_heads_across,
                ref.b_heads_rows,
                ref.sum_send.at[0],
                ref.sum_arrive.at[0],
            )
        ]
    )
    pump(1)
    run(sum_tasks)

    heads_rows = ref.b_heads_rows
    (query_lat, latent_t) = ready(QUERY_LAT, LATENT_T)

    ref.b_latent_block[...] = latent_t[:latent_rank, :].astype(f32).T

    def latents_back(span):
        mine = own_rows(span)
        back, _ = norm_back(2, query_lat[mine, :].astype(f32), heads_rows[span, :query_rank])
        ref.b_query_rows[span, :] = back.astype(bf16)
        back, _ = norm_back(3, ref.b_latent_block[mine, :], heads_rows[span, query_rank:lead])
        ref.b_latent_rows[span, :latent_rank] = back.astype(bf16)
        ref.b_latent_rows[span, latent_rank:] = heads_rows[span, lead:].astype(bf16)

    by_rows(sub, latents_back)
    own = len(placed)
    tensor_tasks = begun(
        [
            over_tensor(ref.b_query_rows, ref.b_dquery_lat, 0, sub),
            over_tensor(ref.b_latent_rows, ref.b_dlatent_all, 0, sub),
        ]
    )
    pump(1)
    run(tensor_tasks)
    for n in (own, own + 1):
        placed[n].wait()
        placed[n] = None

    first, query_down, latent_down = ready(FIRST, QUERY_DOWN, LATENT_DOWN)
    query_cut, latent_cut = query_down.shape[1], latent_down.shape[0]
    dquery_lat = ref.b_dquery_lat[
        :, pl.ds(pl.multiple_of(part * query_cut, LANES), query_cut)
    ]
    ref.b_dlatent_t[...] = ref.b_dlatent_all[...].astype(f32).T
    dlatent_t = ref.b_dlatent_t[
        pl.ds(pl.multiple_of(part * latent_cut, 8), latent_cut), :
    ].astype(bf16)
    ref.b_dquery_cut[...] = dquery_lat

    def query_down_rows(span):
        ref.b_query_down[span, :] = matmul_tn(first[:, span], ref.b_dquery_cut[...]).astype(
            bf16
        )

    rows_loop(width, 256, query_down_rows)
    over_expert(QUERY_DOWN)
    for at in range(0, width, 512):
        ref.b_latent_down[:, at : at + 512] = matmul(dlatent_t, first[:, at : at + 512]).astype(
            bf16
        )
    over_expert(LATENT_DOWN)
    pump(1)
    partial = ref.b_first_partial
    for quarter in range(parts):
        span = slice(quarter * sub, (quarter + 1) * sub)
        partial[quarter // PAIR, quarter % PAIR] = (
            matmul_nt(dquery_lat[span], query_down[...])
            + matmul_tn(dlatent_t[:, span], latent_down[...])
        ).astype(bf16)
    sum_tasks = begun(
        [
            tensor_total(
                link,
                partial,
                ref.b_first_beside,
                ref.b_first_give,
                ref.b_first_across,
                ref.b_first_rows,
                ref.sum_send.at[1],
                ref.sum_arrive.at[1],
            )
        ]
    )
    pump(1)
    run(sum_tasks)

    def first_back(span):
        residual = ref.i_block[own_rows(span), :].astype(f32)
        back, _ = norm_back(0, residual, ref.b_first_rows[span, :])
        ref.b_input_rows[span, :] = (ref.b_middle_grad[span, :] + back).astype(bf16)

    by_rows(sub, first_back)
    input_tasks = begun([over_tensor(ref.b_input_rows, ref.o_input_grad, 0, sub)])
    wide = ref.b_gains.shape[1]
    for i, size in enumerate(sizes):
        span = size * groups
        total = jnp.broadcast_to(sums[i : i + 1, :span], (8, span))
        if span < wide:
            total = jnp.concatenate([total, jnp.zeros((8, wide - span), f32)], axis=1)
            span = wide
        for e in range(groups):
            if size % LANES == 0:
                moved = total[:1, e * size : (e + 1) * size]
                if size < wide:
                    moved = jnp.concatenate([moved, jnp.zeros((1, wide - size), f32)], axis=1)
            else:
                moved = (pltpu.roll(total, span - e * size, 1) if e else total)[:1, :wide]
            ref.b_gains[e * 8 + i : e * 8 + i + 1, :] = moved
    for e in range(groups):
        ref.b_gains[e * 8 + len(sizes) : e * 8 + 8, :] = jnp.zeros((8 - len(sizes), wide), f32)
    over_expert(GAINS)
    pump(len(queue) * deep)
    run(finishing)

    finished = ("o_query_down", "o_latent_down")
    finals = []
    for name, axis in ((QUERY_DOWN, 1), (LATENT_DOWN, 0), (ROUTER, 0), (GAINS, 0)):
        if name not in totals:
            continue
        share = ref["s_" + name]
        whole = ref["o_" + name] if "o_" + name in finished else ref["g_" + name]
        share[...] = ref["r_" + name][...].astype(share.dtype)
        finals.append(over_tensor(share, whole, axis, share.shape[axis]))
    finals = begun(finals)
    for name in (OUT_PROJ, QUERY_UP, LATENT_UP):
        if name in totals:
            leave(name, ref["r_" + name])
    if SHARED in axis_of:
        loading.pop(OWN_SHARED).wait()
        left.append(
            bring(ref.k_shared, ref.o_shared.at[link.me], ref.leave.at[len(left)])
        )
    run(finals)
    for move in placed:
        if move is not None:
            move.wait()
    for name in (ROUTER, GAINS):
        if name in totals:
            size = ref["s_" + name].shape[0]
            total = ref["g_" + name][:size, :]
            for t in range(1, parts):
                total = total + ref["g_" + name][t * size : (t + 1) * size, :]
            ref["f_" + name][...] = total
            leave(name, ref["f_" + name])
    run(block_tasks + input_tasks + shared_tasks)
    link.drain()
    for move in left:
        move.wait()


def back_stage(calls, groups, parts, sizes, held, small, grad_shared):
    deep = groups // PAIR
    bf16, f32 = jnp.bfloat16, jnp.float32
    rows, width = small.block.shape
    sub = rows // parts
    query_rank, latent_rank = held.query_n.shape[1], held.latent_n.shape[1]
    heads, _, head_width = held.queries.shape
    query_cut, latent_cut = held.query_down.shape[1], held.latent_down.shape[0]
    experts = small.router.shape[0]
    gain_wide = -(-max(sizes) // LANES) * LANES
    lead = query_rank + latent_rank + LANES
    half = parts // PAIR
    full = Bag(
        out_proj=(held.out_proj.shape, 1, bf16),
        query_up=(held.query_up.shape, 0, bf16),
        latent_up=(held.latent_up.shape, 0, bf16),
        query_down=((width, query_cut), 0, bf16),
        latent_down=((latent_cut, width), 1, bf16),
        router=((experts, width), 1, bf16),
        gains=((groups * 8, gain_wide), 0, f32),
    )
    reduced, pieces = [], {}
    for name, (shape, axis, dtype) in full.items():
        piece = list(shape)
        piece[axis] //= groups
        if aligned(piece[axis], 1) or axis == 0:
            reduced.append((name, axis))
            pieces[name] = tuple(piece)
    buffers = Bag(
        middle_grad=((sub, width), f32),
        sums=((8, width), f32),
        grad_rows=((sub, width), bf16),
        block_rows=((sub, width), bf16),
        attention_grad=((rows, width), bf16),
        attended_grad=(held.attended.shape, bf16),
        dquery=((rows, heads * head_width), bf16),
        dkeyval=((rows, heads * (NOPE + VD)), bf16),
        heads_partial=((half, PAIR, sub, lead), bf16),
        heads_beside=((half, sub, lead), bf16),
        heads_give=((sub, lead), bf16),
        heads_across=((sub, lead), bf16),
        heads_rows=((sub, lead), f32),
        query_rows=((sub, query_rank), bf16),
        latent_rows=((sub, latent_rank + LANES), bf16),
        latent_block=((rows, latent_rank), f32),
        dquery_lat=((rows, query_rank), bf16),
        dquery_cut=((rows, query_cut), bf16),
        dlatent_all=((rows, latent_rank + LANES), bf16),
        dlatent_t=((latent_rank + LANES, rows), f32),
        first_partial=((half, PAIR, sub, width), bf16),
        first_beside=((half, sub, width), bf16),
        first_give=((sub, width), bf16),
        first_across=((sub, width), bf16),
        first_rows=((sub, width), f32),
        input_rows=((sub, width), bf16),
    )
    for name, (shape, _, dtype) in full.items():
        buffers[name] = (shape, dtype)
    scratch = Bag(("b_" + name, pltpu.VMEM(*spec)) for name, spec in buffers.items())
    for name, array in held.items():
        scratch["l_" + name] = pltpu.VMEM(array.shape, array.dtype)
    outs = Bag(block_out=((rows, width), bf16), input_grad=((rows, width), bf16))
    for name, (shape, axis, dtype) in full.items():
        if name not in pieces:
            outs[name] = (shape, dtype)
            continue
        piece = pieces[name]
        scratch["t_" + name] = pltpu.VMEM((deep, *piece), dtype)
        scratch["d_" + name] = pltpu.VMEM((deep - 1, *piece), dtype)
        scratch["r_" + name] = pltpu.VMEM(piece, f32)
        outs[name] = (piece, f32)
        if name in (QUERY_DOWN, LATENT_DOWN, ROUTER, GAINS):
            kind = bf16 if name in (QUERY_DOWN, LATENT_DOWN) else f32
            along = 1 if name == QUERY_DOWN else 0
            whole = list(piece)
            whole[along] *= parts
            scratch["s_" + name] = pltpu.VMEM(piece, kind)
            if name in (QUERY_DOWN, LATENT_DOWN):
                outs[name] = (tuple(whole), bf16)
            else:
                scratch["g_" + name] = pltpu.VMEM(tuple(whole), kind)
                scratch["f_" + name] = pltpu.VMEM(piece, f32)
    share = grad_shared.shape[1] // groups
    inputs = {"i_" + name: array for name, array in small.items()}
    specs = [IN_VMEM] * len(small)
    if aligned(share, 1):
        reduced.append((SHARED, 1))
        inputs["i_shared"] = grad_shared
        specs.append(ANY)
        outs.shared = ((groups, grad_shared.shape[0], share), bf16)
        scratch.k_shared = pltpu.VMEM((grad_shared.shape[0], share), bf16)
        scratch.shared_send = scratch.shared_arrive = DMA((groups,))
    inputs |= {"h_" + name: array for name, array in held.items()}
    specs += [ANY] * len(held)
    scratch.load = DMA((len(held),))
    scratch.leave = DMA((len(outs) + 1,))
    scratch.place = DMA((12,))
    scratch.rows_send = scratch.rows_arrive = DMA((12, 8))
    scratch.send = scratch.arrive = DMA((len(full), 2 * deep))
    scratch.sum_send = scratch.sum_arrive = DMA((2, 2))
    names = list(inputs) + ["o_" + name for name in outs] + list(scratch)
    reduced = [entry for entry in reduced]
    results = pl.pallas_call(
        functools.partial(back_kernel, groups, tuple(sizes), tuple(reduced), tuple(names)),
        in_specs=specs,
        out_specs=[ANY] * len(outs),
        out_shape=[jax.ShapeDtypeStruct(*spec) for spec in outs.values()],
        scratch_shapes=list(scratch.values()),
        compiler_params=calls.params(),
        name="back",
    )(*inputs.values())
    results = Bag(zip(outs, results))
    for name, (shape, axis, dtype) in full.items():
        if name not in pieces:
            results[name] = scatter_sum(results[name], EXPERT, axis)
            if name == LATENT_DOWN:
                results[name] = gather(results[name].astype(bf16), TENSOR, 0).astype(f32)
            if name == ROUTER:
                results[name] = lax.psum(results[name].astype(bf16), TENSOR).astype(f32)
    if SHARED not in results:
        split = grad_shared.reshape(grad_shared.shape[0], groups, share).transpose(1, 0, 2)
        results.shared = lax.all_to_all(
            split, EXPERT, split_axis=0, concat_axis=0, tiled=True
        )
    return results


ALL = (EXPERT, TENSOR)


def gather(values, axes, dimension):
    return lax.all_gather(values, axes, axis=dimension, tiled=True)


def scatter_sum(values, axes, dimension):
    return lax.psum_scatter(
        values.astype(jnp.bfloat16), axes, scatter_dimension=dimension, tiled=True
    ).astype(jnp.float32)


def aligned(size, axis):
    return size % LANES == 0 if axis else size % 16 == 0


def ready_items(items, part):
    result = []
    for name, array, axis, cut, over, orders, home in items:
        if axis == 1 and array.shape[-1] % LANES:
            if over == SHUFFLE:
                array = lax.all_to_all(array, EXPERT, split_axis=0, concat_axis=0, tiled=True)
                array = array.transpose(1, 0, 2).reshape(array.shape[1], -1)
            else:
                if cut is not None:
                    array = lax.dynamic_slice_in_dim(array, part * cut[1], cut[1], axis=cut[0])
                array = gather(array, EXPERT, axis)
            cut, over, orders, home = None, READY, (), VMEM_
        result.append((name, array, axis, cut, over, orders, home))
    return result


def body(
    calls,
    block_in,
    attention_gain,
    query_down,
    query_gain,
    query_up,
    latent_down,
    latent_gain,
    latent_up,
    out_proj,
    ffn_gain,
    router,
    shared_gate,
    shared_up,
    shared_down,
    expert_gate,
    expert_up,
    expert_down,
    doc_lengths,
    routes,
    out_grad,
):
    groups = lax.axis_size(EXPERT)
    parts = lax.axis_size(TENSOR)
    me = lax.axis_index(EXPERT)
    part = lax.axis_index(TENSOR)
    row_count, width = block_in.shape
    top = routes.shape[1]
    local = expert_gate.shape[0]
    experts = local * groups

    all_gains = (attention_gain, ffn_gain, query_gain, latent_gain)
    gain_sizes = [g.shape[0] for g in all_gains]
    gain_wide = -(-max(gain_sizes) // LANES) * LANES
    gains = sum(
        jnp.pad(g.astype(jnp.float32)[None], ((i, 7 - i), (0, gain_wide - g.shape[0])))
        for i, g in enumerate(all_gains)
    )
    routes_pad = jnp.pad(routes.T, ((0, -top % 8), (0, 0)), constant_values=-1)
    shared = jnp.stack([shared_gate.T, shared_up.T, shared_down])
    shared_units = shared.shape[1] // groups
    shared = shared.reshape(3, groups, shared_units, -1).transpose(1, 0, 2, 3)
    shared = shared.reshape(groups, 3 * shared_units, -1)
    query_cut = query_down.shape[1] // parts
    latent_cut = latent_down.shape[1] // parts
    allowed, cosine, sinusoid = layout(doc_lengths[0], row_count)
    allowed = allowed.astype(jnp.float32)
    tables = [
        jnp.pad(jnp.concatenate(pair, axis=1), ((0, 0), (0, LANES - ROPE)))
        for pair in ((cosine, cosine), (-sinusoid, sinusoid))
    ]
    items = [
        (GAINS, gains, 0, None, EXPERT, ("e",), VMEM_),
        (QUERY_DOWN, query_down, 0, (1, query_cut), EXPERT, ("zx",), VMEM_),
        (LATENT_DOWN, latent_down.T, 1, (0, latent_cut), EXPERT, ("zx",), VMEM_),
        (QUERY_UP, query_up, 0, None, EXPERT, ("zx",), VMEM_),
        (LATENT_UP, latent_up, 0, None, EXPERT, ("zx",), VMEM_),
        (OUT_PROJ, out_proj, 1, None, EXPERT, ("zx",), VMEM_),
        (ROUTER, router.T, 1, None, EXPERT, ("zx",), VMEM_),
        (ROUTES, routes_pad, 1, None, EXPERT, ("e",), "hbm"),
        (SHARED, shared, 1, None, SHUFFLE, (), "hbm"),
        (OUT_GRAD, out_grad, 0, (0, row_count // parts), "all", (ZXYC, "xzyc"), "hbm"),
    ]
    front = front_stage(
        calls,
        groups,
        parts,
        gain_sizes,
        ready_items(items, part),
        block_in,
        routes,
        allowed,
        *tables,
    )
    router_t = front.router
    shared = front.shared
    tokens, gradients = front.tokens, front.out_grad
    lane_pad = -experts % LANES
    own_ids = me * local + jnp.arange(local, dtype=jnp.int32)
    expert_rows, expert_grads, picks, slot_weights = route_stage(
        groups, own_ids, front.routes, tokens, gradients, front.weights
    )
    slot_shape = (groups, local, CAP)
    produced, back_rows, slot_dweights, grad_gate, grad_up, grad_down = expert_stage(
        expert_rows.reshape(*slot_shape, width),
        expert_grads.reshape(*slot_shape, width),
        slot_weights.reshape(*slot_shape, 1),
        expert_gate.transpose(0, 2, 1),
        expert_up.transpose(0, 2, 1),
        expert_down,
    )
    slots = local * CAP
    produced = produced.reshape(groups, slots, width)
    back_rows = back_rows.reshape(groups, slots, width)
    slot_dweights = slot_dweights.reshape(groups, slots, 1)
    slot_lanes = jnp.repeat(own_ids, CAP)[:, None]
    if mix_bytes(groups, row_count, slots, width) < 40 * 2**20:
        dsecond, mixed, grad_shared = mix_stage(
            calls,
            groups,
            parts,
            picks,
            produced,
            back_rows,
            slot_dweights,
            (slot_lanes, experts + lane_pad),
            tokens,
            gradients,
            shared,
        )
    else:
        lane_ids = jnp.arange(experts + lane_pad, dtype=jnp.int32)
        spread_out = jnp.where(slot_lanes == lane_ids[None, :], slot_dweights, 0.0)
        mixed_part, dsecond_part, grad_shared = combine_stage(
            picks,
            produced,
            back_rows,
            spread_out.astype(jnp.bfloat16),
            tokens.reshape(groups, row_count, width),
            gradients.reshape(groups, row_count, width),
            shared.reshape(3, shared_units, width),
        )
        grad_shared = grad_shared.astype(jnp.bfloat16).reshape(3 * shared_units, width)
        dsecond, mixed = sum_all(
            calls,
            groups,
            parts,
            (
                dsecond_part.reshape(-1, width + experts + lane_pad),
                mixed_part.reshape(-1, width),
            ),
        )
    held = Bag(
        (name, front[name])
        for name in (
            ATTENDED,
            OUT_PROJ,
            QUERIES,
            KEYS,
            VALUES,
            QUERY_N,
            LATENT_N,
            QUERY_UP,
            LATENT_UP,
            QUERY_LAT,
            LATENT_T,
            FIRST,
            QUERY_DOWN,
            LATENT_DOWN,
        )
    )
    small = Bag(
        dsecond=dsecond,
        mixed=mixed,
        middle=front.middle,
        chosen=front.chosen,
        router=router_t,
        out_grad=out_grad,
        block=block_in,
        allowed=allowed,
        cosine=tables[0],
        sinusoid=tables[1],
        norms=front.norms,
    )
    back = back_stage(calls, groups, parts, gain_sizes, held, small, grad_shared)
    grad_shared = back.shared.reshape(groups, 3, shared_units, -1).transpose(1, 0, 2, 3)
    grad_shared = grad_shared.astype(jnp.float32).reshape(3, groups * shared_units, -1)
    grad_gains = [back.gains[i, :size] for i, size in enumerate(gain_sizes)]

    return (
        back.block_out,
        back.input_grad,
        grad_gains[0],
        back.query_down.astype(jnp.float32),
        grad_gains[2],
        back.query_up,
        back.latent_down.T.astype(jnp.float32),
        grad_gains[3],
        back.latent_up,
        back.out_proj,
        grad_gains[1],
        back.router.T,
        grad_shared[0].T,
        grad_shared[1].T,
        grad_shared[2],
        grad_gate.transpose(0, 2, 1),
        grad_up.transpose(0, 2, 1),
        grad_down,
    )


def solution(mesh):
    placed = (
        P(EXPERT, None),
        P(EXPERT),
        P(EXPERT, None),
        P(EXPERT),
        P(EXPERT, TENSOR),
        P(EXPERT, None),
        P(EXPERT),
        P(EXPERT, TENSOR),
        P(TENSOR, EXPERT),
        P(EXPERT),
        P(EXPERT, None),
        P(EXPERT, TENSOR),
        P(EXPERT, TENSOR),
        P(TENSOR, EXPERT),
        P(EXPERT, None, TENSOR),
        P(EXPERT, None, TENSOR),
        P(EXPERT, TENSOR, None),
        P(EXPERT, None),
        P(EXPERT, None),
        P(EXPERT, None),
    )
    return jax.shard_map(
        functools.partial(body, Calls()),
        mesh=mesh,
        in_specs=placed,
        out_specs=(
            P(EXPERT, None),
            P(EXPERT, None),
            P(EXPERT),
            P(EXPERT, None),
            P(EXPERT),
            P(EXPERT, TENSOR),
            P(EXPERT, None),
            P(EXPERT),
            P(EXPERT, TENSOR),
            P(TENSOR, EXPERT),
            P(EXPERT),
            P(EXPERT, None),
            P(EXPERT, TENSOR),
            P(EXPERT, TENSOR),
            P(TENSOR, EXPERT),
            P(EXPERT, None, TENSOR),
            P(EXPERT, None, TENSOR),
            P(EXPERT, TENSOR, None),
        ),
        check_vma=False,
    )
```
